32 devices in a mesh: dp: 8 (over y, x, core), tensor: 4 (over z).
Axes of the slice: x: 2, y: 2, z: 4, core: 2. Of those that a mesh axis runs over, the one named last changes fastest.
Arguments:
- tokens: bfloat16 [8192, 2048], P(('dp', 'tensor')), may hold values from -6 to 6
- cotangent: bfloat16 [8192, 2048], P(('dp', 'tensor')), may hold values from -6 to 6
- ln1_gain: bfloat16 [2048], P(('dp', 'tensor')), may hold values from 0.5 to 1.5
- ln1_bias: bfloat16 [2048], P(('dp', 'tensor')), may hold values from -3 to 3
- qkv_weight: bfloat16 [3, 2048, 2048], P(None, 'dp', 'tensor'), may hold values from -0.125 to 0.125
- qv_bias: bfloat16 [2, 2048], P(None, ('tensor', 'dp')), may hold values from -3 to 3
- out_weight: bfloat16 [2048, 2048], P('tensor', 'dp'), may hold values from -2 to 2
- out_bias: bfloat16 [2048], P(('dp', 'tensor')), may hold values from -3 to 3
- ln2_gain: bfloat16 [2048], P(('dp', 'tensor')), may hold values from 0.5 to 1.5
- ln2_bias: bfloat16 [2048], P(('dp', 'tensor')), may hold values from -3 to 3
- up_weight: bfloat16 [2048, 8192], P('dp', 'tensor'), may hold values from -0.125 to 0.125
- up_bias: bfloat16 [8192], P(('tensor', 'dp')), may hold values from -3 to 3
- down_weight: bfloat16 [8192, 2048], P('tensor', 'dp'), may hold values from -0.0625 to 0.0625
- down_bias: bfloat16 [2048], P(('dp', 'tensor')), may hold values from -3 to 3
Outputs:
- layer_out: bfloat16 [8192, 2048], P(('dp', 'tensor'))
- grad_tokens: bfloat16 [8192, 2048], P(('dp', 'tensor'))
- grad_ln1_gain: float32 [2048], P(('dp', 'tensor'))
- grad_ln1_bias: float32 [2048], P(('dp', 'tensor'))
- grad_qkv_weight: float32 [3, 2048, 2048], P(None, 'dp', 'tensor')
- grad_qv_bias: float32 [2, 2048], P(None, ('tensor', 'dp'))
- grad_out_weight: float32 [2048, 2048], P('tensor', 'dp')
- grad_out_bias: float32 [2048], P(('dp', 'tensor'))
- grad_ln2_gain: float32 [2048], P(('dp', 'tensor'))
- grad_ln2_bias: float32 [2048], P(('dp', 'tensor'))
- grad_up_weight: float32 [2048, 8192], P('dp', 'tensor')
- grad_up_bias: float32 [8192], P(('tensor', 'dp'))
- grad_down_weight: float32 [8192, 2048], P('tensor', 'dp')
- grad_down_bias: float32 [2048], P(('dp', 'tensor'))
The draws below stay inside these ranges and needn't reach their ends.
All inputs are finite; a program needn't handle non-finite values.
Results may differ from the reference program's by a relative error of at most 0.012.
Values may be sent and summed in bfloat16 or wider, within the bound.
A program may use at most 192 MiB of HBM per device.

```python
import jax
import jax.numpy as jnp
from jax import lax

D = 2048
HEADS = 16
FF = 8192
HD = 128
LEN = 1024
TOKENS = 8192


def shard_levels(key, shape, pieces, least, largest):
    level = 1.0
    for dim, shards_of in pieces:
        steps = jax.random.uniform(jax.random.fold_in(jax.random.fold_in(key, 6), dim), (shards_of,), jnp.float32, least / len(pieces), largest / len(pieces))
        level = level * jnp.repeat(jnp.exp(steps), shape[dim] // shards_of).reshape((-1,) + (1,) * (len(shape) - 1 - dim))
    return level


def noise(stream_key, dims, spread, limit, cuts=(), dtype=jnp.bfloat16):
    array = spread * jax.random.normal(stream_key, dims, jnp.float32)
    if cuts:
        array = array * shard_levels(stream_key, dims, cuts, -0.22, 0.18)
    return jnp.clip(array, -limit, limit).astype(dtype)


def setup_inputs(seed: int = 0) -> dict:
    key_of = jax.random.split(jax.random.key(seed), 15)
    tokens = noise(key_of[0], (TOKENS, D), 1.0, 6.0, ((0, 32),))
    cotangent = noise(key_of[1], (TOKENS, D), 1.0, 6.0, ((0, 32),))
    ln1_gain = jnp.clip(1.0 + 0.1 * jax.random.normal(key_of[2], (D,), jnp.float32), 0.5, 1.5).astype(jnp.bfloat16)
    ln1_bias = noise(key_of[3], (D,), 0.5, 3.0, ((0, 32),))
    qkv_weight = noise(key_of[4], (3, D, D), D ** -0.5, 0.125, ((1, 8), (2, 4)))
    qv_bias = noise(key_of[5], (2, D), 0.5, 3.0, ((1, 32),))
    out_weight = noise(key_of[6], (D, D), (max(D // 256, 1)) ** -0.5, 2.0, ((0, 4), (1, 8)))
    out_bias = noise(key_of[7], (D,), 0.5, 3.0, ((0, 32),))
    ln2_gain = jnp.clip(1.0 + 0.1 * jax.random.normal(key_of[8], (D,), jnp.float32), 0.5, 1.5).astype(jnp.bfloat16)
    ln2_bias = noise(key_of[9], (D,), 0.5, 3.0, ((0, 32),))
    up_weight = noise(key_of[10], (D, FF), D ** -0.5, 0.125, ((0, 8), (1, 4)))
    up_bias = noise(key_of[11], (FF,), 0.5, 3.0, ((0, 32),))
    down_weight = noise(key_of[12], (FF, D), FF ** -0.5, 0.0625, ((0, 4), (1, 8)))
    down_bias = noise(key_of[13], (D,), 0.5, 3.0, ((0, 32),))
    return {"tokens": tokens, "cotangent": cotangent, "ln1_gain": ln1_gain, "ln1_bias": ln1_bias, "qkv_weight": qkv_weight, "qv_bias": qv_bias, "out_weight": out_weight, "out_bias": out_bias, "ln2_gain": ln2_gain, "ln2_bias": ln2_bias, "up_weight": up_weight, "up_bias": up_bias, "down_weight": down_weight, "down_bias": down_bias}


EPS = 1e-05
HIGH = lax.Precision.HIGHEST

@jax.custom_vjp
def low(v):
    return lax.optimization_barrier(v.astype(jnp.bfloat16)).astype(jnp.float32)

@jax.custom_vjp
def low_back(v):
    return v

def low_keep(v):
    return (low(v), None)

def low_pass(kept, grad):
    return (grad,)

def back_keep(v):
    return (v, None)

def back_low(kept, grad):
    return (low(grad),)
low.defvjp(low_keep, low_pass)
low_back.defvjp(back_keep, back_low)

def layer_norm(row_block, scale_vec, shift_vec):
    row_mean = lax.optimization_barrier(jnp.mean(row_block, axis=-1, keepdims=True))
    centred = row_block - row_mean
    variance = lax.optimization_barrier(jnp.mean(centred * centred, axis=-1, keepdims=True))
    return centred * lax.rsqrt(variance + EPS) * scale_vec + shift_vec

def matmul(left, right):
    return jnp.dot(left, right, precision=HIGH, preferred_element_type=jnp.float32)

def forward(rows_in, ln1_gain, ln1_bias, qkv_weight, qv_bias, out_weight, out_bias, ln2_gain, ln2_bias, up_weight, up_bias, down_weight, down_bias):
    normed_one = low(layer_norm(rows_in, ln1_gain, ln1_bias))
    queries = low(low_back(matmul(normed_one, qkv_weight[0]) + qv_bias[0]))
    key_rows = low(low_back(matmul(normed_one, qkv_weight[1])))
    value_rows = low(low_back(matmul(normed_one, qkv_weight[2]) + qv_bias[1]))
    head_shape = (LEN, HEADS, HD)
    raw_scores = jnp.einsum('qhd,khd->hqk', queries.reshape(head_shape), key_rows.reshape(head_shape), precision=HIGH)
    scores = low_back(raw_scores * HD ** (-0.5))
    positions = jnp.arange(LEN)
    causal = positions[:, None] >= positions[None, :]
    scores = jnp.where(causal[None], scores, -1e+30)
    attention = low(jax.nn.softmax(scores, axis=-1))
    mixture = jnp.einsum('hqk,khd->qhd', attention, value_rows.reshape(head_shape), precision=HIGH).reshape(LEN, D)
    mixture = low(low_back(mixture))
    residual = rows_in + low_back(matmul(mixture, out_weight) + out_bias)
    normed_two = low(layer_norm(residual, ln2_gain, ln2_bias))
    preact = low_back(matmul(normed_two, up_weight) + up_bias)
    hidden = low(jax.nn.gelu(preact, approximate=False))
    return residual + (matmul(hidden, down_weight) + down_bias)

def reference(tokens, cotangent, ln1_gain, ln1_bias, qkv_weight, qv_bias, out_weight, out_bias, ln2_gain, ln2_bias, up_weight, up_bias, down_weight, down_bias):
    params = tuple((weight_arg.astype(jnp.float32) for weight_arg in (ln1_gain, ln1_bias, qkv_weight, qv_bias, out_weight, out_bias, ln2_gain, ln2_bias, up_weight, up_bias, down_weight, down_bias)))
    seq_total = TOKENS // LEN
    inputs = tokens.astype(jnp.float32).reshape(seq_total, LEN, D)
    cotangents = cotangent.astype(jnp.float32).reshape(seq_total, LEN, D)

    def step(carried, pair):
        seq_in, seq_cot = pair
        result, pullback = jax.vjp(forward, seq_in, *params)
        grads = pullback(seq_cot)
        carried = tuple((running + fresh for running, fresh in zip(carried, grads[1:])))
        return (carried, (result.astype(jnp.bfloat16), grads[0].astype(jnp.bfloat16)))
    starting = tuple((jnp.zeros(weight_arg.shape, jnp.float32) for weight_arg in params))
    totals, (outputs, in_grads) = lax.scan(step, starting, (inputs, cotangents))
    return (outputs.reshape(TOKENS, D), in_grads.reshape(TOKENS, D), totals[0], totals[1], totals[2], totals[3], totals[4], totals[5], totals[6], totals[7], totals[8], totals[9], totals[10], totals[11])
```

```python
import jax
import jax.numpy as jnp
from jax import lax
from jax.sharding import PartitionSpec as P

HD = 128
LEN = 1024
EPS = 1e-05
BF = jnp.bfloat16
F32 = jnp.float32


def norm_stats(rows):
    mean = jnp.mean(rows, axis=-1, keepdims=True)
    centred = rows - mean
    variance = jnp.mean(centred * centred, axis=-1, keepdims=True)
    inverse = lax.rsqrt(variance + EPS)
    return centred * inverse, inverse


def norm_back(grad_rows, normal_rows, inverse, gain):
    scaled = grad_rows * gain
    first = jnp.mean(scaled, axis=-1, keepdims=True)
    second = jnp.mean(scaled * normal_rows, axis=-1, keepdims=True)
    return inverse * (scaled - first - normal_rows * second)


def masked_scores(queries, key_rows, positions):
    causal = positions[:, None] >= positions[None, :]
    scores = jnp.einsum("qhd,khd->hqk", queries, key_rows, preferred_element_type=F32) * HD ** (-0.5)
    return jnp.where(causal[None], scores, -1e30)


def attend(queries, key_rows, value_rows, positions):
    scores = masked_scores(queries, key_rows, positions)
    row_top = jnp.max(scores, axis=-1, keepdims=True)
    exponent = jnp.exp(scores - row_top)
    row_total = jnp.sum(exponent, axis=-1, keepdims=True)
    attention = (exponent / row_total).astype(BF)
    mixture = jnp.einsum("hqk,khd->qhd", attention, value_rows, preferred_element_type=F32)
    return mixture.astype(BF), row_top + jnp.log(row_total)


def attend_back(queries, key_rows, value_rows, log_total, grad_mix, positions):
    factor = HD ** (-0.5)
    attention = jnp.exp(masked_scores(queries, key_rows, positions) - log_total)
    grad_value = jnp.einsum("hqk,qhd->khd", attention.astype(BF), grad_mix, preferred_element_type=F32)
    grad_attn = jnp.einsum("qhd,khd->hqk", grad_mix, value_rows, preferred_element_type=F32)
    inner = jnp.sum(attention * grad_attn, axis=-1, keepdims=True)
    grad_scores = (attention * (grad_attn - inner)).astype(BF)
    grad_query = jnp.einsum("hqk,khd->qhd", grad_scores, key_rows, preferred_element_type=F32) * factor
    grad_key = jnp.einsum("hqk,qhd->khd", grad_scores, queries, preferred_element_type=F32) * factor
    return grad_query.astype(BF), grad_key.astype(BF), grad_value.astype(BF)


def gelu_exact(preact):
    return jax.nn.gelu(preact, approximate=False)


class Line:
    def __init__(self, axis, size):
        self.axis, self.n = axis, size
        self.i = lax.axis_index(axis)
        self.first = self.i < size // 2

    def owner(self, k):
        return jnp.where(self.first, self.i + k, self.i - k + self.n) % self.n

    def gather(self, block):
        n = self.n
        down, up = [block], [block]
        for r in range(1, n):
            down.append(lax.ppermute(down[-1], self.axis, [(i, i - 1) for i in range(1, n) if i + r - 1 <= n - 1]))
            up.append(lax.ppermute(up[-1], self.axis, [(i, i + 1) for i in range(n - 1) if i - r + 1 >= 0]))
        slots = [block]
        for k in range(1, n):
            if 2 * k <= n:
                slots.append(jnp.where(self.first, down[k], up[k]))
            else:
                low = jnp.where(self.i + k <= n - 1, down[k], up[n - k])
                high = jnp.where(self.i - k >= 0, up[k], down[n - k])
                slots.append(jnp.where(self.first, low, high))
        return slots

    def scatter_sum(self, parts):
        n = self.n
        right = left = None
        for r in range(1, n):
            term = jnp.where(self.first, parts[n - r], parts[r]).astype(F32)
            term = term if right is None else term + right.astype(F32)
            right = lax.ppermute(term.astype(BF), self.axis, [(i, i + 1) for i in range(min(r, n - 1))])
            term = jnp.where(self.first, parts[r], parts[n - r]).astype(F32)
            term = term if left is None else term + left.astype(F32)
            left = lax.ppermute(term.astype(BF), self.axis, [(i, i - 1) for i in range(max(n - r, 1), n)])
        return parts[0].astype(F32) + (right.astype(F32) + left.astype(F32))


def body(tokens, cotangent, ln1_gain, ln1_bias, qkv_weight, qv_bias, out_weight, out_bias, ln2_gain, ln2_bias,
         up_weight, up_bias, down_weight, down_bias):
    tp = lax.axis_size("tensor")
    dp = lax.axis_size("dp")
    line = Line("tensor", tp)
    rows = tokens.shape[0]
    width = qkv_weight.shape[2]
    heads = width // HD
    piece = ln1_gain.shape[0]

    own = jnp.concatenate([ln1_gain, ln1_bias, out_bias, ln2_gain, ln2_bias, down_bias, qv_bias.reshape(-1), up_bias])
    over_dp = lax.all_gather(own, "dp", axis=0)
    whole = lax.all_gather(over_dp[:, : 6 * piece], "tensor", axis=0)
    whole = whole.reshape(tp, dp, 6, piece).transpose(2, 1, 0, 3).reshape(6, -1).astype(F32)
    gain_one, shift_one, bias_out, gain_two, shift_two, bias_down = [whole[j] for j in range(6)]
    qv = qv_bias.shape[1]
    bias_qv = over_dp[:, 6 * piece : 6 * piece + 2 * qv].reshape(dp, 2, qv).transpose(1, 0, 2).reshape(2, -1).astype(F32)
    bias_up = over_dp[:, 6 * piece + 2 * qv :].reshape(-1).astype(F32)

    w_qkv = lax.all_gather(qkv_weight, "dp", axis=1, tiled=True)
    w_out = lax.all_gather(out_weight, "dp", axis=1, tiled=True)
    w_up = lax.all_gather(up_weight, "dp", axis=0, tiled=True)
    w_down = lax.all_gather(down_weight, "dp", axis=1, tiled=True)

    positions = jnp.concatenate([line.owner(k) * rows + jnp.arange(rows) for k in range(tp)])

    def split(array):
        return [array[k * rows : (k + 1) * rows] for k in range(tp)]

    rows_all = jnp.concatenate(line.gather(tokens), axis=0)
    cot_all = jnp.concatenate(line.gather(cotangent), axis=0)

    normal_all, inverse_all = norm_stats(rows_all.astype(F32))
    attn_in = (normal_all * gain_one + shift_one).astype(BF)
    projected = jnp.einsum("rd,kde->kre", attn_in, w_qkv, preferred_element_type=F32)
    head_shape = (LEN, heads, HD)
    queries = (projected[0] + bias_qv[0]).astype(BF).reshape(head_shape)
    key_rows = projected[1].astype(BF).reshape(head_shape)
    value_rows = (projected[2] + bias_qv[1]).astype(BF).reshape(head_shape)
    mixture, log_totals = attend(queries, key_rows, value_rows, positions)
    mixture = mixture.reshape(LEN, width)
    attn_part = jnp.dot(mixture, w_out, preferred_element_type=F32).astype(BF)
    rows_in = tokens.astype(F32)
    residual = rows_in + (line.scatter_sum(split(attn_part)) + bias_out)

    normal_two, inverse_two = norm_stats(residual)
    mlp_own = (normal_two * gain_two + shift_two).astype(BF)
    mlp_in = jnp.concatenate(line.gather(mlp_own), axis=0)
    preact = jnp.dot(mlp_in, w_up, preferred_element_type=F32) + bias_up
    hidden, gelu_pullback = jax.vjp(gelu_exact, preact)
    hidden = hidden.astype(BF)
    grad_hidden = jnp.einsum("rd,fd->rf", cot_all, w_down, preferred_element_type=F32)
    grad_pre = gelu_pullback(grad_hidden)[0].astype(BF)
    mlp_back = jnp.einsum("rf,df->rd", grad_pre, w_up, preferred_element_type=F32).astype(BF)
    grad_normed_two = line.scatter_sum(split(mlp_back))
    mlp_part = jnp.dot(hidden, w_down, preferred_element_type=F32).astype(BF)
    layer_out = (residual + (line.scatter_sum(split(mlp_part)) + bias_down)).astype(BF)

    grad_out = cotangent.astype(F32)
    grad_resid = grad_out + norm_back(grad_normed_two, normal_two, inverse_two, gain_two)
    branch_cot = grad_resid.astype(BF)
    attn_cot = jnp.concatenate(line.gather(branch_cot), axis=0)
    grad_mix = jnp.einsum("rd,ed->re", attn_cot, w_out, preferred_element_type=F32).astype(BF)
    grad_query, grad_key, grad_value = attend_back(
        queries, key_rows, value_rows, log_totals, grad_mix.reshape(head_shape), positions)
    grad_qkv = jnp.stack((grad_query, grad_key, grad_value)).reshape(3, LEN, width)
    attn_back = jnp.einsum("kre,kde->rd", grad_qkv, w_qkv, preferred_element_type=F32)
    grad_gain_one = jnp.sum(attn_back * normal_all, axis=0)
    grad_shift_one = jnp.sum(attn_back, axis=0)
    grad_normed_one = line.scatter_sum(split(attn_back.astype(BF)))
    grad_tokens = (grad_resid + norm_back(grad_normed_one, normal_all[:rows], inverse_all[:rows], gain_one)).astype(BF)

    grad_down_w = jnp.einsum("rf,rd->fd", hidden, cot_all, preferred_element_type=F32).astype(BF)
    grad_up_w = jnp.einsum("rd,rf->df", mlp_in, grad_pre, preferred_element_type=F32).astype(BF)
    grad_out_w = jnp.einsum("re,rd->ed", mixture, attn_cot, preferred_element_type=F32).astype(BF)
    grad_qkv_w = jnp.einsum("rd,kre->kde", attn_in, grad_qkv, preferred_element_type=F32).astype(BF)
    grad_down_w = lax.psum_scatter(grad_down_w, "dp", scatter_dimension=1, tiled=True).astype(F32)
    grad_up_w = lax.psum_scatter(grad_up_w, "dp", scatter_dimension=0, tiled=True).astype(F32)
    grad_out_w = lax.psum_scatter(grad_out_w, "dp", scatter_dimension=1, tiled=True).astype(F32)
    grad_qkv_w = lax.psum_scatter(grad_qkv_w, "dp", scatter_dimension=1, tiled=True).astype(F32)

    vectors = jnp.stack([
        grad_gain_one,
        grad_shift_one,
        jnp.sum(branch_cot.astype(F32), axis=0),
        jnp.sum(grad_normed_two * normal_two, axis=0),
        jnp.sum(grad_normed_two, axis=0),
        jnp.sum(grad_out, axis=0),
    ])
    vectors = vectors.reshape(6, dp, tp, piece).transpose(1, 2, 0, 3).reshape(dp, tp * 6 * piece)
    grad_qv_b = jnp.sum(grad_qkv[0::2].astype(F32), axis=1).reshape(2, dp, qv).transpose(1, 0, 2).reshape(dp, 2 * qv)
    grad_up_b = jnp.sum(grad_pre.astype(F32), axis=0).reshape(dp, -1)
    packed = jnp.concatenate([vectors, grad_qv_b, grad_up_b], axis=1)
    packed = jnp.sum(lax.all_to_all(packed, "dp", 0, 0), axis=0)
    grad_up_b = packed[tp * 6 * piece + 2 * qv :]
    grad_qv_b = packed[tp * 6 * piece : tp * 6 * piece + 2 * qv].reshape(2, qv)
    vectors = packed[: tp * 6 * piece].reshape(tp, 6 * piece)
    vectors = jnp.sum(lax.all_to_all(vectors, "tensor", 0, 0), axis=0).reshape(6, piece)
    return (layer_out, grad_tokens, vectors[0], vectors[1], grad_qkv_w, grad_qv_b, grad_out_w, vectors[2],
            vectors[3], vectors[4], grad_up_w, grad_up_b, grad_down_w, vectors[5])


def solution(mesh):
    vector, matrix = P(("dp", "tensor")), P(("dp", "tensor"), None)
    in_specs = (matrix, matrix, vector, vector, P(None, "dp", "tensor"), P(None, ("tensor", "dp")), P("tensor", "dp"),
                vector, vector, vector, P("dp", "tensor"), P(("tensor", "dp")), P("tensor", "dp"), vector)
    out_specs = (matrix, matrix, vector, vector, P(None, "dp", "tensor"), P(None, ("tensor", "dp")),
                 P("tensor", "dp"), vector, vector, vector, P("dp", "tensor"), P(("tensor", "dp")), P("tensor", "dp"),
                 vector)
    return jax.shard_map(body, mesh=mesh, in_specs=in_specs, out_specs=out_specs, check_vma=False)
```

```python
import functools

import jax
import jax.numpy as jnp
from jax import lax
from jax.experimental import pallas as pl
from jax.experimental.pallas import tpu as pltpu
from jax.sharding import PartitionSpec as P

HD = 128
LEN = 1024
LANES = 128
EPS = 1e-05
BF = jnp.bfloat16
F32 = jnp.float32
MESH = pl.DeviceIdType.MESH
ANY = pl.BlockSpec(memory_space=pl.ANY)
VM = pl.BlockSpec(memory_space=pltpu.VMEM)
NT = (((1,), (1,)), ((), ()))
TN = (((0,), (0,)), ((), ()))
BIG = 64 * 1024 * 1024 - 65536
RB = 32


def norm_stats(rows):
    mean = jnp.mean(rows, axis=-1, keepdims=True)
    centred = rows - mean
    variance = jnp.mean(centred * centred, axis=-1, keepdims=True)
    inverse = lax.rsqrt(variance + EPS)
    return centred * inverse, inverse


def norm_back(grad_rows, normal_rows, inverse, gain):
    scaled = grad_rows * gain
    first = jnp.mean(scaled, axis=-1, keepdims=True)
    second = jnp.mean(scaled * normal_rows, axis=-1, keepdims=True)
    return inverse * (scaled - first - normal_rows * second)


def loop(count, step):
    def run(i, carry):
        step(i)
        return carry

    lax.fori_loop(0, count, run, 0)


def rows_at(j, size):
    return pl.ds(pl.multiple_of(j * size, size), size)


def remote(src, dst, send, recv, target):
    return pltpu.make_async_remote_copy(src_ref=src, dst_ref=dst, send_sem=send, recv_sem=recv,
                                        device_id={"tensor": target}, device_id_type=MESH)


def greet_neighbours(i, n):
    barrier = pltpu.get_barrier_semaphore()

    @pl.when(i > 0)
    def _():
        pl.semaphore_signal(barrier, inc=1, device_id={"tensor": i - 1}, device_id_type=MESH)

    @pl.when(i < n - 1)
    def _():
        pl.semaphore_signal(barrier, inc=1, device_id={"tensor": i + 1}, device_id_type=MESH)

    pl.semaphore_wait(barrier, jnp.minimum(i, 1) + jnp.minimum(n - 1 - i, 1))


class LineGather:
    def __init__(self, i, n, own, buf, send, recv):
        self.i, self.n, self.own, self.buf, self.send, self.recv = i, n, own, buf, send, recv

    def copy(self, src, j, side, target):
        return remote(src, self.buf.at[j], self.send.at[side, j], self.recv.at[j], target)

    def start(self):
        i, n = self.i, self.n

        @pl.when(i < n - 1)
        def _():
            self.copy(self.own, i, 0, i + 1).start()

        @pl.when(i > 0)
        def _():
            self.copy(self.own, i, 1, i - 1).start()

    def step(self, r):
        i, n = self.i, self.n

        @pl.when(i - r >= 0)
        def _():
            self.copy(self.own, i - r, 0, i).wait_recv()

            @pl.when(i < n - 1)
            def _():
                self.copy(self.buf.at[i - r], i - r, 0, i + 1).start()

        @pl.when(i + r <= n - 1)
        def _():
            self.copy(self.own, i + r, 1, i).wait_recv()

            @pl.when(i > 0)
            def _():
                self.copy(self.buf.at[i + r], i + r, 1, i - 1).start()

    def finish(self):
        i, n = self.i, self.n

        def one(j):
            @pl.when(jnp.logical_and(i < n - 1, j <= i))
            def _():
                self.copy(self.own, j, 0, i + 1).wait_send()

            @pl.when(jnp.logical_and(i > 0, j >= i))
            def _():
                self.copy(self.own, j, 1, i - 1).wait_send()

        loop(n, one)


class LineSum:
    def __init__(self, i, n, part, land, send, recv, pieces):
        self.i, self.n, self.part, self.land, self.send, self.recv = i, n, part, land, send, recv
        self.pieces = pieces
        self.size = part.shape[1] // pieces

    def copy(self, src, d, right, s):
        i, n = self.i, self.n
        target = i + 1 if right else i - 1
        slot = d if right else jnp.where(d == target, n, d)
        here = rows_at(s, self.size)
        return remote(src.at[d, here], self.land.at[slot, here], self.send.at[d, s], self.recv.at[slot, s], target)

    def arrived(self, slot, s):
        here = rows_at(s, self.size)
        remote(self.part.at[0, here], self.land.at[slot, here], self.send.at[0, s], self.recv.at[slot, s],
               self.i).wait_recv()

    def launch(self, d):
        i, n = self.i, self.n

        @pl.when(jnp.logical_and(i == 0, d > 0))
        def _():
            loop(self.pieces, lambda s: self.copy(self.part, d, True, s).start())

        @pl.when(jnp.logical_and(i == n - 1, d < n - 1))
        def _():
            loop(self.pieces, lambda s: self.copy(self.part, d, False, s).start())

    def relay(self, d, right):
        def one(s):
            self.arrived(d, s)
            here = rows_at(s, self.size)
            total = self.land[d, here, :].astype(F32) + self.part[d, here, :].astype(F32)
            self.land[d, here, :] = total.astype(BF)
            self.copy(self.land, d, right, s).start()

        loop(self.pieces, one)

    def own(self):
        i, n = self.i, self.n

        @pl.when(i > 0)
        def _():
            loop(self.pieces, lambda s: self.arrived(i, s))

        @pl.when(i < n - 1)
        def _():
            loop(self.pieces, lambda s: self.arrived(n, s))

    def add(self, here, out):
        i, n = self.i, self.n
        out[...] = self.part[i, here, :].astype(F32)

        @pl.when(i > 0)
        def _():
            out[...] += self.land[i, here, :].astype(F32)

        @pl.when(i < n - 1)
        def _():
            out[...] += self.land[n, here, :].astype(F32)

    def finish(self):
        i, n = self.i, self.n

        def one(d):
            @pl.when(jnp.logical_and(i < n - 1, d > i))
            def _():
                loop(self.pieces, lambda s: self.copy(self.part, d, True, s).wait_send())

            @pl.when(jnp.logical_and(i > 0, d < i))
            def _():
                loop(self.pieces, lambda s: self.copy(self.part, d, False, s).wait_send())

        loop(n, one)


def project_kernel(n, m, pieces, pack_ref, x_ref, w_hbm, a_ref, qkv_ref, vec_ref, buf, w, affine, bias, w_sem, own_sem,
                   send, recv, v_send, v_recv):
    i, row = lax.axis_index("tensor"), lax.axis_index("dp")
    me, total = row * n + i, m * n
    size, width = x_ref.shape[0], w.shape[2]
    barrier = pltpu.get_barrier_semaphore()

    def greet(s):
        other = (me + s + 1) % total
        pl.semaphore_signal(barrier, inc=1, device_id={"dp": other // n, "tensor": other % n}, device_id_type=MESH)

    loop(total - 1, greet)
    pl.semaphore_wait(barrier, total - 1)

    line = LineGather(i, n, x_ref, buf, send, recv)
    line.start()

    def vector(src, other):
        return pltpu.make_async_remote_copy(
            src_ref=pack_ref, dst_ref=vec_ref.at[src], send_sem=v_send.at[other], recv_sem=v_recv.at[src],
            device_id={"dp": other // n, "tensor": other % n}, device_id_type=MESH)

    loop(total - 1, lambda s: vector(me, (me + s + 1) % total).start())
    own_copy = pltpu.make_async_copy(x_ref, buf.at[i], own_sem)
    own_copy.start()
    weights = pltpu.make_async_copy(w_hbm, w, w_sem)
    weights.start()
    vec_ref[me] = pack_ref[...]
    loop(total - 1, lambda s: vector((me + s + 1) % total, me).wait_recv())

    piece, qv_piece = pieces
    depth = affine.shape[1]
    group = LANES // piece
    for tile in range(depth // LANES):
        value = vec_ref[tile * group, 0:2, :]
        for g in range(1, group):
            value = value + vec_ref[tile * group + g, 0:2, :]
        affine[0:2, tile * LANES : (tile + 1) * LANES] = value
    group = LANES // qv_piece
    for tile in range(width // LANES):
        value = vec_ref[tile * group * n + i, 6:8, :]
        for g in range(1, group):
            value = value + vec_ref[(tile * group + g) * n + i, 6:8, :]
        bias[0:2, tile * LANES : (tile + 1) * LANES] = value
    own_copy.wait()
    weights.wait()

    def compute(j):
        def norm(b):
            normal, _ = norm_stats(buf[j, rows_at(b, RB), :].astype(F32))
            here = pl.ds(pl.multiple_of(j * size + b * RB, RB), RB)
            a_ref[here, :] = (normal * affine[0:1, :] + affine[1:2, :]).astype(BF)

        loop(size // RB, norm)
        here = rows_at(j, size)
        for t in range(3):
            value = jnp.dot(a_ref[here, :], w[t], preferred_element_type=F32)
            if t != 1:
                value = value + bias[t // 2 : t // 2 + 1, :]
            qkv_ref[t, here, :] = value.astype(BF)

    def round_of(r):
        @pl.when(r > 0)
        def _():
            line.step(r)

        def side(s):
            j = jnp.where(s == 0, i - r, i + r)

            @pl.when(jnp.logical_and(jnp.logical_and(j >= 0, j <= n - 1), s * r == s * jnp.maximum(r, 1)))
            def _():
                compute(j)

        loop(2, side)

    loop(n, round_of)
    line.finish()
    loop(total - 1, lambda s: vector(me, (me + s + 1) % total).wait_send())


def attend_kernel(n, pieces, qkv_ref, w_ref, x_ref, cot_ref, out_bias, gain, shift, o_ref, h_ref, c_ref, cot_all,
                  part, land, send, recv, s_send, s_recv, own_sem):
    i = lax.axis_index("tensor")
    size = x_ref.shape[0]
    heads = qkv_ref.shape[2] // HD
    depth = w_ref.shape[1]
    greet_neighbours(i, n)
    line = LineGather(i, n, cot_ref, cot_all, send, recv)
    line.start()
    own_copy = pltpu.make_async_copy(cot_ref, cot_all.at[i], own_sem)
    own_copy.start()

    block = 256

    def head(t):
        cols = pl.ds(pl.multiple_of(t * HD, HD), HD)
        for b in range(LEN // block):
            here, keys = slice(b * block, (b + 1) * block), (b + 1) * block
            s = lax.dot_general(qkv_ref[0, here, cols], qkv_ref[1, 0:keys, cols], NT,
                                preferred_element_type=F32) * HD ** (-0.5)
            query = lax.broadcasted_iota(jnp.int32, s.shape, 0) + b * block
            s = jnp.where(query >= lax.broadcasted_iota(jnp.int32, s.shape, 1), s, -1e30)
            e = jnp.exp(s - jnp.max(s, axis=-1, keepdims=True))
            prob = (e / jnp.sum(e, axis=-1, keepdims=True)).astype(BF)
            o_ref[here, cols] = jnp.dot(prob, qkv_ref[2, 0:keys, cols], preferred_element_type=F32).astype(BF)

    loop(heads, head)
    sums = LineSum(i, n, part, land, s_send, s_recv, pieces)
    tile = 512

    def project(t):
        d = jnp.where(i < n // 2, n - 1 - t, t)

        def columns(k):
            cols = rows_at(k, tile)
            part[d, :, cols] = jnp.dot(o_ref[rows_at(d, size), :], w_ref[:, cols], preferred_element_type=F32).astype(BF)

        loop(depth // tile, columns)
        sums.launch(d)

    loop(n, project)

    def round_of(r):
        line.step(r + 1)
        right, left = n - 1 + i - (r + 1), r + 1 - (n - 1 - i)

        @pl.when(jnp.logical_and(i > 0, jnp.logical_and(right > i, right <= n - 1)))
        def _():
            sums.relay(right, True)

        @pl.when(jnp.logical_and(i < n - 1, jnp.logical_and(left >= 0, left < i)))
        def _():
            sums.relay(left, False)

    loop(n - 1, round_of)
    sums.own()

    def norm(b):
        here = rows_at(b, RB)
        sums.add(here, h_ref.at[here, :])
        rows = h_ref[here, :] + (x_ref[here, :].astype(F32) + out_bias[...])
        h_ref[here, :] = rows
        normal, _ = norm_stats(rows)
        c_ref[here, :] = (normal * gain[...] + shift[...]).astype(BF)

    loop(size // RB, norm)
    own_copy.wait()
    line.finish()
    sums.finish()


def hidden_kernel(n, pieces, c_ref, h_ref, cot_hbm, up_hbm, down_hbm, up_bias, gain, c_hbm, g_hbm, du_hbm, dh_ref,
                  db_ref, vec_ref, upb_ref, c_all, g_all, du_all, cot_all, up, down, part, land, send, recv, s_send,
                  s_recv, w_sem, cot_sem, own_sem, c_sem, g_sem, du_sem):
    i = lax.axis_index("tensor")
    size, depth = c_ref.shape
    units = up.shape[1]
    greet_neighbours(i, n)
    line = LineGather(i, n, c_ref, c_all, send, recv)
    line.start()
    own_copy = pltpu.make_async_copy(c_ref, c_all.at[i], own_sem)
    own_copy.start()
    up_copy = pltpu.make_async_copy(up_hbm, up, w_sem.at[0])
    up_copy.start()
    down_copy = pltpu.make_async_copy(down_hbm, down, w_sem.at[1])
    down_copy.start()
    cot_copy = pltpu.make_async_copy(cot_hbm, cot_all, cot_sem)
    cot_copy.start()
    upb_ref[...] = jnp.zeros_like(upb_ref)
    vec_ref[...] = jnp.zeros_like(vec_ref)
    own_copy.wait()
    up_copy.wait()
    down_copy.wait()
    cot_copy.wait()
    sums = LineSum(i, n, part, land, s_send, s_recv, pieces)
    tile = 256

    def out_copy(src, dst, sem, j):
        return pltpu.make_async_copy(src.at[j], dst.at[j], sem.at[j])

    def compute(j):
        def unit(k):
            cols = rows_at(k, tile)
            u = jnp.dot(c_all[j], up[:, cols], preferred_element_type=F32) + up_bias[0:1, cols]
            dg = lax.dot_general(cot_all[j], down[cols, :], NT, preferred_element_type=F32)
            half = 0.5 + 0.5 * lax.erf(u * (0.5 ** 0.5))
            g_all[j, :, cols] = (u * half).astype(BF)
            slope = half + u * (jnp.exp(u * u * -0.5) * 0.3989422804014327)
            du = (slope * dg).astype(BF)
            du_all[j, :, cols] = du
            upb_ref[0:1, cols] += jnp.sum(du.astype(F32), axis=0, keepdims=True)

        loop(units // tile, unit)

        def back(k):
            cols = rows_at(k, tile)
            part[j, :, cols] = lax.dot_general(du_all[j], up[cols, :], NT, preferred_element_type=F32).astype(BF)

        loop(depth // tile, back)
        sums.launch(j)
        out_copy(g_all, g_hbm, g_sem, j).start()
        out_copy(du_all, du_hbm, du_sem, j).start()
        out_copy(c_all, c_hbm, c_sem, j).start()

    def round_of(r):
        @pl.when(r > 0)
        def _():
            line.step(r)

        def side(s):
            j = jnp.where(s == 0, i - r, i + r)

            @pl.when(jnp.logical_and(jnp.logical_and(j >= 0, j <= n - 1), s * r == s * jnp.maximum(r, 1)))
            def _():
                compute(j)

        loop(2, side)

    loop(n, round_of)

    def relay(t):
        right, left = t + 2 - i, 2 * n - 4 - i - t

        @pl.when(jnp.logical_and(i > 0, jnp.logical_and(right > i, right <= n - 1)))
        def _():
            sums.relay(right, True)

        @pl.when(jnp.logical_and(i < n - 1, jnp.logical_and(left >= 0, left < i)))
        def _():
            sums.relay(left, False)

    loop(2 * n - 3, relay)
    sums.own()

    def norm(b):
        here = rows_at(b, RB)
        sums.add(here, dh_ref.at[here, :])
        grad = dh_ref[here, :]
        normal, inverse = norm_stats(h_ref[here, :])
        vec_ref[0:1, :] += jnp.sum(grad * normal, axis=0, keepdims=True)
        vec_ref[1:2, :] += jnp.sum(grad, axis=0, keepdims=True)
        cot = cot_all[i, here, :].astype(F32)
        dh = cot + norm_back(grad, normal, inverse, gain[...])
        dh_ref[here, :] = dh
        db = dh.astype(BF)
        db_ref[here, :] = db
        vec_ref[2:3, :] += jnp.sum(db.astype(F32), axis=0, keepdims=True)
        vec_ref[3:4, :] += jnp.sum(cot, axis=0, keepdims=True)

    loop(size // RB, norm)

    def done(j):
        out_copy(g_all, g_hbm, g_sem, j).wait()
        out_copy(du_all, du_hbm, du_sem, j).wait()
        out_copy(c_all, c_hbm, c_sem, j).wait()

    loop(n, done)
    line.finish()
    sums.finish()


def attend_back_kernel(qkv_ref, do_ref, out_ref, dk, dv):
    heads = qkv_ref.shape[2] // HD
    block = 256
    factor = HD ** (-0.5)

    def head(t):
        cols = pl.ds(pl.multiple_of(t * HD, HD), HD)
        dk[...] = jnp.zeros_like(dk)
        dv[...] = jnp.zeros_like(dv)
        for b in range(LEN // block):
            here, keys = slice(b * block, (b + 1) * block), (b + 1) * block
            q, k, v = qkv_ref[0, here, cols], qkv_ref[1, 0:keys, cols], qkv_ref[2, 0:keys, cols]
            do = do_ref[here, cols]
            s = lax.dot_general(q, k, NT, preferred_element_type=F32) * factor
            query = lax.broadcasted_iota(jnp.int32, s.shape, 0) + b * block
            s = jnp.where(query >= lax.broadcasted_iota(jnp.int32, s.shape, 1), s, -1e30)
            e = jnp.exp(s - jnp.max(s, axis=-1, keepdims=True))
            prob = e / jnp.sum(e, axis=-1, keepdims=True)
            dv[0:keys, :] += lax.dot_general(prob.astype(BF), do, TN, preferred_element_type=F32)
            dp = lax.dot_general(do, v, NT, preferred_element_type=F32)
            ds = (prob * (dp - jnp.sum(prob * dp, axis=-1, keepdims=True))).astype(BF)
            out_ref[0, here, cols] = (jnp.dot(ds, k, preferred_element_type=F32) * factor).astype(BF)
            dk[0:keys, :] += lax.dot_general(ds, q, TN, preferred_element_type=F32)
        out_ref[1, :, cols] = (dk[...] * factor).astype(BF)
        out_ref[2, :, cols] = dv[...].astype(BF)

    loop(heads, head)


def params(collective=None):
    if collective is None:
        return pltpu.CompilerParams(vmem_limit_bytes=BIG)
    return pltpu.CompilerParams(vmem_limit_bytes=BIG, collective_id=collective, has_side_effects=True)


def shape(dims, dtype):
    return jax.ShapeDtypeStruct(dims, dtype)


class Line:
    def __init__(self, axis, size):
        self.axis, self.n = axis, size
        self.i = lax.axis_index(axis)
        self.first = self.i < size // 2

    def owner(self, k):
        return jnp.where(self.first, self.i + k, self.i - k + self.n) % self.n

    def gather(self, block):
        n = self.n
        down, up = [block], [block]
        for r in range(1, n):
            down.append(lax.ppermute(down[-1], self.axis, [(i, i - 1) for i in range(1, n) if i + r - 1 <= n - 1]))
            up.append(lax.ppermute(up[-1], self.axis, [(i, i + 1) for i in range(n - 1) if i - r + 1 >= 0]))
        slots = [block]
        for k in range(1, n):
            if 2 * k <= n:
                slots.append(jnp.where(self.first, down[k], up[k]))
            else:
                low = jnp.where(self.i + k <= n - 1, down[k], up[n - k])
                high = jnp.where(self.i - k >= 0, up[k], down[n - k])
                slots.append(jnp.where(self.first, low, high))
        return slots

    def scatter_sum(self, parts):
        n = self.n
        right = left = None

        def pick(owner):
            return lax.dynamic_index_in_dim(parts, owner % n, 0, keepdims=False).astype(F32)

        for r in range(1, n):
            term = pick(self.i + n - r)
            term = term if right is None else term + right.astype(F32)
            right = lax.ppermute(term.astype(BF), self.axis, [(i, i + 1) for i in range(min(r, n - 1))])
            term = pick(self.i + r)
            term = term if left is None else term + left.astype(F32)
            left = lax.ppermute(term.astype(BF), self.axis, [(i, i - 1) for i in range(max(n - r, 1), n)])
        return pick(self.i) + (right.astype(F32) + left.astype(F32))


def body(tokens, cotangent, ln1_gain, ln1_bias, qkv_weight, qv_bias, out_weight, out_bias, ln2_gain, ln2_bias,
         up_weight, up_bias, down_weight, down_bias):
    n = lax.axis_size("tensor")
    m = lax.axis_size("dp")
    i, row = lax.axis_index("tensor"), lax.axis_index("dp")
    line = Line("tensor", n)
    size, depth = tokens.shape
    width = qkv_weight.shape[2]
    units = up_weight.shape[1]
    piece, qv_piece, up_piece = ln1_gain.shape[0], qv_bias.shape[1], up_bias.shape[0]
    total = m * n

    def lane_rows(value, index):
        count = value.shape[-1]
        if count >= LANES:
            return value.reshape(-1, LANES)
        places = LANES // count
        spread = jnp.tile(value.reshape(-1, count), (1, places))
        return jnp.where((jnp.arange(LANES) // count)[None] == index % places, spread, 0)

    me = row * n + i
    whole = jnp.stack([ln1_gain, ln1_bias, out_bias, ln2_gain, ln2_bias, down_bias])
    pack = jnp.concatenate([lane_rows(whole, me), lane_rows(qv_bias, row), lane_rows(up_bias, row)])
    pack = jnp.pad(pack.astype(F32), ((0, -pack.shape[0] % 8), (0, 0)))
    lanes_up = 8 + max(up_piece // LANES, 1)

    w_qkv = lax.all_gather(qkv_weight, "dp", axis=1, tiled=True)
    w_out = lax.all_gather(out_weight, "dp", axis=1, tiled=True)
    w_up = lax.all_gather(up_weight, "dp", axis=0, tiled=True)
    w_down = lax.all_gather(down_weight, "dp", axis=1, tiled=True)

    dma = pltpu.SemaphoreType.DMA
    attn_in, qkv, vecs = pl.pallas_call(
        functools.partial(project_kernel, n, m, (piece, qv_piece)),
        out_shape=(shape((LEN, depth), BF), shape((3, LEN, width), BF), shape((total,) + pack.shape, F32)),
        in_specs=[VM, VM, ANY], out_specs=(VM, VM, VM),
        scratch_shapes=[pltpu.VMEM((n, size, depth), BF), pltpu.VMEM((3, depth, width), BF), pltpu.VMEM((8, depth), F32),
                        pltpu.VMEM((8, width), F32), dma, dma, dma((2, n)), dma((n,)), dma((total,)), dma((total,))],
        compiler_params=params(0), name="project",
    )(pack, tokens, w_qkv)
    vectors = vecs.reshape(depth // LANES, LANES // piece, -1, LANES).sum(axis=1)
    vectors = vectors[:, 2:6].transpose(1, 0, 2).reshape(4, 1, depth)
    bias_out, gain_two, shift_two, bias_down = [vectors[j] for j in range(4)]
    ups = lax.dynamic_index_in_dim(vecs.reshape(m, n, -1, LANES), i, 1, keepdims=False)[:, 8:lanes_up]
    if up_piece < LANES:
        ups = ups.reshape(units // LANES, LANES // up_piece, LANES).sum(axis=1)
    bias_up = ups.reshape(1, units)

    pieces = 2
    sums = [pltpu.VMEM((n, size, depth), BF), pltpu.VMEM((n + 1, size, depth), BF)]
    mixture, residual, mlp_own, cot_all = pl.pallas_call(
        functools.partial(attend_kernel, n, pieces),
        out_shape=(shape((LEN, width), BF), shape((size, depth), F32), shape((size, depth), BF),
                   shape((n, size, depth), BF)),
        in_specs=[VM] * 7, out_specs=(VM,) * 4,
        scratch_shapes=sums + [dma((2, n)), dma((n,)), dma((n, pieces)), dma((n + 1, pieces)), dma],
        compiler_params=params(1), name="attend",
    )(qkv, w_out, tokens, cotangent, bias_out, gain_two, shift_two)

    pieces = 4
    mlp_in, hidden, grad_pre, grad_resid, branch_cot, vec_two, grad_up_b = pl.pallas_call(
        functools.partial(hidden_kernel, n, pieces),
        out_shape=(shape((n, size, depth), BF), shape((n, size, units), BF), shape((n, size, units), BF),
                   shape((size, depth), F32), shape((size, depth), BF), shape((8, depth), F32), shape((8, units), F32)),
        in_specs=[VM, VM, ANY, ANY, ANY, VM, VM], out_specs=(ANY, ANY, ANY, VM, VM, VM, VM),
        scratch_shapes=[pltpu.VMEM((n, size, depth), BF), pltpu.VMEM((n, size, units), BF),
                        pltpu.VMEM((n, size, units), BF), pltpu.VMEM((n, size, depth), BF),
                        pltpu.VMEM((depth, units), BF), pltpu.VMEM((units, depth), BF)] + sums +
                       [dma((2, n)), dma((n,)), dma((n, pieces)), dma((n + 1, pieces)), dma((2,)), dma, dma,
                        dma((n,)), dma((n,)), dma((n,))],
        compiler_params=params(2), name="hidden",
    )(mlp_own, residual, cot_all, w_up, w_down, bias_up, gain_two)
    mlp_in, hidden, grad_pre = [v.reshape(LEN, -1) for v in (mlp_in, hidden, grad_pre)]
    cot_rows = cot_all.reshape(LEN, depth)

    mlp_part = jnp.dot(hidden, w_down, preferred_element_type=F32).astype(BF)
    layer_out = (residual + (line.scatter_sum(mlp_part.reshape(n, size, depth)) + bias_down)).astype(BF)
    grad_down_w = jnp.einsum("rf,rd->fd", hidden, cot_rows, preferred_element_type=F32).astype(BF)
    grad_up_w = jnp.einsum("rd,rf->df", mlp_in, grad_pre, preferred_element_type=F32).astype(BF)

    slots = line.gather(branch_cot)
    attn_cot = jnp.zeros((LEN, depth), BF)
    for k in range(n):
        attn_cot = lax.dynamic_update_slice(attn_cot, slots[k], (line.owner(k) * size, 0))
    grad_mix = jnp.einsum("rd,ed->re", attn_cot, w_out, preferred_element_type=F32).astype(BF)
    grad_qkv = pl.pallas_call(
        attend_back_kernel, out_shape=shape((3, LEN, width), BF), in_specs=[VM, VM], out_specs=VM,
        scratch_shapes=[pltpu.VMEM((LEN, HD), F32), pltpu.VMEM((LEN, HD), F32)],
        compiler_params=params(), name="attend_back",
        cost_estimate=pl.CostEstimate(flops=14 * LEN * LEN * width // 2, bytes_accessed=14 * LEN * width,
                                      transcendentals=LEN * LEN * width // HD),
    )(qkv, grad_mix)
    attn_back = jnp.einsum("kre,kde->rd", grad_qkv, w_qkv, preferred_element_type=F32).astype(BF)
    grad_normed_one = line.scatter_sum(attn_back.reshape(n, size, depth))
    normal_one, inverse_one = norm_stats(tokens.astype(F32))
    gain_one = vecs.reshape(depth // LANES, LANES // piece, -1, LANES).sum(axis=1)[:, 0].reshape(1, depth)
    grad_tokens = (grad_resid + norm_back(grad_normed_one, normal_one, inverse_one, gain_one)).astype(BF)

    grad_out_w = jnp.einsum("re,rd->ed", mixture, attn_cot, preferred_element_type=F32).astype(BF)
    grad_qkv_w = jnp.einsum("rd,kre->kde", attn_in, grad_qkv, preferred_element_type=F32).astype(BF)
    grad_down_w = lax.psum_scatter(grad_down_w, "dp", scatter_dimension=1, tiled=True).astype(F32)
    grad_up_w = lax.psum_scatter(grad_up_w, "dp", scatter_dimension=0, tiled=True).astype(F32)
    grad_out_w = lax.psum_scatter(grad_out_w, "dp", scatter_dimension=1, tiled=True).astype(F32)
    grad_qkv_w = lax.psum_scatter(grad_qkv_w, "dp", scatter_dimension=1, tiled=True).astype(F32)

    vectors = jnp.stack([
        jnp.sum(grad_normed_one * normal_one, axis=0),
        jnp.sum(grad_normed_one, axis=0),
        vec_two[2], vec_two[0], vec_two[1], vec_two[3],
    ])
    vectors = vectors.reshape(6, m, n, piece).transpose(1, 2, 0, 3).reshape(m, n * 6 * piece)
    grad_qv_b = jnp.sum(grad_qkv[0::2].astype(F32), axis=1).reshape(2, m, qv_piece).transpose(1, 0, 2)
    packed = jnp.concatenate([vectors, grad_qv_b.reshape(m, -1), grad_up_b[0].reshape(m, -1)], axis=1)
    packed = jnp.sum(lax.all_to_all(packed, "dp", 0, 0), axis=0)
    grad_up_b = packed[n * 6 * piece + 2 * qv_piece :]
    grad_qv_b = packed[n * 6 * piece : n * 6 * piece + 2 * qv_piece].reshape(2, qv_piece)
    vectors = packed[: n * 6 * piece].reshape(n, 6 * piece)
    vectors = jnp.sum(lax.all_to_all(vectors, "tensor", 0, 0), axis=0).reshape(6, piece)
    return (layer_out, grad_tokens, vectors[0], vectors[1], grad_qkv_w, grad_qv_b, grad_out_w, vectors[2],
            vectors[3], vectors[4], grad_up_w, grad_up_b, grad_down_w, vectors[5])


def solution(mesh):
    vector, matrix = P(("dp", "tensor")), P(("dp", "tensor"), None)
    in_specs = (matrix, matrix, vector, vector, P(None, "dp", "tensor"), P(None, ("tensor", "dp")), P("tensor", "dp"),
                vector, vector, vector, P("dp", "tensor"), P(("tensor", "dp")), P("tensor", "dp"), vector)
    out_specs = (matrix, matrix, vector, vector, P(None, "dp", "tensor"), P(None, ("tensor", "dp")),
                 P("tensor", "dp"), vector, vector, vector, P("dp", "tensor"), P(("tensor", "dp")), P("tensor", "dp"),
                 vector)
    return jax.shard_map(body, mesh=mesh, in_specs=in_specs, out_specs=out_specs, check_vma=False)
```

```python
import functools

import jax
import jax.numpy as jnp
from jax import lax
from jax.experimental import pallas as pl
from jax.experimental.pallas import tpu as pltpu
from jax.sharding import PartitionSpec as P

HD = 128
LEN = 1024
LANES = 128
EPS = 1e-05
BF = jnp.bfloat16
F32 = jnp.float32
MESH = pl.DeviceIdType.MESH
ANY = pl.BlockSpec(memory_space=pl.ANY)
VM = pl.BlockSpec(memory_space=pltpu.VMEM)
NT = (((1,), (1,)), ((), ()))
TN = (((0,), (0,)), ((), ()))
BIG = 64 * 1024 * 1024 - 65536
RB = 32


def norm_stats(rows):
    mean = jnp.mean(rows, axis=-1, keepdims=True)
    centred = rows - mean
    variance = jnp.mean(centred * centred, axis=-1, keepdims=True)
    inverse = lax.rsqrt(variance + EPS)
    return centred * inverse, inverse


def norm_back(grad_rows, normal_rows, inverse, gain):
    scaled = grad_rows * gain
    first = jnp.mean(scaled, axis=-1, keepdims=True)
    second = jnp.mean(scaled * normal_rows, axis=-1, keepdims=True)
    return inverse * (scaled - first - normal_rows * second)


def loop(count, step):
    def run(i, carry):
        step(i)
        return carry

    lax.fori_loop(0, count, run, 0)


def rows_at(j, size):
    return pl.ds(pl.multiple_of(j * size, size), size)


def remote(src, dst, send, recv, target):
    return pltpu.make_async_remote_copy(src_ref=src, dst_ref=dst, send_sem=send, recv_sem=recv,
                                        device_id={"tensor": target}, device_id_type=MESH)


def greet_neighbours(i, n):
    barrier = pltpu.get_barrier_semaphore()

    @pl.when(i > 0)
    def _():
        pl.semaphore_signal(barrier, inc=1, device_id={"tensor": i - 1}, device_id_type=MESH)

    @pl.when(i < n - 1)
    def _():
        pl.semaphore_signal(barrier, inc=1, device_id={"tensor": i + 1}, device_id_type=MESH)

    pl.semaphore_wait(barrier, jnp.minimum(i, 1) + jnp.minimum(n - 1 - i, 1))


def greet_all(me, n, total):
    barrier = pltpu.get_barrier_semaphore()

    def greet(s):
        other = (me + s + 1) % total
        pl.semaphore_signal(barrier, inc=1, device_id={"dp": other // n, "tensor": other % n}, device_id_type=MESH)

    loop(total - 1, greet)
    pl.semaphore_wait(barrier, total - 1)


def rounds(i, n, line, compute):
    def round_of(r):
        @pl.when(r > 0)
        def _():
            line.step(r)

        def side(s):
            j = jnp.where(s == 0, i - r, i + r)

            @pl.when(jnp.logical_and(jnp.logical_and(j >= 0, j <= n - 1), s * r == s * jnp.maximum(r, 1)))
            def _():
                compute(j)

        loop(2, side)

    loop(n, round_of)


class LineGather:
    def __init__(self, i, n, own, buf, send, recv):
        self.i, self.n, self.own, self.buf, self.send, self.recv = i, n, own, buf, send, recv

    def copy(self, src, j, side, target):
        return remote(src, self.buf.at[j], self.send.at[side, j], self.recv.at[j], target)

    def start(self):
        i, n = self.i, self.n

        @pl.when(i < n - 1)
        def _():
            self.copy(self.own, i, 0, i + 1).start()

        @pl.when(i > 0)
        def _():
            self.copy(self.own, i, 1, i - 1).start()

    def step(self, r):
        i, n = self.i, self.n

        @pl.when(i - r >= 0)
        def _():
            self.copy(self.own, i - r, 0, i).wait_recv()

            @pl.when(i < n - 1)
            def _():
                self.copy(self.buf.at[i - r], i - r, 0, i + 1).start()

        @pl.when(i + r <= n - 1)
        def _():
            self.copy(self.own, i + r, 1, i).wait_recv()

            @pl.when(i > 0)
            def _():
                self.copy(self.buf.at[i + r], i + r, 1, i - 1).start()

    def finish(self):
        i, n = self.i, self.n

        def one(j):
            @pl.when(jnp.logical_and(i < n - 1, j <= i))
            def _():
                self.copy(self.own, j, 0, i + 1).wait_send()

            @pl.when(jnp.logical_and(i > 0, j >= i))
            def _():
                self.copy(self.own, j, 1, i - 1).wait_send()

        loop(n, one)


class LineSum:
    def __init__(self, i, n, part, land, send, recv, pieces):
        self.i, self.n, self.part, self.land, self.send, self.recv = i, n, part, land, send, recv
        self.pieces = pieces
        self.size = part.shape[1] // pieces

    def copy(self, src, d, right, s):
        i, n = self.i, self.n
        target = i + 1 if right else i - 1
        slot = d if right else jnp.where(d == target, n, d)
        here = rows_at(s, self.size)
        return remote(src.at[d, here], self.land.at[slot, here], self.send.at[d, s], self.recv.at[slot, s], target)

    def arrived(self, slot, s):
        here = rows_at(s, self.size)
        remote(self.part.at[0, here], self.land.at[slot, here], self.send.at[0, s], self.recv.at[slot, s],
               self.i).wait_recv()

    def launch(self, d):
        i, n = self.i, self.n

        @pl.when(jnp.logical_and(i == 0, d > 0))
        def _():
            loop(self.pieces, lambda s: self.copy(self.part, d, True, s).start())

        @pl.when(jnp.logical_and(i == n - 1, d < n - 1))
        def _():
            loop(self.pieces, lambda s: self.copy(self.part, d, False, s).start())

    def relay(self, d, right):
        def one(s):
            self.arrived(d, s)
            here = rows_at(s, self.size)
            total = self.land[d, here, :].astype(F32) + self.part[d, here, :].astype(F32)
            self.land[d, here, :] = total.astype(BF)
            self.copy(self.land, d, right, s).start()

        loop(self.pieces, one)

    def own(self):
        i, n = self.i, self.n

        @pl.when(i > 0)
        def _():
            loop(self.pieces, lambda s: self.arrived(i, s))

        @pl.when(i < n - 1)
        def _():
            loop(self.pieces, lambda s: self.arrived(n, s))

    def add(self, here, out):
        i, n = self.i, self.n
        out[...] = self.part[i, here, :].astype(F32)

        @pl.when(i > 0)
        def _():
            out[...] += self.land[i, here, :].astype(F32)

        @pl.when(i < n - 1)
        def _():
            out[...] += self.land[n, here, :].astype(F32)

    def finish(self):
        i, n = self.i, self.n

        def one(d):
            @pl.when(jnp.logical_and(i < n - 1, d > i))
            def _():
                loop(self.pieces, lambda s: self.copy(self.part, d, True, s).wait_send())

            @pl.when(jnp.logical_and(i > 0, d < i))
            def _():
                loop(self.pieces, lambda s: self.copy(self.part, d, False, s).wait_send())

        loop(n, one)


def tokens_kernel(n, m, piece, pack_ref, x_ref, a_ref, vec_ref, buf, affine, own_sem, send, recv, v_send, v_recv):
    i, row = lax.axis_index("tensor"), lax.axis_index("dp")
    me, total = row * n + i, m * n
    size = x_ref.shape[0]
    greet_all(me, n, total)
    line = LineGather(i, n, x_ref, buf, send, recv)
    line.start()

    def vector(src, other):
        return pltpu.make_async_remote_copy(
            src_ref=pack_ref, dst_ref=vec_ref.at[src], send_sem=v_send.at[other], recv_sem=v_recv.at[src],
            device_id={"dp": other // n, "tensor": other % n}, device_id_type=MESH)

    loop(total - 1, lambda s: vector(me, (me + s + 1) % total).start())
    own_copy = pltpu.make_async_copy(x_ref, buf.at[i], own_sem)
    own_copy.start()
    vec_ref[me] = pack_ref[...]
    loop(total - 1, lambda s: vector((me + s + 1) % total, me).wait_recv())
    depth = affine.shape[1]
    group = LANES // piece
    for tile in range(depth // LANES):
        value = vec_ref[tile * group, 0:2, :]
        for g in range(1, group):
            value = value + vec_ref[tile * group + g, 0:2, :]
        affine[0:2, tile * LANES : (tile + 1) * LANES] = value
    own_copy.wait()

    def compute(j):
        def norm(b):
            normal, _ = norm_stats(buf[j, rows_at(b, RB), :].astype(F32))
            here = pl.ds(pl.multiple_of(j * size + b * RB, RB), RB)
            a_ref[here, :] = (normal * affine[0:1, :] + affine[1:2, :]).astype(BF)

        loop(size // RB, norm)

    rounds(i, n, line, compute)
    line.finish()
    loop(total - 1, lambda s: vector(me, (me + s + 1) % total).wait_send())


def attend_kernel(n, pieces, a_hbm, wq_hbm, wo_hbm, x_ref, cot_ref, bias, out_bias, gain, shift, qkv_ref, o_ref, h_ref,
                  c_ref, cot_all, a_ref, wq_ref, w_ref, part, land, send, recv, s_send, s_recv, own_sem, a_sem, w_sem):
    i = lax.axis_index("tensor")
    size = x_ref.shape[0]
    loads = [pltpu.make_async_copy(a_hbm, a_ref, a_sem)]
    loads += [pltpu.make_async_copy(wq_hbm.at[t], wq_ref.at[t], w_sem.at[t]) for t in range(3)]
    loads += [pltpu.make_async_copy(wo_hbm, w_ref, w_sem.at[3])]
    for load in loads:
        load.start()
    heads = qkv_ref.shape[2] // HD
    depth = w_ref.shape[1]
    greet_neighbours(i, n)
    line = LineGather(i, n, cot_ref, cot_all, send, recv)
    line.start()
    own_copy = pltpu.make_async_copy(cot_ref, cot_all.at[i], own_sem)
    own_copy.start()

    loads[0].wait()
    block = 256
    for t in range(3):
        loads[1 + t].wait()

        def project(b):
            here = rows_at(b, block)
            value = jnp.dot(a_ref[here, :], wq_ref[t], preferred_element_type=F32)
            if t != 1:
                value = value + bias[t // 2 : t // 2 + 1, :]
            qkv_ref[t, here, :] = value.astype(BF)

        loop(LEN // block, project)

    def head(t):
        cols = pl.ds(pl.multiple_of(t * HD, HD), HD)
        for b in range(LEN // block):
            here, keys = slice(b * block, (b + 1) * block), (b + 1) * block
            s = lax.dot_general(qkv_ref[0, here, cols], qkv_ref[1, 0:keys, cols], NT,
                                preferred_element_type=F32) * HD ** (-0.5)
            query = lax.broadcasted_iota(jnp.int32, s.shape, 0) + b * block
            s = jnp.where(query >= lax.broadcasted_iota(jnp.int32, s.shape, 1), s, -1e30)
            e = jnp.exp(s - jnp.max(s, axis=-1, keepdims=True))
            prob = (e / jnp.sum(e, axis=-1, keepdims=True)).astype(BF)
            o_ref[here, cols] = jnp.dot(prob, qkv_ref[2, 0:keys, cols], preferred_element_type=F32).astype(BF)

    loop(heads, head)
    loads[4].wait()
    sums = LineSum(i, n, part, land, s_send, s_recv, pieces)
    tile = 512

    def project(t):
        d = jnp.where(i < n // 2, n - 1 - t, t)

        def columns(k):
            cols = rows_at(k, tile)
            part[d, :, cols] = jnp.dot(o_ref[rows_at(d, size), :], w_ref[:, cols], preferred_element_type=F32).astype(BF)

        loop(depth // tile, columns)
        sums.launch(d)

    loop(n, project)

    def round_of(r):
        line.step(r + 1)
        right, left = n - 1 + i - (r + 1), r + 1 - (n - 1 - i)

        @pl.when(jnp.logical_and(i > 0, jnp.logical_and(right > i, right <= n - 1)))
        def _():
            sums.relay(right, True)

        @pl.when(jnp.logical_and(i < n - 1, jnp.logical_and(left >= 0, left < i)))
        def _():
            sums.relay(left, False)

    loop(n - 1, round_of)
    sums.own()

    def norm(b):
        here = rows_at(b, RB)
        sums.add(here, h_ref.at[here, :])
        rows = h_ref[here, :] + (x_ref[here, :].astype(F32) + out_bias[...])
        h_ref[here, :] = rows
        normal, _ = norm_stats(rows)
        c_ref[here, :] = (normal * gain[...] + shift[...]).astype(BF)

    loop(size // RB, norm)
    own_copy.wait()
    line.finish()
    sums.finish()


def hidden_kernel(n, pieces, c_ref, h_ref, cot_hbm, up_hbm, down_hbm, up_bias, gain, c_hbm, g_hbm, du_hbm, dh_ref,
                  db_ref, vec_ref, upb_ref, c_all, g_all, du_all, cot_all, up, down, part, land, send, recv, s_send,
                  s_recv, w_sem, cot_sem, own_sem, c_sem, g_sem, du_sem):
    i = lax.axis_index("tensor")
    size, depth = c_ref.shape
    units = up.shape[1]
    greet_neighbours(i, n)
    line = LineGather(i, n, c_ref, c_all, send, recv)
    line.start()
    own_copy = pltpu.make_async_copy(c_ref, c_all.at[i], own_sem)
    own_copy.start()
    up_copy = pltpu.make_async_copy(up_hbm, up, w_sem.at[0])
    up_copy.start()
    down_copy = pltpu.make_async_copy(down_hbm, down, w_sem.at[1])
    down_copy.start()
    cot_copy = pltpu.make_async_copy(cot_hbm, cot_all, cot_sem)
    cot_copy.start()
    upb_ref[...] = jnp.zeros_like(upb_ref)
    vec_ref[...] = jnp.zeros_like(vec_ref)
    own_copy.wait()
    up_copy.wait()
    down_copy.wait()
    cot_copy.wait()
    sums = LineSum(i, n, part, land, s_send, s_recv, pieces)
    tile = 256

    def out_copy(src, dst, sem, j):
        return pltpu.make_async_copy(src.at[j], dst.at[j], sem.at[j])

    def compute(j):
        def unit(k):
            cols = rows_at(k, tile)
            u = jnp.dot(c_all[j], up[:, cols], preferred_element_type=F32) + up_bias[0:1, cols]
            dg = lax.dot_general(cot_all[j], down[cols, :], NT, preferred_element_type=F32)
            half = 0.5 + 0.5 * lax.erf(u * (0.5 ** 0.5))
            g_all[j, :, cols] = (u * half).astype(BF)
            slope = half + u * (jnp.exp(u * u * -0.5) * 0.3989422804014327)
            du = (slope * dg).astype(BF)
            du_all[j, :, cols] = du
            upb_ref[0:1, cols] += jnp.sum(du.astype(F32), axis=0, keepdims=True)

        loop(units // tile, unit)

        def back(k):
            cols = rows_at(k, tile)
            part[j, :, cols] = lax.dot_general(du_all[j], up[cols, :], NT, preferred_element_type=F32).astype(BF)

        loop(depth // tile, back)
        sums.launch(j)
        out_copy(g_all, g_hbm, g_sem, j).start()
        out_copy(du_all, du_hbm, du_sem, j).start()
        out_copy(c_all, c_hbm, c_sem, j).start()

    rounds(i, n, line, compute)

    def relay(t):
        right, left = t + 2 - i, 2 * n - 4 - i - t

        @pl.when(jnp.logical_and(i > 0, jnp.logical_and(right > i, right <= n - 1)))
        def _():
            sums.relay(right, True)

        @pl.when(jnp.logical_and(i < n - 1, jnp.logical_and(left >= 0, left < i)))
        def _():
            sums.relay(left, False)

    loop(2 * n - 3, relay)
    sums.own()

    def norm(b):
        here = rows_at(b, RB)
        sums.add(here, dh_ref.at[here, :])
        grad = dh_ref[here, :]
        normal, inverse = norm_stats(h_ref[here, :])
        vec_ref[0:1, :] += jnp.sum(grad * normal, axis=0, keepdims=True)
        vec_ref[1:2, :] += jnp.sum(grad, axis=0, keepdims=True)
        cot = cot_all[i, here, :].astype(F32)
        dh = cot + norm_back(grad, normal, inverse, gain[...])
        dh_ref[here, :] = dh
        db = dh.astype(BF)
        db_ref[here, :] = db
        vec_ref[2:3, :] += jnp.sum(db.astype(F32), axis=0, keepdims=True)
        vec_ref[3:4, :] += jnp.sum(cot, axis=0, keepdims=True)

    loop(size // RB, norm)

    def done(j):
        out_copy(g_all, g_hbm, g_sem, j).wait()
        out_copy(du_all, du_hbm, du_sem, j).wait()
        out_copy(c_all, c_hbm, c_sem, j).wait()

    loop(n, done)
    line.finish()
    sums.finish()


def attend_back_kernel(qkv_ref, do_ref, out_ref, dk, dv):
    heads = qkv_ref.shape[2] // HD
    block = 256
    factor = HD ** (-0.5)

    def head(t):
        cols = pl.ds(pl.multiple_of(t * HD, HD), HD)
        dk[...] = jnp.zeros_like(dk)
        dv[...] = jnp.zeros_like(dv)
        for b in range(LEN // block):
            here, keys = slice(b * block, (b + 1) * block), (b + 1) * block
            q, k, v = qkv_ref[0, here, cols], qkv_ref[1, 0:keys, cols], qkv_ref[2, 0:keys, cols]
            do = do_ref[here, cols]
            s = lax.dot_general(q, k, NT, preferred_element_type=F32) * factor
            query = lax.broadcasted_iota(jnp.int32, s.shape, 0) + b * block
            s = jnp.where(query >= lax.broadcasted_iota(jnp.int32, s.shape, 1), s, -1e30)
            e = jnp.exp(s - jnp.max(s, axis=-1, keepdims=True))
            prob = e / jnp.sum(e, axis=-1, keepdims=True)
            dv[0:keys, :] += lax.dot_general(prob.astype(BF), do, TN, preferred_element_type=F32)
            dp = lax.dot_general(do, v, NT, preferred_element_type=F32)
            ds = (prob * (dp - jnp.sum(prob * dp, axis=-1, keepdims=True))).astype(BF)
            out_ref[0, here, cols] = (jnp.dot(ds, k, preferred_element_type=F32) * factor).astype(BF)
            dk[0:keys, :] += lax.dot_general(ds, q, TN, preferred_element_type=F32)
        out_ref[1, :, cols] = (dk[...] * factor).astype(BF)
        out_ref[2, :, cols] = dv[...].astype(BF)

    loop(heads, head)


def share_kernel(n, m, load_ref, every_ref, column_ref, land, send, recv):
    i, row = lax.axis_index("tensor"), lax.axis_index("dp")
    me, total = row * n + i, m * n
    greet_all(me, n, total)

    def copy(src, other):
        return pltpu.make_async_remote_copy(
            src_ref=load_ref.at[other], dst_ref=land.at[src], send_sem=send.at[other], recv_sem=recv.at[src],
            device_id={"dp": other // n, "tensor": other % n}, device_id_type=MESH)

    loop(total - 1, lambda s: copy(me, (me + s + 1) % total).start())
    land[me] = load_ref[me]
    every_ref[...] = jnp.zeros_like(every_ref)
    column_ref[...] = jnp.zeros_like(column_ref)
    loop(total - 1, lambda s: copy((me + s + 1) % total, me).wait_recv())

    def add(d):
        for t in range(n):
            every_ref[...] += land[d * n + t]
        column_ref[...] += land[d * n + i]

    loop(m, add)
    loop(total - 1, lambda s: copy(me, (me + s + 1) % total).wait_send())


def params(collective=None):
    if collective is None:
        return pltpu.CompilerParams(vmem_limit_bytes=BIG)
    return pltpu.CompilerParams(vmem_limit_bytes=BIG, collective_id=collective, has_side_effects=True)


def shape(dims, dtype):
    return jax.ShapeDtypeStruct(dims, dtype)


class Line:
    def __init__(self, axis, size):
        self.axis, self.n = axis, size
        self.i = lax.axis_index(axis)
        self.first = self.i < size // 2

    def owner(self, k):
        return jnp.where(self.first, self.i + k, self.i - k + self.n) % self.n

    def hop(self, block, step, r):
        n = self.n
        if step < 0:
            return lax.ppermute(block, self.axis, [(i, i - 1) for i in range(1, n) if i + r - 1 <= n - 1])
        return lax.ppermute(block, self.axis, [(i, i + 1) for i in range(n - 1) if i - r + 1 >= 0])

    def slots(self, block, down, up):
        n = self.n
        down, up = [block] + down, [block] + up
        slots = [block]
        for k in range(1, n):
            if 2 * k <= n:
                slots.append(jnp.where(self.first, down[k], up[k]))
            else:
                low = jnp.where(self.i + k <= n - 1, down[k], up[n - k])
                high = jnp.where(self.i - k >= 0, up[k], down[n - k])
                slots.append(jnp.where(self.first, low, high))
        return slots

    def scatter_sum(self, parts, work=None):
        n = self.n
        right = left = None
        done = []

        def pick(owner):
            return lax.dynamic_index_in_dim(parts, owner % n, 0, keepdims=False).astype(F32)

        for r in range(1, n):
            term = pick(self.i + n - r)
            term = term if right is None else term + right.astype(F32)
            right = lax.ppermute(term.astype(BF), self.axis, [(i, i + 1) for i in range(min(r, n - 1))])
            term = pick(self.i + r)
            term = term if left is None else term + left.astype(F32)
            left = lax.ppermute(term.astype(BF), self.axis, [(i, i - 1) for i in range(max(n - r, 1), n)])
            if work and r <= len(work):
                right, left, value = lax.optimization_barrier((right, left, work[r - 1]()))
                done.append(value)
        total = pick(self.i) + (right.astype(F32) + left.astype(F32))
        return (total, done) if work else total


def body(tokens, cotangent, ln1_gain, ln1_bias, qkv_weight, qv_bias, out_weight, out_bias, ln2_gain, ln2_bias,
         up_weight, up_bias, down_weight, down_bias):
    n = lax.axis_size("tensor")
    m = lax.axis_size("dp")
    i, row = lax.axis_index("tensor"), lax.axis_index("dp")
    line = Line("tensor", n)
    size, depth = tokens.shape
    width = qkv_weight.shape[2]
    units = up_weight.shape[1]
    piece, qv_piece, up_piece = ln1_gain.shape[0], qv_bias.shape[1], up_bias.shape[0]
    total = m * n

    def lane_rows(value, index):
        count = value.shape[-1]
        if count >= LANES:
            return value.reshape(-1, LANES)
        places = LANES // count
        spread = jnp.tile(value.reshape(-1, count), (1, places))
        return jnp.where((jnp.arange(LANES) // count)[None] == index % places, spread, 0)

    me = row * n + i
    whole = jnp.stack([ln1_gain, ln1_bias, out_bias, ln2_gain, ln2_bias, down_bias])
    pack = jnp.concatenate([lane_rows(whole, me), lane_rows(qv_bias, row), lane_rows(up_bias, row)])
    pack = jnp.pad(pack.astype(F32), ((0, -pack.shape[0] % 8), (0, 0)))
    lanes_up = 8 + max(up_piece // LANES, 1)

    w_qkv = lax.all_gather(qkv_weight, "dp", axis=1, tiled=True)
    w_out = lax.all_gather(out_weight, "dp", axis=1, tiled=True)
    w_up = lax.all_gather(up_weight, "dp", axis=0, tiled=True)
    w_down = lax.all_gather(down_weight, "dp", axis=1, tiled=True)

    dma = pltpu.SemaphoreType.DMA
    attn_in, vecs = pl.pallas_call(
        functools.partial(tokens_kernel, n, m, piece),
        out_shape=(shape((LEN, depth), BF), shape((total,) + pack.shape, F32)),
        in_specs=[VM, VM], out_specs=(VM, VM),
        scratch_shapes=[pltpu.VMEM((n, size, depth), BF), pltpu.VMEM((8, depth), F32), dma, dma((2, n)), dma((n,)),
                        dma((total,)), dma((total,))],
        compiler_params=params(0), name="gather_tokens",
    )(pack, tokens)

    def whole_rows(block, count):
        if count < LANES:
            block = block.reshape(-1, LANES // count, *block.shape[1:]).sum(axis=1)
        return block

    vectors = whole_rows(vecs[:, 0:6], piece).transpose(1, 0, 2).reshape(6, 1, depth)
    gain_one, shift_one, bias_out, gain_two, shift_two, bias_down = [vectors[j] for j in range(6)]
    mine = lax.dynamic_index_in_dim(vecs.reshape(m, n, -1, LANES), i, 1, keepdims=False)
    bias_qv = whole_rows(mine[:, 6:8], qv_piece).transpose(1, 0, 2).reshape(2, width)
    bias_up = whole_rows(mine[:, 8:lanes_up], up_piece).reshape(1, units)

    pieces = 2
    sums = [pltpu.VMEM((n, size, depth), BF), pltpu.VMEM((n + 1, size, depth), BF)]
    qkv, mixture, residual, mlp_own, cot_all = pl.pallas_call(
        functools.partial(attend_kernel, n, pieces),
        out_shape=(shape((3, LEN, width), BF), shape((LEN, width), BF), shape((size, depth), F32),
                   shape((size, depth), BF), shape((n, size, depth), BF)),
        in_specs=[ANY] * 3 + [VM] * 6, out_specs=(VM, VM, VM, VM, ANY),
        scratch_shapes=[pltpu.VMEM((LEN, depth), BF), pltpu.VMEM((3, depth, width), BF), pltpu.VMEM((width, depth), BF)] +
                       sums + [dma((2, n)), dma((n,)), dma((n, pieces)), dma((n + 1, pieces)), dma, dma, dma((4,))],
        compiler_params=params(1), name="attend",
    )(attn_in, w_qkv, w_out, tokens, cotangent, bias_qv, bias_out, gain_two, shift_two)

    pieces = 4
    mlp_in, hidden, grad_pre, grad_resid, branch_cot, vec_two, grad_up_b = pl.pallas_call(
        functools.partial(hidden_kernel, n, pieces),
        out_shape=(shape((n, size, depth), BF), shape((n, size, units), BF), shape((n, size, units), BF),
                   shape((size, depth), F32), shape((size, depth), BF), shape((8, depth), F32), shape((8, units), F32)),
        in_specs=[VM, VM, ANY, ANY, ANY, VM, VM], out_specs=(ANY, ANY, ANY, VM, VM, VM, VM),
        scratch_shapes=[pltpu.VMEM((n, size, depth), BF), pltpu.VMEM((n, size, units), BF),
                        pltpu.VMEM((n, size, units), BF), pltpu.VMEM((n, size, depth), BF),
                        pltpu.VMEM((depth, units), BF), pltpu.VMEM((units, depth), BF)] + sums +
                       [dma((2, n)), dma((n,)), dma((n, pieces)), dma((n + 1, pieces)), dma((2,)), dma, dma,
                        dma((n,)), dma((n,)), dma((n,))],
        compiler_params=params(2), name="hidden",
    )(mlp_own, residual, cot_all, w_up, w_down, bias_up, gain_two)
    mlp_in, hidden, grad_pre = [v.reshape(LEN, -1) for v in (mlp_in, hidden, grad_pre)]
    cot_rows = cot_all.reshape(LEN, depth)

    hold = lax.optimization_barrier
    down, up = line.hop(branch_cot, -1, 1), line.hop(branch_cot, 1, 1)
    downs, ups = [down], [up]
    work = [
        lambda: jnp.einsum("rf,rd->fd", hidden, cot_rows, preferred_element_type=F32).astype(BF),
        lambda: jnp.dot(hidden, w_down, preferred_element_type=F32).astype(BF),
        lambda: jnp.einsum("rd,rf->df", mlp_in, grad_pre, preferred_element_type=F32).astype(BF),
    ]
    done = []
    for r in range(1, n):
        if r - 1 < len(work):
            value = work[r - 1]()
            down, up, value = hold((down, up, value))
            done.append(value)
            downs[-1], ups[-1] = down, up
        if r < n - 1:
            down, up = line.hop(down, -1, r + 1), line.hop(up, 1, r + 1)
            downs.append(down)
            ups.append(up)
    grad_down_w, mlp_part, grad_up_w = done
    slots = line.slots(branch_cot, downs, ups)
    attn_cot = jnp.zeros((LEN, depth), BF)
    for k in range(n):
        attn_cot = lax.dynamic_update_slice(attn_cot, slots[k], (line.owner(k) * size, 0))
    layer_out = (residual + (line.scatter_sum(mlp_part.reshape(n, size, depth)) + bias_down)).astype(BF)
    grad_mix = jnp.einsum("rd,ed->re", attn_cot, w_out, preferred_element_type=F32).astype(BF)
    grad_qkv = pl.pallas_call(
        attend_back_kernel, out_shape=shape((3, LEN, width), BF), in_specs=[VM, VM], out_specs=VM,
        scratch_shapes=[pltpu.VMEM((LEN, HD), F32), pltpu.VMEM((LEN, HD), F32)],
        compiler_params=params(), name="attend_back",
        cost_estimate=pl.CostEstimate(flops=14 * LEN * LEN * width // 2, bytes_accessed=14 * LEN * width,
                                      transcendentals=LEN * LEN * width // HD),
    )(qkv, grad_mix)
    grad_qkv, layer_out = hold((grad_qkv, layer_out))
    attn_back = jnp.einsum("kre,kde->rd", grad_qkv, w_qkv, preferred_element_type=F32).astype(BF)
    work = [
        lambda: jnp.einsum("rd,kre->kde", attn_in, grad_qkv, preferred_element_type=F32).astype(BF),
        lambda: jnp.einsum("re,rd->ed", mixture, attn_cot, preferred_element_type=F32).astype(BF),
    ]
    grad_normed_one, (grad_qkv_w, grad_out_w) = line.scatter_sum(attn_back.reshape(n, size, depth), work)
    normal_one, inverse_one = norm_stats(tokens.astype(F32))
    grad_tokens = (grad_resid + norm_back(grad_normed_one, normal_one, inverse_one, gain_one)).astype(BF)

    grad_down_w = lax.psum_scatter(grad_down_w, "dp", scatter_dimension=1, tiled=True).astype(F32)
    grad_up_w = lax.psum_scatter(grad_up_w, "dp", scatter_dimension=0, tiled=True).astype(F32)
    grad_qkv_w = lax.psum_scatter(grad_qkv_w, "dp", scatter_dimension=1, tiled=True).astype(F32)
    grad_out_w = lax.psum_scatter(grad_out_w, "dp", scatter_dimension=1, tiled=True).astype(F32)

    vectors = jnp.stack([
        jnp.sum(grad_normed_one * normal_one, axis=0),
        jnp.sum(grad_normed_one, axis=0),
        vec_two[2], vec_two[0], vec_two[1], vec_two[3],
    ])
    vectors = vectors.reshape(6, total, piece).transpose(1, 0, 2).reshape(total, 6 * piece)
    local = jnp.concatenate([
        jnp.sum(grad_qkv[0::2].astype(F32), axis=1).reshape(2, m, qv_piece).transpose(1, 0, 2).reshape(m, -1),
        grad_up_b[0].reshape(m, -1)], axis=1)
    local = jnp.broadcast_to(local[:, None], (m, n, local.shape[1])).reshape(total, -1)
    load = jnp.concatenate([vectors, local], axis=1)
    load = jnp.pad(load, ((0, 0), (0, -load.shape[1] % 1024))).reshape(total, -1, LANES)
    everyone, column = pl.pallas_call(
        functools.partial(share_kernel, n, m),
        out_shape=(shape(load.shape[1:], F32),) * 2, in_specs=[VM], out_specs=(VM, VM),
        scratch_shapes=[pltpu.VMEM(load.shape, F32), dma((total,)), dma((total,))],
        compiler_params=params(3), name="share",
    )(load)
    vectors = everyone.reshape(-1)[: 6 * piece].reshape(6, piece)
    local = column.reshape(-1)[6 * piece :]
    grad_qv_b = local[: 2 * qv_piece].reshape(2, qv_piece)
    grad_up_b = local[2 * qv_piece : 2 * qv_piece + up_piece]
    return (layer_out, grad_tokens, vectors[0], vectors[1], grad_qkv_w, grad_qv_b, grad_out_w, vectors[2],
            vectors[3], vectors[4], grad_up_w, grad_up_b, grad_down_w, vectors[5])


def solution(mesh):
    vector, matrix = P(("dp", "tensor")), P(("dp", "tensor"), None)
    in_specs = (matrix, matrix, vector, vector, P(None, "dp", "tensor"), P(None, ("tensor", "dp")), P("tensor", "dp"),
                vector, vector, vector, P("dp", "tensor"), P(("tensor", "dp")), P("tensor", "dp"), vector)
    out_specs = (matrix, matrix, vector, vector, P(None, "dp", "tensor"), P(None, ("tensor", "dp")),
                 P("tensor", "dp"), vector, vector, vector, P("dp", "tensor"), P(("tensor", "dp")), P("tensor", "dp"),
                 vector)
    return jax.shard_map(body, mesh=mesh, in_specs=in_specs, out_specs=out_specs, check_vma=False)
```

```python
import functools

import jax
import jax.numpy as jnp
from jax import lax
from jax.experimental import pallas as pl
from jax.experimental.pallas import tpu as pltpu
from jax.sharding import PartitionSpec as P

HD = 128
LEN = 1024
LANES = 128
EPS = 1e-05
BF = jnp.bfloat16
F32 = jnp.float32
MESH = pl.DeviceIdType.MESH
ANY = pl.BlockSpec(memory_space=pl.ANY)
VM = pl.BlockSpec(memory_space=pltpu.VMEM)
NT = (((1,), (1,)), ((), ()))
TN = (((0,), (0,)), ((), ()))
BIG = 64 * 1024 * 1024 - 65536
RB = 32


def norm_stats(rows):
    mean = jnp.mean(rows, axis=-1, keepdims=True)
    centred = rows - mean
    variance = jnp.mean(centred * centred, axis=-1, keepdims=True)
    inverse = lax.rsqrt(variance + EPS)
    return centred * inverse, inverse


def norm_back(grad_rows, normal_rows, inverse, gain):
    scaled = grad_rows * gain
    first = jnp.mean(scaled, axis=-1, keepdims=True)
    second = jnp.mean(scaled * normal_rows, axis=-1, keepdims=True)
    return inverse * (scaled - first - normal_rows * second)


def loop(count, step):
    def run(i, carry):
        step(i)
        return carry

    lax.fori_loop(0, count, run, 0)


def rows_at(j, size):
    return pl.ds(pl.multiple_of(j * size, size), size)


def remote(src, dst, send, recv, target):
    return pltpu.make_async_remote_copy(src_ref=src, dst_ref=dst, send_sem=send, recv_sem=recv,
                                        device_id={"tensor": target}, device_id_type=MESH)


def greet_neighbours(i, n):
    barrier = pltpu.get_barrier_semaphore()

    @pl.when(i > 0)
    def _():
        pl.semaphore_signal(barrier, inc=1, device_id={"tensor": i - 1}, device_id_type=MESH)

    @pl.when(i < n - 1)
    def _():
        pl.semaphore_signal(barrier, inc=1, device_id={"tensor": i + 1}, device_id_type=MESH)

    pl.semaphore_wait(barrier, jnp.minimum(i, 1) + jnp.minimum(n - 1 - i, 1))


def greet_all(me, n, total):
    barrier = pltpu.get_barrier_semaphore()

    def greet(s):
        other = (me + s + 1) % total
        pl.semaphore_signal(barrier, inc=1, device_id={"dp": other // n, "tensor": other % n}, device_id_type=MESH)

    loop(total - 1, greet)
    pl.semaphore_wait(barrier, total - 1)


def rounds(i, n, line, compute):
    def round_of(r):
        @pl.when(r > 0)
        def _():
            line.step(r)

        def side(s):
            j = jnp.where(s == 0, i - r, i + r)

            @pl.when(jnp.logical_and(jnp.logical_and(j >= 0, j <= n - 1), s * r == s * jnp.maximum(r, 1)))
            def _():
                compute(j)

        loop(2, side)

    loop(n, round_of)


class LineGather:
    def __init__(self, i, n, own, buf, send, recv):
        self.i, self.n, self.own, self.buf, self.send, self.recv = i, n, own, buf, send, recv

    def copy(self, src, j, side, target):
        return remote(src, self.buf.at[j], self.send.at[side, j], self.recv.at[j], target)

    def start(self):
        i, n = self.i, self.n

        @pl.when(i < n - 1)
        def _():
            self.copy(self.own, i, 0, i + 1).start()

        @pl.when(i > 0)
        def _():
            self.copy(self.own, i, 1, i - 1).start()

    def step(self, r):
        i, n = self.i, self.n

        @pl.when(i - r >= 0)
        def _():
            self.copy(self.own, i - r, 0, i).wait_recv()

            @pl.when(i < n - 1)
            def _():
                self.copy(self.buf.at[i - r], i - r, 0, i + 1).start()

        @pl.when(i + r <= n - 1)
        def _():
            self.copy(self.own, i + r, 1, i).wait_recv()

            @pl.when(i > 0)
            def _():
                self.copy(self.buf.at[i + r], i + r, 1, i - 1).start()

    def finish(self):
        i, n = self.i, self.n

        def one(j):
            @pl.when(jnp.logical_and(i < n - 1, j <= i))
            def _():
                self.copy(self.own, j, 0, i + 1).wait_send()

            @pl.when(jnp.logical_and(i > 0, j >= i))
            def _():
                self.copy(self.own, j, 1, i - 1).wait_send()

        loop(n, one)


class LineSum:
    def __init__(self, i, n, part, land, send, recv, pieces):
        self.i, self.n, self.part, self.land, self.send, self.recv = i, n, part, land, send, recv
        self.pieces = pieces
        self.size = part.shape[1] // pieces

    def copy(self, src, d, right, s):
        i, n = self.i, self.n
        target = i + 1 if right else i - 1
        slot = d if right else jnp.where(d == target, n, d)
        here = rows_at(s, self.size)
        return remote(src.at[d, here], self.land.at[slot, here], self.send.at[d, s], self.recv.at[slot, s], target)

    def arrived(self, slot, s):
        here = rows_at(s, self.size)
        remote(self.part.at[0, here], self.land.at[slot, here], self.send.at[0, s], self.recv.at[slot, s],
               self.i).wait_recv()

    def launch(self, d):
        i, n = self.i, self.n

        @pl.when(jnp.logical_and(i == 0, d > 0))
        def _():
            loop(self.pieces, lambda s: self.copy(self.part, d, True, s).start())

        @pl.when(jnp.logical_and(i == n - 1, d < n - 1))
        def _():
            loop(self.pieces, lambda s: self.copy(self.part, d, False, s).start())

    def relay(self, d, right):
        def one(s):
            self.arrived(d, s)
            here = rows_at(s, self.size)
            total = self.land[d, here, :].astype(F32) + self.part[d, here, :].astype(F32)
            self.land[d, here, :] = total.astype(BF)
            self.copy(self.land, d, right, s).start()

        loop(self.pieces, one)

    def own(self):
        i, n = self.i, self.n

        @pl.when(i > 0)
        def _():
            loop(self.pieces, lambda s: self.arrived(i, s))

        @pl.when(i < n - 1)
        def _():
            loop(self.pieces, lambda s: self.arrived(n, s))

    def add(self, here, out):
        i, n = self.i, self.n
        out[...] = self.part[i, here, :].astype(F32)

        @pl.when(i > 0)
        def _():
            out[...] += self.land[i, here, :].astype(F32)

        @pl.when(i < n - 1)
        def _():
            out[...] += self.land[n, here, :].astype(F32)

    def finish(self):
        i, n = self.i, self.n

        def one(d):
            @pl.when(jnp.logical_and(i < n - 1, d > i))
            def _():
                loop(self.pieces, lambda s: self.copy(self.part, d, True, s).wait_send())

            @pl.when(jnp.logical_and(i > 0, d < i))
            def _():
                loop(self.pieces, lambda s: self.copy(self.part, d, False, s).wait_send())

        loop(n, one)


def tokens_kernel(n, m, piece, pack_ref, x_ref, a_ref, vec_ref, buf, affine, own_sem, send, recv, v_send, v_recv):
    i, row = lax.axis_index("tensor"), lax.axis_index("dp")
    me, total = row * n + i, m * n
    size = x_ref.shape[0]
    greet_all(me, n, total)
    line = LineGather(i, n, x_ref, buf, send, recv)

    def vector(src, other):
        return pltpu.make_async_remote_copy(
            src_ref=pack_ref, dst_ref=vec_ref.at[src], send_sem=v_send.at[other], recv_sem=v_recv.at[src],
            device_id={"dp": other // n, "tensor": other % n}, device_id_type=MESH)

    loop(total - 1, lambda s: vector(me, (me + s + 1) % total).start())
    line.start()
    own_copy = pltpu.make_async_copy(x_ref, buf.at[i], own_sem)
    own_copy.start()
    vec_ref[me] = pack_ref[...]
    loop(total - 1, lambda s: vector((me + s + 1) % total, me).wait_recv())
    depth = affine.shape[1]
    group = LANES // piece
    for tile in range(depth // LANES):
        value = vec_ref[tile * group, 0:2, :].astype(F32)
        for g in range(1, group):
            value = value + vec_ref[tile * group + g, 0:2, :].astype(F32)
        affine[0:2, tile * LANES : (tile + 1) * LANES] = value
    own_copy.wait()

    def compute(j):
        def norm(b):
            normal, _ = norm_stats(buf[j, rows_at(b, RB), :].astype(F32))
            here = pl.ds(pl.multiple_of(j * size + b * RB, RB), RB)
            a_ref[here, :] = (normal * affine[0:1, :] + affine[1:2, :]).astype(BF)

        loop(size // RB, norm)

    rounds(i, n, line, compute)
    line.finish()
    loop(total - 1, lambda s: vector(me, (me + s + 1) % total).wait_send())


def attend_kernel(n, pieces, a_hbm, wq_hbm, wo_hbm, x_ref, cot_ref, bias, out_bias, gain, shift, qkv_ref, o_ref, h_ref,
                  c_ref, cot_all, a_ref, wq_ref, w_ref, part, land, send, recv, s_send, s_recv, own_sem, a_sem, w_sem):
    i = lax.axis_index("tensor")
    size = x_ref.shape[0]
    loads = [pltpu.make_async_copy(a_hbm, a_ref, a_sem)]
    loads += [pltpu.make_async_copy(wq_hbm.at[t], wq_ref.at[t], w_sem.at[t]) for t in range(3)]
    loads += [pltpu.make_async_copy(wo_hbm, w_ref, w_sem.at[3])]
    for load in loads:
        load.start()
    heads = qkv_ref.shape[2] // HD
    depth = w_ref.shape[1]
    greet_neighbours(i, n)
    line = LineGather(i, n, cot_ref, cot_all, send, recv)
    line.start()
    own_copy = pltpu.make_async_copy(cot_ref, cot_all.at[i], own_sem)
    own_copy.start()

    loads[0].wait()
    block = 256
    for t in range(3):
        loads[1 + t].wait()

        def project(b):
            here = rows_at(b, block)
            value = jnp.dot(a_ref[here, :], wq_ref[t], preferred_element_type=F32)
            if t != 1:
                value = value + bias[t // 2 : t // 2 + 1, :]
            qkv_ref[t, here, :] = value.astype(BF)

        loop(LEN // block, project)

    def head(t):
        cols = pl.ds(pl.multiple_of(t * HD, HD), HD)
        for b in range(LEN // block):
            here, keys = slice(b * block, (b + 1) * block), (b + 1) * block
            s = lax.dot_general(qkv_ref[0, here, cols], qkv_ref[1, 0:keys, cols], NT,
                                preferred_element_type=F32) * HD ** (-0.5)
            query = lax.broadcasted_iota(jnp.int32, s.shape, 0) + b * block
            s = jnp.where(query >= lax.broadcasted_iota(jnp.int32, s.shape, 1), s, -1e30)
            e = jnp.exp(s - jnp.max(s, axis=-1, keepdims=True))
            prob = (e / jnp.sum(e, axis=-1, keepdims=True)).astype(BF)
            o_ref[here, cols] = jnp.dot(prob, qkv_ref[2, 0:keys, cols], preferred_element_type=F32).astype(BF)

    loop(heads, head)
    loads[4].wait()
    sums = LineSum(i, n, part, land, s_send, s_recv, pieces)
    tile = 512

    def project(t):
        d = jnp.where(i < n // 2, n - 1 - t, t)

        def columns(k):
            cols = rows_at(k, tile)
            part[d, :, cols] = jnp.dot(o_ref[rows_at(d, size), :], w_ref[:, cols], preferred_element_type=F32).astype(BF)

        loop(depth // tile, columns)
        sums.launch(d)

    loop(n, project)

    def round_of(r):
        line.step(r + 1)
        right, left = n - 1 + i - (r + 1), r + 1 - (n - 1 - i)

        @pl.when(jnp.logical_and(i > 0, jnp.logical_and(right > i, right <= n - 1)))
        def _():
            sums.relay(right, True)

        @pl.when(jnp.logical_and(i < n - 1, jnp.logical_and(left >= 0, left < i)))
        def _():
            sums.relay(left, False)

    loop(n - 1, round_of)
    sums.own()

    def norm(b):
        here = rows_at(b, RB)
        sums.add(here, h_ref.at[here, :])
        rows = h_ref[here, :] + (x_ref[here, :].astype(F32) + out_bias[...])
        h_ref[here, :] = rows
        normal, _ = norm_stats(rows)
        c_ref[here, :] = (normal * gain[...] + shift[...]).astype(BF)

    loop(size // RB, norm)
    own_copy.wait()
    line.finish()
    sums.finish()


def hidden_kernel(n, pieces, c_ref, h_ref, cot_hbm, up_hbm, down_hbm, up_bias, gain, c_hbm, g_hbm, du_hbm, mlp_hbm, dh_ref,
                  db_ref, vec_ref, upb_ref, c_all, g_all, du_all, cot_all, up, down, part, land, send, recv, s_send,
                  s_recv, w_sem, cot_sem, own_sem, c_sem, g_sem, du_sem, mlp, mlp_sem):
    i = lax.axis_index("tensor")
    size, depth = c_ref.shape
    units = up.shape[1]
    greet_neighbours(i, n)
    line = LineGather(i, n, c_ref, c_all, send, recv)
    line.start()
    own_copy = pltpu.make_async_copy(c_ref, c_all.at[i], own_sem)
    own_copy.start()
    up_copy = pltpu.make_async_copy(up_hbm, up, w_sem.at[0])
    up_copy.start()
    down_copy = pltpu.make_async_copy(down_hbm, down, w_sem.at[1])
    down_copy.start()
    cot_copy = pltpu.make_async_copy(cot_hbm, cot_all, cot_sem)
    cot_copy.start()
    upb_ref[...] = jnp.zeros_like(upb_ref)
    vec_ref[...] = jnp.zeros_like(vec_ref)
    own_copy.wait()
    up_copy.wait()
    down_copy.wait()
    cot_copy.wait()
    sums = LineSum(i, n, part, land, s_send, s_recv, pieces)
    tile = 256

    def out_copy(src, dst, sem, j):
        return pltpu.make_async_copy(src.at[j], dst.at[j], sem.at[j])

    def compute(j):
        def unit(k):
            cols = rows_at(k, tile)
            u = jnp.dot(c_all[j], up[:, cols], preferred_element_type=F32) + up_bias[0:1, cols]
            dg = lax.dot_general(cot_all[j], down[cols, :], NT, preferred_element_type=F32)
            half = 0.5 + 0.5 * lax.erf(u * (0.5 ** 0.5))
            g_all[j, :, cols] = (u * half).astype(BF)
            slope = half + u * (jnp.exp(u * u * -0.5) * 0.3989422804014327)
            du = (slope * dg).astype(BF)
            du_all[j, :, cols] = du
            upb_ref[0:1, cols] += jnp.sum(du.astype(F32), axis=0, keepdims=True)

        loop(units // tile, unit)

        def back(k):
            cols = rows_at(k, tile)
            part[j, :, cols] = lax.dot_general(du_all[j], up[cols, :], NT, preferred_element_type=F32).astype(BF)

        loop(depth // tile, back)
        sums.launch(j)
        out_copy(g_all, g_hbm, g_sem, j).start()
        out_copy(du_all, du_hbm, du_sem, j).start()
        out_copy(c_all, c_hbm, c_sem, j).start()

    rounds(i, n, line, compute)

    def forward(j):
        def columns(k):
            cols = rows_at(k, tile)
            mlp[j, :, cols] = jnp.dot(g_all[j], down[:, cols], preferred_element_type=F32).astype(BF)

        loop(depth // tile, columns)
        out_copy(mlp, mlp_hbm, mlp_sem, j).start()

    loop(n, forward)

    def relay(t):
        right, left = t + 2 - i, 2 * n - 4 - i - t

        @pl.when(jnp.logical_and(i > 0, jnp.logical_and(right > i, right <= n - 1)))
        def _():
            sums.relay(right, True)

        @pl.when(jnp.logical_and(i < n - 1, jnp.logical_and(left >= 0, left < i)))
        def _():
            sums.relay(left, False)

    loop(2 * n - 3, relay)
    sums.own()

    def norm(b):
        here = rows_at(b, RB)
        sums.add(here, dh_ref.at[here, :])
        grad = dh_ref[here, :]
        normal, inverse = norm_stats(h_ref[here, :])
        vec_ref[0:1, :] += jnp.sum(grad * normal, axis=0, keepdims=True)
        vec_ref[1:2, :] += jnp.sum(grad, axis=0, keepdims=True)
        cot = cot_all[i, here, :].astype(F32)
        dh = cot + norm_back(grad, normal, inverse, gain[...])
        dh_ref[here, :] = dh
        db = dh.astype(BF)
        db_ref[here, :] = db
        vec_ref[2:3, :] += jnp.sum(db.astype(F32), axis=0, keepdims=True)
        vec_ref[3:4, :] += jnp.sum(cot, axis=0, keepdims=True)

    loop(size // RB, norm)

    def done(j):
        out_copy(g_all, g_hbm, g_sem, j).wait()
        out_copy(du_all, du_hbm, du_sem, j).wait()
        out_copy(c_all, c_hbm, c_sem, j).wait()
        out_copy(mlp, mlp_hbm, mlp_sem, j).wait()

    loop(n, done)
    line.finish()
    sums.finish()


def attend_back_kernel(qkv_ref, do_ref, out_ref, dk, dv):
    heads = qkv_ref.shape[2] // HD
    block = 256
    factor = HD ** (-0.5)

    def head(t):
        cols = pl.ds(pl.multiple_of(t * HD, HD), HD)
        dk[...] = jnp.zeros_like(dk)
        dv[...] = jnp.zeros_like(dv)
        for b in range(LEN // block):
            here, keys = slice(b * block, (b + 1) * block), (b + 1) * block
            q, k, v = qkv_ref[0, here, cols], qkv_ref[1, 0:keys, cols], qkv_ref[2, 0:keys, cols]
            do = do_ref[here, cols]
            s = lax.dot_general(q, k, NT, preferred_element_type=F32) * factor
            query = lax.broadcasted_iota(jnp.int32, s.shape, 0) + b * block
            s = jnp.where(query >= lax.broadcasted_iota(jnp.int32, s.shape, 1), s, -1e30)
            e = jnp.exp(s - jnp.max(s, axis=-1, keepdims=True))
            prob = e / jnp.sum(e, axis=-1, keepdims=True)
            dv[0:keys, :] += lax.dot_general(prob.astype(BF), do, TN, preferred_element_type=F32)
            dp = lax.dot_general(do, v, NT, preferred_element_type=F32)
            ds = (prob * (dp - jnp.sum(prob * dp, axis=-1, keepdims=True))).astype(BF)
            out_ref[0, here, cols] = (jnp.dot(ds, k, preferred_element_type=F32) * factor).astype(BF)
            dk[0:keys, :] += lax.dot_general(ds, q, TN, preferred_element_type=F32)
        out_ref[1, :, cols] = (dk[...] * factor).astype(BF)
        out_ref[2, :, cols] = dv[...].astype(BF)

    loop(heads, head)


def partner(row, bit):
    return row + bit * (1 - 2 * ((row // bit) % 2))


class PlaneSum:
    def __init__(self, row, m, terms, land, halves, send, recv, h_send, h_recv):
        self.row, self.m, self.terms, self.land, self.halves = row, m, terms, land, halves
        self.send, self.recv, self.h_send, self.h_recv = send, recv, h_send, h_recv
        bits = [1 << k for k in range(1, m.bit_length() - 1)]
        self.plan = []
        for order in (bits, bits[::-1]):
            left, at, stages = [e for e in range(m) if e % 2 == 0], 0, []
            for bit in order:
                out = [e for e in left if e & bit]
                stages.append((bit, [(e, e ^ bit, at + k) for k, e in enumerate(out)]))
                left, at = [e for e in left if not e & bit], at + len(out)
            self.plan.append(stages)
        self.stages = len(bits)

    def owner(self, e):
        d = self.row
        for k in range(self.m.bit_length() - 1):
            if e & (1 << k):
                d = d + (partner(self.row, 1 << k) - self.row)
        return d

    def whole(self, e):
        return pltpu.make_async_remote_copy(
            src_ref=self.terms.at[e], dst_ref=self.land.at[e // 2], send_sem=self.send.at[e // 2],
            recv_sem=self.recv.at[e // 2], device_id={"dp": partner(self.row, 1)}, device_id_type=MESH)

    def half(self, h, bit, e, at):
        size = self.halves.shape[2]
        return pltpu.make_async_remote_copy(
            src_ref=self.terms.at[e, pl.ds(h * size, size)], dst_ref=self.halves.at[h, at],
            send_sem=self.h_send.at[h, at], recv_sem=self.h_recv.at[h, at],
            device_id={"dp": partner(self.row, bit)}, device_id_type=MESH)

    def merge(self):
        for e in range(0, self.m, 2):
            self.whole(e + 1).wait_recv()

            def add(b):
                here = rows_at(b, RB)
                total = self.terms[e, here, :].astype(F32) + self.land[e // 2, here, :].astype(F32)
                self.terms[e, here, :] = total.astype(BF)

            loop(self.terms.shape[1] // RB, add)

    def push(self, stage):
        for h in range(2):
            bit, moves = self.plan[h][stage]
            for e, _, at in moves:
                self.half(h, bit, e, at).start()

    def take(self, stage, out=None):
        size = self.halves.shape[2]
        for h in range(2):
            bit, moves = self.plan[h][stage]
            for e, into, at in moves:
                self.half(h, bit, e, at).wait_recv()

                def add(b):
                    here, there = rows_at(b, RB), pl.ds(pl.multiple_of(h * size + b * RB, RB), RB)
                    total = self.terms[into, there, :].astype(F32) + self.halves[h, at, here, :].astype(F32)
                    if out is None:
                        self.terms[into, there, :] = total.astype(BF)
                    else:
                        out(there, total)

                loop(size // RB, add)

    def finish(self):
        for e in range(1, self.m, 2):
            self.whole(e).wait_send()
        for h in range(2):
            for bit, moves in self.plan[h]:
                for e, _, at in moves:
                    self.half(h, bit, e, at).wait_send()


def greet_cross(i, n, row, m):
    barrier = pltpu.get_barrier_semaphore()

    @pl.when(i > 0)
    def _():
        pl.semaphore_signal(barrier, inc=1, device_id={"tensor": i - 1}, device_id_type=MESH)

    @pl.when(i < n - 1)
    def _():
        pl.semaphore_signal(barrier, inc=1, device_id={"tensor": i + 1}, device_id_type=MESH)

    bits = [1 << k for k in range(m.bit_length() - 1)]
    for bit in bits:
        pl.semaphore_signal(barrier, inc=1, device_id={"dp": partner(row, bit)}, device_id_type=MESH)
    pl.semaphore_wait(barrier, jnp.minimum(i, 1) + jnp.minimum(n - 1 - i, 1) + len(bits))


def relays(sums, i, n, r):
    right, left = n - 1 + i - r, r - (n - 1 - i)

    @pl.when(jnp.logical_and(i > 0, jnp.logical_and(right > i, right <= n - 1)))
    def _():
        sums.relay(right, True)

    @pl.when(jnp.logical_and(i < n - 1, jnp.logical_and(left >= 0, left < i)))
    def _():
        sums.relay(left, False)


def block_terms(plane, e, pairs):
    size = plane.terms.shape[1]
    cols = rows_at(plane.owner(e), size)
    for lhs, rhs, first in pairs:
        width = rhs.shape[1]
        tile = min(512, width)

        def columns(k):
            there = pl.ds(pl.multiple_of(first + k * tile, tile), tile)
            plane.terms[e, :, there] = lax.dot_general(
                lhs[:, cols], rhs[:, rows_at(k, tile)], TN, preferred_element_type=F32).astype(BF)

        loop(width // tile, columns)


def branch_kernel(n, m, pieces, db_ref, h_ref, down_bias, mlp_hbm, g_hbm, cot_hbm, c_hbm, du_hbm, db_all, lo_ref,
                  down_ref, up_ref, lhs, rhs, part, land, terms_a, land_a, half_a, terms_b, land_b, half_b, acc, send,
                  recv, s_send, s_recv, own_sem, part_sem, in_sem, p_send, p_recv, h_send, h_recv):
    i, row = lax.axis_index("tensor"), lax.axis_index("dp")
    size = db_ref.shape[0]
    greet_cross(i, n, row, m)
    line = LineGather(i, n, db_ref, db_all, send, recv)
    line.start()
    part_copy = pltpu.make_async_copy(mlp_hbm, part, part_sem)
    part_copy.start()
    own_copy = pltpu.make_async_copy(db_ref, db_all.at[i], own_sem)
    own_copy.start()

    def load(left, right):
        return [pltpu.make_async_copy(left, lhs, in_sem.at[0]), pltpu.make_async_copy(right, rhs, in_sem.at[1])]

    loads = load(cot_hbm, g_hbm)
    for copy in loads:
        copy.start()
    sums = LineSum(i, n, part, land, s_send, s_recv, pieces)
    part_copy.wait()
    loop(n, lambda t: sums.launch(jnp.where(i < n // 2, n - 1 - t, t)))
    planes = [PlaneSum(row, m, terms_a, land_a, half_a, p_send.at[0], p_recv.at[0], h_send.at[0], h_recv.at[0]),
              PlaneSum(row, m, terms_b, land_b, half_b, p_send.at[1], p_recv.at[1], h_send.at[1], h_recv.at[1])]

    def line_round(r):
        line.step(r)
        relays(sums, i, n, r)

    first, second = planes
    for copy in loads:
        copy.wait()
    for e in range(1, m, 2):
        block_terms(first, e, [(lhs, rhs, 0)])
        first.whole(e).start()
    for e in range(m - 2, -1, -2):
        block_terms(first, e, [(lhs, rhs, 0)])
    loads = load(c_hbm, du_hbm)
    for copy in loads:
        copy.start()
    first.merge()
    first.push(0)
    for copy in loads:
        copy.wait()
    for e in range(1, m, 2):
        block_terms(second, e, [(lhs, rhs, 0)])
        second.whole(e).start()
    line_round(1)
    for e in range(m - 2, -1, -2):
        block_terms(second, e, [(lhs, rhs, 0)])
    second.merge()
    second.push(0)

    def keep(ref):
        def out(here, total):
            ref[here, :] = total

        return out

    def advance(plane, stage, ref):
        if stage < plane.stages - 1:
            plane.take(stage)
            plane.push(stage + 1)
        else:
            plane.take(stage, keep(ref))

    advance(first, 0, down_ref)
    line_round(2)
    advance(second, 0, up_ref)
    for r in range(3, n):
        line_round(r)
    for stage in range(1, first.stages):
        advance(first, stage, down_ref)
        advance(second, stage, up_ref)
    sums.own()

    def output(b):
        here = rows_at(b, RB)
        sums.add(here, acc)
        lo_ref[here, :] = (h_ref[here, :] + (acc[...] + down_bias[...])).astype(BF)

    loop(size // RB, output)
    own_copy.wait()
    line.finish()
    sums.finish()
    for plane in planes:
        plane.finish()


def input_kernel(n, m, pieces, dqkv_ref, wq_hbm, x_ref, dh_ref, gain, a_hbm, db_hbm, o_hbm, gt_ref, gqkv_ref, gout_ref,
                 vec_ref, qv_ref, wq, a_ref, db_ref, o_ref, part, land, terms, land_p, half_p, acc, s_send, s_recv,
                 in_sem, p_send, p_recv, h_send, h_recv):
    i, row = lax.axis_index("tensor"), lax.axis_index("dp")
    size = x_ref.shape[0]
    width = dqkv_ref.shape[2]
    depth = part.shape[2]
    loads = [pltpu.make_async_copy(wq_hbm, wq, in_sem.at[0]), pltpu.make_async_copy(a_hbm, a_ref, in_sem.at[1]),
             pltpu.make_async_copy(db_hbm, db_ref, in_sem.at[2]), pltpu.make_async_copy(o_hbm, o_ref, in_sem.at[3])]
    for copy in loads:
        copy.start()
    greet_cross(i, n, row, m)
    sums = LineSum(i, n, part, land, s_send, s_recv, pieces)
    vec_ref[...] = jnp.zeros_like(vec_ref)
    qv_ref[...] = jnp.zeros_like(qv_ref)
    loads[0].wait()
    tile = 512

    def term(t):
        d = jnp.where(i < n // 2, n - 1 - t, t)
        here = rows_at(d, size)

        def columns(k):
            cols = rows_at(k, tile)
            total = lax.dot_general(dqkv_ref[0, here, :], wq[0, cols, :], NT, preferred_element_type=F32)
            for p in range(1, 3):
                total += lax.dot_general(dqkv_ref[p, here, :], wq[p, cols, :], NT, preferred_element_type=F32)
            part[d, :, cols] = total.astype(BF)

        loop(depth // tile, columns)
        sums.launch(d)
        for p in range(2):
            qv_ref[p : p + 1, :] += jnp.sum(dqkv_ref[2 * p, here, :].astype(F32), axis=0, keepdims=True)

    loop(n, term)
    for copy in loads[1:]:
        copy.wait()
    plane = PlaneSum(row, m, terms, land_p, half_p, p_send, p_recv, h_send, h_recv)
    pairs = [(a_ref, dqkv_ref.at[p], p * width) for p in range(3)] + [(db_ref, o_ref, 3 * width)]
    for e in range(1, m, 2):
        block_terms(plane, e, pairs)
        plane.whole(e).start()
    for e in range(m - 2, -1, -2):
        block_terms(plane, e, pairs)
    plane.merge()
    plane.push(0)

    def out(here, total):
        for p in range(3):
            gqkv_ref[p, here, :] = total[:, p * width : (p + 1) * width]
        gout_ref[here, :] = total[:, 3 * width :]

    stage = 0
    for r in range(1, n):
        relays(sums, i, n, r)
        if r > 1 and stage < plane.stages:
            if stage < plane.stages - 1:
                plane.take(stage)
                plane.push(stage + 1)
            else:
                plane.take(stage, out)
            stage += 1
    sums.own()

    def norm(b):
        here = rows_at(b, RB)
        sums.add(here, acc)
        grad = acc[...]
        normal, inverse = norm_stats(x_ref[here, :].astype(F32))
        vec_ref[0:1, :] += jnp.sum(grad * normal, axis=0, keepdims=True)
        vec_ref[1:2, :] += jnp.sum(grad, axis=0, keepdims=True)
        gt_ref[here, :] = (dh_ref[here, :] + norm_back(grad, normal, inverse, gain[...])).astype(BF)

    loop(size // RB, norm)
    while stage < plane.stages:
        if stage < plane.stages - 1:
            plane.take(stage)
            plane.push(stage + 1)
        else:
            plane.take(stage, out)
        stage += 1
    sums.finish()
    plane.finish()


def share_kernel(n, m, load_ref, every_ref, column_ref, land, send, recv):
    i, row = lax.axis_index("tensor"), lax.axis_index("dp")
    me, total = row * n + i, m * n
    greet_all(me, n, total)

    def copy(src, other):
        return pltpu.make_async_remote_copy(
            src_ref=load_ref.at[other], dst_ref=land.at[src], send_sem=send.at[other], recv_sem=recv.at[src],
            device_id={"dp": other // n, "tensor": other % n}, device_id_type=MESH)

    loop(total - 1, lambda s: copy(me, (me + s + 1) % total).start())
    land[me] = load_ref[me]
    every_ref[...] = jnp.zeros_like(every_ref)
    column_ref[...] = jnp.zeros_like(column_ref)
    loop(total - 1, lambda s: copy((me + s + 1) % total, me).wait_recv())

    def add(d):
        for t in range(n):
            every_ref[...] += land[d * n + t]
        column_ref[...] += land[d * n + i]

    loop(m, add)
    loop(total - 1, lambda s: copy(me, (me + s + 1) % total).wait_send())


def params(collective=None):
    if collective is None:
        return pltpu.CompilerParams(vmem_limit_bytes=BIG)
    return pltpu.CompilerParams(vmem_limit_bytes=BIG, collective_id=collective, has_side_effects=True)


def shape(dims, dtype):
    return jax.ShapeDtypeStruct(dims, dtype)


def body(tokens, cotangent, ln1_gain, ln1_bias, qkv_weight, qv_bias, out_weight, out_bias, ln2_gain, ln2_bias,
         up_weight, up_bias, down_weight, down_bias):
    n = lax.axis_size("tensor")
    m = lax.axis_size("dp")
    i, row = lax.axis_index("tensor"), lax.axis_index("dp")
    size, depth = tokens.shape
    width = qkv_weight.shape[2]
    units = up_weight.shape[1]
    piece, qv_piece, up_piece = ln1_gain.shape[0], qv_bias.shape[1], up_bias.shape[0]
    total = m * n

    def lane_rows(value, index):
        count = value.shape[-1]
        if count >= LANES:
            return value.reshape(-1, LANES)
        places = LANES // count
        spread = jnp.tile(value.reshape(-1, count), (1, places))
        return jnp.where((jnp.arange(LANES) // count)[None] == index % places, spread, 0)

    me = row * n + i
    whole = jnp.stack([ln1_gain, ln1_bias, out_bias, ln2_gain, ln2_bias, down_bias])
    pack = jnp.concatenate([lane_rows(whole, me), lane_rows(qv_bias, row), lane_rows(up_bias, row)])
    pack = jnp.pad(pack, ((0, -pack.shape[0] % 16), (0, 0)))
    lanes_up = 8 + max(up_piece // LANES, 1)

    w_qkv = lax.all_gather(qkv_weight, "dp", axis=1, tiled=True)
    w_out = lax.all_gather(out_weight, "dp", axis=1, tiled=True)
    w_up = lax.all_gather(up_weight, "dp", axis=0, tiled=True)
    w_down = lax.all_gather(down_weight, "dp", axis=1, tiled=True)

    dma = pltpu.SemaphoreType.DMA
    attn_in, vecs = pl.pallas_call(
        functools.partial(tokens_kernel, n, m, piece),
        out_shape=(shape((LEN, depth), BF), shape((total,) + pack.shape, BF)),
        in_specs=[VM, VM], out_specs=(VM, VM),
        scratch_shapes=[pltpu.VMEM((n, size, depth), BF), pltpu.VMEM((8, depth), F32), dma, dma((2, n)), dma((n,)),
                        dma((total,)), dma((total,))],
        compiler_params=params(0), name="gather_tokens",
    )(pack, tokens)
    vecs = vecs.astype(F32)

    def whole_rows(block, count):
        if count < LANES:
            block = block.reshape(-1, LANES // count, *block.shape[1:]).sum(axis=1)
        return block

    vectors = whole_rows(vecs[:, 0:6], piece).transpose(1, 0, 2).reshape(6, 1, depth)
    gain_one, shift_one, bias_out, gain_two, shift_two, bias_down = [vectors[j] for j in range(6)]
    mine = lax.dynamic_index_in_dim(vecs.reshape(m, n, -1, LANES), i, 1, keepdims=False)
    bias_qv = whole_rows(mine[:, 6:8], qv_piece).transpose(1, 0, 2).reshape(2, width)
    bias_up = whole_rows(mine[:, 8:lanes_up], up_piece).reshape(1, units)

    pieces = 2
    sums = [pltpu.VMEM((n, size, depth), BF), pltpu.VMEM((n + 1, size, depth), BF)]
    qkv, mixture, residual, mlp_own, cot_all = pl.pallas_call(
        functools.partial(attend_kernel, n, pieces),
        out_shape=(shape((3, LEN, width), BF), shape((LEN, width), BF), shape((size, depth), F32),
                   shape((size, depth), BF), shape((n, size, depth), BF)),
        in_specs=[ANY] * 3 + [VM] * 6, out_specs=(VM, VM, VM, VM, ANY),
        scratch_shapes=[pltpu.VMEM((LEN, depth), BF), pltpu.VMEM((3, depth, width), BF), pltpu.VMEM((width, depth), BF)] +
                       sums + [dma((2, n)), dma((n,)), dma((n, pieces)), dma((n + 1, pieces)), dma, dma, dma((4,))],
        compiler_params=params(1), name="attend",
    )(attn_in, w_qkv, w_out, tokens, cotangent, bias_qv, bias_out, gain_two, shift_two)

    pieces = 4
    mlp_in, hidden, grad_pre, mlp_part, grad_resid, branch_cot, vec_two, grad_up_b = pl.pallas_call(
        functools.partial(hidden_kernel, n, pieces),
        out_shape=(shape((n, size, depth), BF), shape((n, size, units), BF), shape((n, size, units), BF),
                   shape((n, size, depth), BF), shape((size, depth), F32), shape((size, depth), BF),
                   shape((8, depth), F32), shape((8, units), F32)),
        in_specs=[VM, VM, ANY, ANY, ANY, VM, VM], out_specs=(ANY, ANY, ANY, ANY, VM, VM, VM, VM),
        scratch_shapes=[pltpu.VMEM((n, size, depth), BF), pltpu.VMEM((n, size, units), BF),
                        pltpu.VMEM((n, size, units), BF), pltpu.VMEM((n, size, depth), BF),
                        pltpu.VMEM((depth, units), BF), pltpu.VMEM((units, depth), BF)] + sums +
                       [dma((2, n)), dma((n,)), dma((n, pieces)), dma((n + 1, pieces)), dma((2,)), dma, dma,
                        dma((n,)), dma((n,)), dma((n,)), pltpu.VMEM((n, size, depth), BF), dma((n,))],
        compiler_params=params(2), name="hidden",
    )(mlp_own, residual, cot_all, w_up, w_down, bias_up, gain_two)
    mlp_in, hidden, grad_pre, cot_rows = [v.reshape(LEN, -1) for v in (mlp_in, hidden, grad_pre, cot_all)]

    def plane_scratch(columns):
        rows = depth // m
        return [pltpu.VMEM((m, rows, columns), BF), pltpu.VMEM((m // 2, rows, columns), BF),
                pltpu.VMEM((2, m // 2 - 1, rows // 2, columns), BF)]

    pieces = 2
    sum_sems = [dma((n, pieces)), dma((n + 1, pieces))]
    attn_cot, layer_out, grad_down_w, grad_up_w = pl.pallas_call(
        functools.partial(branch_kernel, n, m, pieces),
        out_shape=(shape((n, size, depth), BF), shape((size, depth), BF), shape((depth // m, units), F32),
                   shape((depth // m, units), F32)),
        in_specs=[VM] * 3 + [ANY] * 5, out_specs=(ANY, VM, VM, VM),
        scratch_shapes=[pltpu.VMEM((LEN, depth), BF), pltpu.VMEM((LEN, units), BF)] + sums + plane_scratch(units) * 2 +
                       [pltpu.VMEM((RB, depth), F32), dma((2, n)), dma((n,))] + sum_sems +
                       [dma, dma, dma((2,)), dma((2, m // 2)), dma((2, m // 2)), dma((2, 2, m // 2 - 1)),
                        dma((2, 2, m // 2 - 1))],
        compiler_params=params(4), name="branch",
    )(branch_cot, residual, bias_down, mlp_part, hidden, cot_rows, mlp_in, grad_pre)
    attn_cot = attn_cot.reshape(LEN, depth)
    grad_mix = jnp.einsum("rd,ed->re", attn_cot, w_out, preferred_element_type=F32).astype(BF)
    grad_qkv = pl.pallas_call(
        attend_back_kernel, out_shape=shape((3, LEN, width), BF), in_specs=[VM, VM], out_specs=VM,
        scratch_shapes=[pltpu.VMEM((LEN, HD), F32), pltpu.VMEM((LEN, HD), F32)],
        compiler_params=params(), name="attend_back",
    )(qkv, grad_mix)
    grad_tokens, grad_qkv_w, grad_out_w, vec_one, grad_qv_b = pl.pallas_call(
        functools.partial(input_kernel, n, m, pieces),
        out_shape=(shape((size, depth), BF), shape((3, depth // m, width), F32), shape((depth // m, width), F32),
                   shape((8, depth), F32), shape((8, width), F32)),
        in_specs=[VM, ANY, VM, VM, VM, ANY, ANY, ANY], out_specs=(VM,) * 5,
        scratch_shapes=[pltpu.VMEM((3, depth, width), BF), pltpu.VMEM((LEN, depth), BF), pltpu.VMEM((LEN, depth), BF),
                        pltpu.VMEM((LEN, width), BF)] + sums + plane_scratch(4 * width) +
                       [pltpu.VMEM((RB, depth), F32)] + sum_sems +
                       [dma((4,)), dma((m // 2,)), dma((m // 2,)), dma((2, m // 2 - 1)), dma((2, m // 2 - 1))],
        compiler_params=params(5), name="input",
    )(grad_qkv, w_qkv, tokens, grad_resid, gain_one, attn_in, attn_cot, mixture)
    grad_down_w, grad_out_w = grad_down_w.T, grad_out_w.T

    vectors = jnp.stack([
        vec_one[0], vec_one[1], vec_two[2], vec_two[0], vec_two[1], vec_two[3],
    ])
    vectors = vectors.reshape(6, total, piece).transpose(1, 0, 2).reshape(total, 6 * piece)
    local = jnp.concatenate([
        grad_qv_b[:2].reshape(2, m, qv_piece).transpose(1, 0, 2).reshape(m, -1),
        grad_up_b[0].reshape(m, -1)], axis=1)
    local = jnp.broadcast_to(local[:, None], (m, n, local.shape[1])).reshape(total, -1)
    load = jnp.concatenate([vectors, local], axis=1)
    load = jnp.pad(load, ((0, 0), (0, -load.shape[1] % 1024))).reshape(total, -1, LANES)
    everyone, column = pl.pallas_call(
        functools.partial(share_kernel, n, m),
        out_shape=(shape(load.shape[1:], F32),) * 2, in_specs=[VM], out_specs=(VM, VM),
        scratch_shapes=[pltpu.VMEM(load.shape, F32), dma((total,)), dma((total,))],
        compiler_params=params(3), name="share",
    )(load)
    vectors = everyone.reshape(-1)[: 6 * piece].reshape(6, piece)
    local = column.reshape(-1)[6 * piece :]
    grad_qv_b = local[: 2 * qv_piece].reshape(2, qv_piece)
    grad_up_b = local[2 * qv_piece : 2 * qv_piece + up_piece]
    return (layer_out, grad_tokens, vectors[0], vectors[1], grad_qkv_w, grad_qv_b, grad_out_w, vectors[2],
            vectors[3], vectors[4], grad_up_w, grad_up_b, grad_down_w, vectors[5])


def solution(mesh):
    vector, matrix = P(("dp", "tensor")), P(("dp", "tensor"), None)
    in_specs = (matrix, matrix, vector, vector, P(None, "dp", "tensor"), P(None, ("tensor", "dp")), P("tensor", "dp"),
                vector, vector, vector, P("dp", "tensor"), P(("tensor", "dp")), P("tensor", "dp"), vector)
    out_specs = (matrix, matrix, vector, vector, P(None, "dp", "tensor"), P(None, ("tensor", "dp")),
                 P("tensor", "dp"), vector, vector, vector, P("dp", "tensor"), P(("tensor", "dp")), P("tensor", "dp"),
                 vector)
    return jax.shard_map(body, mesh=mesh, in_specs=in_specs, out_specs=out_specs, check_vma=False)
```

```python
import functools

import jax
import jax.numpy as jnp
from jax import lax
from jax.experimental import pallas as pl
from jax.experimental.pallas import tpu as pltpu
from jax.sharding import PartitionSpec as P

HD = 128
LEN = 1024
LANES = 128
EPS = 1e-05
BF = jnp.bfloat16
F32 = jnp.float32
MESH = pl.DeviceIdType.MESH
ANY = pl.BlockSpec(memory_space=pl.ANY)
VM = pl.BlockSpec(memory_space=pltpu.VMEM)
NT = (((1,), (1,)), ((), ()))
TN = (((0,), (0,)), ((), ()))
BIG = 64 * 1024 * 1024 - 65536
RB = 32


def norm_stats(rows):
    mean = jnp.mean(rows, axis=-1, keepdims=True)
    centred = rows - mean
    variance = jnp.mean(centred * centred, axis=-1, keepdims=True)
    inverse = lax.rsqrt(variance + EPS)
    return centred * inverse, inverse


def norm_back(grad_rows, normal_rows, inverse, gain):
    scaled = grad_rows * gain
    first = jnp.mean(scaled, axis=-1, keepdims=True)
    second = jnp.mean(scaled * normal_rows, axis=-1, keepdims=True)
    return inverse * (scaled - first - normal_rows * second)


def loop(count, step):
    def run(i, carry):
        step(i)
        return carry

    lax.fori_loop(0, count, run, 0)


def rows_at(j, size):
    return pl.ds(pl.multiple_of(j * size, size), size)


def remote(src, dst, send, recv, target):
    return pltpu.make_async_remote_copy(src_ref=src, dst_ref=dst, send_sem=send, recv_sem=recv,
                                        device_id={"tensor": target}, device_id_type=MESH)


def greet_neighbours(i, n):
    barrier = pltpu.get_barrier_semaphore()

    @pl.when(i > 0)
    def _():
        pl.semaphore_signal(barrier, inc=1, device_id={"tensor": i - 1}, device_id_type=MESH)

    @pl.when(i < n - 1)
    def _():
        pl.semaphore_signal(barrier, inc=1, device_id={"tensor": i + 1}, device_id_type=MESH)

    pl.semaphore_wait(barrier, jnp.minimum(i, 1) + jnp.minimum(n - 1 - i, 1))


def greet_all(me, n, total):
    barrier = pltpu.get_barrier_semaphore()

    def greet(s):
        other = (me + s + 1) % total
        pl.semaphore_signal(barrier, inc=1, device_id={"dp": other // n, "tensor": other % n}, device_id_type=MESH)

    loop(total - 1, greet)
    pl.semaphore_wait(barrier, total - 1)


def rounds(i, n, line, compute):
    def round_of(r):
        @pl.when(r > 0)
        def _():
            line.step(r)

        def side(s):
            j = jnp.where(s == 0, i - r, i + r)

            @pl.when(jnp.logical_and(jnp.logical_and(j >= 0, j <= n - 1), s * r == s * jnp.maximum(r, 1)))
            def _():
                compute(j)

        loop(2, side)

    loop(n, round_of)


class LineGather:
    def __init__(self, i, n, own, buf, send, recv):
        self.i, self.n, self.own, self.buf, self.send, self.recv = i, n, own, buf, send, recv

    def copy(self, src, j, side, target):
        return remote(src, self.buf.at[j], self.send.at[side, j], self.recv.at[j], target)

    def start(self):
        i, n = self.i, self.n

        @pl.when(i < n - 1)
        def _():
            self.copy(self.own, i, 0, i + 1).start()

        @pl.when(i > 0)
        def _():
            self.copy(self.own, i, 1, i - 1).start()

    def step(self, r):
        i, n = self.i, self.n

        @pl.when(i - r >= 0)
        def _():
            self.copy(self.own, i - r, 0, i).wait_recv()

            @pl.when(i < n - 1)
            def _():
                self.copy(self.buf.at[i - r], i - r, 0, i + 1).start()

        @pl.when(i + r <= n - 1)
        def _():
            self.copy(self.own, i + r, 1, i).wait_recv()

            @pl.when(i > 0)
            def _():
                self.copy(self.buf.at[i + r], i + r, 1, i - 1).start()

    def finish(self):
        i, n = self.i, self.n

        def one(j):
            @pl.when(jnp.logical_and(i < n - 1, j <= i))
            def _():
                self.copy(self.own, j, 0, i + 1).wait_send()

            @pl.when(jnp.logical_and(i > 0, j >= i))
            def _():
                self.copy(self.own, j, 1, i - 1).wait_send()

        loop(n, one)


class LineSum:
    def __init__(self, i, n, part, land, send, recv, pieces):
        self.i, self.n, self.part, self.land, self.send, self.recv = i, n, part, land, send, recv
        self.pieces = pieces
        self.size = part.shape[1] // pieces

    def copy(self, src, d, right, s):
        i, n = self.i, self.n
        target = i + 1 if right else i - 1
        slot = d if right else jnp.where(d == target, n, d)
        here = rows_at(s, self.size)
        return remote(src.at[d, here], self.land.at[slot, here], self.send.at[d, s], self.recv.at[slot, s], target)

    def arrived(self, slot, s):
        here = rows_at(s, self.size)
        remote(self.part.at[0, here], self.land.at[slot, here], self.send.at[0, s], self.recv.at[slot, s],
               self.i).wait_recv()

    def launch(self, d):
        i, n = self.i, self.n

        @pl.when(jnp.logical_and(i == 0, d > 0))
        def _():
            loop(self.pieces, lambda s: self.copy(self.part, d, True, s).start())

        @pl.when(jnp.logical_and(i == n - 1, d < n - 1))
        def _():
            loop(self.pieces, lambda s: self.copy(self.part, d, False, s).start())

    def relay(self, d, right):
        def one(s):
            self.arrived(d, s)
            here = rows_at(s, self.size)
            total = self.land[d, here, :].astype(F32) + self.part[d, here, :].astype(F32)
            self.land[d, here, :] = total.astype(BF)
            self.copy(self.land, d, right, s).start()

        loop(self.pieces, one)

    def own(self):
        i, n = self.i, self.n

        @pl.when(i > 0)
        def _():
            loop(self.pieces, lambda s: self.arrived(i, s))

        @pl.when(i < n - 1)
        def _():
            loop(self.pieces, lambda s: self.arrived(n, s))

    def add(self, here, out):
        i, n = self.i, self.n
        out[...] = self.part[i, here, :].astype(F32)

        @pl.when(i > 0)
        def _():
            out[...] += self.land[i, here, :].astype(F32)

        @pl.when(i < n - 1)
        def _():
            out[...] += self.land[n, here, :].astype(F32)

    def finish(self):
        i, n = self.i, self.n

        def one(d):
            @pl.when(jnp.logical_and(i < n - 1, d > i))
            def _():
                loop(self.pieces, lambda s: self.copy(self.part, d, True, s).wait_send())

            @pl.when(jnp.logical_and(i > 0, d < i))
            def _():
                loop(self.pieces, lambda s: self.copy(self.part, d, False, s).wait_send())

        loop(n, one)


def tokens_kernel(n, m, piece, pack_ref, x_ref, a_ref, vec_ref, buf, affine, own_sem, send, recv, v_send, v_recv):
    i, row = lax.axis_index("tensor"), lax.axis_index("dp")
    me, total = row * n + i, m * n
    size = x_ref.shape[0]
    greet_all(me, n, total)
    line = LineGather(i, n, x_ref, buf, send, recv)

    def vector(src, other):
        return pltpu.make_async_remote_copy(
            src_ref=pack_ref, dst_ref=vec_ref.at[src], send_sem=v_send.at[other], recv_sem=v_recv.at[src],
            device_id={"dp": other // n, "tensor": other % n}, device_id_type=MESH)

    loop(total - 1, lambda s: vector(me, (me + s + 1) % total).start())
    line.start()
    own_copy = pltpu.make_async_copy(x_ref, buf.at[i], own_sem)
    own_copy.start()
    vec_ref[me] = pack_ref[...]
    loop(total - 1, lambda s: vector((me + s + 1) % total, me).wait_recv())
    depth = affine.shape[1]
    group = LANES // piece
    for tile in range(depth // LANES):
        value = vec_ref[tile * group, 0:2, :].astype(F32)
        for g in range(1, group):
            value = value + vec_ref[tile * group + g, 0:2, :].astype(F32)
        affine[0:2, tile * LANES : (tile + 1) * LANES] = value
    own_copy.wait()

    def compute(j):
        def norm(b):
            normal, _ = norm_stats(buf[j, rows_at(b, RB), :].astype(F32))
            here = pl.ds(pl.multiple_of(j * size + b * RB, RB), RB)
            a_ref[here, :] = (normal * affine[0:1, :] + affine[1:2, :]).astype(BF)

        loop(size // RB, norm)

    rounds(i, n, line, compute)
    line.finish()
    loop(total - 1, lambda s: vector(me, (me + s + 1) % total).wait_send())


def attend_kernel(n, pieces, a_hbm, wq_hbm, wo_hbm, x_ref, cot_ref, bias, out_bias, gain, shift, qkv_ref, o_ref, h_ref,
                  c_ref, cot_all, a_ref, wq_ref, w_ref, part, land, send, recv, s_send, s_recv, own_sem, a_sem, w_sem):
    i = lax.axis_index("tensor")
    size = x_ref.shape[0]
    loads = [pltpu.make_async_copy(a_hbm, a_ref, a_sem)]
    loads += [pltpu.make_async_copy(wq_hbm.at[t], wq_ref.at[t], w_sem.at[t]) for t in range(3)]
    loads += [pltpu.make_async_copy(wo_hbm, w_ref, w_sem.at[3])]
    for load in loads:
        load.start()
    heads = qkv_ref.shape[2] // HD
    depth = w_ref.shape[1]
    greet_neighbours(i, n)
    line = LineGather(i, n, cot_ref, cot_all, send, recv)
    line.start()
    own_copy = pltpu.make_async_copy(cot_ref, cot_all.at[i], own_sem)
    own_copy.start()

    loads[0].wait()
    block = 256
    for t in range(3):
        loads[1 + t].wait()

        def project(b):
            here = rows_at(b, block)
            value = jnp.dot(a_ref[here, :], wq_ref[t], preferred_element_type=F32)
            if t != 1:
                value = value + bias[t // 2 : t // 2 + 1, :]
            qkv_ref[t, here, :] = value.astype(BF)

        loop(LEN // block, project)

    def head(t):
        cols = pl.ds(pl.multiple_of(t * HD, HD), HD)
        for b in range(LEN // block):
            here, keys = slice(b * block, (b + 1) * block), (b + 1) * block
            s = lax.dot_general(qkv_ref[0, here, cols], qkv_ref[1, 0:keys, cols], NT,
                                preferred_element_type=F32) * HD ** (-0.5)
            query = lax.broadcasted_iota(jnp.int32, s.shape, 0) + b * block
            s = jnp.where(query >= lax.broadcasted_iota(jnp.int32, s.shape, 1), s, -1e30)
            e = jnp.exp(s - jnp.max(s, axis=-1, keepdims=True))
            prob = (e / jnp.sum(e, axis=-1, keepdims=True)).astype(BF)
            o_ref[here, cols] = jnp.dot(prob, qkv_ref[2, 0:keys, cols], preferred_element_type=F32).astype(BF)

    loop(heads, head)
    loads[4].wait()
    sums = LineSum(i, n, part, land, s_send, s_recv, pieces)
    tile = 512

    def project(t):
        d = jnp.where(i < n // 2, n - 1 - t, t)

        def columns(k):
            cols = rows_at(k, tile)
            part[d, :, cols] = jnp.dot(o_ref[rows_at(d, size), :], w_ref[:, cols], preferred_element_type=F32).astype(BF)

        loop(depth // tile, columns)
        sums.launch(d)

    loop(n, project)

    def round_of(r):
        line.step(r + 1)
        right, left = n - 1 + i - (r + 1), r + 1 - (n - 1 - i)

        @pl.when(jnp.logical_and(i > 0, jnp.logical_and(right > i, right <= n - 1)))
        def _():
            sums.relay(right, True)

        @pl.when(jnp.logical_and(i < n - 1, jnp.logical_and(left >= 0, left < i)))
        def _():
            sums.relay(left, False)

    loop(n - 1, round_of)
    sums.own()

    def norm(b):
        here = rows_at(b, RB)
        sums.add(here, h_ref.at[here, :])
        rows = h_ref[here, :] + (x_ref[here, :].astype(F32) + out_bias[...])
        h_ref[here, :] = rows
        normal, _ = norm_stats(rows)
        c_ref[here, :] = (normal * gain[...] + shift[...]).astype(BF)

    loop(size // RB, norm)
    own_copy.wait()
    line.finish()
    sums.finish()


def hidden_kernel(n, pieces, c_ref, h_ref, cot_hbm, up_hbm, down_hbm, up_bias, gain, c_hbm, g_hbm, du_hbm, mlp_hbm, dh_ref,
                  db_ref, vec_ref, upb_ref, c_all, g_all, du_all, cot_all, up, down, part, land, send, recv, s_send,
                  s_recv, w_sem, cot_sem, own_sem, c_sem, g_sem, du_sem, mlp, mlp_sem):
    i = lax.axis_index("tensor")
    size, depth = c_ref.shape
    units = up.shape[1]
    greet_neighbours(i, n)
    line = LineGather(i, n, c_ref, c_all, send, recv)
    line.start()
    own_copy = pltpu.make_async_copy(c_ref, c_all.at[i], own_sem)
    own_copy.start()
    up_copy = pltpu.make_async_copy(up_hbm, up, w_sem.at[0])
    up_copy.start()
    down_copy = pltpu.make_async_copy(down_hbm, down, w_sem.at[1])
    down_copy.start()
    cot_copy = pltpu.make_async_copy(cot_hbm, cot_all, cot_sem)
    cot_copy.start()
    upb_ref[...] = jnp.zeros_like(upb_ref)
    vec_ref[...] = jnp.zeros_like(vec_ref)
    own_copy.wait()
    up_copy.wait()
    down_copy.wait()
    cot_copy.wait()
    sums = LineSum(i, n, part, land, s_send, s_recv, pieces)
    tile = 256

    def out_copy(src, dst, sem, j):
        return pltpu.make_async_copy(src.at[j], dst.at[j], sem.at[j])

    def compute(j):
        def unit(k):
            cols = rows_at(k, tile)
            u = jnp.dot(c_all[j], up[:, cols], preferred_element_type=F32) + up_bias[0:1, cols]
            dg = lax.dot_general(cot_all[j], down[cols, :], NT, preferred_element_type=F32)
            half = 0.5 + 0.5 * lax.erf(u * (0.5 ** 0.5))
            g_all[j, :, cols] = (u * half).astype(BF)
            slope = half + u * (jnp.exp(u * u * -0.5) * 0.3989422804014327)
            du = (slope * dg).astype(BF)
            du_all[j, :, cols] = du
            upb_ref[0:1, cols] += jnp.sum(du.astype(F32), axis=0, keepdims=True)

        loop(units // tile, unit)

        def back(k):
            cols = rows_at(k, tile)
            part[j, :, cols] = lax.dot_general(du_all[j], up[cols, :], NT, preferred_element_type=F32).astype(BF)

        loop(depth // tile, back)
        sums.launch(j)
        out_copy(g_all, g_hbm, g_sem, j).start()
        out_copy(du_all, du_hbm, du_sem, j).start()
        out_copy(c_all, c_hbm, c_sem, j).start()

    rounds(i, n, line, compute)

    def forward(j):
        def columns(k):
            cols = rows_at(k, tile)
            mlp[j, :, cols] = jnp.dot(g_all[j], down[:, cols], preferred_element_type=F32).astype(BF)

        loop(depth // tile, columns)
        out_copy(mlp, mlp_hbm, mlp_sem, j).start()

    loop(n, forward)

    def relay(t):
        right, left = t + 2 - i, 2 * n - 4 - i - t

        @pl.when(jnp.logical_and(i > 0, jnp.logical_and(right > i, right <= n - 1)))
        def _():
            sums.relay(right, True)

        @pl.when(jnp.logical_and(i < n - 1, jnp.logical_and(left >= 0, left < i)))
        def _():
            sums.relay(left, False)

    loop(2 * n - 3, relay)
    sums.own()

    def norm(b):
        here = rows_at(b, RB)
        sums.add(here, dh_ref.at[here, :])
        grad = dh_ref[here, :]
        normal, inverse = norm_stats(h_ref[here, :])
        vec_ref[0:1, :] += jnp.sum(grad * normal, axis=0, keepdims=True)
        vec_ref[1:2, :] += jnp.sum(grad, axis=0, keepdims=True)
        cot = cot_all[i, here, :].astype(F32)
        dh = cot + norm_back(grad, normal, inverse, gain[...])
        dh_ref[here, :] = dh
        db = dh.astype(BF)
        db_ref[here, :] = db
        vec_ref[2:3, :] += jnp.sum(db.astype(F32), axis=0, keepdims=True)
        vec_ref[3:4, :] += jnp.sum(cot, axis=0, keepdims=True)

    loop(size // RB, norm)

    def done(j):
        out_copy(g_all, g_hbm, g_sem, j).wait()
        out_copy(du_all, du_hbm, du_sem, j).wait()
        out_copy(c_all, c_hbm, c_sem, j).wait()
        out_copy(mlp, mlp_hbm, mlp_sem, j).wait()

    loop(n, done)
    line.finish()
    sums.finish()


def attend_back(q_of, k_of, v_of, do_of, heads, put, dk, dv):
    block = 256
    factor = HD ** (-0.5)

    def head(t):
        dk[...] = jnp.zeros_like(dk)
        dv[...] = jnp.zeros_like(dv)
        for b in range(LEN // block):
            here, keys = slice(b * block, (b + 1) * block), slice(0, (b + 1) * block)
            q, k, v, do = q_of(here, t), k_of(keys, t), v_of(keys, t), do_of(here, t)
            s = lax.dot_general(q, k, NT, preferred_element_type=F32) * factor
            query = lax.broadcasted_iota(jnp.int32, s.shape, 0) + b * block
            s = jnp.where(query >= lax.broadcasted_iota(jnp.int32, s.shape, 1), s, -1e30)
            e = jnp.exp(s - jnp.max(s, axis=-1, keepdims=True))
            prob = e / jnp.sum(e, axis=-1, keepdims=True)
            dv[keys, :] += lax.dot_general(prob.astype(BF), do, TN, preferred_element_type=F32)
            dp = lax.dot_general(do, v, NT, preferred_element_type=F32)
            ds = (prob * (dp - jnp.sum(prob * dp, axis=-1, keepdims=True))).astype(BF)
            put(0, here, t, (jnp.dot(ds, k, preferred_element_type=F32) * factor).astype(BF))
            dk[keys, :] += lax.dot_general(ds, q, TN, preferred_element_type=F32)
        put(1, slice(0, LEN), t, (dk[...] * factor).astype(BF))
        put(2, slice(0, LEN), t, dv[...].astype(BF))

    loop(heads, head)


def partner(row, bit):
    return row + bit * (1 - 2 * ((row // bit) % 2))


class PlaneSum:
    def __init__(self, row, m, out, terms, land, halves, send, recv, h_send, h_recv):
        self.row, self.m, self.out, self.terms, self.land, self.halves = row, m, out, terms, land, halves
        self.send, self.recv, self.h_send, self.h_recv = send, recv, h_send, h_recv
        bits = [1 << k for k in range(1, m.bit_length() - 1)]
        self.plan = []
        for order in (bits, bits[::-1]):
            left, at, stages = [e for e in range(m) if e % 2 == 0], 0, []
            for bit in order:
                out = [e for e in left if e & bit]
                stages.append((bit, [(e, e ^ bit, at + k) for k, e in enumerate(out)]))
                left, at = [e for e in left if not e & bit], at + len(out)
            self.plan.append(stages)
        self.stages = len(bits)

    def owner(self, e):
        d = self.row
        for k in range(self.m.bit_length() - 1):
            if e & (1 << k):
                d = d + (partner(self.row, 1 << k) - self.row)
        return d

    def whole(self, e):
        return pltpu.make_async_remote_copy(
            src_ref=self.out.at[e // 2], dst_ref=self.land.at[e // 2], send_sem=self.send.at[e // 2],
            recv_sem=self.recv.at[e // 2], device_id={"dp": partner(self.row, 1)}, device_id_type=MESH)

    def half(self, h, bit, e, at):
        size = self.halves.shape[2]
        return pltpu.make_async_remote_copy(
            src_ref=self.terms.at[e // 2, pl.ds(h * size, size)], dst_ref=self.halves.at[h, at],
            send_sem=self.h_send.at[h, at], recv_sem=self.h_recv.at[h, at],
            device_id={"dp": partner(self.row, bit)}, device_id_type=MESH)

    def merge(self):
        for e in range(0, self.m, 2):
            self.whole(e + 1).wait_recv()

            def add(b):
                here = rows_at(b, RB)
                total = self.terms[e // 2, here, :].astype(F32) + self.land[e // 2, here, :].astype(F32)
                self.terms[e // 2, here, :] = total.astype(BF)

            loop(self.terms.shape[1] // RB, add)

    def push(self, stage):
        for h in range(2):
            bit, moves = self.plan[h][stage]
            for e, _, at in moves:
                self.half(h, bit, e, at).start()

    def take(self, stage, out=None):
        size = self.halves.shape[2]
        for h in range(2):
            bit, moves = self.plan[h][stage]
            for e, into, at in moves:
                self.half(h, bit, e, at).wait_recv()

                def add(b):
                    here, there = rows_at(b, RB), pl.ds(pl.multiple_of(h * size + b * RB, RB), RB)
                    total = self.terms[into // 2, there, :].astype(F32) + self.halves[h, at, here, :].astype(F32)
                    if out is None:
                        self.terms[into // 2, there, :] = total.astype(BF)
                    else:
                        out(there, total)

                loop(size // RB, add)

    def sent(self):
        for e in range(1, self.m, 2):
            self.whole(e).wait_send()

    def finish(self):
        for h in range(2):
            for bit, moves in self.plan[h]:
                for e, _, at in moves:
                    self.half(h, bit, e, at).wait_send()


class VectorSum:
    def __init__(self, me, count, device, vectors, piece, land, out, send, recv):
        self.me, self.count, self.device, self.vectors, self.piece = me, count, device, vectors, piece
        self.land, self.out, self.send, self.recv = land, out, send, recv

    def lanes(self, owner):
        size = self.land.shape[2]
        return pl.ds(pl.multiple_of(owner * self.piece // size * size, size), size)

    def copy(self, src, other):
        return pltpu.make_async_remote_copy(
            src_ref=self.vectors.at[:, self.lanes(other)], dst_ref=self.land.at[src], send_sem=self.send.at[other],
            recv_sem=self.recv.at[src], device_id=self.device(other), device_id_type=MESH)

    def start(self):
        loop(self.count - 1, lambda s: self.copy(self.me, (self.me + s + 1) % self.count).start())

    def finish(self):
        self.out[...] = self.vectors[:, self.lanes(self.me)]

        def take(s):
            src = (self.me + s + 1) % self.count
            self.copy(src, self.me).wait_recv()
            self.out[...] += self.land[src]

        loop(self.count - 1, take)
        loop(self.count - 1, lambda s: self.copy(self.me, (self.me + s + 1) % self.count).wait_send())


def greet_cross(i, n, row, m):
    barrier = pltpu.get_barrier_semaphore()

    @pl.when(i > 0)
    def _():
        pl.semaphore_signal(barrier, inc=1, device_id={"tensor": i - 1}, device_id_type=MESH)

    @pl.when(i < n - 1)
    def _():
        pl.semaphore_signal(barrier, inc=1, device_id={"tensor": i + 1}, device_id_type=MESH)

    bits = [1 << k for k in range(m.bit_length() - 1)]
    for bit in bits:
        pl.semaphore_signal(barrier, inc=1, device_id={"dp": partner(row, bit)}, device_id_type=MESH)
    pl.semaphore_wait(barrier, jnp.minimum(i, 1) + jnp.minimum(n - 1 - i, 1) + len(bits))


def relays(sums, i, n, r):
    right, left = n - 1 + i - r, r - (n - 1 - i)

    @pl.when(jnp.logical_and(i > 0, jnp.logical_and(right > i, right <= n - 1)))
    def _():
        sums.relay(right, True)

    @pl.when(jnp.logical_and(i < n - 1, jnp.logical_and(left >= 0, left < i)))
    def _():
        sums.relay(left, False)


def block_terms(plane, e, pairs):
    size = plane.terms.shape[1]
    cols = rows_at(plane.owner(e), size)
    for lhs, rhs, first in pairs:
        width = rhs.shape[1]
        tile = min(512, width)

        def columns(k):
            there = pl.ds(pl.multiple_of(first + k * tile, tile), tile)
            (plane.out if e % 2 else plane.terms)[e // 2, :, there] = lax.dot_general(
                lhs[:, cols], rhs[:, rows_at(k, tile)], TN, preferred_element_type=F32).astype(BF)

        loop(width // tile, columns)


def branch_kernel(n, m, pieces, db_ref, h_ref, down_bias, mlp_hbm, g_hbm, cot_hbm, c_hbm, du_hbm, qkv_hbm, wo_hbm,
                  db_all, lo_ref, down_ref, up_ref, dqkv_ref, lhs, rhs, wo, dk, dv, part, land, out, terms_a, land_a,
                  half_a, terms_b, land_b, half_b, acc, send, recv, s_send, s_recv, own_sem, part_sem, in_sem, qkv_sem,
                  db_sem, p_send, p_recv, h_send, h_recv):
    i, row = lax.axis_index("tensor"), lax.axis_index("dp")
    size = db_ref.shape[0]
    width = wo.shape[0]
    greet_cross(i, n, row, m)
    line = LineGather(i, n, db_ref, db_all, send, recv)
    line.start()
    part_copy = pltpu.make_async_copy(mlp_hbm, part, part_sem)
    part_copy.start()
    own_copy = pltpu.make_async_copy(db_ref, db_all.at[i], own_sem)
    own_copy.start()

    def load(left, right):
        return [pltpu.make_async_copy(left, lhs, in_sem.at[0]), pltpu.make_async_copy(right, rhs, in_sem.at[1])]

    loads = load(cot_hbm, g_hbm)
    for copy in loads:
        copy.start()
    wo_copy = pltpu.make_async_copy(wo_hbm, wo, in_sem.at[2])
    wo_copy.start()
    sums = LineSum(i, n, part, land, s_send, s_recv, pieces)
    part_copy.wait()
    loop(n, lambda t: sums.launch(jnp.where(i < n // 2, n - 1 - t, t)))
    planes = [PlaneSum(row, m, out, terms_a, land_a, half_a, p_send.at[0], p_recv.at[0], h_send.at[0], h_recv.at[0]),
              PlaneSum(row, m, out, terms_b, land_b, half_b, p_send.at[1], p_recv.at[1], h_send.at[1], h_recv.at[1])]
    first, second = planes
    for copy in loads:
        copy.wait()
    left, right = lhs.at[:, 0 : lhs.shape[1]], rhs.at[:, 0 : down_ref.shape[1]]
    for e in range(1, m, 2):
        block_terms(first, e, [(left, right, 0)])
        first.whole(e).start()
    for e in range(m - 2, -1, -2):
        block_terms(first, e, [(left, right, 0)])
    loads = load(c_hbm, du_hbm)
    for copy in loads:
        copy.start()
    first.merge()
    first.push(0)
    first.sent()
    for copy in loads:
        copy.wait()
    for e in range(1, m, 2):
        block_terms(second, e, [(left, right, 0)])
        second.whole(e).start()

    def line_round(r):
        line.step(r)
        relays(sums, i, n, r)

    line_round(1)
    for e in range(m - 2, -1, -2):
        block_terms(second, e, [(left, right, 0)])
    qkv_copies = [pltpu.make_async_copy(qkv_hbm.at[p], rhs.at[:, p * width : (p + 1) * width], qkv_sem.at[p])
                  for p in range(3)]
    for copy in qkv_copies:
        copy.start()
    second.merge()
    second.push(0)
    own_copy.wait()
    wo_copy.wait()

    def mixture_back(j):
        here = rows_at(j, size)
        copy = pltpu.make_async_copy(db_all.at[j], lhs.at[here], db_sem.at[j])
        copy.start()
        copy.wait()
        rhs[here, 3 * width : 4 * width] = lax.dot_general(
            lhs[here, :], wo[...], NT, preferred_element_type=F32).astype(BF)

    def round_back(r):
        def side(s):
            j = jnp.where(s == 0, i - r, i + r)

            @pl.when(jnp.logical_and(j >= 0, j <= n - 1))
            def _():
                mixture_back(j)

        loop(2, side)

    def keep(ref):
        def put(here, total):
            ref[here, :] = total

        return put

    def advance(plane, stage, ref):
        if stage < plane.stages - 1:
            plane.take(stage)
            plane.push(stage + 1)
        else:
            plane.take(stage, keep(ref))

    mixture_back(i)
    round_back(1)
    advance(first, 0, down_ref)
    line_round(2)
    round_back(2)
    advance(second, 0, up_ref)

    def rest(r):
        line_round(r)
        round_back(r)

    for r in range(3, n):
        rest(r)
    for copy in qkv_copies:
        copy.wait()

    def column(p):
        def get(here, t):
            return rhs[here, pl.ds(pl.multiple_of(p * width + t * HD, HD), HD)]

        return get

    def put(p, here, t, value):
        dqkv_ref[p, here, pl.ds(pl.multiple_of(t * HD, HD), HD)] = value

    attend_back(column(0), column(1), column(2), column(3), width // HD, put, dk, dv)
    for stage in range(1, first.stages):
        advance(first, stage, down_ref)
        advance(second, stage, up_ref)
    sums.own()

    def output(b):
        here = rows_at(b, RB)
        sums.add(here, acc)
        lo_ref[here, :] = (h_ref[here, :] + (acc[...] + down_bias[...])).astype(BF)

    loop(size // RB, output)
    line.finish()
    sums.finish()
    second.sent()
    for plane in planes:
        plane.finish()


def input_kernel(n, m, pieces, widths, dqkv_ref, wq_hbm, x_ref, dh_ref, gain, early_ref, up_ref, a_hbm, db_hbm, o_hbm,
                 gt_ref, gqkv_ref, gout_ref, early_out, late_out, up_out, qv_out, vec_ref, qv_ref, wq, a_ref, db_ref,
                 o_ref, part, land, out_p, terms, land_p, half_p, acc, early_land, late_land, up_land, qv_land, s_send,
                 s_recv, in_sem, p_send, p_recv, h_send, h_recv, e_send, e_recv, l_send, l_recv, u_send, u_recv, q_send,
                 q_recv):
    i, row = lax.axis_index("tensor"), lax.axis_index("dp")
    me, total_devices = row * n + i, m * n
    size = x_ref.shape[0]
    width = dqkv_ref.shape[2]
    piece, up_piece, qv_piece = widths
    depth = part.shape[2]
    loads = [pltpu.make_async_copy(wq_hbm, wq, in_sem.at[0]), pltpu.make_async_copy(a_hbm, a_ref, in_sem.at[1]),
             pltpu.make_async_copy(db_hbm, db_ref, in_sem.at[2]), pltpu.make_async_copy(o_hbm, o_ref, in_sem.at[3])]
    for copy in loads:
        copy.start()
    greet_all(me, n, total_devices)
    every = [VectorSum(me, total_devices, lambda g: {"dp": g // n, "tensor": g % n}, early_ref, piece, early_land, early_out,
                       e_send, e_recv),
             VectorSum(me, total_devices, lambda g: {"dp": g // n, "tensor": g % n}, vec_ref, piece, late_land, late_out,
                       l_send, l_recv)]
    column = [VectorSum(row, m, lambda g: {"dp": g}, up_ref, up_piece, up_land, up_out, u_send, u_recv),
              VectorSum(row, m, lambda g: {"dp": g}, qv_ref, qv_piece, qv_land, qv_out, q_send, q_recv)]
    every[0].start()
    column[0].start()
    sums = LineSum(i, n, part, land, s_send, s_recv, pieces)
    vec_ref[...] = jnp.zeros_like(vec_ref)
    qv_ref[...] = jnp.zeros_like(qv_ref)
    loads[0].wait()
    tile = 512

    def term(t):
        d = jnp.where(i < n // 2, n - 1 - t, t)
        here = rows_at(d, size)

        def columns(k):
            cols = rows_at(k, tile)
            total = lax.dot_general(dqkv_ref[0, here, :], wq[0, cols, :], NT, preferred_element_type=F32)
            for p in range(1, 3):
                total += lax.dot_general(dqkv_ref[p, here, :], wq[p, cols, :], NT, preferred_element_type=F32)
            part[d, :, cols] = total.astype(BF)

        loop(depth // tile, columns)
        sums.launch(d)
        for p in range(2):
            qv_ref[p : p + 1, :] += jnp.sum(dqkv_ref[2 * p, here, :].astype(F32), axis=0, keepdims=True)

    loop(n, term)
    column[1].start()
    for copy in loads[1:]:
        copy.wait()
    plane = PlaneSum(row, m, out_p, terms, land_p, half_p, p_send, p_recv, h_send, h_recv)
    pairs = [(a_ref, dqkv_ref.at[p], p * width) for p in range(3)] + [(db_ref, o_ref, 3 * width)]
    for e in range(1, m, 2):
        block_terms(plane, e, pairs)
        plane.whole(e).start()
    for e in range(m - 2, -1, -2):
        block_terms(plane, e, pairs)
    plane.merge()
    plane.push(0)

    def out(here, total):
        for p in range(3):
            gqkv_ref[p, here, :] = total[:, p * width : (p + 1) * width]
        gout_ref[here, :] = total[:, 3 * width :]

    stage = 0
    for r in range(1, n):
        relays(sums, i, n, r)
        if r > 1 and stage < plane.stages:
            if stage < plane.stages - 1:
                plane.take(stage)
                plane.push(stage + 1)
            else:
                plane.take(stage, out)
            stage += 1
    sums.own()

    def norm(b):
        here = rows_at(b, RB)
        sums.add(here, acc)
        grad = acc[...]
        normal, inverse = norm_stats(x_ref[here, :].astype(F32))
        vec_ref[0:1, :] += jnp.sum(grad * normal, axis=0, keepdims=True)
        vec_ref[1:2, :] += jnp.sum(grad, axis=0, keepdims=True)
        gt_ref[here, :] = (dh_ref[here, :] + norm_back(grad, normal, inverse, gain[...])).astype(BF)

    loop(size // RB, norm)
    every[1].start()
    while stage < plane.stages:
        if stage < plane.stages - 1:
            plane.take(stage)
            plane.push(stage + 1)
        else:
            plane.take(stage, out)
        stage += 1
    sums.finish()
    plane.sent()
    plane.finish()
    for group in (every[0], column[0], column[1], every[1]):
        group.finish()


def params(collective=None):
    if collective is None:
        return pltpu.CompilerParams(vmem_limit_bytes=BIG)
    return pltpu.CompilerParams(vmem_limit_bytes=BIG, collective_id=collective, has_side_effects=True)


def shape(dims, dtype):
    return jax.ShapeDtypeStruct(dims, dtype)


def body(tokens, cotangent, ln1_gain, ln1_bias, qkv_weight, qv_bias, out_weight, out_bias, ln2_gain, ln2_bias,
         up_weight, up_bias, down_weight, down_bias):
    n = lax.axis_size("tensor")
    m = lax.axis_size("dp")
    i, row = lax.axis_index("tensor"), lax.axis_index("dp")
    size, depth = tokens.shape
    width = qkv_weight.shape[2]
    units = up_weight.shape[1]
    piece, qv_piece, up_piece = ln1_gain.shape[0], qv_bias.shape[1], up_bias.shape[0]
    total = m * n

    def lane_rows(value, index):
        count = value.shape[-1]
        if count >= LANES:
            return value.reshape(-1, LANES)
        places = LANES // count
        spread = jnp.tile(value.reshape(-1, count), (1, places))
        return jnp.where((jnp.arange(LANES) // count)[None] == index % places, spread, 0)

    me = row * n + i
    whole = jnp.stack([ln1_gain, ln1_bias, out_bias, ln2_gain, ln2_bias, down_bias])
    pack = jnp.concatenate([lane_rows(whole, me), lane_rows(qv_bias, row), lane_rows(up_bias, row)])
    pack = jnp.pad(pack, ((0, -pack.shape[0] % 16), (0, 0)))
    lanes_up = 8 + max(up_piece // LANES, 1)

    w_qkv = lax.all_gather(qkv_weight, "dp", axis=1, tiled=True)
    w_out = lax.all_gather(out_weight, "dp", axis=1, tiled=True)
    w_up = lax.all_gather(up_weight, "dp", axis=0, tiled=True)
    w_down = lax.all_gather(down_weight, "dp", axis=1, tiled=True)

    dma = pltpu.SemaphoreType.DMA
    attn_in, vecs = pl.pallas_call(
        functools.partial(tokens_kernel, n, m, piece),
        out_shape=(shape((LEN, depth), BF), shape((total,) + pack.shape, BF)),
        in_specs=[VM, VM], out_specs=(VM, VM),
        scratch_shapes=[pltpu.VMEM((n, size, depth), BF), pltpu.VMEM((8, depth), F32), dma, dma((2, n)), dma((n,)),
                        dma((total,)), dma((total,))],
        compiler_params=params(0), name="gather_tokens",
    )(pack, tokens)
    vecs = vecs.astype(F32)

    def whole_rows(block, count):
        if count < LANES:
            block = block.reshape(-1, LANES // count, *block.shape[1:]).sum(axis=1)
        return block

    vectors = whole_rows(vecs[:, 0:6], piece).transpose(1, 0, 2).reshape(6, 1, depth)
    gain_one, shift_one, bias_out, gain_two, shift_two, bias_down = [vectors[j] for j in range(6)]
    mine = lax.dynamic_index_in_dim(vecs.reshape(m, n, -1, LANES), i, 1, keepdims=False)
    bias_qv = whole_rows(mine[:, 6:8], qv_piece).transpose(1, 0, 2).reshape(2, width)
    bias_up = whole_rows(mine[:, 8:lanes_up], up_piece).reshape(1, units)

    pieces = 2
    sums = [pltpu.VMEM((n, size, depth), BF), pltpu.VMEM((n + 1, size, depth), BF)]
    qkv, mixture, residual, mlp_own, cot_all = pl.pallas_call(
        functools.partial(attend_kernel, n, pieces),
        out_shape=(shape((3, LEN, width), BF), shape((LEN, width), BF), shape((size, depth), F32),
                   shape((size, depth), BF), shape((n, size, depth), BF)),
        in_specs=[ANY] * 3 + [VM] * 6, out_specs=(VM, VM, VM, VM, ANY),
        scratch_shapes=[pltpu.VMEM((LEN, depth), BF), pltpu.VMEM((3, depth, width), BF), pltpu.VMEM((width, depth), BF)] +
                       sums + [dma((2, n)), dma((n,)), dma((n, pieces)), dma((n + 1, pieces)), dma, dma, dma((4,))],
        compiler_params=params(1), name="attend",
    )(attn_in, w_qkv, w_out, tokens, cotangent, bias_qv, bias_out, gain_two, shift_two)

    pieces = 4
    mlp_in, hidden, grad_pre, mlp_part, grad_resid, branch_cot, vec_two, grad_up_b = pl.pallas_call(
        functools.partial(hidden_kernel, n, pieces),
        out_shape=(shape((n, size, depth), BF), shape((n, size, units), BF), shape((n, size, units), BF),
                   shape((n, size, depth), BF), shape((size, depth), F32), shape((size, depth), BF),
                   shape((8, depth), F32), shape((8, units), F32)),
        in_specs=[VM, VM, ANY, ANY, ANY, VM, VM], out_specs=(ANY, ANY, ANY, ANY, VM, VM, VM, VM),
        scratch_shapes=[pltpu.VMEM((n, size, depth), BF), pltpu.VMEM((n, size, units), BF),
                        pltpu.VMEM((n, size, units), BF), pltpu.VMEM((n, size, depth), BF),
                        pltpu.VMEM((depth, units), BF), pltpu.VMEM((units, depth), BF)] + sums +
                       [dma((2, n)), dma((n,)), dma((n, pieces)), dma((n + 1, pieces)), dma((2,)), dma, dma,
                        dma((n,)), dma((n,)), dma((n,)), pltpu.VMEM((n, size, depth), BF), dma((n,))],
        compiler_params=params(2), name="hidden",
    )(mlp_own, residual, cot_all, w_up, w_down, bias_up, gain_two)
    mlp_in, hidden, grad_pre, cot_rows = [v.reshape(LEN, -1) for v in (mlp_in, hidden, grad_pre, cot_all)]

    def plane_scratch(columns):
        rows = depth // m
        return [pltpu.VMEM((m // 2, rows, columns), BF), pltpu.VMEM((m // 2, rows, columns), BF),
                pltpu.VMEM((2, m // 2 - 1, rows // 2, columns), BF)]

    pieces = 2
    sum_sems = [dma((n, pieces)), dma((n + 1, pieces))]
    attn_cot, layer_out, grad_down_w, grad_up_w, grad_qkv = pl.pallas_call(
        functools.partial(branch_kernel, n, m, pieces),
        out_shape=(shape((n, size, depth), BF), shape((size, depth), BF), shape((depth // m, units), F32),
                   shape((depth // m, units), F32), shape((3, LEN, width), BF)),
        in_specs=[VM] * 3 + [ANY] * 7, out_specs=(ANY, VM, VM, VM, VM),
        scratch_shapes=[pltpu.VMEM((LEN, depth), BF), pltpu.VMEM((LEN, units), BF), pltpu.VMEM((width, depth), BF),
                        pltpu.VMEM((LEN, HD), F32), pltpu.VMEM((LEN, HD), F32)] + sums +
                       [pltpu.VMEM((m // 2, depth // m, units), BF)] + plane_scratch(units) * 2 +
                       [pltpu.VMEM((RB, depth), F32), dma((2, n)), dma((n,))] + sum_sems +
                       [dma, dma, dma((3,)), dma((3,)), dma((n,)), dma((2, m // 2)), dma((2, m // 2)),
                        dma((2, 2, m // 2 - 1)), dma((2, 2, m // 2 - 1))],
        compiler_params=params(4), name="branch",
    )(branch_cot, residual, bias_down, mlp_part, hidden, cot_rows, mlp_in, grad_pre, qkv, w_out)
    attn_cot = attn_cot.reshape(LEN, depth)

    tiles = [max(v, LANES) for v in (piece, up_piece, qv_piece)]
    grad_tokens, grad_qkv_w, grad_out_w, early, late, grad_up_b, grad_qv_b = pl.pallas_call(
        functools.partial(input_kernel, n, m, pieces, (piece, up_piece, qv_piece)),
        out_shape=(shape((size, depth), BF), shape((3, depth // m, width), F32), shape((depth // m, width), F32),
                   shape((8, tiles[0]), F32), shape((8, tiles[0]), F32), shape((8, tiles[1]), F32),
                   shape((8, tiles[2]), F32)),
        in_specs=[VM, ANY, VM, VM, VM, VM, VM, ANY, ANY, ANY], out_specs=(VM,) * 7,
        scratch_shapes=[pltpu.VMEM((8, depth), F32), pltpu.VMEM((8, width), F32),
                        pltpu.VMEM((3, depth, width), BF), pltpu.VMEM((LEN, depth), BF), pltpu.VMEM((LEN, depth), BF),
                        pltpu.VMEM((LEN, width), BF)] + sums + [pltpu.VMEM((m // 2, depth // m, 4 * width), BF)] +
                       plane_scratch(4 * width) +
                       [pltpu.VMEM((RB, depth), F32), pltpu.VMEM((total, 8, tiles[0]), F32),
                        pltpu.VMEM((total, 8, tiles[0]), F32), pltpu.VMEM((m, 8, tiles[1]), F32),
                        pltpu.VMEM((m, 8, tiles[2]), F32)] + sum_sems +
                       [dma((4,)), dma((m // 2,)), dma((m // 2,)), dma((2, m // 2 - 1)), dma((2, m // 2 - 1))] +
                       [dma((total,))] * 4 + [dma((m,))] * 4,
        compiler_params=params(5), name="input",
    )(grad_qkv, w_qkv, tokens, grad_resid, gain_one, vec_two, grad_up_b, attn_in, attn_cot, mixture)
    grad_down_w, grad_out_w = grad_down_w.T, grad_out_w.T

    def own_lanes(block, index, count):
        return lax.dynamic_slice_in_dim(block, index * count % block.shape[1], count, axis=1)

    early, late = own_lanes(early, me, piece), own_lanes(late, me, piece)
    vectors = [late[0], late[1], early[2], early[0], early[1], early[3]]
    grad_qv_b = own_lanes(grad_qv_b, row, qv_piece)[:2]
    grad_up_b = own_lanes(grad_up_b, row, up_piece)[0]
    return (layer_out, grad_tokens, vectors[0], vectors[1], grad_qkv_w, grad_qv_b, grad_out_w, vectors[2],
            vectors[3], vectors[4], grad_up_w, grad_up_b, grad_down_w, vectors[5])


def solution(mesh):
    vector, matrix = P(("dp", "tensor")), P(("dp", "tensor"), None)
    in_specs = (matrix, matrix, vector, vector, P(None, "dp", "tensor"), P(None, ("tensor", "dp")), P("tensor", "dp"),
                vector, vector, vector, P("dp", "tensor"), P(("tensor", "dp")), P("tensor", "dp"), vector)
    out_specs = (matrix, matrix, vector, vector, P(None, "dp", "tensor"), P(None, ("tensor", "dp")),
                 P("tensor", "dp"), vector, vector, vector, P("dp", "tensor"), P(("tensor", "dp")), P("tensor", "dp"),
                 vector)
    return jax.shard_map(body, mesh=mesh, in_specs=in_specs, out_specs=out_specs, check_vma=False)
```

```python
import functools

import jax
import jax.numpy as jnp
from jax import lax
from jax.experimental import pallas as pl
from jax.experimental.pallas import tpu as pltpu
from jax.sharding import PartitionSpec as P

HD = 128
LEN = 1024
LANES = 128
EPS = 1e-05
BF = jnp.bfloat16
F32 = jnp.float32
MESH = pl.DeviceIdType.MESH
ANY = pl.BlockSpec(memory_space=pl.ANY)
VM = pl.BlockSpec(memory_space=pltpu.VMEM)
NT = (((1,), (1,)), ((), ()))
TN = (((0,), (0,)), ((), ()))
BIG = 64 * 1024 * 1024 - 65536
RB = 32


def norm_stats(rows):
    mean = jnp.mean(rows, axis=-1, keepdims=True)
    centred = rows - mean
    variance = jnp.mean(centred * centred, axis=-1, keepdims=True)
    inverse = lax.rsqrt(variance + EPS)
    return centred * inverse, inverse


def norm_back(grad_rows, normal_rows, inverse, gain):
    scaled = grad_rows * gain
    first = jnp.mean(scaled, axis=-1, keepdims=True)
    second = jnp.mean(scaled * normal_rows, axis=-1, keepdims=True)
    return inverse * (scaled - first - normal_rows * second)


def loop(count, step):
    def run(i, carry):
        step(i)
        return carry

    lax.fori_loop(0, count, run, 0)


def rows_at(j, size):
    return pl.ds(pl.multiple_of(j * size, size), size)


def remote(src, dst, send, recv, target):
    return pltpu.make_async_remote_copy(src_ref=src, dst_ref=dst, send_sem=send, recv_sem=recv,
                                        device_id={"tensor": target}, device_id_type=MESH)


def greet_neighbours(i, n):
    barrier = pltpu.get_barrier_semaphore()

    @pl.when(i > 0)
    def _():
        pl.semaphore_signal(barrier, inc=1, device_id={"tensor": i - 1}, device_id_type=MESH)

    @pl.when(i < n - 1)
    def _():
        pl.semaphore_signal(barrier, inc=1, device_id={"tensor": i + 1}, device_id_type=MESH)

    pl.semaphore_wait(barrier, jnp.minimum(i, 1) + jnp.minimum(n - 1 - i, 1))


def greet_all(me, n, total):
    barrier = pltpu.get_barrier_semaphore()

    def greet(s):
        other = (me + s + 1) % total
        pl.semaphore_signal(barrier, inc=1, device_id={"dp": other // n, "tensor": other % n}, device_id_type=MESH)

    loop(total - 1, greet)
    pl.semaphore_wait(barrier, total - 1)


def rounds(i, n, line, compute):
    def round_of(r):
        @pl.when(r > 0)
        def _():
            line.step(r)

        def side(s):
            j = jnp.where(s == 0, i - r, i + r)

            @pl.when(jnp.logical_and(jnp.logical_and(j >= 0, j <= n - 1), s * r == s * jnp.maximum(r, 1)))
            def _():
                compute(j)

        loop(2, side)

    loop(n, round_of)


class LineGather:
    PIECES = 2

    def __init__(self, i, n, own, buf, send, recv):
        self.i, self.n, self.own, self.buf, self.send, self.recv = i, n, own, buf, send, recv
        self.size = own.shape[0] // self.PIECES

    def copy(self, src, j, side, s, target):
        here = pl.ds(s * self.size, self.size)
        return remote(src.at[here], self.buf.at[j, here], self.send.at[side, j, s], self.recv.at[j, s], target)

    def start(self):
        i, n = self.i, self.n
        for s in range(self.PIECES):
            @pl.when(i < n - 1)
            def _():
                self.copy(self.own, i, 0, s, i + 1).start()

            @pl.when(i > 0)
            def _():
                self.copy(self.own, i, 1, s, i - 1).start()

    def step(self, r):
        i, n = self.i, self.n
        for s in range(self.PIECES):
            @pl.when(i - r >= 0)
            def _():
                self.copy(self.own, i - r, 0, s, i).wait_recv()

                @pl.when(i < n - 1)
                def _():
                    self.copy(self.buf.at[i - r], i - r, 0, s, i + 1).start()

            @pl.when(i + r <= n - 1)
            def _():
                self.copy(self.own, i + r, 1, s, i).wait_recv()

                @pl.when(i > 0)
                def _():
                    self.copy(self.buf.at[i + r], i + r, 1, s, i - 1).start()

    def finish(self):
        i, n = self.i, self.n

        def one(j):
            for s in range(self.PIECES):
                @pl.when(jnp.logical_and(i < n - 1, j <= i))
                def _():
                    self.copy(self.own, j, 0, s, i + 1).wait_send()

                @pl.when(jnp.logical_and(i > 0, j >= i))
                def _():
                    self.copy(self.own, j, 1, s, i - 1).wait_send()

        loop(n, one)


class LineSum:
    def __init__(self, i, n, part, land, send, recv, pieces):
        self.i, self.n, self.part, self.land, self.send, self.recv = i, n, part, land, send, recv
        self.pieces = pieces
        self.size = part.shape[1] // pieces

    def copy(self, src, d, right, s):
        i, n = self.i, self.n
        target = i + 1 if right else i - 1
        slot = d if right else jnp.where(d == target, n, d)
        here = rows_at(s, self.size)
        return remote(src.at[d, here], self.land.at[slot, here], self.send.at[d, s], self.recv.at[slot, s], target)

    def arrived(self, slot, s):
        here = rows_at(s, self.size)
        remote(self.part.at[0, here], self.land.at[slot, here], self.send.at[0, s], self.recv.at[slot, s],
               self.i).wait_recv()

    def launch(self, d):
        i, n = self.i, self.n

        @pl.when(jnp.logical_and(i == 0, d > 0))
        def _():
            loop(self.pieces, lambda s: self.copy(self.part, d, True, s).start())

        @pl.when(jnp.logical_and(i == n - 1, d < n - 1))
        def _():
            loop(self.pieces, lambda s: self.copy(self.part, d, False, s).start())

    def relay(self, right, left):
        i, n = self.i, self.n

        def move(d, to_right, s):
            self.arrived(d, s)
            here = rows_at(s, self.size)
            total = self.land[d, here, :].astype(F32) + self.part[d, here, :].astype(F32)
            self.land[d, here, :] = total.astype(BF)
            self.copy(self.land, d, to_right, s).start()

        def one(s):
            @pl.when(jnp.logical_and(i > 0, jnp.logical_and(right > i, right <= n - 1)))
            def _():
                move(right, True, s)

            @pl.when(jnp.logical_and(i < n - 1, jnp.logical_and(left >= 0, left < i)))
            def _():
                move(left, False, s)

        loop(self.pieces, one)

    def own(self, step):
        i, n = self.i, self.n

        def one(s):
            @pl.when(i > 0)
            def _():
                self.arrived(i, s)

            @pl.when(i < n - 1)
            def _():
                self.arrived(n, s)

            loop(self.size // RB, lambda b: step(s * (self.size // RB) + b))

        loop(self.pieces, one)

    def add(self, here, out):
        i, n = self.i, self.n
        out[...] = self.part[i, here, :].astype(F32)

        @pl.when(i > 0)
        def _():
            out[...] += self.land[i, here, :].astype(F32)

        @pl.when(i < n - 1)
        def _():
            out[...] += self.land[n, here, :].astype(F32)

    def finish(self):
        i, n = self.i, self.n

        def one(d):
            @pl.when(jnp.logical_and(i < n - 1, d > i))
            def _():
                loop(self.pieces, lambda s: self.copy(self.part, d, True, s).wait_send())

            @pl.when(jnp.logical_and(i > 0, d < i))
            def _():
                loop(self.pieces, lambda s: self.copy(self.part, d, False, s).wait_send())

        loop(n, one)


def tokens_kernel(n, m, piece, pack_ref, x_ref, a_ref, n_ref, vec_ref, buf, affine, own_sem, send, recv, v_send, v_recv):
    i, row = lax.axis_index("tensor"), lax.axis_index("dp")
    me, total = row * n + i, m * n
    size = x_ref.shape[0]
    greet_all(me, n, total)
    line = LineGather(i, n, x_ref, buf, send, recv)

    def vector(src, other):
        return pltpu.make_async_remote_copy(
            src_ref=pack_ref, dst_ref=vec_ref.at[src], send_sem=v_send.at[other], recv_sem=v_recv.at[src],
            device_id={"dp": other // n, "tensor": other % n}, device_id_type=MESH)

    loop(total - 1, lambda s: vector(me, (me + s + 1) % total).start())
    line.start()
    own_copy = pltpu.make_async_copy(x_ref, buf.at[i], own_sem)
    own_copy.start()
    vec_ref[me] = pack_ref[...]
    loop(total - 1, lambda s: vector((me + s + 1) % total, me).wait_recv())
    depth = affine.shape[1]
    group = LANES // piece
    for tile in range(depth // LANES):
        value = vec_ref[tile * group, 0:2, :].astype(F32)
        for g in range(1, group):
            value = value + vec_ref[tile * group + g, 0:2, :].astype(F32)
        affine[0:2, tile * LANES : (tile + 1) * LANES] = value
    own_copy.wait()

    def compute(j):
        def norm(b):
            normal, _ = norm_stats(buf[j, rows_at(b, RB), :].astype(F32))
            here = pl.ds(pl.multiple_of(j * size + b * RB, RB), RB)
            n_ref[here, :] = normal.astype(BF)
            a_ref[here, :] = (normal * affine[0:1, :] + affine[1:2, :]).astype(BF)

        loop(size // RB, norm)

    rounds(i, n, line, compute)
    line.finish()
    loop(total - 1, lambda s: vector(me, (me + s + 1) % total).wait_send())


def attend_kernel(n, pieces, a_hbm, wq_hbm, wo_hbm, x_ref, cot_ref, bias, out_bias, gain, shift, qkv_ref, o_ref, h_ref,
                  c_ref, cot_all, a_ref, wq_ref, w_ref, part, land, send, recv, s_send, s_recv, own_sem, a_sem, w_sem):
    i = lax.axis_index("tensor")
    size = x_ref.shape[0]
    loads = [pltpu.make_async_copy(a_hbm, a_ref, a_sem)]
    loads += [pltpu.make_async_copy(wq_hbm.at[t], wq_ref.at[t], w_sem.at[t]) for t in range(3)]
    loads += [pltpu.make_async_copy(wo_hbm, w_ref, w_sem.at[3])]
    for load in loads:
        load.start()
    heads = qkv_ref.shape[2] // HD
    depth = w_ref.shape[1]
    greet_neighbours(i, n)
    line = LineGather(i, n, cot_ref, cot_all, send, recv)
    line.start()
    own_copy = pltpu.make_async_copy(cot_ref, cot_all.at[i], own_sem)
    own_copy.start()

    loads[0].wait()
    block = 256
    for t in range(3):
        loads[1 + t].wait()

        def project(b):
            here = rows_at(b, block)
            value = jnp.dot(a_ref[here, :], wq_ref[t], preferred_element_type=F32)
            if t != 1:
                value = value + bias[t // 2 : t // 2 + 1, :]
            qkv_ref[t, here, :] = value.astype(BF)

        loop(LEN // block, project)

    def head(t):
        cols = pl.ds(pl.multiple_of(t * HD, HD), HD)
        for b in range(LEN // block):
            here, keys = slice(b * block, (b + 1) * block), (b + 1) * block
            s = lax.dot_general(qkv_ref[0, here, cols], qkv_ref[1, 0:keys, cols], NT,
                                preferred_element_type=F32) * HD ** (-0.5)
            query = lax.broadcasted_iota(jnp.int32, s.shape, 0) + b * block
            s = jnp.where(query >= lax.broadcasted_iota(jnp.int32, s.shape, 1), s, -1e30)
            e = jnp.exp(s - jnp.max(s, axis=-1, keepdims=True))
            prob = (e / jnp.sum(e, axis=-1, keepdims=True)).astype(BF)
            o_ref[here, cols] = jnp.dot(prob, qkv_ref[2, 0:keys, cols], preferred_element_type=F32).astype(BF)

    loop(heads, head)
    loads[4].wait()
    sums = LineSum(i, n, part, land, s_send, s_recv, pieces)
    tile = 512

    def project(t):
        d = jnp.where(i < n // 2, n - 1 - t, t)

        def columns(k):
            cols = rows_at(k, tile)
            part[d, :, cols] = jnp.dot(o_ref[rows_at(d, size), :], w_ref[:, cols], preferred_element_type=F32).astype(BF)

        loop(depth // tile, columns)
        sums.launch(d)

    loop(n, project)

    def round_of(r):
        line.step(r + 1)
        relays(sums, i, n, r + 1)

    loop(n - 1, round_of)

    def norm(b):
        here = rows_at(b, RB)
        sums.add(here, h_ref.at[here, :])
        rows = h_ref[here, :] + (x_ref[here, :].astype(F32) + out_bias[...])
        h_ref[here, :] = rows
        normal, _ = norm_stats(rows)
        c_ref[here, :] = (normal * gain[...] + shift[...]).astype(BF)

    sums.own(norm)
    own_copy.wait()
    line.finish()
    sums.finish()


def hidden_kernel(n, pieces, c_ref, h_ref, cot_hbm, up_hbm, down_hbm, up_bias, gain, c_hbm, g_hbm, du_hbm, mlp_hbm, dh_ref,
                  db_ref, vec_ref, upb_ref, c_all, g_all, du_all, cot_all, up, down, part, land, send, recv, s_send,
                  s_recv, w_sem, cot_sem, own_sem, c_sem, g_sem, du_sem, mlp, mlp_sem):
    i = lax.axis_index("tensor")
    size, depth = c_ref.shape
    units = up.shape[1]
    greet_neighbours(i, n)
    line = LineGather(i, n, c_ref, c_all, send, recv)
    line.start()
    own_copy = pltpu.make_async_copy(c_ref, c_all.at[i], own_sem)
    own_copy.start()
    up_copy = pltpu.make_async_copy(up_hbm, up, w_sem.at[0])
    up_copy.start()
    down_copy = pltpu.make_async_copy(down_hbm, down, w_sem.at[1])
    down_copy.start()
    cot_copy = pltpu.make_async_copy(cot_hbm, cot_all, cot_sem)
    cot_copy.start()
    upb_ref[...] = jnp.zeros_like(upb_ref)
    vec_ref[...] = jnp.zeros_like(vec_ref)
    own_copy.wait()
    up_copy.wait()
    down_copy.wait()
    cot_copy.wait()
    sums = LineSum(i, n, part, land, s_send, s_recv, pieces)
    tile = 256

    def out_copy(src, dst, sem, j):
        return pltpu.make_async_copy(src.at[j], dst.at[j], sem.at[j])

    def compute(j):
        def unit(k):
            cols = rows_at(k, tile)
            u = jnp.dot(c_all[j], up[:, cols], preferred_element_type=F32) + up_bias[0:1, cols]
            dg = lax.dot_general(cot_all[j], down[cols, :], NT, preferred_element_type=F32)
            half = 0.5 + 0.5 * lax.erf(u * (0.5 ** 0.5))
            g_all[j, :, cols] = (u * half).astype(BF)
            slope = half + u * (jnp.exp(u * u * -0.5) * 0.3989422804014327)
            du = (slope * dg).astype(BF)
            du_all[j, :, cols] = du
            upb_ref[0:1, cols] += jnp.sum(du.astype(F32), axis=0, keepdims=True)

        loop(units // tile, unit)

        def back(k):
            cols = rows_at(k, tile)
            part[j, :, cols] = lax.dot_general(du_all[j], up[cols, :], NT, preferred_element_type=F32).astype(BF)

        loop(depth // tile, back)
        sums.launch(j)
        out_copy(g_all, g_hbm, g_sem, j).start()
        out_copy(du_all, du_hbm, du_sem, j).start()
        out_copy(c_all, c_hbm, c_sem, j).start()

    rounds(i, n, line, compute)

    def forward(j):
        def columns(k):
            cols = rows_at(k, tile)
            mlp[j, :, cols] = jnp.dot(g_all[j], down[:, cols], preferred_element_type=F32).astype(BF)

        loop(depth // tile, columns)
        out_copy(mlp, mlp_hbm, mlp_sem, j).start()

    loop(n, forward)

    def relay(t):
        early = jnp.where(i < n // 2, 1, 0)
        sums.relay(t + 3 - early - i, 2 * n - 4 - i - t - early)

    loop(2 * n - 3, relay)

    def norm(b):
        here = rows_at(b, RB)
        sums.add(here, dh_ref.at[here, :])
        grad = dh_ref[here, :]
        normal, inverse = norm_stats(h_ref[here, :])
        vec_ref[0:1, :] += jnp.sum(grad * normal, axis=0, keepdims=True)
        vec_ref[1:2, :] += jnp.sum(grad, axis=0, keepdims=True)
        cot = cot_all[i, here, :].astype(F32)
        dh = cot + norm_back(grad, normal, inverse, gain[...])
        dh_ref[here, :] = dh
        db = dh.astype(BF)
        db_ref[here, :] = db
        vec_ref[2:3, :] += jnp.sum(db.astype(F32), axis=0, keepdims=True)
        vec_ref[3:4, :] += jnp.sum(cot, axis=0, keepdims=True)

    sums.own(norm)

    def done(j):
        out_copy(g_all, g_hbm, g_sem, j).wait()
        out_copy(du_all, du_hbm, du_sem, j).wait()
        out_copy(c_all, c_hbm, c_sem, j).wait()
        out_copy(mlp, mlp_hbm, mlp_sem, j).wait()

    loop(n, done)
    line.finish()
    sums.finish()


def attend_back(q_of, k_of, v_of, do_of, heads, put, dk, dv):
    block = 256
    factor = HD ** (-0.5)

    def head(t):
        dk[...] = jnp.zeros_like(dk)
        dv[...] = jnp.zeros_like(dv)
        for b in range(LEN // block):
            here, keys = slice(b * block, (b + 1) * block), slice(0, (b + 1) * block)
            q, k, v, do = q_of(here, t), k_of(keys, t), v_of(keys, t), do_of(here, t)
            s = lax.dot_general(q, k, NT, preferred_element_type=F32) * factor
            query = lax.broadcasted_iota(jnp.int32, s.shape, 0) + b * block
            s = jnp.where(query >= lax.broadcasted_iota(jnp.int32, s.shape, 1), s, -1e30)
            e = jnp.exp(s - jnp.max(s, axis=-1, keepdims=True))
            prob = e / jnp.sum(e, axis=-1, keepdims=True)
            dv[keys, :] += lax.dot_general(prob.astype(BF), do, TN, preferred_element_type=F32)
            dp = lax.dot_general(do, v, NT, preferred_element_type=F32)
            ds = (prob * (dp - jnp.sum(prob * dp, axis=-1, keepdims=True))).astype(BF)
            put(0, here, t, (jnp.dot(ds, k, preferred_element_type=F32) * factor).astype(BF))
            dk[keys, :] += lax.dot_general(ds, q, TN, preferred_element_type=F32)
        put(1, slice(0, LEN), t, (dk[...] * factor).astype(BF))
        put(2, slice(0, LEN), t, dv[...].astype(BF))

    loop(heads, head)


def partner(row, bit):
    return row + bit * (1 - 2 * ((row // bit) % 2))


class PlaneSum:
    def __init__(self, row, m, out, terms, land, halves, send, recv, h_send, h_recv):
        self.row, self.m, self.out, self.terms, self.land, self.halves = row, m, out, terms, land, halves
        self.send, self.recv, self.h_send, self.h_recv = send, recv, h_send, h_recv
        bits = [1 << k for k in range(1, m.bit_length() - 1)]
        self.plan = []
        for order in (bits, bits[::-1]):
            left, at, stages = [e for e in range(m) if e % 2 == 0], 0, []
            for bit in order:
                out = [e for e in left if e & bit]
                stages.append((bit, [(e, e ^ bit, at + k) for k, e in enumerate(out)]))
                left, at = [e for e in left if not e & bit], at + len(out)
            self.plan.append(stages)
        self.stages = len(bits)

    def owner(self, e):
        d = self.row
        for k in range(self.m.bit_length() - 1):
            if e & (1 << k):
                d = d + (partner(self.row, 1 << k) - self.row)
        return d

    def whole(self, e):
        return pltpu.make_async_remote_copy(
            src_ref=self.out.at[e // 2], dst_ref=self.land.at[e // 2], send_sem=self.send.at[e // 2],
            recv_sem=self.recv.at[e // 2], device_id={"dp": partner(self.row, 1)}, device_id_type=MESH)

    def half(self, h, bit, e, at):
        size = self.halves.shape[2]
        return pltpu.make_async_remote_copy(
            src_ref=self.terms.at[e // 2, pl.ds(h * size, size)], dst_ref=self.halves.at[h, at],
            send_sem=self.h_send.at[h, at], recv_sem=self.h_recv.at[h, at],
            device_id={"dp": partner(self.row, bit)}, device_id_type=MESH)

    def merge(self):
        for e in range(0, self.m, 2):
            self.whole(e + 1).wait_recv()

            def add(b):
                here = rows_at(b, RB)
                total = self.terms[e // 2, here, :].astype(F32) + self.land[e // 2, here, :].astype(F32)
                self.terms[e // 2, here, :] = total.astype(BF)

            loop(self.terms.shape[1] // RB, add)

    def push(self, stage):
        for h in range(2):
            bit, moves = self.plan[h][stage]
            for e, _, at in moves:
                self.half(h, bit, e, at).start()

    def take(self, stage, out=None):
        size = self.halves.shape[2]
        for h in range(2):
            bit, moves = self.plan[h][stage]
            for e, into, at in moves:
                self.half(h, bit, e, at).wait_recv()

                def add(b):
                    here, there = rows_at(b, RB), pl.ds(pl.multiple_of(h * size + b * RB, RB), RB)
                    total = self.terms[into // 2, there, :].astype(F32) + self.halves[h, at, here, :].astype(F32)
                    if out is None:
                        self.terms[into // 2, there, :] = total.astype(BF)
                    else:
                        out(there, total)

                loop(size // RB, add)

    def sent(self):
        for e in range(1, self.m, 2):
            self.whole(e).wait_send()

    def finish(self):
        for h in range(2):
            for bit, moves in self.plan[h]:
                for e, _, at in moves:
                    self.half(h, bit, e, at).wait_send()


class VectorSum:
    def __init__(self, me, count, device, vectors, piece, land, out, send, recv):
        self.me, self.count, self.device, self.vectors, self.piece = me, count, device, vectors, piece
        self.land, self.out, self.send, self.recv = land, out, send, recv

    def lanes(self, owner):
        size = self.land.shape[2]
        return pl.ds(pl.multiple_of(owner * self.piece // size * size, size), size)

    def copy(self, src, other):
        return pltpu.make_async_remote_copy(
            src_ref=self.vectors.at[:, self.lanes(other)], dst_ref=self.land.at[src], send_sem=self.send.at[other],
            recv_sem=self.recv.at[src], device_id=self.device(other), device_id_type=MESH)

    def start(self):
        loop(self.count - 1, lambda s: self.copy(self.me, (self.me + s + 1) % self.count).start())

    def finish(self):
        self.out[...] = self.vectors[:, self.lanes(self.me)]

        def take(s):
            src = (self.me + s + 1) % self.count
            self.copy(src, self.me).wait_recv()
            self.out[...] += self.land[src]

        loop(self.count - 1, take)
        loop(self.count - 1, lambda s: self.copy(self.me, (self.me + s + 1) % self.count).wait_send())


def greet_cross(i, n, row, m):
    barrier = pltpu.get_barrier_semaphore()

    @pl.when(i > 0)
    def _():
        pl.semaphore_signal(barrier, inc=1, device_id={"tensor": i - 1}, device_id_type=MESH)

    @pl.when(i < n - 1)
    def _():
        pl.semaphore_signal(barrier, inc=1, device_id={"tensor": i + 1}, device_id_type=MESH)

    bits = [1 << k for k in range(m.bit_length() - 1)]
    for bit in bits:
        pl.semaphore_signal(barrier, inc=1, device_id={"dp": partner(row, bit)}, device_id_type=MESH)
    pl.semaphore_wait(barrier, jnp.minimum(i, 1) + jnp.minimum(n - 1 - i, 1) + len(bits))


def relays(sums, i, n, r):
    sums.relay(n - 1 + i - r, r - (n - 1 - i))


def block_terms(plane, e, pairs):
    size = plane.terms.shape[1]
    cols = rows_at(plane.owner(e), size)
    for lhs, rhs, first in pairs:
        width = rhs.shape[1]
        tile = min(512, width)

        def columns(k):
            there = pl.ds(pl.multiple_of(first + k * tile, tile), tile)
            (plane.out if e % 2 else plane.terms)[e // 2, :, there] = lax.dot_general(
                lhs[:, cols], rhs[:, rows_at(k, tile)], TN, preferred_element_type=F32).astype(BF)

        loop(width // tile, columns)


def branch_kernel(n, m, pieces, db_ref, h_ref, down_bias, mlp_hbm, g_hbm, cot_hbm, c_hbm, du_hbm, qkv_hbm, wo_hbm,
                  db_all, lo_ref, down_ref, up_ref, dqkv_ref, lhs, rhs, wo, dk, dv, part, land, out, terms_a, land_a,
                  half_a, terms_b, land_b, half_b, acc, send, recv, s_send, s_recv, own_sem, part_sem, in_sem, qkv_sem,
                  db_sem, p_send, p_recv, h_send, h_recv):
    i, row = lax.axis_index("tensor"), lax.axis_index("dp")
    size = db_ref.shape[0]
    width = wo.shape[0]
    greet_cross(i, n, row, m)
    line = LineGather(i, n, db_ref, db_all, send, recv)
    line.start()
    part_copy = pltpu.make_async_copy(mlp_hbm, part, part_sem)
    part_copy.start()
    own_copy = pltpu.make_async_copy(db_ref, db_all.at[i], own_sem)
    own_copy.start()

    def load(left, right):
        return [pltpu.make_async_copy(left, lhs, in_sem.at[0]), pltpu.make_async_copy(right, rhs, in_sem.at[1])]

    loads = load(cot_hbm, g_hbm)
    for copy in loads:
        copy.start()
    wo_copy = pltpu.make_async_copy(wo_hbm, wo, in_sem.at[2])
    wo_copy.start()
    sums = LineSum(i, n, part, land, s_send, s_recv, pieces)
    part_copy.wait()
    loop(n, lambda t: sums.launch(jnp.where(i < n // 2, n - 1 - t, t)))
    planes = [PlaneSum(row, m, out, terms_a, land_a, half_a, p_send.at[0], p_recv.at[0], h_send.at[0], h_recv.at[0]),
              PlaneSum(row, m, out, terms_b, land_b, half_b, p_send.at[1], p_recv.at[1], h_send.at[1], h_recv.at[1])]
    first, second = planes
    for copy in loads:
        copy.wait()
    left, right = lhs.at[:, 0 : lhs.shape[1]], rhs.at[:, 0 : down_ref.shape[1]]
    for e in range(1, m, 2):
        block_terms(first, e, [(left, right, 0)])
        first.whole(e).start()
    for e in range(m - 2, -1, -2):
        block_terms(first, e, [(left, right, 0)])
    loads = load(c_hbm, du_hbm)
    for copy in loads:
        copy.start()
    first.merge()
    first.push(0)
    first.sent()
    for copy in loads:
        copy.wait()
    for e in range(1, m, 2):
        block_terms(second, e, [(left, right, 0)])
        second.whole(e).start()

    line.step(1)
    for e in range(m - 2, -1, -2):
        block_terms(second, e, [(left, right, 0)])
    qkv_copies = [pltpu.make_async_copy(qkv_hbm.at[p], rhs.at[:, p * width : (p + 1) * width], qkv_sem.at[p])
                  for p in range(3)]
    for copy in qkv_copies:
        copy.start()
    second.merge()
    second.push(0)
    own_copy.wait()
    wo_copy.wait()

    def mixture_back(j):
        here = rows_at(j, size)
        copy = pltpu.make_async_copy(db_all.at[j], lhs.at[here], db_sem.at[j])
        copy.start()
        copy.wait()
        rhs[here, 3 * width : 4 * width] = lax.dot_general(
            lhs[here, :], wo[...], NT, preferred_element_type=F32).astype(BF)

    def round_back(r):
        def side(s):
            j = jnp.where(s == 0, i - r, i + r)

            @pl.when(jnp.logical_and(j >= 0, j <= n - 1))
            def _():
                mixture_back(j)

        loop(2, side)

    def keep(ref):
        def put(here, total):
            ref[here, :] = total

        return put

    def advance(plane, stage, ref):
        if stage < plane.stages - 1:
            plane.take(stage)
            plane.push(stage + 1)
        else:
            plane.take(stage, keep(ref))

    mixture_back(i)
    round_back(1)
    advance(first, 0, down_ref)
    for r in range(2, n):
        line.step(r)
        relays(sums, i, n, r - 1)
        round_back(r)
        if r == 2:
            advance(second, 0, up_ref)
    if n == 2:
        advance(second, 0, up_ref)
    relays(sums, i, n, n - 1)
    for copy in qkv_copies:
        copy.wait()

    def column(p):
        def get(here, t):
            return rhs[here, pl.ds(pl.multiple_of(p * width + t * HD, HD), HD)]

        return get

    def put(p, here, t, value):
        dqkv_ref[p, here, pl.ds(pl.multiple_of(t * HD, HD), HD)] = value

    attend_back(column(0), column(1), column(2), column(3), width // HD, put, dk, dv)
    for stage in range(1, first.stages):
        advance(first, stage, down_ref)
        advance(second, stage, up_ref)

    def output(b):
        here = rows_at(b, RB)
        sums.add(here, acc)
        lo_ref[here, :] = (h_ref[here, :] + (acc[...] + down_bias[...])).astype(BF)

    sums.own(output)
    line.finish()
    sums.finish()
    second.sent()
    for plane in planes:
        plane.finish()


def input_kernel(n, m, pieces, widths, dqkv_ref, wq_hbm, x_ref, dh_ref, gain, early_ref, up_ref, a_hbm, db_hbm, o_hbm,
                 n_hbm, gt_ref, gqkv_ref, gout_ref, early_out, late_out, up_out, qv_out, vec_ref, qv_ref, wq, a_ref, db_ref,
                 o_ref, n_ref, part, land, out_p, terms, land_p, half_p, acc, early_land, late_land, up_land, qv_land, s_send,
                 s_recv, in_sem, p_send, p_recv, h_send, h_recv, e_send, e_recv, l_send, l_recv, u_send, u_recv, q_send,
                 q_recv):
    i, row = lax.axis_index("tensor"), lax.axis_index("dp")
    me, total_devices = row * n + i, m * n
    size = x_ref.shape[0]
    width = dqkv_ref.shape[2]
    piece, up_piece, qv_piece = widths
    depth = part.shape[2]
    loads = [pltpu.make_async_copy(wq_hbm, wq, in_sem.at[0]), pltpu.make_async_copy(a_hbm, a_ref, in_sem.at[1]),
             pltpu.make_async_copy(db_hbm, db_ref, in_sem.at[2]), pltpu.make_async_copy(o_hbm, o_ref, in_sem.at[3]),
             pltpu.make_async_copy(n_hbm, n_ref, in_sem.at[4])]
    for copy in loads:
        copy.start()
    greet_all(me, n, total_devices)
    every = [VectorSum(me, total_devices, lambda g: {"dp": g // n, "tensor": g % n}, early_ref, piece, early_land, early_out,
                       e_send, e_recv),
             VectorSum(me, total_devices, lambda g: {"dp": g // n, "tensor": g % n}, vec_ref, piece, late_land, late_out,
                       l_send, l_recv)]
    column = [VectorSum(row, m, lambda g: {"dp": g}, up_ref, up_piece, up_land, up_out, u_send, u_recv),
              VectorSum(row, m, lambda g: {"dp": g}, qv_ref, qv_piece, qv_land, qv_out, q_send, q_recv)]
    every[0].start()
    column[0].start()
    sums = LineSum(i, n, part, land, s_send, s_recv, pieces)
    vec_ref[...] = jnp.zeros_like(vec_ref)
    qv_ref[...] = jnp.zeros_like(qv_ref)
    loads[0].wait()
    loads[4].wait()
    tile = 512

    def term(t):
        d = jnp.where(i < n // 2, n - 1 - t, t)
        here = rows_at(d, size)

        def columns(k):
            cols = rows_at(k, tile)
            total = lax.dot_general(dqkv_ref[0, here, :], wq[0, cols, :], NT, preferred_element_type=F32)
            for p in range(1, 3):
                total += lax.dot_general(dqkv_ref[p, here, :], wq[p, cols, :], NT, preferred_element_type=F32)
            part[d, :, cols] = total.astype(BF)
            vec_ref[0:1, cols] += jnp.sum(total * n_ref[here, cols].astype(F32), axis=0, keepdims=True)
            vec_ref[1:2, cols] += jnp.sum(total, axis=0, keepdims=True)

        loop(depth // tile, columns)
        sums.launch(d)
        for p in range(2):
            qv_ref[p : p + 1, :] += jnp.sum(dqkv_ref[2 * p, here, :].astype(F32), axis=0, keepdims=True)

    loop(n, term)
    column[1].start()
    every[1].start()
    for copy in loads[1:4]:
        copy.wait()
    plane = PlaneSum(row, m, out_p, terms, land_p, half_p, p_send, p_recv, h_send, h_recv)
    pairs = [(a_ref, dqkv_ref.at[p], p * width) for p in range(3)] + [(db_ref, o_ref, 3 * width)]
    for e in range(1, m, 2):
        block_terms(plane, e, pairs)
        plane.whole(e).start()
    for e in range(m - 2, -1, -2):
        block_terms(plane, e, pairs)
    plane.merge()
    plane.push(0)

    def out(here, total):
        for p in range(3):
            gqkv_ref[p, here, :] = total[:, p * width : (p + 1) * width]
        gout_ref[here, :] = total[:, 3 * width :]

    stage = 0
    for r in range(1, n):
        relays(sums, i, n, r)
        if r > 1 and stage < plane.stages:
            if stage < plane.stages - 1:
                plane.take(stage)
                plane.push(stage + 1)
            else:
                plane.take(stage, out)
            stage += 1

    def norm(b):
        here = rows_at(b, RB)
        sums.add(here, acc)
        grad = acc[...]
        normal, inverse = norm_stats(x_ref[here, :].astype(F32))
        gt_ref[here, :] = (dh_ref[here, :] + norm_back(grad, normal, inverse, gain[...])).astype(BF)

    while stage < plane.stages:
        if stage < plane.stages - 1:
            plane.take(stage)
            plane.push(stage + 1)
        else:
            plane.take(stage, out)
        stage += 1
    for group in (every[0], column[0], column[1], every[1]):
        group.finish()
    sums.own(norm)
    sums.finish()
    plane.sent()
    plane.finish()


def params(collective=None):
    if collective is None:
        return pltpu.CompilerParams(vmem_limit_bytes=BIG)
    return pltpu.CompilerParams(vmem_limit_bytes=BIG, collective_id=collective, has_side_effects=True)


def shape(dims, dtype):
    return jax.ShapeDtypeStruct(dims, dtype)


def body(tokens, cotangent, ln1_gain, ln1_bias, qkv_weight, qv_bias, out_weight, out_bias, ln2_gain, ln2_bias,
         up_weight, up_bias, down_weight, down_bias):
    n = lax.axis_size("tensor")
    m = lax.axis_size("dp")
    i, row = lax.axis_index("tensor"), lax.axis_index("dp")
    size, depth = tokens.shape
    width = qkv_weight.shape[2]
    units = up_weight.shape[1]
    piece, qv_piece, up_piece = ln1_gain.shape[0], qv_bias.shape[1], up_bias.shape[0]
    total = m * n

    def lane_rows(value, index):
        count = value.shape[-1]
        if count >= LANES:
            return value.reshape(-1, LANES)
        places = LANES // count
        spread = jnp.tile(value.reshape(-1, count), (1, places))
        return jnp.where((jnp.arange(LANES) // count)[None] == index % places, spread, 0)

    me = row * n + i
    whole = jnp.stack([ln1_gain, ln1_bias, out_bias, ln2_gain, ln2_bias, down_bias])
    pack = jnp.concatenate([lane_rows(whole, me), lane_rows(qv_bias, row), lane_rows(up_bias, row)])
    pack = jnp.pad(pack, ((0, -pack.shape[0] % 16), (0, 0)))
    lanes_up = 8 + max(up_piece // LANES, 1)

    w_qkv = lax.all_gather(qkv_weight, "dp", axis=1, tiled=True)
    w_out = lax.all_gather(out_weight, "dp", axis=1, tiled=True)
    w_up = lax.all_gather(up_weight, "dp", axis=0, tiled=True)
    w_down = lax.all_gather(down_weight, "dp", axis=1, tiled=True)

    dma = pltpu.SemaphoreType.DMA
    attn_in, normal_one, vecs = pl.pallas_call(
        functools.partial(tokens_kernel, n, m, piece),
        out_shape=(shape((LEN, depth), BF), shape((LEN, depth), BF), shape((total,) + pack.shape, BF)),
        in_specs=[VM, VM], out_specs=(VM, VM, VM),
        scratch_shapes=[pltpu.VMEM((n, size, depth), BF), pltpu.VMEM((8, depth), F32), dma, dma((2, n, LineGather.PIECES)), dma((n, LineGather.PIECES)),
                        dma((total,)), dma((total,))],
        compiler_params=params(0), name="gather_tokens",
    )(pack, tokens)
    vecs = vecs.astype(F32)

    def whole_rows(block, count):
        if count < LANES:
            block = block.reshape(-1, LANES // count, *block.shape[1:]).sum(axis=1)
        return block

    vectors = whole_rows(vecs[:, 0:6], piece).transpose(1, 0, 2).reshape(6, 1, depth)
    gain_one, shift_one, bias_out, gain_two, shift_two, bias_down = [vectors[j] for j in range(6)]
    mine = lax.dynamic_index_in_dim(vecs.reshape(m, n, -1, LANES), i, 1, keepdims=False)
    bias_qv = whole_rows(mine[:, 6:8], qv_piece).transpose(1, 0, 2).reshape(2, width)
    bias_up = whole_rows(mine[:, 8:lanes_up], up_piece).reshape(1, units)

    pieces = 2
    sums = [pltpu.VMEM((n, size, depth), BF), pltpu.VMEM((n + 1, size, depth), BF)]
    qkv, mixture, residual, mlp_own, cot_all = pl.pallas_call(
        functools.partial(attend_kernel, n, pieces),
        out_shape=(shape((3, LEN, width), BF), shape((LEN, width), BF), shape((size, depth), F32),
                   shape((size, depth), BF), shape((n, size, depth), BF)),
        in_specs=[ANY] * 3 + [VM] * 6, out_specs=(VM, VM, VM, VM, ANY),
        scratch_shapes=[pltpu.VMEM((LEN, depth), BF), pltpu.VMEM((3, depth, width), BF), pltpu.VMEM((width, depth), BF)] +
                       sums + [dma((2, n, LineGather.PIECES)), dma((n, LineGather.PIECES)), dma((n, pieces)), dma((n + 1, pieces)), dma, dma, dma((4,))],
        compiler_params=params(1), name="attend",
    )(attn_in, w_qkv, w_out, tokens, cotangent, bias_qv, bias_out, gain_two, shift_two)

    pieces = 4
    mlp_in, hidden, grad_pre, mlp_part, grad_resid, branch_cot, vec_two, grad_up_b = pl.pallas_call(
        functools.partial(hidden_kernel, n, pieces),
        out_shape=(shape((n, size, depth), BF), shape((n, size, units), BF), shape((n, size, units), BF),
                   shape((n, size, depth), BF), shape((size, depth), F32), shape((size, depth), BF),
                   shape((8, depth), F32), shape((8, units), F32)),
        in_specs=[VM, VM, ANY, ANY, ANY, VM, VM], out_specs=(ANY, ANY, ANY, ANY, VM, VM, VM, VM),
        scratch_shapes=[pltpu.VMEM((n, size, depth), BF), pltpu.VMEM((n, size, units), BF),
                        pltpu.VMEM((n, size, units), BF), pltpu.VMEM((n, size, depth), BF),
                        pltpu.VMEM((depth, units), BF), pltpu.VMEM((units, depth), BF)] + sums +
                       [dma((2, n, LineGather.PIECES)), dma((n, LineGather.PIECES)), dma((n, pieces)), dma((n + 1, pieces)), dma((2,)), dma, dma,
                        dma((n,)), dma((n,)), dma((n,)), pltpu.VMEM((n, size, depth), BF), dma((n,))],
        compiler_params=params(2), name="hidden",
    )(mlp_own, residual, cot_all, w_up, w_down, bias_up, gain_two)
    mlp_in, hidden, grad_pre, cot_rows = [v.reshape(LEN, -1) for v in (mlp_in, hidden, grad_pre, cot_all)]

    def plane_scratch(columns):
        rows = depth // m
        return [pltpu.VMEM((m // 2, rows, columns), BF), pltpu.VMEM((m // 2, rows, columns), BF),
                pltpu.VMEM((2, m // 2 - 1, rows // 2, columns), BF)]

    pieces = 2
    sum_sems = [dma((n, pieces)), dma((n + 1, pieces))]
    attn_cot, layer_out, grad_down_w, grad_up_w, grad_qkv = pl.pallas_call(
        functools.partial(branch_kernel, n, m, pieces),
        out_shape=(shape((n, size, depth), BF), shape((size, depth), BF), shape((depth // m, units), F32),
                   shape((depth // m, units), F32), shape((3, LEN, width), BF)),
        in_specs=[VM] * 3 + [ANY] * 7, out_specs=(ANY, VM, VM, VM, VM),
        scratch_shapes=[pltpu.VMEM((LEN, depth), BF), pltpu.VMEM((LEN, units), BF), pltpu.VMEM((width, depth), BF),
                        pltpu.VMEM((LEN, HD), F32), pltpu.VMEM((LEN, HD), F32)] + sums +
                       [pltpu.VMEM((m // 2, depth // m, units), BF)] + plane_scratch(units) * 2 +
                       [pltpu.VMEM((RB, depth), F32), dma((2, n, LineGather.PIECES)), dma((n, LineGather.PIECES))] + sum_sems +
                       [dma, dma, dma((3,)), dma((3,)), dma((n,)), dma((2, m // 2)), dma((2, m // 2)),
                        dma((2, 2, m // 2 - 1)), dma((2, 2, m // 2 - 1))],
        compiler_params=params(4), name="branch",
    )(branch_cot, residual, bias_down, mlp_part, hidden, cot_rows, mlp_in, grad_pre, qkv, w_out)
    attn_cot = attn_cot.reshape(LEN, depth)

    tiles = [max(v, LANES) for v in (piece, up_piece, qv_piece)]
    grad_tokens, grad_qkv_w, grad_out_w, early, late, grad_up_b, grad_qv_b = pl.pallas_call(
        functools.partial(input_kernel, n, m, pieces, (piece, up_piece, qv_piece)),
        out_shape=(shape((size, depth), BF), shape((3, depth // m, width), F32), shape((depth // m, width), F32),
                   shape((8, tiles[0]), F32), shape((8, tiles[0]), F32), shape((8, tiles[1]), F32),
                   shape((8, tiles[2]), F32)),
        in_specs=[VM, ANY, VM, VM, VM, VM, VM, ANY, ANY, ANY, ANY], out_specs=(VM,) * 7,
        scratch_shapes=[pltpu.VMEM((8, depth), F32), pltpu.VMEM((8, width), F32),
                        pltpu.VMEM((3, depth, width), BF), pltpu.VMEM((LEN, depth), BF), pltpu.VMEM((LEN, depth), BF),
                        pltpu.VMEM((LEN, width), BF), pltpu.VMEM((LEN, depth), BF)] + sums +
                       [pltpu.VMEM((m // 2, depth // m, 4 * width), BF)] +
                       plane_scratch(4 * width) +
                       [pltpu.VMEM((RB, depth), F32), pltpu.VMEM((total, 8, tiles[0]), F32),
                        pltpu.VMEM((total, 8, tiles[0]), F32), pltpu.VMEM((m, 8, tiles[1]), F32),
                        pltpu.VMEM((m, 8, tiles[2]), F32)] + sum_sems +
                       [dma((5,)), dma((m // 2,)), dma((m // 2,)), dma((2, m // 2 - 1)), dma((2, m // 2 - 1))] +
                       [dma((total,))] * 4 + [dma((m,))] * 4,
        compiler_params=params(5), name="input",
    )(grad_qkv, w_qkv, tokens, grad_resid, gain_one, vec_two, grad_up_b, attn_in, attn_cot, mixture, normal_one)
    grad_down_w, grad_out_w = grad_down_w.T, grad_out_w.T

    def own_lanes(block, index, count):
        return lax.dynamic_slice_in_dim(block, index * count % block.shape[1], count, axis=1)

    early, late = own_lanes(early, me, piece), own_lanes(late, me, piece)
    vectors = [late[0], late[1], early[2], early[0], early[1], early[3]]
    grad_qv_b = own_lanes(grad_qv_b, row, qv_piece)[:2]
    grad_up_b = own_lanes(grad_up_b, row, up_piece)[0]
    return (layer_out, grad_tokens, vectors[0], vectors[1], grad_qkv_w, grad_qv_b, grad_out_w, vectors[2],
            vectors[3], vectors[4], grad_up_w, grad_up_b, grad_down_w, vectors[5])


def solution(mesh):
    vector, matrix = P(("dp", "tensor")), P(("dp", "tensor"), None)
    in_specs = (matrix, matrix, vector, vector, P(None, "dp", "tensor"), P(None, ("tensor", "dp")), P("tensor", "dp"),
                vector, vector, vector, P("dp", "tensor"), P(("tensor", "dp")), P("tensor", "dp"), vector)
    out_specs = (matrix, matrix, vector, vector, P(None, "dp", "tensor"), P(None, ("tensor", "dp")),
                 P("tensor", "dp"), vector, vector, vector, P("dp", "tensor"), P(("tensor", "dp")), P("tensor", "dp"),
                 vector)
    return jax.shard_map(body, mesh=mesh, in_specs=in_specs, out_specs=out_specs, check_vma=False)
```

```python
import functools

import jax
import jax.numpy as jnp
from jax import lax
from jax.experimental import pallas as pl
from jax.experimental.pallas import tpu as pltpu
from jax.sharding import PartitionSpec as P

HD = 128
LEN = 1024
LANES = 128
EPS = 1e-05
BF = jnp.bfloat16
F32 = jnp.float32
MESH = pl.DeviceIdType.MESH
ANY = pl.BlockSpec(memory_space=pl.ANY)
VM = pl.BlockSpec(memory_space=pltpu.VMEM)
NT = (((1,), (1,)), ((), ()))
TN = (((0,), (0,)), ((), ()))
BIG = 64 * 1024 * 1024 - 65536
RB = 32


def norm_stats(rows):
    mean = jnp.mean(rows, axis=-1, keepdims=True)
    centred = rows - mean
    variance = jnp.mean(centred * centred, axis=-1, keepdims=True)
    inverse = lax.rsqrt(variance + EPS)
    return centred * inverse, inverse


def norm_back(grad_rows, normal_rows, inverse, gain):
    scaled = grad_rows * gain
    first = jnp.mean(scaled, axis=-1, keepdims=True)
    second = jnp.mean(scaled * normal_rows, axis=-1, keepdims=True)
    return inverse * (scaled - first - normal_rows * second)


def loop(count, step):
    def run(i, carry):
        step(i)
        return carry

    lax.fori_loop(0, count, run, 0)


def rows_at(j, size):
    return pl.ds(pl.multiple_of(j * size, size), size)


def remote(src, dst, send, recv, target):
    return pltpu.make_async_remote_copy(src_ref=src, dst_ref=dst, send_sem=send, recv_sem=recv,
                                        device_id={"tensor": target}, device_id_type=MESH)


def greet_neighbours(i, n):
    barrier = pltpu.get_barrier_semaphore()

    @pl.when(i > 0)
    def _():
        pl.semaphore_signal(barrier, inc=1, device_id={"tensor": i - 1}, device_id_type=MESH)

    @pl.when(i < n - 1)
    def _():
        pl.semaphore_signal(barrier, inc=1, device_id={"tensor": i + 1}, device_id_type=MESH)

    pl.semaphore_wait(barrier, jnp.minimum(i, 1) + jnp.minimum(n - 1 - i, 1))


def greet_all(me, n, total):
    barrier = pltpu.get_barrier_semaphore()

    def greet(s):
        other = (me + s + 1) % total
        pl.semaphore_signal(barrier, inc=1, device_id={"dp": other // n, "tensor": other % n}, device_id_type=MESH)

    loop(total - 1, greet)
    pl.semaphore_wait(barrier, total - 1)


def rounds(i, n, line, compute):
    def round_of(r):
        @pl.when(r > 0)
        def _():
            line.step(r)

        def side(s):
            j = jnp.where(s == 0, i - r, i + r)

            @pl.when(jnp.logical_and(jnp.logical_and(j >= 0, j <= n - 1), s * r == s * jnp.maximum(r, 1)))
            def _():
                compute(j)

        loop(2, side)

    loop(n, round_of)


class LineGather:
    PIECES = 2

    def __init__(self, i, n, own, buf, send, recv):
        self.i, self.n, self.own, self.buf, self.send, self.recv = i, n, own, buf, send, recv
        self.size = own.shape[0] // self.PIECES

    def copy(self, src, j, side, s, target):
        here = pl.ds(s * self.size, self.size)
        return remote(src.at[here], self.buf.at[j, here], self.send.at[side, j, s], self.recv.at[j, s], target)

    def start(self):
        i, n = self.i, self.n
        for s in range(self.PIECES):
            @pl.when(i < n - 1)
            def _():
                self.copy(self.own, i, 0, s, i + 1).start()

            @pl.when(i > 0)
            def _():
                self.copy(self.own, i, 1, s, i - 1).start()

    def step(self, r):
        i, n = self.i, self.n
        for s in range(self.PIECES):
            @pl.when(i - r >= 0)
            def _():
                self.copy(self.own, i - r, 0, s, i).wait_recv()

                @pl.when(i < n - 1)
                def _():
                    self.copy(self.buf.at[i - r], i - r, 0, s, i + 1).start()

            @pl.when(i + r <= n - 1)
            def _():
                self.copy(self.own, i + r, 1, s, i).wait_recv()

                @pl.when(i > 0)
                def _():
                    self.copy(self.buf.at[i + r], i + r, 1, s, i - 1).start()

    def finish(self):
        i, n = self.i, self.n

        def one(j):
            for s in range(self.PIECES):
                @pl.when(jnp.logical_and(i < n - 1, j <= i))
                def _():
                    self.copy(self.own, j, 0, s, i + 1).wait_send()

                @pl.when(jnp.logical_and(i > 0, j >= i))
                def _():
                    self.copy(self.own, j, 1, s, i - 1).wait_send()

        loop(n, one)


class LineSum:
    def __init__(self, i, n, part, land, send, recv, pieces):
        self.i, self.n, self.part, self.land, self.send, self.recv = i, n, part, land, send, recv
        self.pieces = pieces
        self.size = part.shape[1] // pieces

    def copy(self, src, d, right, s):
        i, n = self.i, self.n
        target = i + 1 if right else i - 1
        slot = d if right else jnp.where(d == target, n, d)
        here = rows_at(s, self.size)
        return remote(src.at[d, here], self.land.at[slot, here], self.send.at[d, s], self.recv.at[slot, s], target)

    def arrived(self, slot, s):
        here = rows_at(s, self.size)
        remote(self.part.at[0, here], self.land.at[slot, here], self.send.at[0, s], self.recv.at[slot, s],
               self.i).wait_recv()

    def launch(self, d):
        i, n = self.i, self.n

        @pl.when(jnp.logical_and(i == 0, d > 0))
        def _():
            loop(self.pieces, lambda s: self.copy(self.part, d, True, s).start())

        @pl.when(jnp.logical_and(i == n - 1, d < n - 1))
        def _():
            loop(self.pieces, lambda s: self.copy(self.part, d, False, s).start())

    def relay(self, right, left):
        i, n = self.i, self.n

        def move(d, to_right, s):
            self.arrived(d, s)
            here = rows_at(s, self.size)
            total = self.land[d, here, :].astype(F32) + self.part[d, here, :].astype(F32)
            self.land[d, here, :] = total.astype(BF)
            self.copy(self.land, d, to_right, s).start()

        first = jnp.where(i < n // 2, 0, 1)

        def one(s):
            turn, s = (s + first) % 2, s // 2

            @pl.when(jnp.logical_and(turn == 0, jnp.logical_and(i > 0, jnp.logical_and(right > i, right <= n - 1))))
            def _():
                move(right, True, s)

            @pl.when(jnp.logical_and(turn == 1, jnp.logical_and(i < n - 1, jnp.logical_and(left >= 0, left < i))))
            def _():
                move(left, False, s)

        loop(2 * self.pieces, one)

    def own(self, step):
        i, n = self.i, self.n

        def one(s):
            @pl.when(i > 0)
            def _():
                self.arrived(i, s)

            @pl.when(i < n - 1)
            def _():
                self.arrived(n, s)

            loop(self.size // RB, lambda b: step(s * (self.size // RB) + b))

        loop(self.pieces, one)

    def add(self, here, out):
        i, n = self.i, self.n
        out[...] = self.part[i, here, :].astype(F32)

        @pl.when(i > 0)
        def _():
            out[...] += self.land[i, here, :].astype(F32)

        @pl.when(i < n - 1)
        def _():
            out[...] += self.land[n, here, :].astype(F32)

    def finish(self):
        i, n = self.i, self.n

        def one(d):
            @pl.when(jnp.logical_and(i < n - 1, d > i))
            def _():
                loop(self.pieces, lambda s: self.copy(self.part, d, True, s).wait_send())

            @pl.when(jnp.logical_and(i > 0, d < i))
            def _():
                loop(self.pieces, lambda s: self.copy(self.part, d, False, s).wait_send())

        loop(n, one)


def tokens_kernel(n, m, piece, pack_ref, x_ref, a_hbm, n_hbm, vec_ref, buf, affine, a_ref, n_ref, out_sem, own_sem, send, recv, v_send, v_recv):
    i, row = lax.axis_index("tensor"), lax.axis_index("dp")
    me, total = row * n + i, m * n
    size = x_ref.shape[0]
    greet_all(me, n, total)
    line = LineGather(i, n, x_ref, buf, send, recv)

    def vector(src, other):
        return pltpu.make_async_remote_copy(
            src_ref=pack_ref, dst_ref=vec_ref.at[src], send_sem=v_send.at[other], recv_sem=v_recv.at[src],
            device_id={"dp": other // n, "tensor": other % n}, device_id_type=MESH)

    loop(total - 1, lambda s: vector(me, (me + s + 1) % total).start())
    line.start()
    own_copy = pltpu.make_async_copy(x_ref, buf.at[i], own_sem)
    own_copy.start()
    vec_ref[me] = pack_ref[...]
    loop(total - 1, lambda s: vector((me + s + 1) % total, me).wait_recv())
    depth = affine.shape[1]
    group = LANES // piece
    for tile in range(depth // LANES):
        value = vec_ref[tile * group, 0:2, :].astype(F32)
        for g in range(1, group):
            value = value + vec_ref[tile * group + g, 0:2, :].astype(F32)
        affine[0:2, tile * LANES : (tile + 1) * LANES] = value
    own_copy.wait()

    def compute(j):
        def norm(b):
            normal, _ = norm_stats(buf[j, rows_at(b, RB), :].astype(F32))
            here = pl.ds(pl.multiple_of(j * size + b * RB, RB), RB)
            n_ref[here, :] = normal.astype(BF)
            a_ref[here, :] = (normal * affine[0:1, :] + affine[1:2, :]).astype(BF)

        loop(size // RB, norm)
        for copy in leave(j):
            copy.start()

    def leave(j):
        here = rows_at(j, size)
        return [pltpu.make_async_copy(a_ref.at[here], a_hbm.at[here], out_sem.at[0, j]),
                pltpu.make_async_copy(n_ref.at[here], n_hbm.at[here], out_sem.at[1, j])]

    def left(j):
        for copy in leave(j):
            copy.wait()

    rounds(i, n, line, compute)
    line.finish()
    loop(n, left)
    loop(total - 1, lambda s: vector(me, (me + s + 1) % total).wait_send())


def attend_kernel(n, pieces, a_hbm, wq_hbm, wo_hbm, x_ref, cot_ref, bias, out_bias, gain, shift, qkv_hbm, o_hbm, h_ref,
                  c_ref, cot_all, qkv_ref, o_ref, out_sem, a_ref, wq_ref, w_ref, part, land, send, recv, s_send, s_recv, own_sem, a_sem, w_sem):
    i = lax.axis_index("tensor")
    size = x_ref.shape[0]
    loads = [pltpu.make_async_copy(a_hbm, a_ref, a_sem)]
    loads += [pltpu.make_async_copy(wq_hbm.at[t], wq_ref.at[t], w_sem.at[t]) for t in range(3)]
    loads += [pltpu.make_async_copy(wo_hbm, w_ref, w_sem.at[3])]
    for load in loads:
        load.start()
    heads = qkv_ref.shape[2] // HD
    depth = w_ref.shape[1]
    greet_neighbours(i, n)
    line = LineGather(i, n, cot_ref, cot_all, send, recv)
    line.start()
    own_copy = pltpu.make_async_copy(cot_ref, cot_all.at[i], own_sem)
    own_copy.start()

    loads[0].wait()
    block = 256
    for t in range(3):
        loads[1 + t].wait()

        def project(b):
            here = rows_at(b, block)
            value = jnp.dot(a_ref[here, :], wq_ref[t], preferred_element_type=F32)
            if t != 1:
                value = value + bias[t // 2 : t // 2 + 1, :]
            qkv_ref[t, here, :] = value.astype(BF)

        loop(LEN // block, project)

    def head(t):
        cols = pl.ds(pl.multiple_of(t * HD, HD), HD)
        for b in range(LEN // block):
            here, keys = slice(b * block, (b + 1) * block), (b + 1) * block
            s = lax.dot_general(qkv_ref[0, here, cols], qkv_ref[1, 0:keys, cols], NT,
                                preferred_element_type=F32) * HD ** (-0.5)
            query = lax.broadcasted_iota(jnp.int32, s.shape, 0) + b * block
            s = jnp.where(query >= lax.broadcasted_iota(jnp.int32, s.shape, 1), s, -1e30)
            e = jnp.exp(s - jnp.max(s, axis=-1, keepdims=True))
            prob = (e / jnp.sum(e, axis=-1, keepdims=True)).astype(BF)
            o_ref[here, cols] = jnp.dot(prob, qkv_ref[2, 0:keys, cols], preferred_element_type=F32).astype(BF)

    loop(heads, head)
    leave = [pltpu.make_async_copy(qkv_ref, qkv_hbm, out_sem.at[0]), pltpu.make_async_copy(o_ref, o_hbm, out_sem.at[1])]
    for copy in leave:
        copy.start()
    loads[4].wait()
    sums = LineSum(i, n, part, land, s_send, s_recv, pieces)
    tile = 512

    def project(t):
        d = jnp.where(i < n // 2, n - 1 - t, t)

        def columns(k):
            cols = rows_at(k, tile)
            part[d, :, cols] = jnp.dot(o_ref[rows_at(d, size), :], w_ref[:, cols], preferred_element_type=F32).astype(BF)

        loop(depth // tile, columns)
        sums.launch(d)

    loop(n, project)

    def round_of(r):
        line.step(r + 1)
        relays(sums, i, n, r + 1)

    loop(n - 1, round_of)

    def norm(b):
        here = rows_at(b, RB)
        sums.add(here, h_ref.at[here, :])
        rows = h_ref[here, :] + (x_ref[here, :].astype(F32) + out_bias[...])
        h_ref[here, :] = rows
        normal, _ = norm_stats(rows)
        c_ref[here, :] = (normal * gain[...] + shift[...]).astype(BF)

    sums.own(norm)
    own_copy.wait()
    for copy in leave:
        copy.wait()
    line.finish()
    sums.finish()


def hidden_kernel(n, pieces, c_ref, h_ref, cot_hbm, up_hbm, down_hbm, up_bias, gain, c_hbm, g_hbm, du_hbm, mlp_hbm, dh_ref,
                  db_ref, vec_ref, upb_ref, c_all, g_all, du_all, cot_all, up, down, part, land, send, recv, s_send,
                  s_recv, w_sem, cot_sem, own_sem, c_sem, g_sem, du_sem, mlp, mlp_sem):
    i = lax.axis_index("tensor")
    size, depth = c_ref.shape
    units = up.shape[1]
    greet_neighbours(i, n)
    line = LineGather(i, n, c_ref, c_all, send, recv)
    line.start()
    own_copy = pltpu.make_async_copy(c_ref, c_all.at[i], own_sem)
    own_copy.start()
    up_copy = pltpu.make_async_copy(up_hbm, up, w_sem.at[0])
    up_copy.start()
    down_copy = pltpu.make_async_copy(down_hbm, down, w_sem.at[1])
    down_copy.start()
    cot_copy = pltpu.make_async_copy(cot_hbm, cot_all, cot_sem)
    cot_copy.start()
    upb_ref[...] = jnp.zeros_like(upb_ref)
    vec_ref[...] = jnp.zeros_like(vec_ref)
    own_copy.wait()
    up_copy.wait()
    down_copy.wait()
    cot_copy.wait()
    sums = LineSum(i, n, part, land, s_send, s_recv, pieces)
    tile = 256

    def out_copy(src, dst, sem, j):
        return pltpu.make_async_copy(src.at[j], dst.at[j], sem.at[j])

    def compute(j):
        def unit(k):
            cols = rows_at(k, tile)
            u = jnp.dot(c_all[j], up[:, cols], preferred_element_type=F32) + up_bias[0:1, cols]
            dg = lax.dot_general(cot_all[j], down[cols, :], NT, preferred_element_type=F32)
            half = 0.5 + 0.5 * lax.erf(u * (0.5 ** 0.5))
            g_all[j, :, cols] = (u * half).astype(BF)
            slope = half + u * (jnp.exp(u * u * -0.5) * 0.3989422804014327)
            du = (slope * dg).astype(BF)
            du_all[j, :, cols] = du
            upb_ref[0:1, cols] += jnp.sum(du.astype(F32), axis=0, keepdims=True)

        loop(units // tile, unit)

        def back(k):
            cols = rows_at(k, tile)
            part[j, :, cols] = lax.dot_general(du_all[j], up[cols, :], NT, preferred_element_type=F32).astype(BF)

        loop(depth // tile, back)
        sums.launch(j)
        out_copy(g_all, g_hbm, g_sem, j).start()
        out_copy(du_all, du_hbm, du_sem, j).start()
        out_copy(c_all, c_hbm, c_sem, j).start()

    rounds(i, n, line, compute)

    def forward(j):
        def columns(k):
            cols = rows_at(k, tile)
            mlp[j, :, cols] = jnp.dot(g_all[j], down[:, cols], preferred_element_type=F32).astype(BF)

        loop(depth // tile, columns)
        out_copy(mlp, mlp_hbm, mlp_sem, j).start()

    loop(n, forward)

    def relay(t):
        early = jnp.where(i < n // 2, 1, 0)
        sums.relay(t + 3 - early - i, 2 * n - 4 - i - t - early)

    loop(2 * n - 3, relay)

    def norm(b):
        here = rows_at(b, RB)
        sums.add(here, dh_ref.at[here, :])
        grad = dh_ref[here, :]
        normal, inverse = norm_stats(h_ref[here, :])
        vec_ref[0:1, :] += jnp.sum(grad * normal, axis=0, keepdims=True)
        vec_ref[1:2, :] += jnp.sum(grad, axis=0, keepdims=True)
        cot = cot_all[i, here, :].astype(F32)
        dh = cot + norm_back(grad, normal, inverse, gain[...])
        dh_ref[here, :] = dh
        db = dh.astype(BF)
        db_ref[here, :] = db
        vec_ref[2:3, :] += jnp.sum(db.astype(F32), axis=0, keepdims=True)
        vec_ref[3:4, :] += jnp.sum(cot, axis=0, keepdims=True)

    sums.own(norm)

    def done(j):
        out_copy(g_all, g_hbm, g_sem, j).wait()
        out_copy(du_all, du_hbm, du_sem, j).wait()
        out_copy(c_all, c_hbm, c_sem, j).wait()
        out_copy(mlp, mlp_hbm, mlp_sem, j).wait()

    loop(n, done)
    line.finish()
    sums.finish()


def attend_back(q_of, k_of, v_of, do_of, heads, put, dk, dv):
    block = 256
    factor = HD ** (-0.5)

    def head(t):
        dk[...] = jnp.zeros_like(dk)
        dv[...] = jnp.zeros_like(dv)
        for b in range(LEN // block):
            here, keys = slice(b * block, (b + 1) * block), slice(0, (b + 1) * block)
            q, k, v, do = q_of(here, t), k_of(keys, t), v_of(keys, t), do_of(here, t)
            s = lax.dot_general(q, k, NT, preferred_element_type=F32) * factor
            query = lax.broadcasted_iota(jnp.int32, s.shape, 0) + b * block
            s = jnp.where(query >= lax.broadcasted_iota(jnp.int32, s.shape, 1), s, -1e30)
            e = jnp.exp(s - jnp.max(s, axis=-1, keepdims=True))
            prob = e / jnp.sum(e, axis=-1, keepdims=True)
            dv[keys, :] += lax.dot_general(prob.astype(BF), do, TN, preferred_element_type=F32)
            dp = lax.dot_general(do, v, NT, preferred_element_type=F32)
            ds = (prob * (dp - jnp.sum(prob * dp, axis=-1, keepdims=True))).astype(BF)
            put(0, here, t, (jnp.dot(ds, k, preferred_element_type=F32) * factor).astype(BF))
            dk[keys, :] += lax.dot_general(ds, q, TN, preferred_element_type=F32)
        put(1, slice(0, LEN), t, (dk[...] * factor).astype(BF))
        put(2, slice(0, LEN), t, dv[...].astype(BF))

    loop(heads, head)


def partner(row, bit):
    return row + bit * (1 - 2 * ((row // bit) % 2))


class PlaneSum:
    def __init__(self, row, m, out, terms, land, halves, send, recv, h_send, h_recv):
        self.row, self.m, self.out, self.terms, self.land, self.halves = row, m, out, terms, land, halves
        self.send, self.recv, self.h_send, self.h_recv = send, recv, h_send, h_recv
        bits = [1 << k for k in range(1, m.bit_length() - 1)]
        self.plan = []
        for order in (bits, bits[::-1]):
            left, at, stages = [e for e in range(m) if e % 2 == 0], 0, []
            for bit in order:
                out = [e for e in left if e & bit]
                stages.append((bit, [(e, e ^ bit, at + k) for k, e in enumerate(out)]))
                left, at = [e for e in left if not e & bit], at + len(out)
            self.plan.append(stages)
        self.stages = len(bits)

    def owner(self, e):
        d = self.row
        for k in range(self.m.bit_length() - 1):
            if e & (1 << k):
                d = d + (partner(self.row, 1 << k) - self.row)
        return d

    def whole(self, e):
        return pltpu.make_async_remote_copy(
            src_ref=self.out.at[e // 2], dst_ref=self.land.at[e // 2], send_sem=self.send.at[e // 2],
            recv_sem=self.recv.at[e // 2], device_id={"dp": partner(self.row, 1)}, device_id_type=MESH)

    def half(self, h, bit, e, at):
        size = self.halves.shape[2]
        return pltpu.make_async_remote_copy(
            src_ref=self.terms.at[e // 2, pl.ds(h * size, size)], dst_ref=self.halves.at[h, at],
            send_sem=self.h_send.at[h, at], recv_sem=self.h_recv.at[h, at],
            device_id={"dp": partner(self.row, bit)}, device_id_type=MESH)

    def merge(self):
        for e in range(0, self.m, 2):
            self.whole(e + 1).wait_recv()

            def add(b):
                here = rows_at(b, RB)
                total = self.terms[e // 2, here, :].astype(F32) + self.land[e // 2, here, :].astype(F32)
                self.terms[e // 2, here, :] = total.astype(BF)

            loop(self.terms.shape[1] // RB, add)

    def push(self, stage):
        for h in range(2):
            bit, moves = self.plan[h][stage]
            for e, _, at in moves:
                self.half(h, bit, e, at).start()

    def take(self, stage, out=None):
        size = self.halves.shape[2]
        for h in range(2):
            bit, moves = self.plan[h][stage]
            for e, into, at in moves:
                self.half(h, bit, e, at).wait_recv()

                def add(b):
                    here, there = rows_at(b, RB), pl.ds(pl.multiple_of(h * size + b * RB, RB), RB)
                    total = self.terms[into // 2, there, :].astype(F32) + self.halves[h, at, here, :].astype(F32)
                    if out is None:
                        self.terms[into // 2, there, :] = total.astype(BF)
                    else:
                        out(there, total)

                loop(size // RB, add)

    def sent(self):
        for e in range(1, self.m, 2):
            self.whole(e).wait_send()

    def finish(self):
        for h in range(2):
            for bit, moves in self.plan[h]:
                for e, _, at in moves:
                    self.half(h, bit, e, at).wait_send()


class VectorSum:
    def __init__(self, me, count, device, vectors, piece, land, out, send, recv):
        self.me, self.count, self.device, self.vectors, self.piece = me, count, device, vectors, piece
        self.land, self.out, self.send, self.recv = land, out, send, recv

    def lanes(self, owner):
        size = self.land.shape[2]
        return pl.ds(pl.multiple_of(owner * self.piece // size * size, size), size)

    def copy(self, src, other):
        return pltpu.make_async_remote_copy(
            src_ref=self.vectors.at[:, self.lanes(other)], dst_ref=self.land.at[src], send_sem=self.send.at[other],
            recv_sem=self.recv.at[src], device_id=self.device(other), device_id_type=MESH)

    def start(self):
        loop(self.count - 1, lambda s: self.copy(self.me, (self.me + s + 1) % self.count).start())

    def finish(self):
        self.out[...] = self.vectors[:, self.lanes(self.me)]

        def take(s):
            src = (self.me + s + 1) % self.count
            self.copy(src, self.me).wait_recv()
            self.out[...] += self.land[src]

        loop(self.count - 1, take)
        loop(self.count - 1, lambda s: self.copy(self.me, (self.me + s + 1) % self.count).wait_send())


def greet_cross(i, n, row, m):
    barrier = pltpu.get_barrier_semaphore()

    @pl.when(i > 0)
    def _():
        pl.semaphore_signal(barrier, inc=1, device_id={"tensor": i - 1}, device_id_type=MESH)

    @pl.when(i < n - 1)
    def _():
        pl.semaphore_signal(barrier, inc=1, device_id={"tensor": i + 1}, device_id_type=MESH)

    bits = [1 << k for k in range(m.bit_length() - 1)]
    for bit in bits:
        pl.semaphore_signal(barrier, inc=1, device_id={"dp": partner(row, bit)}, device_id_type=MESH)
    pl.semaphore_wait(barrier, jnp.minimum(i, 1) + jnp.minimum(n - 1 - i, 1) + len(bits))


def relays(sums, i, n, r):
    sums.relay(n - 1 + i - r, r - (n - 1 - i))


def block_terms(plane, e, pairs):
    size = plane.terms.shape[1]
    cols = rows_at(plane.owner(e), size)
    for lhs, rhs, first in pairs:
        width = rhs.shape[1]
        tile = min(512, width)

        def columns(k):
            there = pl.ds(pl.multiple_of(first + k * tile, tile), tile)
            (plane.out if e % 2 else plane.terms)[e // 2, :, there] = lax.dot_general(
                lhs[:, cols], rhs[:, rows_at(k, tile)], TN, preferred_element_type=F32).astype(BF)

        loop(width // tile, columns)


def branch_kernel(n, m, pieces, db_ref, h_ref, down_bias, mlp_hbm, g_hbm, cot_hbm, c_hbm, du_hbm, qkv_hbm, wo_hbm,
                  db_all, lo_ref, down_ref, up_ref, dqkv_hbm, dqkv_ref, out_sem, lhs, rhs, wo, dk, dv, part, land, out, terms_a, land_a,
                  half_a, terms_b, land_b, half_b, acc, send, recv, s_send, s_recv, own_sem, part_sem, in_sem, qkv_sem,
                  db_sem, p_send, p_recv, h_send, h_recv):
    i, row = lax.axis_index("tensor"), lax.axis_index("dp")
    size = db_ref.shape[0]
    width = wo.shape[0]
    greet_cross(i, n, row, m)
    line = LineGather(i, n, db_ref, db_all, send, recv)
    line.start()
    part_copy = pltpu.make_async_copy(mlp_hbm, part, part_sem)
    part_copy.start()
    own_copy = pltpu.make_async_copy(db_ref, db_all.at[i], own_sem)
    own_copy.start()

    def load(left, right):
        return [pltpu.make_async_copy(left, lhs, in_sem.at[0]), pltpu.make_async_copy(right, rhs, in_sem.at[1])]

    loads = load(cot_hbm, g_hbm)
    for copy in loads:
        copy.start()
    wo_copy = pltpu.make_async_copy(wo_hbm, wo, in_sem.at[2])
    wo_copy.start()
    sums = LineSum(i, n, part, land, s_send, s_recv, pieces)
    part_copy.wait()
    loop(n, lambda t: sums.launch(jnp.where(i < n // 2, n - 1 - t, t)))
    planes = [PlaneSum(row, m, out, terms_a, land_a, half_a, p_send.at[0], p_recv.at[0], h_send.at[0], h_recv.at[0]),
              PlaneSum(row, m, out, terms_b, land_b, half_b, p_send.at[1], p_recv.at[1], h_send.at[1], h_recv.at[1])]
    first, second = planes
    for copy in loads:
        copy.wait()
    left, right = lhs.at[:, 0 : lhs.shape[1]], rhs.at[:, 0 : down_ref.shape[1]]
    for e in range(1, m, 2):
        block_terms(first, e, [(left, right, 0)])
        first.whole(e).start()
    for e in range(m - 2, -1, -2):
        block_terms(first, e, [(left, right, 0)])
    loads = load(c_hbm, du_hbm)
    for copy in loads:
        copy.start()
    first.merge()
    first.push(0)
    first.sent()
    for copy in loads:
        copy.wait()
    for e in range(1, m, 2):
        block_terms(second, e, [(left, right, 0)])
        second.whole(e).start()

    line.step(1)
    for e in range(m - 2, -1, -2):
        block_terms(second, e, [(left, right, 0)])
    qkv_copies = [pltpu.make_async_copy(qkv_hbm.at[p], rhs.at[:, p * width : (p + 1) * width], qkv_sem.at[p])
                  for p in range(3)]
    for copy in qkv_copies:
        copy.start()
    second.merge()
    second.push(0)
    own_copy.wait()
    wo_copy.wait()

    def mixture_back(j):
        here = rows_at(j, size)
        copy = pltpu.make_async_copy(db_all.at[j], lhs.at[here], db_sem.at[j])
        copy.start()
        copy.wait()
        rhs[here, 3 * width : 4 * width] = lax.dot_general(
            lhs[here, :], wo[...], NT, preferred_element_type=F32).astype(BF)

    def round_back(r):
        def side(s):
            j = jnp.where(s == 0, i - r, i + r)

            @pl.when(jnp.logical_and(j >= 0, j <= n - 1))
            def _():
                mixture_back(j)

        loop(2, side)

    def keep(ref):
        def put(here, total):
            ref[here, :] = total

        return put

    def advance(plane, stage, ref):
        if stage < plane.stages - 1:
            plane.take(stage)
            plane.push(stage + 1)
        else:
            plane.take(stage, keep(ref))

    mixture_back(i)
    round_back(1)
    advance(first, 0, down_ref)
    for r in range(2, n):
        line.step(r)
        relays(sums, i, n, r - 1)
        round_back(r)
        if r == 2:
            advance(second, 0, up_ref)
    if n == 2:
        advance(second, 0, up_ref)
    relays(sums, i, n, n - 1)
    for copy in qkv_copies:
        copy.wait()

    def column(p):
        def get(here, t):
            return rhs[here, pl.ds(pl.multiple_of(p * width + t * HD, HD), HD)]

        return get

    def put(p, here, t, value):
        dqkv_ref[p, here, pl.ds(pl.multiple_of(t * HD, HD), HD)] = value

    attend_back(column(0), column(1), column(2), column(3), width // HD, put, dk, dv)
    leave = pltpu.make_async_copy(dqkv_ref, dqkv_hbm, out_sem)
    leave.start()
    for stage in range(1, first.stages):
        advance(first, stage, down_ref)
        advance(second, stage, up_ref)

    def output(b):
        here = rows_at(b, RB)
        sums.add(here, acc)
        lo_ref[here, :] = (h_ref[here, :] + (acc[...] + down_bias[...])).astype(BF)

    sums.own(output)
    line.finish()
    sums.finish()
    second.sent()
    for plane in planes:
        plane.finish()
    leave.wait()


def input_kernel(n, m, pieces, widths, dqkv_ref, wq_hbm, x_hbm, dh_hbm, gain, early_ref, up_ref, a_hbm, db_hbm, o_hbm,
                 n_hbm, gt_ref, gqkv_ref, gout_ref, early_out, late_out, up_out, qv_out, vec_ref, qv_ref, wq, a_ref, db_ref,
                 o_ref, n_ref, x_ref, dh_ref, part, land, out_p, terms, land_p, half_p, acc, early_land, late_land, up_land, qv_land, s_send,
                 s_recv, in_sem, p_send, p_recv, h_send, h_recv, e_send, e_recv, l_send, l_recv, u_send, u_recv, q_send,
                 q_recv):
    i, row = lax.axis_index("tensor"), lax.axis_index("dp")
    me, total_devices = row * n + i, m * n
    size = x_hbm.shape[0]
    width = dqkv_ref.shape[2]
    piece, up_piece, qv_piece = widths
    depth = part.shape[2]
    loads = [pltpu.make_async_copy(src, dst, in_sem.at[k]) for k, (src, dst) in enumerate(
        [(wq_hbm, wq), (a_hbm, a_ref), (db_hbm, db_ref), (o_hbm, o_ref), (n_hbm, n_ref), (x_hbm, x_ref), (dh_hbm, dh_ref)])]
    loads[0].start()
    loads[4].start()
    greet_all(me, n, total_devices)
    every = [VectorSum(me, total_devices, lambda g: {"dp": g // n, "tensor": g % n}, early_ref, piece, early_land, early_out,
                       e_send, e_recv),
             VectorSum(me, total_devices, lambda g: {"dp": g // n, "tensor": g % n}, vec_ref, piece, late_land, late_out,
                       l_send, l_recv)]
    column = [VectorSum(row, m, lambda g: {"dp": g}, up_ref, up_piece, up_land, up_out, u_send, u_recv),
              VectorSum(row, m, lambda g: {"dp": g}, qv_ref, qv_piece, qv_land, qv_out, q_send, q_recv)]
    every[0].start()
    column[0].start()
    sums = LineSum(i, n, part, land, s_send, s_recv, pieces)
    vec_ref[...] = jnp.zeros_like(vec_ref)
    qv_ref[...] = jnp.zeros_like(qv_ref)
    loads[0].wait()
    loads[4].wait()
    for k in (1, 2, 3, 5, 6):
        loads[k].start()
    tile = 512

    def term(t):
        d = jnp.where(i < n // 2, n - 1 - t, t)
        here = rows_at(d, size)

        def columns(k):
            cols = rows_at(k, tile)
            total = lax.dot_general(dqkv_ref[0, here, :], wq[0, cols, :], NT, preferred_element_type=F32)
            for p in range(1, 3):
                total += lax.dot_general(dqkv_ref[p, here, :], wq[p, cols, :], NT, preferred_element_type=F32)
            part[d, :, cols] = total.astype(BF)
            vec_ref[0:1, cols] += jnp.sum(total * n_ref[here, cols].astype(F32), axis=0, keepdims=True)
            vec_ref[1:2, cols] += jnp.sum(total, axis=0, keepdims=True)

        loop(depth // tile, columns)
        sums.launch(d)
        for p in range(2):
            qv_ref[p : p + 1, :] += jnp.sum(dqkv_ref[2 * p, here, :].astype(F32), axis=0, keepdims=True)

    loop(n, term)
    column[1].start()
    every[1].start()
    for k in (1, 2, 3, 5, 6):
        loads[k].wait()
    plane = PlaneSum(row, m, out_p, terms, land_p, half_p, p_send, p_recv, h_send, h_recv)
    pairs = [(a_ref, dqkv_ref.at[p], p * width) for p in range(3)] + [(db_ref, o_ref, 3 * width)]
    for e in range(1, m, 2):
        block_terms(plane, e, pairs)
        plane.whole(e).start()
    for e in range(m - 2, -1, -2):
        block_terms(plane, e, pairs)
    plane.merge()
    plane.push(0)

    def out(here, total):
        for p in range(3):
            gqkv_ref[p, here, :] = total[:, p * width : (p + 1) * width]
        gout_ref[here, :] = total[:, 3 * width :]

    stage = 0
    for r in range(1, n):
        relays(sums, i, n, r)
        if r > 1 and stage < plane.stages:
            if stage < plane.stages - 1:
                plane.take(stage)
                plane.push(stage + 1)
            else:
                plane.take(stage, out)
            stage += 1

    def norm(b):
        here = rows_at(b, RB)
        sums.add(here, acc)
        grad = acc[...]
        normal, inverse = norm_stats(x_ref[here, :].astype(F32))
        gt_ref[here, :] = (dh_ref[here, :] + norm_back(grad, normal, inverse, gain[...])).astype(BF)

    while stage < plane.stages:
        if stage < plane.stages - 1:
            plane.take(stage)
            plane.push(stage + 1)
        else:
            plane.take(stage, out)
        stage += 1
    for group in (every[0], column[0], column[1], every[1]):
        group.finish()
    sums.own(norm)
    sums.finish()
    plane.sent()
    plane.finish()


def params(collective=None):
    if collective is None:
        return pltpu.CompilerParams(vmem_limit_bytes=BIG)
    return pltpu.CompilerParams(vmem_limit_bytes=BIG, collective_id=collective, has_side_effects=True)


def shape(dims, dtype):
    return jax.ShapeDtypeStruct(dims, dtype)


def body(tokens, cotangent, ln1_gain, ln1_bias, qkv_weight, qv_bias, out_weight, out_bias, ln2_gain, ln2_bias,
         up_weight, up_bias, down_weight, down_bias):
    n = lax.axis_size("tensor")
    m = lax.axis_size("dp")
    i, row = lax.axis_index("tensor"), lax.axis_index("dp")
    size, depth = tokens.shape
    width = qkv_weight.shape[2]
    units = up_weight.shape[1]
    piece, qv_piece, up_piece = ln1_gain.shape[0], qv_bias.shape[1], up_bias.shape[0]
    total = m * n

    def lane_rows(value, index):
        count = value.shape[-1]
        if count >= LANES:
            return value.reshape(-1, LANES)
        places = LANES // count
        spread = jnp.tile(value.reshape(-1, count), (1, places))
        return jnp.where((jnp.arange(LANES) // count)[None] == index % places, spread, 0)

    me = row * n + i
    whole = jnp.stack([ln1_gain, ln1_bias, out_bias, ln2_gain, ln2_bias, down_bias])
    pack = jnp.concatenate([lane_rows(whole, me), lane_rows(qv_bias, row), lane_rows(up_bias, row)])
    pack = jnp.pad(pack, ((0, -pack.shape[0] % 16), (0, 0)))
    lanes_up = 8 + max(up_piece // LANES, 1)

    w_qkv = lax.all_gather(qkv_weight, "dp", axis=1, tiled=True)
    w_out = lax.all_gather(out_weight, "dp", axis=1, tiled=True)
    w_up = lax.all_gather(up_weight, "dp", axis=0, tiled=True)
    w_down = lax.all_gather(down_weight, "dp", axis=1, tiled=True)

    dma = pltpu.SemaphoreType.DMA
    attn_in, normal_one, vecs = pl.pallas_call(
        functools.partial(tokens_kernel, n, m, piece),
        out_shape=(shape((LEN, depth), BF), shape((LEN, depth), BF), shape((total,) + pack.shape, BF)),
        in_specs=[VM, VM], out_specs=(ANY, ANY, VM),
        scratch_shapes=[pltpu.VMEM((n, size, depth), BF), pltpu.VMEM((8, depth), F32), pltpu.VMEM((LEN, depth), BF),
                        pltpu.VMEM((LEN, depth), BF), dma((2, n)), dma, dma((2, n, LineGather.PIECES)), dma((n, LineGather.PIECES)),
                        dma((total,)), dma((total,))],
        compiler_params=params(0), name="gather_tokens",
    )(pack, tokens)
    vecs = vecs.astype(F32)

    def whole_rows(block, count):
        if count < LANES:
            block = block.reshape(-1, LANES // count, *block.shape[1:]).sum(axis=1)
        return block

    vectors = whole_rows(vecs[:, 0:6], piece).transpose(1, 0, 2).reshape(6, 1, depth)
    gain_one, shift_one, bias_out, gain_two, shift_two, bias_down = [vectors[j] for j in range(6)]
    mine = lax.dynamic_index_in_dim(vecs.reshape(m, n, -1, LANES), i, 1, keepdims=False)
    bias_qv = whole_rows(mine[:, 6:8], qv_piece).transpose(1, 0, 2).reshape(2, width)
    bias_up = whole_rows(mine[:, 8:lanes_up], up_piece).reshape(1, units)

    pieces = 2
    sums = [pltpu.VMEM((n, size, depth), BF), pltpu.VMEM((n + 1, size, depth), BF)]
    qkv, mixture, residual, mlp_own, cot_all = pl.pallas_call(
        functools.partial(attend_kernel, n, pieces),
        out_shape=(shape((3, LEN, width), BF), shape((LEN, width), BF), shape((size, depth), F32),
                   shape((size, depth), BF), shape((n, size, depth), BF)),
        in_specs=[ANY] * 3 + [VM] * 6, out_specs=(ANY, ANY, VM, VM, ANY),
        scratch_shapes=[pltpu.VMEM((3, LEN, width), BF), pltpu.VMEM((LEN, width), BF), dma((2,)),
                        pltpu.VMEM((LEN, depth), BF), pltpu.VMEM((3, depth, width), BF), pltpu.VMEM((width, depth), BF)] +
                       sums + [dma((2, n, LineGather.PIECES)), dma((n, LineGather.PIECES)), dma((n, pieces)), dma((n + 1, pieces)), dma, dma, dma((4,))],
        compiler_params=params(1), name="attend",
    )(attn_in, w_qkv, w_out, tokens, cotangent, bias_qv, bias_out, gain_two, shift_two)

    pieces = 4
    mlp_in, hidden, grad_pre, mlp_part, grad_resid, branch_cot, vec_two, grad_up_b = pl.pallas_call(
        functools.partial(hidden_kernel, n, pieces),
        out_shape=(shape((n, size, depth), BF), shape((n, size, units), BF), shape((n, size, units), BF),
                   shape((n, size, depth), BF), shape((size, depth), F32), shape((size, depth), BF),
                   shape((8, depth), F32), shape((8, units), F32)),
        in_specs=[VM, VM, ANY, ANY, ANY, VM, VM], out_specs=(ANY, ANY, ANY, ANY, VM, VM, VM, VM),
        scratch_shapes=[pltpu.VMEM((n, size, depth), BF), pltpu.VMEM((n, size, units), BF),
                        pltpu.VMEM((n, size, units), BF), pltpu.VMEM((n, size, depth), BF),
                        pltpu.VMEM((depth, units), BF), pltpu.VMEM((units, depth), BF)] + sums +
                       [dma((2, n, LineGather.PIECES)), dma((n, LineGather.PIECES)), dma((n, pieces)), dma((n + 1, pieces)), dma((2,)), dma, dma,
                        dma((n,)), dma((n,)), dma((n,)), pltpu.VMEM((n, size, depth), BF), dma((n,))],
        compiler_params=params(2), name="hidden",
    )(mlp_own, residual, cot_all, w_up, w_down, bias_up, gain_two)
    mlp_in, hidden, grad_pre, cot_rows = [v.reshape(LEN, -1) for v in (mlp_in, hidden, grad_pre, cot_all)]

    def plane_scratch(columns):
        rows = depth // m
        return [pltpu.VMEM((m // 2, rows, columns), BF), pltpu.VMEM((m // 2, rows, columns), BF),
                pltpu.VMEM((2, m // 2 - 1, rows // 2, columns), BF)]

    pieces = 2
    sum_sems = [dma((n, pieces)), dma((n + 1, pieces))]
    attn_cot, layer_out, grad_down_w, grad_up_w, grad_qkv = pl.pallas_call(
        functools.partial(branch_kernel, n, m, pieces),
        out_shape=(shape((n, size, depth), BF), shape((size, depth), BF), shape((depth // m, units), F32),
                   shape((depth // m, units), F32), shape((3, LEN, width), BF)),
        in_specs=[VM] * 3 + [ANY] * 7, out_specs=(ANY, VM, VM, VM, ANY),
        scratch_shapes=[pltpu.VMEM((3, LEN, width), BF), dma, pltpu.VMEM((LEN, depth), BF), pltpu.VMEM((LEN, units), BF), pltpu.VMEM((width, depth), BF),
                        pltpu.VMEM((LEN, HD), F32), pltpu.VMEM((LEN, HD), F32)] + sums +
                       [pltpu.VMEM((m // 2, depth // m, units), BF)] + plane_scratch(units) * 2 +
                       [pltpu.VMEM((RB, depth), F32), dma((2, n, LineGather.PIECES)), dma((n, LineGather.PIECES))] + sum_sems +
                       [dma, dma, dma((3,)), dma((3,)), dma((n,)), dma((2, m // 2)), dma((2, m // 2)),
                        dma((2, 2, m // 2 - 1)), dma((2, 2, m // 2 - 1))],
        compiler_params=params(4), name="branch",
    )(branch_cot, residual, bias_down, mlp_part, hidden, cot_rows, mlp_in, grad_pre, qkv, w_out)
    attn_cot = attn_cot.reshape(LEN, depth)

    tiles = [max(v, LANES) for v in (piece, up_piece, qv_piece)]
    grad_tokens, grad_qkv_w, grad_out_w, early, late, grad_up_b, grad_qv_b = pl.pallas_call(
        functools.partial(input_kernel, n, m, pieces, (piece, up_piece, qv_piece)),
        out_shape=(shape((size, depth), BF), shape((3, depth // m, width), F32), shape((depth // m, width), F32),
                   shape((8, tiles[0]), F32), shape((8, tiles[0]), F32), shape((8, tiles[1]), F32),
                   shape((8, tiles[2]), F32)),
        in_specs=[VM, ANY, ANY, ANY, VM, VM, VM, ANY, ANY, ANY, ANY], out_specs=(VM,) * 7,
        scratch_shapes=[pltpu.VMEM((8, depth), F32), pltpu.VMEM((8, width), F32),
                        pltpu.VMEM((3, depth, width), BF), pltpu.VMEM((LEN, depth), BF), pltpu.VMEM((LEN, depth), BF),
                        pltpu.VMEM((LEN, width), BF), pltpu.VMEM((LEN, depth), BF), pltpu.VMEM((size, depth), BF),
                        pltpu.VMEM((size, depth), F32)] + sums +
                       [pltpu.VMEM((m // 2, depth // m, 4 * width), BF)] +
                       plane_scratch(4 * width) +
                       [pltpu.VMEM((RB, depth), F32), pltpu.VMEM((total, 8, tiles[0]), F32),
                        pltpu.VMEM((total, 8, tiles[0]), F32), pltpu.VMEM((m, 8, tiles[1]), F32),
                        pltpu.VMEM((m, 8, tiles[2]), F32)] + sum_sems +
                       [dma((7,)), dma((m // 2,)), dma((m // 2,)), dma((2, m // 2 - 1)), dma((2, m // 2 - 1))] +
                       [dma((total,))] * 4 + [dma((m,))] * 4,
        compiler_params=params(5), name="input",
    )(grad_qkv, w_qkv, tokens, grad_resid, gain_one, vec_two, grad_up_b, attn_in, attn_cot, mixture, normal_one)
    grad_down_w, grad_out_w = grad_down_w.T, grad_out_w.T

    def own_lanes(block, index, count):
        return lax.dynamic_slice_in_dim(block, index * count % block.shape[1], count, axis=1)

    early, late = own_lanes(early, me, piece), own_lanes(late, me, piece)
    vectors = [late[0], late[1], early[2], early[0], early[1], early[3]]
    grad_qv_b = own_lanes(grad_qv_b, row, qv_piece)[:2]
    grad_up_b = own_lanes(grad_up_b, row, up_piece)[0]
    return (layer_out, grad_tokens, vectors[0], vectors[1], grad_qkv_w, grad_qv_b, grad_out_w, vectors[2],
            vectors[3], vectors[4], grad_up_w, grad_up_b, grad_down_w, vectors[5])


def solution(mesh):
    vector, matrix = P(("dp", "tensor")), P(("dp", "tensor"), None)
    in_specs = (matrix, matrix, vector, vector, P(None, "dp", "tensor"), P(None, ("tensor", "dp")), P("tensor", "dp"),
                vector, vector, vector, P("dp", "tensor"), P(("tensor", "dp")), P("tensor", "dp"), vector)
    out_specs = (matrix, matrix, vector, vector, P(None, "dp", "tensor"), P(None, ("tensor", "dp")),
                 P("tensor", "dp"), vector, vector, vector, P("dp", "tensor"), P(("tensor", "dp")), P("tensor", "dp"),
                 vector)
    return jax.shard_map(body, mesh=mesh, in_specs=in_specs, out_specs=out_specs, check_vma=False)
```

```python
import functools

import jax
import jax.numpy as jnp
from jax import lax
from jax.experimental import pallas as pl
from jax.experimental.pallas import tpu as pltpu
from jax.sharding import PartitionSpec as P

HD = 128
LEN = 1024
LANES = 128
EPS = 1e-05
BF = jnp.bfloat16
F32 = jnp.float32
MESH = pl.DeviceIdType.MESH
ANY = pl.BlockSpec(memory_space=pl.ANY)
VM = pl.BlockSpec(memory_space=pltpu.VMEM)
NT = (((1,), (1,)), ((), ()))
TN = (((0,), (0,)), ((), ()))
BIG = 64 * 1024 * 1024 - 65536
RB = 32


def norm_stats(rows):
    mean = jnp.mean(rows, axis=-1, keepdims=True)
    centred = rows - mean
    variance = jnp.mean(centred * centred, axis=-1, keepdims=True)
    inverse = lax.rsqrt(variance + EPS)
    return centred * inverse, inverse


def norm_back(grad_rows, normal_rows, inverse, gain):
    scaled = grad_rows * gain
    first = jnp.mean(scaled, axis=-1, keepdims=True)
    second = jnp.mean(scaled * normal_rows, axis=-1, keepdims=True)
    return inverse * (scaled - first - normal_rows * second)


def loop(count, step):
    def run(i, carry):
        step(i)
        return carry

    lax.fori_loop(0, count, run, 0)


def rows_at(j, size):
    return pl.ds(pl.multiple_of(j * size, size), size)


def remote(src, dst, send, recv, target):
    return pltpu.make_async_remote_copy(src_ref=src, dst_ref=dst, send_sem=send, recv_sem=recv,
                                        device_id={"tensor": target}, device_id_type=MESH)


def greet_neighbours(i, n):
    barrier = pltpu.get_barrier_semaphore()

    @pl.when(i > 0)
    def _():
        pl.semaphore_signal(barrier, inc=1, device_id={"tensor": i - 1}, device_id_type=MESH)

    @pl.when(i < n - 1)
    def _():
        pl.semaphore_signal(barrier, inc=1, device_id={"tensor": i + 1}, device_id_type=MESH)

    pl.semaphore_wait(barrier, jnp.minimum(i, 1) + jnp.minimum(n - 1 - i, 1))


def greet_all(me, n, total):
    barrier = pltpu.get_barrier_semaphore()

    def greet(s):
        other = (me + s + 1) % total
        pl.semaphore_signal(barrier, inc=1, device_id={"dp": other // n, "tensor": other % n}, device_id_type=MESH)

    loop(total - 1, greet)
    pl.semaphore_wait(barrier, total - 1)


def rounds(i, n, line, compute, between=None):
    def round_of(r):
        @pl.when(r > 0)
        def _():
            line.step(r)

        if between is not None:
            between(r)

        def side(s):
            j = jnp.where(s == 0, i - r, i + r)

            @pl.when(jnp.logical_and(jnp.logical_and(j >= 0, j <= n - 1), s * r == s * jnp.maximum(r, 1)))
            def _():
                compute(j)

        loop(2, side)

    loop(n, round_of)


class LineGather:
    PIECES = 2

    def __init__(self, i, n, own, buf, send, recv):
        self.i, self.n, self.own, self.buf, self.send, self.recv = i, n, own, buf, send, recv
        self.size = own.shape[0] // self.PIECES

    def copy(self, src, j, side, s, target):
        here = pl.ds(s * self.size, self.size)
        return remote(src.at[here], self.buf.at[j, here], self.send.at[side, j, s], self.recv.at[j, s], target)

    def start(self):
        i, n = self.i, self.n
        for s in range(self.PIECES):
            @pl.when(i < n - 1)
            def _():
                self.copy(self.own, i, 0, s, i + 1).start()

            @pl.when(i > 0)
            def _():
                self.copy(self.own, i, 1, s, i - 1).start()

    def step(self, r):
        i, n = self.i, self.n
        for s in range(self.PIECES):
            @pl.when(i - r >= 0)
            def _():
                self.copy(self.own, i - r, 0, s, i).wait_recv()

                @pl.when(i < n - 1)
                def _():
                    self.copy(self.buf.at[i - r], i - r, 0, s, i + 1).start()

            @pl.when(i + r <= n - 1)
            def _():
                self.copy(self.own, i + r, 1, s, i).wait_recv()

                @pl.when(i > 0)
                def _():
                    self.copy(self.buf.at[i + r], i + r, 1, s, i - 1).start()

    def finish(self):
        i, n = self.i, self.n

        def one(j):
            for s in range(self.PIECES):
                @pl.when(jnp.logical_and(i < n - 1, j <= i))
                def _():
                    self.copy(self.own, j, 0, s, i + 1).wait_send()

                @pl.when(jnp.logical_and(i > 0, j >= i))
                def _():
                    self.copy(self.own, j, 1, s, i - 1).wait_send()

        loop(n, one)


class LineSum:
    def __init__(self, i, n, part, land, send, recv, pieces):
        self.i, self.n, self.part, self.land, self.send, self.recv = i, n, part, land, send, recv
        self.pieces = pieces
        self.size = part.shape[1] // pieces

    def copy(self, src, d, right, s):
        i, n = self.i, self.n
        target = i + 1 if right else i - 1
        slot = d if right else jnp.where(d == target, n, d)
        here = rows_at(s, self.size)
        return remote(src.at[d, here], self.land.at[slot, here], self.send.at[d, s], self.recv.at[slot, s], target)

    def arrived(self, slot, s):
        here = rows_at(s, self.size)
        remote(self.part.at[0, here], self.land.at[slot, here], self.send.at[0, s], self.recv.at[slot, s],
               self.i).wait_recv()

    def launch(self, d):
        i, n = self.i, self.n

        @pl.when(jnp.logical_and(i == 0, d > 0))
        def _():
            loop(self.pieces, lambda s: self.copy(self.part, d, True, s).start())

        @pl.when(jnp.logical_and(i == n - 1, d < n - 1))
        def _():
            loop(self.pieces, lambda s: self.copy(self.part, d, False, s).start())

    def relay(self, right, left):
        i, n = self.i, self.n

        def move(d, to_right, s):
            self.arrived(d, s)
            here = rows_at(s, self.size)
            total = self.land[d, here, :].astype(F32) + self.part[d, here, :].astype(F32)
            self.land[d, here, :] = total.astype(BF)
            self.copy(self.land, d, to_right, s).start()

        first = jnp.where(i < n // 2, 0, 1)

        def one(s):
            turn, s = (s + first) % 2, s // 2

            @pl.when(jnp.logical_and(turn == 0, jnp.logical_and(i > 0, jnp.logical_and(right > i, right <= n - 1))))
            def _():
                move(right, True, s)

            @pl.when(jnp.logical_and(turn == 1, jnp.logical_and(i < n - 1, jnp.logical_and(left >= 0, left < i))))
            def _():
                move(left, False, s)

        loop(2 * self.pieces, one)

    def own(self, step):
        i, n = self.i, self.n

        def one(s):
            @pl.when(i > 0)
            def _():
                self.arrived(i, s)

            @pl.when(i < n - 1)
            def _():
                self.arrived(n, s)

            loop(self.size // RB, lambda b: step(s * (self.size // RB) + b))

        loop(self.pieces, one)

    def add(self, here, out):
        i, n = self.i, self.n
        out[...] = self.part[i, here, :].astype(F32)

        @pl.when(i > 0)
        def _():
            out[...] += self.land[i, here, :].astype(F32)

        @pl.when(i < n - 1)
        def _():
            out[...] += self.land[n, here, :].astype(F32)

    def finish(self):
        i, n = self.i, self.n

        def one(d):
            @pl.when(jnp.logical_and(i < n - 1, d > i))
            def _():
                loop(self.pieces, lambda s: self.copy(self.part, d, True, s).wait_send())

            @pl.when(jnp.logical_and(i > 0, d < i))
            def _():
                loop(self.pieces, lambda s: self.copy(self.part, d, False, s).wait_send())

        loop(n, one)


def partner(row, bit):
    return row + bit * (1 - 2 * ((row // bit) % 2))


class PlaneGather:
    def __init__(self, row, m, items, send, recv, local):
        self.row, self.m, self.items, self.send, self.recv, self.local = row, m, items, send, recv, local
        bits = [1 << k for k in range(1, m.bit_length() - 1)]
        self.plan = []
        for order in (bits + [1], bits[::-1] + [1]):
            have, at, stages = [0], 0, []
            for bit in order:
                stages.append((bit, [(e, at + k) for k, e in enumerate(have)]))
                at, have = at + len(have), have + [e ^ bit for e in have]
            self.plan.append(stages)
        self.stages = len(bits) + 1

    def owner(self, e):
        d = self.row
        for k in range(self.m.bit_length() - 1):
            if e & (1 << k):
                d = d + (partner(self.row, 1 << k) - self.row)
        return d

    def copies(self, stage):
        for k, (own, whole, own_half, half) in enumerate(self.items):
            for h in range(2):
                bit, moves = self.plan[h][stage]
                for e, at in moves:
                    there = half(whole, self.owner(e), h)
                    src = own_half(own, h) if e == 0 else there
                    yield pltpu.make_async_remote_copy(
                        src_ref=src, dst_ref=there, send_sem=self.send.at[k, h, at], recv_sem=self.recv.at[k, h, e ^ bit],
                        device_id={"dp": partner(self.row, bit)}, device_id_type=MESH)

    def landed(self, stage):
        for k, (own, whole, own_half, half) in enumerate(self.items):
            for h in range(2):
                bit, moves = self.plan[h][stage]
                for e, at in moves:
                    there = half(whole, self.owner(e ^ bit), h)
                    pltpu.make_async_remote_copy(
                        src_ref=there, dst_ref=there, send_sem=self.send.at[k, h, at], recv_sem=self.recv.at[k, h, e ^ bit],
                        device_id={"dp": partner(self.row, bit)}, device_id_type=MESH).wait_recv()

    def locals(self):
        return [pltpu.make_async_copy(own_half(own, h), half(whole, self.row, h), self.local.at[k, h])
                for k, (own, whole, own_half, half) in enumerate(self.items) for h in range(2)]

    def start(self):
        for copy in self.copies(0):
            copy.start()
        for copy in self.locals():
            copy.start()

    def advance(self, stage):
        self.landed(stage - 1)
        for copy in self.copies(stage):
            copy.start()

    def finish(self):
        self.landed(self.stages - 1)
        for stage in range(self.stages):
            for copy in self.copies(stage):
                copy.wait_send()
        for copy in self.locals():
            copy.wait()


def half_rows(own, h):
    size = own.shape[-2] // 2
    return own.at[..., pl.ds(h * size, size), :]


def row_blocks(m):
    def half(whole, d, h):
        size = whole.shape[-2] // m // 2
        return whole.at[..., pl.ds(pl.multiple_of((2 * d + h) * size, size), size), :]

    return half


def column_blocks(m):
    def half(whole, d, h):
        size, width = whole.shape[-2] // 2, whole.shape[-1] // m
        return whole.at[pl.ds(h * size, size), pl.ds(pl.multiple_of(d * width, width), width)]

    return half


def tokens_kernel(n, m, piece, pack_ref, x_ref, wq_ref, wo_ref, a_hbm, n_hbm, vec_ref, wq_all, wo_all, buf, affine,
                  a_ref, n_ref, out_sem, w_send, w_recv, w_local, own_sem, send, recv, v_send, v_recv):
    i, row = lax.axis_index("tensor"), lax.axis_index("dp")
    me, total = row * n + i, m * n
    size = x_ref.shape[0]
    greet_all(me, n, total)
    line = LineGather(i, n, x_ref, buf, send, recv)

    def vector(src, other):
        return pltpu.make_async_remote_copy(
            src_ref=pack_ref, dst_ref=vec_ref.at[src], send_sem=v_send.at[other], recv_sem=v_recv.at[src],
            device_id={"dp": other // n, "tensor": other % n}, device_id_type=MESH)

    loop(total - 1, lambda s: vector(me, (me + s + 1) % total).start())
    line.start()
    weights = PlaneGather(row, m, [(wq_ref, wq_all, half_rows, row_blocks(m)), (wo_ref, wo_all, half_rows, column_blocks(m))],
                          w_send, w_recv, w_local)
    weights.start()
    own_copy = pltpu.make_async_copy(x_ref, buf.at[i], own_sem)
    own_copy.start()
    vec_ref[me] = pack_ref[...]
    loop(total - 1, lambda s: vector((me + s + 1) % total, me).wait_recv())
    depth = affine.shape[1]
    group = LANES // piece
    for tile in range(depth // LANES):
        value = vec_ref[tile * group, 0:2, :].astype(F32)
        for g in range(1, group):
            value = value + vec_ref[tile * group + g, 0:2, :].astype(F32)
        affine[0:2, tile * LANES : (tile + 1) * LANES] = value
    own_copy.wait()

    def compute(j):
        def norm(b):
            normal, _ = norm_stats(buf[j, rows_at(b, RB), :].astype(F32))
            here = pl.ds(pl.multiple_of(j * size + b * RB, RB), RB)
            n_ref[here, :] = normal.astype(BF)
            a_ref[here, :] = (normal * affine[0:1, :] + affine[1:2, :]).astype(BF)

        loop(size // RB, norm)
        for copy in leave(j):
            copy.start()

    def leave(j):
        here = rows_at(j, size)
        return [pltpu.make_async_copy(a_ref.at[here], a_hbm.at[here], out_sem.at[0, j]),
                pltpu.make_async_copy(n_ref.at[here], n_hbm.at[here], out_sem.at[1, j])]

    def left(j):
        for copy in leave(j):
            copy.wait()

    def between(r):
        for stage in range(1, weights.stages):
            @pl.when(r == stage)
            def _():
                weights.advance(stage)

    rounds(i, n, line, compute, between)
    line.finish()
    weights.finish()
    loop(n, left)
    loop(total - 1, lambda s: vector(me, (me + s + 1) % total).wait_send())


def attend_kernel(n, m, pieces, a_hbm, wq_hbm, wo_hbm, up_ref, down_ref, x_ref, cot_ref, bias, out_bias, gain, shift,
                  qkv_hbm, o_hbm, h_ref, c_ref, cot_all, up_all, down_all, w_send, w_recv, w_local, qkv_ref, o_ref, out_sem, a_ref, wq_ref, w_ref, part, land, send, recv, s_send, s_recv, own_sem, a_sem, w_sem):
    i, row = lax.axis_index("tensor"), lax.axis_index("dp")
    size = x_ref.shape[0]
    loads = [pltpu.make_async_copy(a_hbm, a_ref, a_sem)]
    loads += [pltpu.make_async_copy(wq_hbm.at[t], wq_ref.at[t], w_sem.at[t]) for t in range(3)]
    loads += [pltpu.make_async_copy(wo_hbm, w_ref, w_sem.at[3])]
    for load in loads:
        load.start()
    heads = qkv_ref.shape[2] // HD
    depth = w_ref.shape[1]
    greet_cross(i, n, row, m)
    line = LineGather(i, n, cot_ref, cot_all, send, recv)
    line.start()
    weights = PlaneGather(row, m, [(up_ref, up_all, half_rows, row_blocks(m)), (down_ref, down_all, half_rows, column_blocks(m))],
                          w_send, w_recv, w_local)
    weights.start()
    own_copy = pltpu.make_async_copy(cot_ref, cot_all.at[i], own_sem)
    own_copy.start()

    loads[0].wait()
    block = 256
    for t in range(3):
        loads[1 + t].wait()

        def project(b):
            here = rows_at(b, block)
            value = jnp.dot(a_ref[here, :], wq_ref[t], preferred_element_type=F32)
            if t != 1:
                value = value + bias[t // 2 : t // 2 + 1, :]
            qkv_ref[t, here, :] = value.astype(BF)

        loop(LEN // block, project)

    def head(t):
        cols = pl.ds(pl.multiple_of(t * HD, HD), HD)
        for b in range(LEN // block):
            here, keys = slice(b * block, (b + 1) * block), (b + 1) * block
            s = lax.dot_general(qkv_ref[0, here, cols], qkv_ref[1, 0:keys, cols], NT,
                                preferred_element_type=F32) * HD ** (-0.5)
            query = lax.broadcasted_iota(jnp.int32, s.shape, 0) + b * block
            s = jnp.where(query >= lax.broadcasted_iota(jnp.int32, s.shape, 1), s, -1e30)
            e = jnp.exp(s - jnp.max(s, axis=-1, keepdims=True))
            prob = (e / jnp.sum(e, axis=-1, keepdims=True)).astype(BF)
            o_ref[here, cols] = jnp.dot(prob, qkv_ref[2, 0:keys, cols], preferred_element_type=F32).astype(BF)

    loop(heads, head)
    leave = [pltpu.make_async_copy(qkv_ref, qkv_hbm, out_sem.at[0]), pltpu.make_async_copy(o_ref, o_hbm, out_sem.at[1])]
    for copy in leave:
        copy.start()
    loads[4].wait()
    sums = LineSum(i, n, part, land, s_send, s_recv, pieces)
    tile = 512

    def project(t):
        d = jnp.where(i < n // 2, n - 1 - t, t)

        def columns(k):
            cols = rows_at(k, tile)
            part[d, :, cols] = jnp.dot(o_ref[rows_at(d, size), :], w_ref[:, cols], preferred_element_type=F32).astype(BF)

        loop(depth // tile, columns)
        sums.launch(d)

    loop(n, project)
    weights.advance(1)
    for r in range(1, n):
        line.step(r)
        for stage in range(2, weights.stages):
            if r == min(2 * stage - 1, n - 1):
                weights.advance(stage)
        relays(sums, i, n, r)

    def norm(b):
        here = rows_at(b, RB)
        sums.add(here, h_ref.at[here, :])
        rows = h_ref[here, :] + (x_ref[here, :].astype(F32) + out_bias[...])
        h_ref[here, :] = rows
        normal, _ = norm_stats(rows)
        c_ref[here, :] = (normal * gain[...] + shift[...]).astype(BF)

    sums.own(norm)
    own_copy.wait()
    for copy in leave:
        copy.wait()
    weights.finish()
    line.finish()
    sums.finish()


def hidden_kernel(n, pieces, c_ref, h_ref, cot_hbm, up_hbm, down_hbm, up_bias, gain, c_hbm, g_hbm, du_hbm, mlp_hbm, dh_ref,
                  db_ref, vec_ref, upb_ref, c_all, g_all, du_all, cot_all, up, down, part, land, send, recv, s_send,
                  s_recv, w_sem, cot_sem, own_sem, c_sem, g_sem, du_sem, mlp, mlp_sem):
    i = lax.axis_index("tensor")
    size, depth = c_ref.shape
    units = up.shape[1]
    greet_neighbours(i, n)
    line = LineGather(i, n, c_ref, c_all, send, recv)
    line.start()
    own_copy = pltpu.make_async_copy(c_ref, c_all.at[i], own_sem)
    own_copy.start()
    up_copy = pltpu.make_async_copy(up_hbm, up, w_sem.at[0])
    up_copy.start()
    down_copy = pltpu.make_async_copy(down_hbm, down, w_sem.at[1])
    down_copy.start()
    cot_copy = pltpu.make_async_copy(cot_hbm, cot_all, cot_sem)
    cot_copy.start()
    upb_ref[...] = jnp.zeros_like(upb_ref)
    vec_ref[...] = jnp.zeros_like(vec_ref)
    own_copy.wait()
    up_copy.wait()
    down_copy.wait()
    cot_copy.wait()
    sums = LineSum(i, n, part, land, s_send, s_recv, pieces)
    tile = 256

    def out_copy(src, dst, sem, j):
        return pltpu.make_async_copy(src.at[j], dst.at[j], sem.at[j])

    def compute(j):
        def unit(k):
            cols = rows_at(k, tile)
            u = jnp.dot(c_all[j], up[:, cols], preferred_element_type=F32) + up_bias[0:1, cols]
            dg = lax.dot_general(cot_all[j], down[cols, :], NT, preferred_element_type=F32)
            half = 0.5 + 0.5 * lax.erf(u * (0.5 ** 0.5))
            g_all[j, :, cols] = (u * half).astype(BF)
            slope = half + u * (jnp.exp(u * u * -0.5) * 0.3989422804014327)
            du = (slope * dg).astype(BF)
            du_all[j, :, cols] = du
            upb_ref[0:1, cols] += jnp.sum(du.astype(F32), axis=0, keepdims=True)

        loop(units // tile, unit)

        def back(k):
            cols = rows_at(k, tile)
            part[j, :, cols] = lax.dot_general(du_all[j], up[cols, :], NT, preferred_element_type=F32).astype(BF)

        loop(depth // tile, back)
        sums.launch(j)
        out_copy(g_all, g_hbm, g_sem, j).start()
        out_copy(du_all, du_hbm, du_sem, j).start()
        out_copy(c_all, c_hbm, c_sem, j).start()

    rounds(i, n, line, compute)

    def forward(j):
        def columns(k):
            cols = rows_at(k, tile)
            mlp[j, :, cols] = jnp.dot(g_all[j], down[:, cols], preferred_element_type=F32).astype(BF)

        loop(depth // tile, columns)
        out_copy(mlp, mlp_hbm, mlp_sem, j).start()

    loop(n, forward)

    def relay(t):
        early = jnp.where(i < n // 2, 1, 0)
        sums.relay(t + 3 - early - i, 2 * n - 4 - i - t - early)

    loop(2 * n - 3, relay)

    def norm(b):
        here = rows_at(b, RB)
        sums.add(here, dh_ref.at[here, :])
        grad = dh_ref[here, :]
        normal, inverse = norm_stats(h_ref[here, :])
        vec_ref[0:1, :] += jnp.sum(grad * normal, axis=0, keepdims=True)
        vec_ref[1:2, :] += jnp.sum(grad, axis=0, keepdims=True)
        cot = cot_all[i, here, :].astype(F32)
        dh = cot + norm_back(grad, normal, inverse, gain[...])
        dh_ref[here, :] = dh
        db = dh.astype(BF)
        db_ref[here, :] = db
        vec_ref[2:3, :] += jnp.sum(db.astype(F32), axis=0, keepdims=True)
        vec_ref[3:4, :] += jnp.sum(cot, axis=0, keepdims=True)

    sums.own(norm)

    def done(j):
        out_copy(g_all, g_hbm, g_sem, j).wait()
        out_copy(du_all, du_hbm, du_sem, j).wait()
        out_copy(c_all, c_hbm, c_sem, j).wait()
        out_copy(mlp, mlp_hbm, mlp_sem, j).wait()

    loop(n, done)
    line.finish()
    sums.finish()


def attend_back(q_of, k_of, v_of, do_of, heads, put, dk, dv):
    block = 256
    factor = HD ** (-0.5)

    def head(t):
        dk[...] = jnp.zeros_like(dk)
        dv[...] = jnp.zeros_like(dv)
        for b in range(LEN // block):
            here, keys = slice(b * block, (b + 1) * block), slice(0, (b + 1) * block)
            q, k, v, do = q_of(here, t), k_of(keys, t), v_of(keys, t), do_of(here, t)
            s = lax.dot_general(q, k, NT, preferred_element_type=F32) * factor
            query = lax.broadcasted_iota(jnp.int32, s.shape, 0) + b * block
            s = jnp.where(query >= lax.broadcasted_iota(jnp.int32, s.shape, 1), s, -1e30)
            e = jnp.exp(s - jnp.max(s, axis=-1, keepdims=True))
            prob = e / jnp.sum(e, axis=-1, keepdims=True)
            dv[keys, :] += lax.dot_general(prob.astype(BF), do, TN, preferred_element_type=F32)
            dp = lax.dot_general(do, v, NT, preferred_element_type=F32)
            ds = (prob * (dp - jnp.sum(prob * dp, axis=-1, keepdims=True))).astype(BF)
            put(0, here, t, (jnp.dot(ds, k, preferred_element_type=F32) * factor).astype(BF))
            dk[keys, :] += lax.dot_general(ds, q, TN, preferred_element_type=F32)
        put(1, slice(0, LEN), t, (dk[...] * factor).astype(BF))
        put(2, slice(0, LEN), t, dv[...].astype(BF))

    loop(heads, head)


class PlaneSum:
    def __init__(self, row, m, out, terms, land, halves, send, recv, h_send, h_recv):
        self.row, self.m, self.out, self.terms, self.land, self.halves = row, m, out, terms, land, halves
        self.send, self.recv, self.h_send, self.h_recv = send, recv, h_send, h_recv
        bits = [1 << k for k in range(1, m.bit_length() - 1)]
        self.plan = []
        for order in (bits, bits[::-1]):
            left, at, stages = [e for e in range(m) if e % 2 == 0], 0, []
            for bit in order:
                out = [e for e in left if e & bit]
                stages.append((bit, [(e, e ^ bit, at + k) for k, e in enumerate(out)]))
                left, at = [e for e in left if not e & bit], at + len(out)
            self.plan.append(stages)
        self.stages = len(bits)

    def owner(self, e):
        d = self.row
        for k in range(self.m.bit_length() - 1):
            if e & (1 << k):
                d = d + (partner(self.row, 1 << k) - self.row)
        return d

    def whole(self, e):
        return pltpu.make_async_remote_copy(
            src_ref=self.out.at[e // 2], dst_ref=self.land.at[e // 2], send_sem=self.send.at[e // 2],
            recv_sem=self.recv.at[e // 2], device_id={"dp": partner(self.row, 1)}, device_id_type=MESH)

    def half(self, h, bit, e, at):
        size = self.halves.shape[2]
        return pltpu.make_async_remote_copy(
            src_ref=self.terms.at[e // 2, pl.ds(h * size, size)], dst_ref=self.halves.at[h, at],
            send_sem=self.h_send.at[h, at], recv_sem=self.h_recv.at[h, at],
            device_id={"dp": partner(self.row, bit)}, device_id_type=MESH)

    def merge(self):
        for e in range(0, self.m, 2):
            self.whole(e + 1).wait_recv()

            def add(b):
                here = rows_at(b, RB)
                total = self.terms[e // 2, here, :].astype(F32) + self.land[e // 2, here, :].astype(F32)
                self.terms[e // 2, here, :] = total.astype(BF)

            loop(self.terms.shape[1] // RB, add)

    def push(self, stage):
        for h in range(2):
            bit, moves = self.plan[h][stage]
            for e, _, at in moves:
                self.half(h, bit, e, at).start()

    def take(self, stage, out=None):
        size = self.halves.shape[2]
        for h in range(2):
            bit, moves = self.plan[h][stage]
            for e, into, at in moves:
                self.half(h, bit, e, at).wait_recv()

                def add(b):
                    here, there = rows_at(b, RB), pl.ds(pl.multiple_of(h * size + b * RB, RB), RB)
                    total = self.terms[into // 2, there, :].astype(F32) + self.halves[h, at, here, :].astype(F32)
                    if out is None:
                        self.terms[into // 2, there, :] = total.astype(BF)
                    else:
                        out(there, total)

                loop(size // RB, add)

    def sent(self):
        for e in range(1, self.m, 2):
            self.whole(e).wait_send()

    def finish(self):
        for h in range(2):
            for bit, moves in self.plan[h]:
                for e, _, at in moves:
                    self.half(h, bit, e, at).wait_send()


class VectorSum:
    def __init__(self, me, count, device, vectors, piece, land, out, send, recv):
        self.me, self.count, self.device, self.vectors, self.piece = me, count, device, vectors, piece
        self.land, self.out, self.send, self.recv = land, out, send, recv

    def lanes(self, owner):
        size = self.land.shape[2]
        return pl.ds(pl.multiple_of(owner * self.piece // size * size, size), size)

    def copy(self, src, other):
        return pltpu.make_async_remote_copy(
            src_ref=self.vectors.at[:, self.lanes(other)], dst_ref=self.land.at[src], send_sem=self.send.at[other],
            recv_sem=self.recv.at[src], device_id=self.device(other), device_id_type=MESH)

    def start(self):
        loop(self.count - 1, lambda s: self.copy(self.me, (self.me + s + 1) % self.count).start())

    def finish(self):
        self.out[...] = self.vectors[:, self.lanes(self.me)]

        def take(s):
            src = (self.me + s + 1) % self.count
            self.copy(src, self.me).wait_recv()
            self.out[...] += self.land[src]

        loop(self.count - 1, take)
        loop(self.count - 1, lambda s: self.copy(self.me, (self.me + s + 1) % self.count).wait_send())


def greet_cross(i, n, row, m):
    barrier = pltpu.get_barrier_semaphore()

    @pl.when(i > 0)
    def _():
        pl.semaphore_signal(barrier, inc=1, device_id={"tensor": i - 1}, device_id_type=MESH)

    @pl.when(i < n - 1)
    def _():
        pl.semaphore_signal(barrier, inc=1, device_id={"tensor": i + 1}, device_id_type=MESH)

    bits = [1 << k for k in range(m.bit_length() - 1)]
    for bit in bits:
        pl.semaphore_signal(barrier, inc=1, device_id={"dp": partner(row, bit)}, device_id_type=MESH)
    pl.semaphore_wait(barrier, jnp.minimum(i, 1) + jnp.minimum(n - 1 - i, 1) + len(bits))


def relays(sums, i, n, r):
    sums.relay(n - 1 + i - r, r - (n - 1 - i))


def block_terms(plane, e, pairs):
    size = plane.terms.shape[1]
    cols = rows_at(plane.owner(e), size)
    for lhs, rhs, first in pairs:
        width = rhs.shape[1]
        tile = min(512, width)

        def columns(k):
            there = pl.ds(pl.multiple_of(first + k * tile, tile), tile)
            (plane.out if e % 2 else plane.terms)[e // 2, :, there] = lax.dot_general(
                lhs[:, cols], rhs[:, rows_at(k, tile)], TN, preferred_element_type=F32).astype(BF)

        loop(width // tile, columns)


def branch_kernel(n, m, pieces, db_ref, h_ref, down_bias, mlp_hbm, g_hbm, cot_hbm, c_hbm, du_hbm, qkv_hbm, wo_hbm,
                  db_all, lo_ref, down_ref, up_ref, dqkv_hbm, dqkv_ref, out_sem, lhs, rhs, wo, dk, dv, part, land, out, terms_a, land_a,
                  half_a, terms_b, land_b, half_b, acc, send, recv, s_send, s_recv, own_sem, part_sem, in_sem, qkv_sem,
                  db_sem, p_send, p_recv, h_send, h_recv):
    i, row = lax.axis_index("tensor"), lax.axis_index("dp")
    size = db_ref.shape[0]
    width = wo.shape[0]
    greet_cross(i, n, row, m)
    line = LineGather(i, n, db_ref, db_all, send, recv)
    line.start()
    part_copy = pltpu.make_async_copy(mlp_hbm, part, part_sem)
    part_copy.start()
    own_copy = pltpu.make_async_copy(db_ref, db_all.at[i], own_sem)
    own_copy.start()

    def load(left, right):
        return [pltpu.make_async_copy(left, lhs, in_sem.at[0]), pltpu.make_async_copy(right, rhs, in_sem.at[1])]

    loads = load(cot_hbm, g_hbm)
    for copy in loads:
        copy.start()
    wo_copy = pltpu.make_async_copy(wo_hbm, wo, in_sem.at[2])
    wo_copy.start()
    sums = LineSum(i, n, part, land, s_send, s_recv, pieces)
    part_copy.wait()
    loop(n, lambda t: sums.launch(jnp.where(i < n // 2, n - 1 - t, t)))
    planes = [PlaneSum(row, m, out, terms_a, land_a, half_a, p_send.at[0], p_recv.at[0], h_send.at[0], h_recv.at[0]),
              PlaneSum(row, m, out, terms_b, land_b, half_b, p_send.at[1], p_recv.at[1], h_send.at[1], h_recv.at[1])]
    first, second = planes
    for copy in loads:
        copy.wait()
    left, right = lhs.at[:, 0 : lhs.shape[1]], rhs.at[:, 0 : down_ref.shape[1]]
    for e in range(1, m, 2):
        block_terms(first, e, [(left, right, 0)])
        first.whole(e).start()
    for e in range(m - 2, -1, -2):
        block_terms(first, e, [(left, right, 0)])
    loads = load(c_hbm, du_hbm)
    for copy in loads:
        copy.start()
    first.merge()
    first.push(0)
    first.sent()
    for copy in loads:
        copy.wait()
    for e in range(1, m, 2):
        block_terms(second, e, [(left, right, 0)])
        second.whole(e).start()

    line.step(1)
    for e in range(m - 2, -1, -2):
        block_terms(second, e, [(left, right, 0)])
    qkv_copies = [pltpu.make_async_copy(qkv_hbm.at[p], rhs.at[:, p * width : (p + 1) * width], qkv_sem.at[p])
                  for p in range(3)]
    for copy in qkv_copies:
        copy.start()
    second.merge()
    second.push(0)
    own_copy.wait()
    wo_copy.wait()

    def mixture_back(j):
        here = rows_at(j, size)
        copy = pltpu.make_async_copy(db_all.at[j], lhs.at[here], db_sem.at[j])
        copy.start()
        copy.wait()
        rhs[here, 3 * width : 4 * width] = lax.dot_general(
            lhs[here, :], wo[...], NT, preferred_element_type=F32).astype(BF)

    def round_back(r):
        def side(s):
            j = jnp.where(s == 0, i - r, i + r)

            @pl.when(jnp.logical_and(j >= 0, j <= n - 1))
            def _():
                mixture_back(j)

        loop(2, side)

    def keep(ref):
        def put(here, total):
            ref[here, :] = total

        return put

    def advance(plane, stage, ref):
        if stage < plane.stages - 1:
            plane.take(stage)
            plane.push(stage + 1)
        else:
            plane.take(stage, keep(ref))

    mixture_back(i)
    round_back(1)
    advance(first, 0, down_ref)
    for r in range(2, n):
        line.step(r)
        relays(sums, i, n, r - 1)
        round_back(r)
        if r == 2:
            advance(second, 0, up_ref)
    if n == 2:
        advance(second, 0, up_ref)
    relays(sums, i, n, n - 1)
    for copy in qkv_copies:
        copy.wait()

    def column(p):
        def get(here, t):
            return rhs[here, pl.ds(pl.multiple_of(p * width + t * HD, HD), HD)]

        return get

    def put(p, here, t, value):
        dqkv_ref[p, here, pl.ds(pl.multiple_of(t * HD, HD), HD)] = value

    attend_back(column(0), column(1), column(2), column(3), width // HD, put, dk, dv)
    leave = pltpu.make_async_copy(dqkv_ref, dqkv_hbm, out_sem)
    leave.start()
    for stage in range(1, first.stages):
        advance(first, stage, down_ref)
        advance(second, stage, up_ref)

    def output(b):
        here = rows_at(b, RB)
        sums.add(here, acc)
        lo_ref[here, :] = (h_ref[here, :] + (acc[...] + down_bias[...])).astype(BF)

    sums.own(output)
    line.finish()
    sums.finish()
    second.sent()
    for plane in planes:
        plane.finish()
    leave.wait()


def input_kernel(n, m, pieces, widths, dqkv_ref, wq_hbm, x_hbm, dh_hbm, gain, early_ref, up_ref, a_hbm, db_hbm, o_hbm,
                 n_hbm, gt_ref, gqkv_ref, gout_ref, early_out, late_out, up_out, qv_out, vec_ref, qv_ref, wq, a_ref, db_ref,
                 o_ref, n_ref, x_ref, dh_ref, part, land, out_p, terms, land_p, half_p, acc, early_land, late_land, up_land, qv_land, s_send,
                 s_recv, in_sem, p_send, p_recv, h_send, h_recv, e_send, e_recv, l_send, l_recv, u_send, u_recv, q_send,
                 q_recv):
    i, row = lax.axis_index("tensor"), lax.axis_index("dp")
    me, total_devices = row * n + i, m * n
    size = x_hbm.shape[0]
    width = dqkv_ref.shape[2]
    piece, up_piece, qv_piece = widths
    depth = part.shape[2]
    loads = [pltpu.make_async_copy(src, dst, in_sem.at[k]) for k, (src, dst) in enumerate(
        [(wq_hbm, wq), (a_hbm, a_ref), (db_hbm, db_ref), (o_hbm, o_ref), (n_hbm, n_ref), (x_hbm, x_ref), (dh_hbm, dh_ref)])]
    loads[0].start()
    loads[4].start()
    greet_all(me, n, total_devices)
    every = [VectorSum(me, total_devices, lambda g: {"dp": g // n, "tensor": g % n}, early_ref, piece, early_land, early_out,
                       e_send, e_recv),
             VectorSum(me, total_devices, lambda g: {"dp": g // n, "tensor": g % n}, vec_ref, piece, late_land, late_out,
                       l_send, l_recv)]
    column = [VectorSum(row, m, lambda g: {"dp": g}, up_ref, up_piece, up_land, up_out, u_send, u_recv),
              VectorSum(row, m, lambda g: {"dp": g}, qv_ref, qv_piece, qv_land, qv_out, q_send, q_recv)]
    every[0].start()
    column[0].start()
    sums = LineSum(i, n, part, land, s_send, s_recv, pieces)
    vec_ref[...] = jnp.zeros_like(vec_ref)
    qv_ref[...] = jnp.zeros_like(qv_ref)
    loads[0].wait()
    loads[4].wait()
    for k in (1, 2, 3, 5, 6):
        loads[k].start()
    tile = 512

    def term(t):
        d = jnp.where(i < n // 2, n - 1 - t, t)
        here = rows_at(d, size)

        def columns(k):
            cols = rows_at(k, tile)
            total = lax.dot_general(dqkv_ref[0, here, :], wq[0, cols, :], NT, preferred_element_type=F32)
            for p in range(1, 3):
                total += lax.dot_general(dqkv_ref[p, here, :], wq[p, cols, :], NT, preferred_element_type=F32)
            part[d, :, cols] = total.astype(BF)
            vec_ref[0:1, cols] += jnp.sum(total * n_ref[here, cols].astype(F32), axis=0, keepdims=True)
            vec_ref[1:2, cols] += jnp.sum(total, axis=0, keepdims=True)

        loop(depth // tile, columns)

        @pl.when(t == 0)
        def _():
            sums.launch(d)

        for p in range(2):
            qv_ref[p : p + 1, :] += jnp.sum(dqkv_ref[2 * p, here, :].astype(F32), axis=0, keepdims=True)

    loop(n, term)
    every[1].start()
    column[1].start()
    loop(n - 1, lambda t: sums.launch(jnp.where(i < n // 2, n - 2 - t, t + 1)))
    for k in (1, 2, 3, 5, 6):
        loads[k].wait()
    plane = PlaneSum(row, m, out_p, terms, land_p, half_p, p_send, p_recv, h_send, h_recv)
    pairs = [(a_ref, dqkv_ref.at[p], p * width) for p in range(3)] + [(db_ref, o_ref, 3 * width)]
    for e in range(1, m, 2):
        block_terms(plane, e, pairs)
        plane.whole(e).start()
    for e in range(m - 2, -1, -2):
        block_terms(plane, e, pairs)
    plane.merge()
    plane.push(0)

    def out(here, total):
        for p in range(3):
            gqkv_ref[p, here, :] = total[:, p * width : (p + 1) * width]
        gout_ref[here, :] = total[:, 3 * width :]

    stage = 0
    for r in range(1, n):
        relays(sums, i, n, r)
        if r > 1 and stage < plane.stages:
            if stage < plane.stages - 1:
                plane.take(stage)
                plane.push(stage + 1)
            else:
                plane.take(stage, out)
            stage += 1

    def norm(b):
        here = rows_at(b, RB)
        sums.add(here, acc)
        grad = acc[...]
        normal, inverse = norm_stats(x_ref[here, :].astype(F32))
        gt_ref[here, :] = (dh_ref[here, :] + norm_back(grad, normal, inverse, gain[...])).astype(BF)

    while stage < plane.stages:
        if stage < plane.stages - 1:
            plane.take(stage)
            plane.push(stage + 1)
        else:
            plane.take(stage, out)
        stage += 1
    for group in (every[0], column[0], column[1], every[1]):
        group.finish()
    sums.own(norm)
    sums.finish()
    plane.sent()
    plane.finish()


def params(collective=None):
    if collective is None:
        return pltpu.CompilerParams(vmem_limit_bytes=BIG)
    return pltpu.CompilerParams(vmem_limit_bytes=BIG, collective_id=collective, has_side_effects=True)


def shape(dims, dtype):
    return jax.ShapeDtypeStruct(dims, dtype)


def body(tokens, cotangent, ln1_gain, ln1_bias, qkv_weight, qv_bias, out_weight, out_bias, ln2_gain, ln2_bias,
         up_weight, up_bias, down_weight, down_bias):
    n = lax.axis_size("tensor")
    m = lax.axis_size("dp")
    i, row = lax.axis_index("tensor"), lax.axis_index("dp")
    size, depth = tokens.shape
    width = qkv_weight.shape[2]
    units = up_weight.shape[1]
    piece, qv_piece, up_piece = ln1_gain.shape[0], qv_bias.shape[1], up_bias.shape[0]
    total = m * n

    def lane_rows(value, index):
        count = value.shape[-1]
        if count >= LANES:
            return value.reshape(-1, LANES)
        places = LANES // count
        spread = jnp.tile(value.reshape(-1, count), (1, places))
        return jnp.where((jnp.arange(LANES) // count)[None] == index % places, spread, 0)

    me = row * n + i
    whole = jnp.stack([ln1_gain, ln1_bias, out_bias, ln2_gain, ln2_bias, down_bias])
    pack = jnp.concatenate([lane_rows(whole, me), lane_rows(qv_bias, row), lane_rows(up_bias, row)])
    pack = jnp.pad(pack, ((0, -pack.shape[0] % 16), (0, 0)))
    lanes_up = 8 + max(up_piece // LANES, 1)

    dma = pltpu.SemaphoreType.DMA
    weight_sems = [dma((2, 2, m - 1)), dma((2, 2, m)), dma((2, 2))]
    attn_in, normal_one, vecs, w_qkv, w_out = pl.pallas_call(
        functools.partial(tokens_kernel, n, m, piece),
        out_shape=(shape((LEN, depth), BF), shape((LEN, depth), BF), shape((total,) + pack.shape, BF),
                   shape((3, depth, width), BF), shape((width, depth), BF)),
        in_specs=[VM] * 4, out_specs=(ANY, ANY, VM, ANY, ANY),
        scratch_shapes=[pltpu.VMEM((n, size, depth), BF), pltpu.VMEM((8, depth), F32), pltpu.VMEM((LEN, depth), BF),
                        pltpu.VMEM((LEN, depth), BF), dma((2, n))] + weight_sems + [dma, dma((2, n, LineGather.PIECES)), dma((n, LineGather.PIECES)),
                        dma((total,)), dma((total,))],
        compiler_params=params(0), name="gather_tokens",
    )(pack, tokens, qkv_weight, out_weight)
    vecs = vecs.astype(F32)

    def whole_rows(block, count):
        if count < LANES:
            block = block.reshape(-1, LANES // count, *block.shape[1:]).sum(axis=1)
        return block

    vectors = whole_rows(vecs[:, 0:6], piece).transpose(1, 0, 2).reshape(6, 1, depth)
    gain_one, shift_one, bias_out, gain_two, shift_two, bias_down = [vectors[j] for j in range(6)]
    mine = lax.dynamic_index_in_dim(vecs.reshape(m, n, -1, LANES), i, 1, keepdims=False)
    bias_qv = whole_rows(mine[:, 6:8], qv_piece).transpose(1, 0, 2).reshape(2, width)
    bias_up = whole_rows(mine[:, 8:lanes_up], up_piece).reshape(1, units)

    pieces = 2
    sums = [pltpu.VMEM((n, size, depth), BF), pltpu.VMEM((n + 1, size, depth), BF)]
    qkv, mixture, residual, mlp_own, cot_all, w_up, w_down = pl.pallas_call(
        functools.partial(attend_kernel, n, m, pieces),
        out_shape=(shape((3, LEN, width), BF), shape((LEN, width), BF), shape((size, depth), F32),
                   shape((size, depth), BF), shape((n, size, depth), BF), shape((depth, units), BF), shape((units, depth), BF)),
        in_specs=[ANY] * 3 + [VM] * 8, out_specs=(ANY, ANY, VM, VM, ANY, ANY, ANY),
        scratch_shapes=weight_sems + [pltpu.VMEM((3, LEN, width), BF), pltpu.VMEM((LEN, width), BF), dma((2,)),
                        pltpu.VMEM((LEN, depth), BF), pltpu.VMEM((3, depth, width), BF), pltpu.VMEM((width, depth), BF)] +
                       sums + [dma((2, n, LineGather.PIECES)), dma((n, LineGather.PIECES)), dma((n, pieces)), dma((n + 1, pieces)), dma, dma, dma((4,))],
        compiler_params=params(1), name="attend",
    )(attn_in, w_qkv, w_out, up_weight, down_weight, tokens, cotangent, bias_qv, bias_out, gain_two, shift_two)

    pieces = size // RB
    mlp_in, hidden, grad_pre, mlp_part, grad_resid, branch_cot, vec_two, grad_up_b = pl.pallas_call(
        functools.partial(hidden_kernel, n, pieces),
        out_shape=(shape((n, size, depth), BF), shape((n, size, units), BF), shape((n, size, units), BF),
                   shape((n, size, depth), BF), shape((size, depth), F32), shape((size, depth), BF),
                   shape((8, depth), F32), shape((8, units), F32)),
        in_specs=[VM, VM, ANY, ANY, ANY, VM, VM], out_specs=(ANY, ANY, ANY, ANY, VM, VM, VM, VM),
        scratch_shapes=[pltpu.VMEM((n, size, depth), BF), pltpu.VMEM((n, size, units), BF),
                        pltpu.VMEM((n, size, units), BF), pltpu.VMEM((n, size, depth), BF),
                        pltpu.VMEM((depth, units), BF), pltpu.VMEM((units, depth), BF)] + sums +
                       [dma((2, n, LineGather.PIECES)), dma((n, LineGather.PIECES)), dma((n, pieces)), dma((n + 1, pieces)), dma((2,)), dma, dma,
                        dma((n,)), dma((n,)), dma((n,)), pltpu.VMEM((n, size, depth), BF), dma((n,))],
        compiler_params=params(2), name="hidden",
    )(mlp_own, residual, cot_all, w_up, w_down, bias_up, gain_two)
    mlp_in, hidden, grad_pre, cot_rows = [v.reshape(LEN, -1) for v in (mlp_in, hidden, grad_pre, cot_all)]

    def plane_scratch(columns):
        rows = depth // m
        return [pltpu.VMEM((m // 2, rows, columns), BF), pltpu.VMEM((m // 2, rows, columns), BF),
                pltpu.VMEM((2, m // 2 - 1, rows // 2, columns), BF)]

    pieces = 2
    sum_sems = [dma((n, pieces)), dma((n + 1, pieces))]
    attn_cot, layer_out, grad_down_w, grad_up_w, grad_qkv = pl.pallas_call(
        functools.partial(branch_kernel, n, m, pieces),
        out_shape=(shape((n, size, depth), BF), shape((size, depth), BF), shape((depth // m, units), F32),
                   shape((depth // m, units), F32), shape((3, LEN, width), BF)),
        in_specs=[VM] * 3 + [ANY] * 7, out_specs=(ANY, VM, VM, VM, ANY),
        scratch_shapes=[pltpu.VMEM((3, LEN, width), BF), dma, pltpu.VMEM((LEN, depth), BF), pltpu.VMEM((LEN, units), BF), pltpu.VMEM((width, depth), BF),
                        pltpu.VMEM((LEN, HD), F32), pltpu.VMEM((LEN, HD), F32)] + sums +
                       [pltpu.VMEM((m // 2, depth // m, units), BF)] + plane_scratch(units) * 2 +
                       [pltpu.VMEM((RB, depth), F32), dma((2, n, LineGather.PIECES)), dma((n, LineGather.PIECES))] + sum_sems +
                       [dma, dma, dma((3,)), dma((3,)), dma((n,)), dma((2, m // 2)), dma((2, m // 2)),
                        dma((2, 2, m // 2 - 1)), dma((2, 2, m // 2 - 1))],
        compiler_params=params(4), name="branch",
    )(branch_cot, residual, bias_down, mlp_part, hidden, cot_rows, mlp_in, grad_pre, qkv, w_out)
    attn_cot = attn_cot.reshape(LEN, depth)

    tiles = [max(v, LANES) for v in (piece, up_piece, qv_piece)]
    grad_tokens, grad_qkv_w, grad_out_w, early, late, grad_up_b, grad_qv_b = pl.pallas_call(
        functools.partial(input_kernel, n, m, pieces, (piece, up_piece, qv_piece)),
        out_shape=(shape((size, depth), BF), shape((3, depth // m, width), F32), shape((depth // m, width), F32),
                   shape((8, tiles[0]), F32), shape((8, tiles[0]), F32), shape((8, tiles[1]), F32),
                   shape((8, tiles[2]), F32)),
        in_specs=[VM, ANY, ANY, ANY, VM, VM, VM, ANY, ANY, ANY, ANY], out_specs=(VM,) * 7,
        scratch_shapes=[pltpu.VMEM((8, depth), F32), pltpu.VMEM((8, width), F32),
                        pltpu.VMEM((3, depth, width), BF), pltpu.VMEM((LEN, depth), BF), pltpu.VMEM((LEN, depth), BF),
                        pltpu.VMEM((LEN, width), BF), pltpu.VMEM((LEN, depth), BF), pltpu.VMEM((size, depth), BF),
                        pltpu.VMEM((size, depth), F32)] + sums +
                       [pltpu.VMEM((m // 2, depth // m, 4 * width), BF)] +
                       plane_scratch(4 * width) +
                       [pltpu.VMEM((RB, depth), F32), pltpu.VMEM((total, 8, tiles[0]), F32),
                        pltpu.VMEM((total, 8, tiles[0]), F32), pltpu.VMEM((m, 8, tiles[1]), F32),
                        pltpu.VMEM((m, 8, tiles[2]), F32)] + sum_sems +
                       [dma((7,)), dma((m // 2,)), dma((m // 2,)), dma((2, m // 2 - 1)), dma((2, m // 2 - 1))] +
                       [dma((total,))] * 4 + [dma((m,))] * 4,
        compiler_params=params(5), name="input",
    )(grad_qkv, w_qkv, tokens, grad_resid, gain_one, vec_two, grad_up_b, attn_in, attn_cot, mixture, normal_one)
    grad_down_w, grad_out_w = grad_down_w.T, grad_out_w.T

    def own_lanes(block, index, count):
        return lax.dynamic_slice_in_dim(block, index * count % block.shape[1], count, axis=1)

    early, late = own_lanes(early, me, piece), own_lanes(late, me, piece)
    vectors = [late[0], late[1], early[2], early[0], early[1], early[3]]
    grad_qv_b = own_lanes(grad_qv_b, row, qv_piece)[:2]
    grad_up_b = own_lanes(grad_up_b, row, up_piece)[0]
    return (layer_out, grad_tokens, vectors[0], vectors[1], grad_qkv_w, grad_qv_b, grad_out_w, vectors[2],
            vectors[3], vectors[4], grad_up_w, grad_up_b, grad_down_w, vectors[5])


def solution(mesh):
    vector, matrix = P(("dp", "tensor")), P(("dp", "tensor"), None)
    in_specs = (matrix, matrix, vector, vector, P(None, "dp", "tensor"), P(None, ("tensor", "dp")), P("tensor", "dp"),
                vector, vector, vector, P("dp", "tensor"), P(("tensor", "dp")), P("tensor", "dp"), vector)
    out_specs = (matrix, matrix, vector, vector, P(None, "dp", "tensor"), P(None, ("tensor", "dp")),
                 P("tensor", "dp"), vector, vector, vector, P("dp", "tensor"), P(("tensor", "dp")), P("tensor", "dp"),
                 vector)
    return jax.shard_map(body, mesh=mesh, in_specs=in_specs, out_specs=out_specs, check_vma=False)
```

```python
import functools

import jax
import jax.numpy as jnp
from jax import lax
from jax.experimental import pallas as pl
from jax.experimental.pallas import tpu as pltpu
from jax.sharding import PartitionSpec as P

HD = 128
LEN = 1024
LANES = 128
EPS = 1e-05
BF = jnp.bfloat16
F32 = jnp.float32
MESH = pl.DeviceIdType.MESH
ANY = pl.BlockSpec(memory_space=pl.ANY)
VM = pl.BlockSpec(memory_space=pltpu.VMEM)
NT = (((1,), (1,)), ((), ()))
TN = (((0,), (0,)), ((), ()))
BIG = 64 * 1024 * 1024 - 65536
RB = 32


def norm_stats(rows):
    mean = jnp.mean(rows, axis=-1, keepdims=True)
    centred = rows - mean
    variance = jnp.mean(centred * centred, axis=-1, keepdims=True)
    inverse = lax.rsqrt(variance + EPS)
    return centred * inverse, inverse


def norm_back(grad_rows, normal_rows, inverse, gain):
    scaled = grad_rows * gain
    first = jnp.mean(scaled, axis=-1, keepdims=True)
    second = jnp.mean(scaled * normal_rows, axis=-1, keepdims=True)
    return inverse * (scaled - first - normal_rows * second)


def loop(count, step):
    def run(i, carry):
        step(i)
        return carry

    lax.fori_loop(0, count, run, 0)


def rows_at(j, size):
    return pl.ds(pl.multiple_of(j * size, size), size)


def remote(src, dst, send, recv, target):
    return pltpu.make_async_remote_copy(src_ref=src, dst_ref=dst, send_sem=send, recv_sem=recv,
                                        device_id={"tensor": target}, device_id_type=MESH)


def greet_neighbours(i, n):
    barrier = pltpu.get_barrier_semaphore()

    @pl.when(i > 0)
    def _():
        pl.semaphore_signal(barrier, inc=1, device_id={"tensor": i - 1}, device_id_type=MESH)

    @pl.when(i < n - 1)
    def _():
        pl.semaphore_signal(barrier, inc=1, device_id={"tensor": i + 1}, device_id_type=MESH)

    pl.semaphore_wait(barrier, jnp.minimum(i, 1) + jnp.minimum(n - 1 - i, 1))


def greet_all(me, n, total):
    barrier = pltpu.get_barrier_semaphore()

    def greet(s):
        other = (me + s + 1) % total
        pl.semaphore_signal(barrier, inc=1, device_id={"dp": other // n, "tensor": other % n}, device_id_type=MESH)

    loop(total - 1, greet)
    pl.semaphore_wait(barrier, total - 1)


def rounds(i, n, line, compute, between=None):
    def round_of(r):
        @pl.when(r > 0)
        def _():
            line.step(r)

        if between is not None:
            between(r)

        def side(s):
            j = jnp.where(s == 0, i - r, i + r)

            @pl.when(jnp.logical_and(jnp.logical_and(j >= 0, j <= n - 1), s * r == s * jnp.maximum(r, 1)))
            def _():
                compute(j)

        loop(2, side)

    loop(n, round_of)


class LineGather:
    PIECES = 2

    def __init__(self, i, n, own, buf, send, recv):
        self.i, self.n, self.own, self.buf, self.send, self.recv = i, n, own, buf, send, recv
        self.size = own.shape[0] // self.PIECES

    def copy(self, src, j, side, s, target):
        here = pl.ds(s * self.size, self.size)
        return remote(src.at[here], self.buf.at[j, here], self.send.at[side, j, s], self.recv.at[j, s], target)

    def start(self):
        i, n = self.i, self.n
        for s in range(self.PIECES):
            @pl.when(i < n - 1)
            def _():
                self.copy(self.own, i, 0, s, i + 1).start()

            @pl.when(i > 0)
            def _():
                self.copy(self.own, i, 1, s, i - 1).start()

    def step(self, r):
        i, n = self.i, self.n
        for s in range(self.PIECES):
            @pl.when(i - r >= 0)
            def _():
                self.copy(self.own, i - r, 0, s, i).wait_recv()

                @pl.when(i < n - 1)
                def _():
                    self.copy(self.buf.at[i - r], i - r, 0, s, i + 1).start()

            @pl.when(i + r <= n - 1)
            def _():
                self.copy(self.own, i + r, 1, s, i).wait_recv()

                @pl.when(i > 0)
                def _():
                    self.copy(self.buf.at[i + r], i + r, 1, s, i - 1).start()

    def finish(self):
        i, n = self.i, self.n

        def one(j):
            for s in range(self.PIECES):
                @pl.when(jnp.logical_and(i < n - 1, j <= i))
                def _():
                    self.copy(self.own, j, 0, s, i + 1).wait_send()

                @pl.when(jnp.logical_and(i > 0, j >= i))
                def _():
                    self.copy(self.own, j, 1, s, i - 1).wait_send()

        loop(n, one)


class LineSum:
    def __init__(self, i, n, part, land, send, recv, pieces):
        self.i, self.n, self.part, self.land, self.send, self.recv = i, n, part, land, send, recv
        self.pieces = pieces
        self.size = part.shape[1] // pieces

    def copy(self, src, d, right, s):
        i, n = self.i, self.n
        target = i + 1 if right else i - 1
        slot = d if right else jnp.where(d == target, n, d)
        here = rows_at(s, self.size)
        return remote(src.at[d, here], self.land.at[slot, here], self.send.at[d, s], self.recv.at[slot, s], target)

    def arrived(self, slot, s):
        here = rows_at(s, self.size)
        remote(self.part.at[0, here], self.land.at[slot, here], self.send.at[0, s], self.recv.at[slot, s],
               self.i).wait_recv()

    def launch(self, d):
        i, n = self.i, self.n

        @pl.when(jnp.logical_and(i == 0, d > 0))
        def _():
            loop(self.pieces, lambda s: self.copy(self.part, d, True, s).start())

        @pl.when(jnp.logical_and(i == n - 1, d < n - 1))
        def _():
            loop(self.pieces, lambda s: self.copy(self.part, d, False, s).start())

    def relay(self, right, left):
        i, n = self.i, self.n

        def move(d, to_right, s):
            self.arrived(d, s)
            here = rows_at(s, self.size)
            total = self.land[d, here, :].astype(F32) + self.part[d, here, :].astype(F32)
            self.land[d, here, :] = total.astype(BF)
            self.copy(self.land, d, to_right, s).start()

        first = jnp.where(i < n // 2, 0, 1)

        def one(s):
            turn, s = (s + first) % 2, s // 2

            @pl.when(jnp.logical_and(turn == 0, jnp.logical_and(i > 0, jnp.logical_and(right > i, right <= n - 1))))
            def _():
                move(right, True, s)

            @pl.when(jnp.logical_and(turn == 1, jnp.logical_and(i < n - 1, jnp.logical_and(left >= 0, left < i))))
            def _():
                move(left, False, s)

        loop(2 * self.pieces, one)

    def own(self, step):
        i, n = self.i, self.n

        def one(s):
            @pl.when(i > 0)
            def _():
                self.arrived(i, s)

            @pl.when(i < n - 1)
            def _():
                self.arrived(n, s)

            loop(self.size // RB, lambda b: step(s * (self.size // RB) + b))

        loop(self.pieces, one)

    def add(self, here, out):
        i, n = self.i, self.n
        out[...] = self.part[i, here, :].astype(F32)

        @pl.when(i > 0)
        def _():
            out[...] += self.land[i, here, :].astype(F32)

        @pl.when(i < n - 1)
        def _():
            out[...] += self.land[n, here, :].astype(F32)

    def finish(self):
        i, n = self.i, self.n

        def one(d):
            @pl.when(jnp.logical_and(i < n - 1, d > i))
            def _():
                loop(self.pieces, lambda s: self.copy(self.part, d, True, s).wait_send())

            @pl.when(jnp.logical_and(i > 0, d < i))
            def _():
                loop(self.pieces, lambda s: self.copy(self.part, d, False, s).wait_send())

        loop(n, one)


def partner(row, bit):
    return row + bit * (1 - 2 * ((row // bit) % 2))


class PlaneGather:
    def __init__(self, row, m, items, send, recv, local):
        self.row, self.m, self.items, self.send, self.recv, self.local = row, m, items, send, recv, local
        bits = [1 << k for k in range(1, m.bit_length() - 1)]
        self.plan = []
        for order in (bits + [1], bits[::-1] + [1]):
            have, at, stages = [0], 0, []
            for bit in order:
                stages.append((bit, [(e, at + k) for k, e in enumerate(have)]))
                at, have = at + len(have), have + [e ^ bit for e in have]
            self.plan.append(stages)
        self.stages = len(bits) + 1

    def owner(self, e):
        d = self.row
        for k in range(self.m.bit_length() - 1):
            if e & (1 << k):
                d = d + (partner(self.row, 1 << k) - self.row)
        return d

    def copies(self, stage):
        for k, (own, whole, own_half, half) in enumerate(self.items):
            for h in range(2):
                bit, moves = self.plan[h][stage]
                for e, at in moves:
                    there = half(whole, self.owner(e), h)
                    src = own_half(own, h) if e == 0 else there
                    yield pltpu.make_async_remote_copy(
                        src_ref=src, dst_ref=there, send_sem=self.send.at[k, h, at], recv_sem=self.recv.at[k, h, e ^ bit],
                        device_id={"dp": partner(self.row, bit)}, device_id_type=MESH)

    def landed(self, stage):
        for k, (own, whole, own_half, half) in enumerate(self.items):
            for h in range(2):
                bit, moves = self.plan[h][stage]
                for e, at in moves:
                    there = half(whole, self.owner(e ^ bit), h)
                    pltpu.make_async_remote_copy(
                        src_ref=there, dst_ref=there, send_sem=self.send.at[k, h, at], recv_sem=self.recv.at[k, h, e ^ bit],
                        device_id={"dp": partner(self.row, bit)}, device_id_type=MESH).wait_recv()

    def locals(self):
        return [pltpu.make_async_copy(own_half(own, h), half(whole, self.row, h), self.local.at[k, h])
                for k, (own, whole, own_half, half) in enumerate(self.items) for h in range(2)]

    def start(self):
        for copy in self.copies(0):
            copy.start()
        for copy in self.locals():
            copy.start()

    def advance(self, stage):
        self.landed(stage - 1)
        for copy in self.copies(stage):
            copy.start()

    def finish(self):
        self.landed(self.stages - 1)
        for stage in range(self.stages):
            for copy in self.copies(stage):
                copy.wait_send()
        for copy in self.locals():
            copy.wait()


def half_rows(own, h):
    size = own.shape[-2] // 2
    return own.at[..., pl.ds(h * size, size), :]


def row_blocks(m):
    def half(whole, d, h):
        size = whole.shape[-2] // m // 2
        return whole.at[..., pl.ds(pl.multiple_of((2 * d + h) * size, size), size), :]

    return half


def column_blocks(m):
    def half(whole, d, h):
        size, width = whole.shape[-2] // 2, whole.shape[-1] // m
        return whole.at[pl.ds(h * size, size), pl.ds(pl.multiple_of(d * width, width), width)]

    return half


def tokens_kernel(n, m, widths, pack_ref, x_ref, wq_ref, wo_ref, a_hbm, n_hbm, affine, qv_bias, up_bias, wq_all, wo_all,
                  vec_ref, buf, a_ref, n_ref, out_sem, w_send, w_recv, w_local, own_sem, send, recv, v_send, v_recv):
    i, row = lax.axis_index("tensor"), lax.axis_index("dp")
    me, total = row * n + i, m * n
    size = x_ref.shape[0]
    greet_all(me, n, total)
    line = LineGather(i, n, x_ref, buf, send, recv)

    def vector(src, other):
        return pltpu.make_async_remote_copy(
            src_ref=pack_ref, dst_ref=vec_ref.at[src], send_sem=v_send.at[other], recv_sem=v_recv.at[src],
            device_id={"dp": other // n, "tensor": other % n}, device_id_type=MESH)

    loop(total - 1, lambda s: vector(me, (me + s + 1) % total).start())
    line.start()
    weights = PlaneGather(row, m, [(wq_ref, wq_all, half_rows, row_blocks(m)), (wo_ref, wo_all, half_rows, column_blocks(m))],
                          w_send, w_recv, w_local)
    weights.start()
    own_copy = pltpu.make_async_copy(x_ref, buf.at[i], own_sem)
    own_copy.start()
    vec_ref[me] = pack_ref[...]
    loop(total - 1, lambda s: vector((me + s + 1) % total, me).wait_recv())
    piece, qv_piece, up_piece = widths

    def assemble(out, piece, first, rows, device):
        group = max(LANES // piece, 1)
        split = max(piece // LANES, 1)
        for tile in range(out.shape[1] // LANES):
            if split > 1:
                at = first + tile % split
                value = vec_ref[device(tile // split), at : at + 1, :].astype(F32)
            else:
                value = vec_ref[device(tile * group), first : first + rows, :].astype(F32)
                for g in range(1, group):
                    value = value + vec_ref[device(tile * group + g), first : first + rows, :].astype(F32)
            out[0:rows, tile * LANES : (tile + 1) * LANES] = value

    assemble(affine, piece, 0, 6, lambda g: g)
    assemble(qv_bias, qv_piece, 6, 2, lambda d: d * n + i)
    assemble(up_bias, up_piece, 8, 1, lambda d: d * n + i)
    own_copy.wait()

    def compute(j):
        def norm(b):
            normal, _ = norm_stats(buf[j, rows_at(b, RB), :].astype(F32))
            here = pl.ds(pl.multiple_of(j * size + b * RB, RB), RB)
            n_ref[here, :] = normal.astype(BF)
            a_ref[here, :] = (normal * affine[0:1, :] + affine[1:2, :]).astype(BF)

        loop(size // RB, norm)
        for copy in leave(j):
            copy.start()

    def leave(j):
        here = rows_at(j, size)
        return [pltpu.make_async_copy(a_ref.at[here], a_hbm.at[here], out_sem.at[0, j]),
                pltpu.make_async_copy(n_ref.at[here], n_hbm.at[here], out_sem.at[1, j])]

    def left(j):
        for copy in leave(j):
            copy.wait()

    def between(r):
        for stage in range(1, weights.stages):
            @pl.when(r == stage)
            def _():
                weights.advance(stage)

    rounds(i, n, line, compute, between)
    line.finish()
    weights.finish()
    loop(n, left)
    loop(total - 1, lambda s: vector(me, (me + s + 1) % total).wait_send())


def attend_kernel(n, m, pieces, a_hbm, wq_hbm, wo_hbm, up_ref, down_ref, x_ref, cot_ref, bias, vec,
                  qkv_hbm, o_hbm, h_ref, c_ref, cot_all, up_all, down_all, w_send, w_recv, w_local, qkv_ref, o_ref, out_sem, a_ref, wq_ref, w_ref, part, land, send, recv, s_send, s_recv, own_sem, a_sem, w_sem):
    i, row = lax.axis_index("tensor"), lax.axis_index("dp")
    size = x_ref.shape[0]
    loads = [pltpu.make_async_copy(a_hbm, a_ref, a_sem)]
    loads += [pltpu.make_async_copy(wq_hbm.at[t], wq_ref.at[t], w_sem.at[t]) for t in range(3)]
    loads += [pltpu.make_async_copy(wo_hbm, w_ref, w_sem.at[3])]
    for load in loads:
        load.start()
    heads = qkv_ref.shape[2] // HD
    depth = w_ref.shape[1]
    greet_cross(i, n, row, m)
    line = LineGather(i, n, cot_ref, cot_all, send, recv)
    line.start()
    weights = PlaneGather(row, m, [(up_ref, up_all, half_rows, row_blocks(m)), (down_ref, down_all, half_rows, column_blocks(m))],
                          w_send, w_recv, w_local)
    weights.start()
    own_copy = pltpu.make_async_copy(cot_ref, cot_all.at[i], own_sem)
    own_copy.start()

    loads[0].wait()
    block = 256
    for t in range(3):
        loads[1 + t].wait()

        def project(b):
            here = rows_at(b, block)
            value = jnp.dot(a_ref[here, :], wq_ref[t], preferred_element_type=F32)
            if t != 1:
                value = value + bias[t // 2 : t // 2 + 1, :]
            qkv_ref[t, here, :] = value.astype(BF)

        loop(LEN // block, project)

    def head(t):
        cols = pl.ds(pl.multiple_of(t * HD, HD), HD)
        for b in range(LEN // block):
            here, keys = slice(b * block, (b + 1) * block), (b + 1) * block
            s = lax.dot_general(qkv_ref[0, here, cols], qkv_ref[1, 0:keys, cols], NT,
                                preferred_element_type=F32) * HD ** (-0.5)
            query = lax.broadcasted_iota(jnp.int32, s.shape, 0) + b * block
            s = jnp.where(query >= lax.broadcasted_iota(jnp.int32, s.shape, 1), s, -1e30)
            e = jnp.exp(s - jnp.max(s, axis=-1, keepdims=True))
            prob = (e / jnp.sum(e, axis=-1, keepdims=True)).astype(BF)
            o_ref[here, cols] = jnp.dot(prob, qkv_ref[2, 0:keys, cols], preferred_element_type=F32).astype(BF)

    loop(heads, head)
    leave = [pltpu.make_async_copy(qkv_ref, qkv_hbm, out_sem.at[0]), pltpu.make_async_copy(o_ref, o_hbm, out_sem.at[1])]
    for copy in leave:
        copy.start()
    loads[4].wait()
    sums = LineSum(i, n, part, land, s_send, s_recv, pieces)
    tile = 512

    def project(t):
        d = jnp.where(i < n // 2, n - 1 - t, t)

        def columns(k):
            cols = rows_at(k, tile)
            part[d, :, cols] = jnp.dot(o_ref[rows_at(d, size), :], w_ref[:, cols], preferred_element_type=F32).astype(BF)

        loop(depth // tile, columns)
        sums.launch(d)

    loop(n, project)
    weights.advance(1)
    for r in range(1, n):
        line.step(r)
        for stage in range(2, weights.stages):
            if r == min(2 * stage - 1, n - 1):
                weights.advance(stage)
        relays(sums, i, n, r)

    def norm(b):
        here = rows_at(b, RB)
        sums.add(here, h_ref.at[here, :])
        rows = h_ref[here, :] + (x_ref[here, :].astype(F32) + vec[2:3, :])
        h_ref[here, :] = rows
        normal, _ = norm_stats(rows)
        c_ref[here, :] = (normal * vec[3:4, :] + vec[4:5, :]).astype(BF)

    sums.own(norm)
    own_copy.wait()
    for copy in leave:
        copy.wait()
    weights.finish()
    line.finish()
    sums.finish()


def hidden_kernel(n, pieces, c_ref, h_ref, cot_hbm, up_hbm, down_hbm, up_bias, vec, c_hbm, g_hbm, du_hbm, mlp_hbm, dh_ref,
                  db_ref, vec_ref, upb_ref, c_all, g_all, du_all, cot_all, up, down, part, land, send, recv, s_send,
                  s_recv, w_sem, cot_sem, own_sem, c_sem, g_sem, du_sem, mlp, mlp_sem):
    i = lax.axis_index("tensor")
    size, depth = c_ref.shape
    units = up.shape[1]
    greet_neighbours(i, n)
    line = LineGather(i, n, c_ref, c_all, send, recv)
    line.start()
    own_copy = pltpu.make_async_copy(c_ref, c_all.at[i], own_sem)
    own_copy.start()
    up_copy = pltpu.make_async_copy(up_hbm, up, w_sem.at[0])
    up_copy.start()
    down_copy = pltpu.make_async_copy(down_hbm, down, w_sem.at[1])
    down_copy.start()
    cot_copy = pltpu.make_async_copy(cot_hbm, cot_all, cot_sem)
    cot_copy.start()
    upb_ref[...] = jnp.zeros_like(upb_ref)
    vec_ref[...] = jnp.zeros_like(vec_ref)
    own_copy.wait()
    up_copy.wait()
    down_copy.wait()
    cot_copy.wait()
    sums = LineSum(i, n, part, land, s_send, s_recv, pieces)
    tile = 256

    def out_copy(src, dst, sem, j):
        return pltpu.make_async_copy(src.at[j], dst.at[j], sem.at[j])

    def compute(j):
        def unit(k):
            cols = rows_at(k, tile)
            u = jnp.dot(c_all[j], up[:, cols], preferred_element_type=F32) + up_bias[0:1, cols]
            dg = lax.dot_general(cot_all[j], down[cols, :], NT, preferred_element_type=F32)
            half = 0.5 + 0.5 * lax.erf(u * (0.5 ** 0.5))
            g_all[j, :, cols] = (u * half).astype(BF)
            slope = half + u * (jnp.exp(u * u * -0.5) * 0.3989422804014327)
            du = (slope * dg).astype(BF)
            du_all[j, :, cols] = du
            upb_ref[0:1, cols] += jnp.sum(du.astype(F32), axis=0, keepdims=True)

        loop(units // tile, unit)

        def back(k):
            cols = rows_at(k, tile)
            part[j, :, cols] = lax.dot_general(du_all[j], up[cols, :], NT, preferred_element_type=F32).astype(BF)

        loop(depth // tile, back)
        sums.launch(j)
        out_copy(g_all, g_hbm, g_sem, j).start()
        out_copy(du_all, du_hbm, du_sem, j).start()
        out_copy(c_all, c_hbm, c_sem, j).start()

    rounds(i, n, line, compute)

    def forward(j):
        def columns(k):
            cols = rows_at(k, tile)
            mlp[j, :, cols] = jnp.dot(g_all[j], down[:, cols], preferred_element_type=F32).astype(BF)

        loop(depth // tile, columns)
        out_copy(mlp, mlp_hbm, mlp_sem, j).start()

    def relay(t):
        early = jnp.where(i < n // 2, 1, 0)
        sums.relay(t + 3 - early - i, 2 * n - 4 - i - t - early)

        @pl.when(t < n // 2)
        def _():
            loop(2, lambda k: forward(2 * t + k))

    loop(2 * n - 3, relay)

    def norm(b):
        here = rows_at(b, RB)
        sums.add(here, dh_ref.at[here, :])
        grad = dh_ref[here, :]
        normal, inverse = norm_stats(h_ref[here, :])
        vec_ref[0:1, :] += jnp.sum(grad * normal, axis=0, keepdims=True)
        vec_ref[1:2, :] += jnp.sum(grad, axis=0, keepdims=True)
        cot = cot_all[i, here, :].astype(F32)
        dh = cot + norm_back(grad, normal, inverse, vec[3:4, :])
        dh_ref[here, :] = dh
        db = dh.astype(BF)
        db_ref[here, :] = db
        vec_ref[2:3, :] += jnp.sum(db.astype(F32), axis=0, keepdims=True)
        vec_ref[3:4, :] += jnp.sum(cot, axis=0, keepdims=True)

    sums.own(norm)

    def done(j):
        out_copy(g_all, g_hbm, g_sem, j).wait()
        out_copy(du_all, du_hbm, du_sem, j).wait()
        out_copy(c_all, c_hbm, c_sem, j).wait()
        out_copy(mlp, mlp_hbm, mlp_sem, j).wait()

    loop(n, done)
    line.finish()
    sums.finish()


def attend_back(q_of, k_of, v_of, do_of, heads, put, dk, dv):
    block = 256
    factor = HD ** (-0.5)

    def head(t):
        dk[...] = jnp.zeros_like(dk)
        dv[...] = jnp.zeros_like(dv)
        for b in range(LEN // block):
            here, keys = slice(b * block, (b + 1) * block), slice(0, (b + 1) * block)
            q, k, v, do = q_of(here, t), k_of(keys, t), v_of(keys, t), do_of(here, t)
            s = lax.dot_general(q, k, NT, preferred_element_type=F32) * factor
            query = lax.broadcasted_iota(jnp.int32, s.shape, 0) + b * block
            s = jnp.where(query >= lax.broadcasted_iota(jnp.int32, s.shape, 1), s, -1e30)
            e = jnp.exp(s - jnp.max(s, axis=-1, keepdims=True))
            prob = e / jnp.sum(e, axis=-1, keepdims=True)
            dv[keys, :] += lax.dot_general(prob.astype(BF), do, TN, preferred_element_type=F32)
            dp = lax.dot_general(do, v, NT, preferred_element_type=F32)
            ds = (prob * (dp - jnp.sum(prob * dp, axis=-1, keepdims=True))).astype(BF)
            put(0, here, t, (jnp.dot(ds, k, preferred_element_type=F32) * factor).astype(BF))
            dk[keys, :] += lax.dot_general(ds, q, TN, preferred_element_type=F32)
        put(1, slice(0, LEN), t, (dk[...] * factor).astype(BF))
        put(2, slice(0, LEN), t, dv[...].astype(BF))

    loop(heads, head)


class PlaneSum:
    def __init__(self, row, m, out, terms, land, halves, send, recv, h_send, h_recv):
        self.row, self.m, self.out, self.terms, self.land, self.halves = row, m, out, terms, land, halves
        self.send, self.recv, self.h_send, self.h_recv = send, recv, h_send, h_recv
        bits = [1 << k for k in range(1, m.bit_length() - 1)]
        self.plan = []
        for order in (bits, bits[::-1]):
            left, at, stages = [e for e in range(m) if e % 2 == 0], 0, []
            for bit in order:
                out = [e for e in left if e & bit]
                stages.append((bit, [(e, e ^ bit, at + k) for k, e in enumerate(out)]))
                left, at = [e for e in left if not e & bit], at + len(out)
            self.plan.append(stages)
        self.stages = len(bits)

    def owner(self, e):
        d = self.row
        for k in range(self.m.bit_length() - 1):
            if e & (1 << k):
                d = d + (partner(self.row, 1 << k) - self.row)
        return d

    def whole(self, e):
        return pltpu.make_async_remote_copy(
            src_ref=self.out.at[e // 2], dst_ref=self.land.at[e // 2], send_sem=self.send.at[e // 2],
            recv_sem=self.recv.at[e // 2], device_id={"dp": partner(self.row, 1)}, device_id_type=MESH)

    def half(self, h, bit, e, at):
        size = self.halves.shape[2]
        return pltpu.make_async_remote_copy(
            src_ref=self.terms.at[e // 2, pl.ds(h * size, size)], dst_ref=self.halves.at[h, at],
            send_sem=self.h_send.at[h, at], recv_sem=self.h_recv.at[h, at],
            device_id={"dp": partner(self.row, bit)}, device_id_type=MESH)

    def merge(self):
        for e in range(0, self.m, 2):
            self.whole(e + 1).wait_recv()

            def add(b):
                here = rows_at(b, RB)
                total = self.terms[e // 2, here, :].astype(F32) + self.land[e // 2, here, :].astype(F32)
                self.terms[e // 2, here, :] = total.astype(BF)

            loop(self.terms.shape[1] // RB, add)

    def push(self, stage):
        for h in range(2):
            bit, moves = self.plan[h][stage]
            for e, _, at in moves:
                self.half(h, bit, e, at).start()

    def take(self, stage, out=None):
        size = self.halves.shape[2]
        for h in range(2):
            bit, moves = self.plan[h][stage]
            for e, into, at in moves:
                self.half(h, bit, e, at).wait_recv()

                def add(b):
                    here, there = rows_at(b, RB), pl.ds(pl.multiple_of(h * size + b * RB, RB), RB)
                    total = self.terms[into // 2, there, :].astype(F32) + self.halves[h, at, here, :].astype(F32)
                    if out is None:
                        self.terms[into // 2, there, :] = total.astype(BF)
                    else:
                        out(there, total)

                loop(size // RB, add)

    def sent(self):
        for e in range(1, self.m, 2):
            self.whole(e).wait_send()

    def finish(self):
        for h in range(2):
            for bit, moves in self.plan[h]:
                for e, _, at in moves:
                    self.half(h, bit, e, at).wait_send()


class VectorSum:
    def __init__(self, me, count, device, vectors, piece, land, acc, send, recv):
        self.me, self.count, self.device, self.vectors, self.piece = me, count, device, vectors, piece
        self.land, self.acc, self.send, self.recv = land, acc, send, recv

    def lanes(self, owner):
        size = self.land.shape[2]
        return pl.ds(pl.multiple_of(owner * self.piece // size * size, size), size)

    def copy(self, src, other):
        return pltpu.make_async_remote_copy(
            src_ref=self.vectors.at[:, self.lanes(other)], dst_ref=self.land.at[src], send_sem=self.send.at[other],
            recv_sem=self.recv.at[src], device_id=self.device(other), device_id_type=MESH)

    def start(self):
        loop(self.count - 1, lambda s: self.copy(self.me, (self.me + s + 1) % self.count).start())

    def finish(self):
        self.acc[...] = self.vectors[:, self.lanes(self.me)]

        def take(s):
            src = (self.me + s + 1) % self.count
            self.copy(src, self.me).wait_recv()
            self.acc[...] += self.land[src]

        loop(self.count - 1, take)
        loop(self.count - 1, lambda s: self.copy(self.me, (self.me + s + 1) % self.count).wait_send())
        places = self.land.shape[2] // self.piece
        own = self.acc[:, 0 : self.piece]
        for k in range(1, places):
            own = jnp.where(self.me % places == k, self.acc[:, k * self.piece : (k + 1) * self.piece], own)
        return own


def greet_cross(i, n, row, m):
    barrier = pltpu.get_barrier_semaphore()

    @pl.when(i > 0)
    def _():
        pl.semaphore_signal(barrier, inc=1, device_id={"tensor": i - 1}, device_id_type=MESH)

    @pl.when(i < n - 1)
    def _():
        pl.semaphore_signal(barrier, inc=1, device_id={"tensor": i + 1}, device_id_type=MESH)

    bits = [1 << k for k in range(m.bit_length() - 1)]
    for bit in bits:
        pl.semaphore_signal(barrier, inc=1, device_id={"dp": partner(row, bit)}, device_id_type=MESH)
    pl.semaphore_wait(barrier, jnp.minimum(i, 1) + jnp.minimum(n - 1 - i, 1) + len(bits))


def relays(sums, i, n, r):
    sums.relay(n - 1 + i - r, r - (n - 1 - i))


def block_terms(plane, e, pairs):
    size = plane.terms.shape[1]
    cols = rows_at(plane.owner(e), size)
    for lhs, rhs, first in pairs:
        width = rhs.shape[1]
        tile = min(512, width)

        def columns(k):
            there = pl.ds(pl.multiple_of(first + k * tile, tile), tile)
            (plane.out if e % 2 else plane.terms)[e // 2, :, there] = lax.dot_general(
                lhs[:, cols], rhs[:, rows_at(k, tile)], TN, preferred_element_type=F32).astype(BF)

        loop(width // tile, columns)


def branch_kernel(n, m, pieces, db_ref, h_ref, vec, mlp_hbm, g_hbm, cot_hbm, c_hbm, du_hbm, qkv_hbm, wo_hbm,
                  db_all, lo_ref, down_ref, up_ref, dqkv_hbm, dqkv_ref, out_sem, lhs, rhs, wo, dk, dv, part, land, out, terms_a, land_a,
                  half_a, terms_b, land_b, half_b, acc, send, recv, s_send, s_recv, own_sem, part_sem, in_sem, qkv_sem,
                  db_sem, p_send, p_recv, h_send, h_recv):
    i, row = lax.axis_index("tensor"), lax.axis_index("dp")
    size = db_ref.shape[0]
    width = wo.shape[0]
    greet_cross(i, n, row, m)
    line = LineGather(i, n, db_ref, db_all, send, recv)
    line.start()
    part_copy = pltpu.make_async_copy(mlp_hbm, part, part_sem)
    part_copy.start()
    own_copy = pltpu.make_async_copy(db_ref, db_all.at[i], own_sem)
    own_copy.start()

    def load(left, right):
        return [pltpu.make_async_copy(left, lhs, in_sem.at[0]), pltpu.make_async_copy(right, rhs, in_sem.at[1])]

    loads = load(cot_hbm, g_hbm)
    for copy in loads:
        copy.start()
    wo_copy = pltpu.make_async_copy(wo_hbm, wo, in_sem.at[2])
    wo_copy.start()
    sums = LineSum(i, n, part, land, s_send, s_recv, pieces)
    part_copy.wait()
    loop(n, lambda t: sums.launch(jnp.where(i < n // 2, n - 1 - t, t)))
    planes = [PlaneSum(row, m, out, terms_a, land_a, half_a, p_send.at[0], p_recv.at[0], h_send.at[0], h_recv.at[0]),
              PlaneSum(row, m, out, terms_b, land_b, half_b, p_send.at[1], p_recv.at[1], h_send.at[1], h_recv.at[1])]
    first, second = planes
    for copy in loads:
        copy.wait()
    left, right = lhs.at[:, 0 : lhs.shape[1]], rhs.at[:, 0 : down_ref.shape[1]]
    for e in range(1, m, 2):
        block_terms(first, e, [(left, right, 0)])
        first.whole(e).start()
    for e in range(m - 2, -1, -2):
        block_terms(first, e, [(left, right, 0)])
    loads = load(c_hbm, du_hbm)
    for copy in loads:
        copy.start()
    first.merge()
    first.push(0)
    first.sent()
    for copy in loads:
        copy.wait()
    for e in range(1, m, 2):
        block_terms(second, e, [(left, right, 0)])
        second.whole(e).start()

    line.step(1)
    for e in range(m - 2, -1, -2):
        block_terms(second, e, [(left, right, 0)])
    qkv_copies = [pltpu.make_async_copy(qkv_hbm.at[p], rhs.at[:, p * width : (p + 1) * width], qkv_sem.at[p])
                  for p in range(3)]
    for copy in qkv_copies:
        copy.start()
    second.merge()
    second.push(0)
    own_copy.wait()
    wo_copy.wait()

    def mixture_back(j):
        here = rows_at(j, size)
        copy = pltpu.make_async_copy(db_all.at[j], lhs.at[here], db_sem.at[j])
        copy.start()
        copy.wait()
        rhs[here, 3 * width : 4 * width] = lax.dot_general(
            lhs[here, :], wo[...], NT, preferred_element_type=F32).astype(BF)

    def round_back(r):
        def side(s):
            j = jnp.where(s == 0, i - r, i + r)

            @pl.when(jnp.logical_and(j >= 0, j <= n - 1))
            def _():
                mixture_back(j)

        loop(2, side)

    def keep(ref):
        def put(here, total):
            ref[here, :] = total

        return put

    def advance(plane, stage, ref):
        if stage < plane.stages - 1:
            plane.take(stage)
            plane.push(stage + 1)
        else:
            plane.take(stage, keep(ref))

    mixture_back(i)
    round_back(1)
    advance(first, 0, down_ref)
    for r in range(2, n):
        line.step(r)
        relays(sums, i, n, r - 1)
        round_back(r)
        if r == 2:
            advance(second, 0, up_ref)
    if n == 2:
        advance(second, 0, up_ref)
    relays(sums, i, n, n - 1)
    for copy in qkv_copies:
        copy.wait()

    def column(p):
        def get(here, t):
            return rhs[here, pl.ds(pl.multiple_of(p * width + t * HD, HD), HD)]

        return get

    def put(p, here, t, value):
        dqkv_ref[p, here, pl.ds(pl.multiple_of(t * HD, HD), HD)] = value

    attend_back(column(0), column(1), column(2), column(3), width // HD, put, dk, dv)
    leave = pltpu.make_async_copy(dqkv_ref, dqkv_hbm, out_sem)
    leave.start()
    for stage in range(1, first.stages):
        advance(first, stage, down_ref)
        advance(second, stage, up_ref)

    def output(b):
        here = rows_at(b, RB)
        sums.add(here, acc)
        lo_ref[here, :] = (h_ref[here, :] + (acc[...] + vec[5:6, :])).astype(BF)

    sums.own(output)
    line.finish()
    sums.finish()
    second.sent()
    for plane in planes:
        plane.finish()
    leave.wait()


def input_kernel(n, m, pieces, widths, dqkv_ref, wq_hbm, x_hbm, dh_hbm, vec, early_ref, up_ref, a_hbm, db_hbm, o_hbm,
                 n_hbm, gt_ref, gqkv_ref, gout_ref, vec_out, up_out, qv_out, early_acc, late_acc, up_acc, qv_acc, vec_ref, qv_ref, wq, a_ref, db_ref,
                 o_ref, n_ref, x_ref, dh_ref, part, land, out_p, terms, land_p, half_p, acc, early_land, late_land, up_land, qv_land, s_send,
                 s_recv, in_sem, p_send, p_recv, h_send, h_recv, e_send, e_recv, l_send, l_recv, u_send, u_recv, q_send,
                 q_recv):
    i, row = lax.axis_index("tensor"), lax.axis_index("dp")
    me, total_devices = row * n + i, m * n
    size = x_hbm.shape[0]
    width = dqkv_ref.shape[2]
    piece, up_piece, qv_piece = widths
    depth = part.shape[2]
    loads = [pltpu.make_async_copy(src, dst, in_sem.at[k]) for k, (src, dst) in enumerate(
        [(wq_hbm, wq), (a_hbm, a_ref), (db_hbm, db_ref), (o_hbm, o_ref), (n_hbm, n_ref), (x_hbm, x_ref), (dh_hbm, dh_ref)])]
    loads[0].start()
    loads[4].start()
    greet_all(me, n, total_devices)
    every = [VectorSum(me, total_devices, lambda g: {"dp": g // n, "tensor": g % n}, early_ref, piece, early_land, early_acc,
                       e_send, e_recv),
             VectorSum(me, total_devices, lambda g: {"dp": g // n, "tensor": g % n}, vec_ref, piece, late_land, late_acc,
                       l_send, l_recv)]
    column = [VectorSum(row, m, lambda g: {"dp": g}, up_ref, up_piece, up_land, up_acc, u_send, u_recv),
              VectorSum(row, m, lambda g: {"dp": g}, qv_ref, qv_piece, qv_land, qv_acc, q_send, q_recv)]
    every[0].start()
    column[0].start()
    sums = LineSum(i, n, part, land, s_send, s_recv, pieces)
    vec_ref[...] = jnp.zeros_like(vec_ref)
    qv_ref[...] = jnp.zeros_like(qv_ref)
    loads[0].wait()
    loads[4].wait()
    for k in (1, 2, 3, 5, 6):
        loads[k].start()
    tile = 512

    def term(t):
        d = jnp.where(i < n // 2, n - 1 - t, t)
        here = rows_at(d, size)

        def columns(k):
            cols = rows_at(k, tile)
            total = lax.dot_general(dqkv_ref[0, here, :], wq[0, cols, :], NT, preferred_element_type=F32)
            for p in range(1, 3):
                total += lax.dot_general(dqkv_ref[p, here, :], wq[p, cols, :], NT, preferred_element_type=F32)
            part[d, :, cols] = total.astype(BF)
            vec_ref[0:1, cols] += jnp.sum(total * n_ref[here, cols].astype(F32), axis=0, keepdims=True)
            vec_ref[1:2, cols] += jnp.sum(total, axis=0, keepdims=True)

        loop(depth // tile, columns)

        @pl.when(t == 0)
        def _():
            sums.launch(d)

        for p in range(2):
            qv_ref[p : p + 1, :] += jnp.sum(dqkv_ref[2 * p, here, :].astype(F32), axis=0, keepdims=True)

    loop(n, term)
    every[1].start()
    column[1].start()
    loop(n - 1, lambda t: sums.launch(jnp.where(i < n // 2, n - 2 - t, t + 1)))
    for k in (1, 2, 3, 5, 6):
        loads[k].wait()
    plane = PlaneSum(row, m, out_p, terms, land_p, half_p, p_send, p_recv, h_send, h_recv)
    pairs = [(a_ref, dqkv_ref.at[p], p * width) for p in range(3)] + [(db_ref, o_ref, 3 * width)]
    for e in range(1, m, 2):
        block_terms(plane, e, pairs)
        plane.whole(e).start()
    for e in range(m - 2, -1, -2):
        block_terms(plane, e, pairs)
    plane.merge()
    plane.push(0)

    def out(here, total):
        for p in range(3):
            gqkv_ref[p, here, :] = total[:, p * width : (p + 1) * width]
        gout_ref[here, :] = total[:, 3 * width :]

    stage = 0
    for r in range(1, n):
        relays(sums, i, n, r)
        if r > 1 and stage < plane.stages:
            if stage < plane.stages - 1:
                plane.take(stage)
                plane.push(stage + 1)
            else:
                plane.take(stage, out)
            stage += 1

    def norm(b):
        here = rows_at(b, RB)
        sums.add(here, acc)
        grad = acc[...]
        normal, inverse = norm_stats(x_ref[here, :].astype(F32))
        gt_ref[here, :] = (dh_ref[here, :] + norm_back(grad, normal, inverse, vec[0:1, :])).astype(BF)

    while stage < plane.stages:
        if stage < plane.stages - 1:
            plane.take(stage)
            plane.push(stage + 1)
        else:
            plane.take(stage, out)
        stage += 1
    early, late = every[0].finish(), every[1].finish()
    for k, (rows, at) in enumerate([(late, 0), (late, 1), (early, 2), (early, 0), (early, 1), (early, 3)]):
        vec_out[k : k + 1, :] = rows[at : at + 1, :]
    up_out[...] = column[0].finish()
    qv_out[...] = column[1].finish()
    sums.own(norm)
    sums.finish()
    plane.sent()
    plane.finish()


def params(collective=None):
    if collective is None:
        return pltpu.CompilerParams(vmem_limit_bytes=BIG)
    return pltpu.CompilerParams(vmem_limit_bytes=BIG, collective_id=collective, has_side_effects=True)


def shape(dims, dtype):
    return jax.ShapeDtypeStruct(dims, dtype)


def body(tokens, cotangent, ln1_gain, ln1_bias, qkv_weight, qv_bias, out_weight, out_bias, ln2_gain, ln2_bias,
         up_weight, up_bias, down_weight, down_bias):
    n = lax.axis_size("tensor")
    m = lax.axis_size("dp")
    i, row = lax.axis_index("tensor"), lax.axis_index("dp")
    size, depth = tokens.shape
    width = qkv_weight.shape[2]
    units = up_weight.shape[1]
    piece, qv_piece, up_piece = ln1_gain.shape[0], qv_bias.shape[1], up_bias.shape[0]
    total = m * n

    def lane_rows(value, index):
        count = value.shape[-1]
        if count >= LANES:
            return value.reshape(-1, LANES)
        places = LANES // count
        spread = jnp.tile(value.reshape(-1, count), (1, places))
        return jnp.where((jnp.arange(LANES) // count)[None] == index % places, spread, 0)

    me = row * n + i
    whole = jnp.stack([ln1_gain, ln1_bias, out_bias, ln2_gain, ln2_bias, down_bias])
    pack = jnp.concatenate([lane_rows(whole, me), lane_rows(qv_bias, row), lane_rows(up_bias, row)])
    pack = jnp.pad(pack, ((0, -pack.shape[0] % 16), (0, 0)))
    lanes_up = 8 + max(up_piece // LANES, 1)

    dma = pltpu.SemaphoreType.DMA
    weight_sems = [dma((2, 2, m - 1)), dma((2, 2, m)), dma((2, 2))]
    attn_in, normal_one, vectors, bias_qv, bias_up, w_qkv, w_out = pl.pallas_call(
        functools.partial(tokens_kernel, n, m, (piece, qv_piece, up_piece)),
        out_shape=(shape((LEN, depth), BF), shape((LEN, depth), BF), shape((8, depth), F32), shape((8, width), F32),
                   shape((8, units), F32), shape((3, depth, width), BF), shape((width, depth), BF)),
        in_specs=[VM] * 4, out_specs=(ANY, ANY, VM, VM, VM, ANY, ANY),
        scratch_shapes=[pltpu.VMEM((total,) + pack.shape, BF), pltpu.VMEM((n, size, depth), BF), pltpu.VMEM((LEN, depth), BF),
                        pltpu.VMEM((LEN, depth), BF), dma((2, n))] + weight_sems +
                       [dma, dma((2, n, LineGather.PIECES)), dma((n, LineGather.PIECES)), dma((total,)), dma((total,))],
        compiler_params=params(0), name="gather_tokens",
    )(pack, tokens, qkv_weight, out_weight)

    pieces = 2
    sums = [pltpu.VMEM((n, size, depth), BF), pltpu.VMEM((n + 1, size, depth), BF)]
    qkv, mixture, residual, mlp_own, cot_all, w_up, w_down = pl.pallas_call(
        functools.partial(attend_kernel, n, m, pieces),
        out_shape=(shape((3, LEN, width), BF), shape((LEN, width), BF), shape((size, depth), F32),
                   shape((size, depth), BF), shape((n, size, depth), BF), shape((depth, units), BF), shape((units, depth), BF)),
        in_specs=[ANY] * 3 + [VM] * 6, out_specs=(ANY, ANY, VM, VM, ANY, ANY, ANY),
        scratch_shapes=weight_sems + [pltpu.VMEM((3, LEN, width), BF), pltpu.VMEM((LEN, width), BF), dma((2,)),
                        pltpu.VMEM((LEN, depth), BF), pltpu.VMEM((3, depth, width), BF), pltpu.VMEM((width, depth), BF)] +
                       sums + [dma((2, n, LineGather.PIECES)), dma((n, LineGather.PIECES)), dma((n, pieces)), dma((n + 1, pieces)), dma, dma, dma((4,))],
        compiler_params=params(1), name="attend",
    )(attn_in, w_qkv, w_out, up_weight, down_weight, tokens, cotangent, bias_qv, vectors)

    pieces = min(4, size // RB)
    mlp_in, hidden, grad_pre, mlp_part, grad_resid, branch_cot, vec_two, grad_up_b = pl.pallas_call(
        functools.partial(hidden_kernel, n, pieces),
        out_shape=(shape((n, size, depth), BF), shape((n, size, units), BF), shape((n, size, units), BF),
                   shape((n, size, depth), BF), shape((size, depth), F32), shape((size, depth), BF),
                   shape((8, depth), F32), shape((8, units), F32)),
        in_specs=[VM, VM, ANY, ANY, ANY, VM, VM], out_specs=(ANY, ANY, ANY, ANY, VM, VM, VM, VM),
        scratch_shapes=[pltpu.VMEM((n, size, depth), BF), pltpu.VMEM((n, size, units), BF),
                        pltpu.VMEM((n, size, units), BF), pltpu.VMEM((n, size, depth), BF),
                        pltpu.VMEM((depth, units), BF), pltpu.VMEM((units, depth), BF)] + sums +
                       [dma((2, n, LineGather.PIECES)), dma((n, LineGather.PIECES)), dma((n, pieces)), dma((n + 1, pieces)), dma((2,)), dma, dma,
                        dma((n,)), dma((n,)), dma((n,)), pltpu.VMEM((n, size, depth), BF), dma((n,))],
        compiler_params=params(2), name="hidden",
    )(mlp_own, residual, cot_all, w_up, w_down, bias_up, vectors)
    mlp_in, hidden, grad_pre, cot_rows = [v.reshape(LEN, -1) for v in (mlp_in, hidden, grad_pre, cot_all)]

    def plane_scratch(columns):
        rows = depth // m
        return [pltpu.VMEM((m // 2, rows, columns), BF), pltpu.VMEM((m // 2, rows, columns), BF),
                pltpu.VMEM((2, m // 2 - 1, rows // 2, columns), BF)]

    pieces = 2
    sum_sems = [dma((n, pieces)), dma((n + 1, pieces))]
    attn_cot, layer_out, grad_down_w, grad_up_w, grad_qkv = pl.pallas_call(
        functools.partial(branch_kernel, n, m, pieces),
        out_shape=(shape((n, size, depth), BF), shape((size, depth), BF), shape((depth // m, units), F32),
                   shape((depth // m, units), F32), shape((3, LEN, width), BF)),
        in_specs=[VM] * 3 + [ANY] * 7, out_specs=(ANY, VM, VM, VM, ANY),
        scratch_shapes=[pltpu.VMEM((3, LEN, width), BF), dma, pltpu.VMEM((LEN, depth), BF), pltpu.VMEM((LEN, units), BF), pltpu.VMEM((width, depth), BF),
                        pltpu.VMEM((LEN, HD), F32), pltpu.VMEM((LEN, HD), F32)] + sums +
                       [pltpu.VMEM((m // 2, depth // m, units), BF)] + plane_scratch(units) * 2 +
                       [pltpu.VMEM((RB, depth), F32), dma((2, n, LineGather.PIECES)), dma((n, LineGather.PIECES))] + sum_sems +
                       [dma, dma, dma((3,)), dma((3,)), dma((n,)), dma((2, m // 2)), dma((2, m // 2)),
                        dma((2, 2, m // 2 - 1)), dma((2, 2, m // 2 - 1))],
        compiler_params=params(4), name="branch",
    )(branch_cot, residual, vectors, mlp_part, hidden, cot_rows, mlp_in, grad_pre, qkv, w_out)
    attn_cot = attn_cot.reshape(LEN, depth)

    tiles = [max(v, LANES) for v in (piece, up_piece, qv_piece)]
    grad_tokens, grad_qkv_w, grad_out_w, vector_grads, grad_up_b, grad_qv_b = pl.pallas_call(
        functools.partial(input_kernel, n, m, pieces, (piece, up_piece, qv_piece)),
        out_shape=(shape((size, depth), BF), shape((3, depth // m, width), F32), shape((depth // m, width), F32),
                   shape((8, piece), F32), shape((8, up_piece), F32), shape((8, qv_piece), F32)),
        in_specs=[VM, ANY, ANY, ANY, VM, VM, VM, ANY, ANY, ANY, ANY], out_specs=(VM,) * 6,
        scratch_shapes=[pltpu.VMEM((8, tiles[k]), F32) for k in (0, 0, 1, 2)] + [
                        pltpu.VMEM((8, depth), F32), pltpu.VMEM((8, width), F32),
                        pltpu.VMEM((3, depth, width), BF), pltpu.VMEM((LEN, depth), BF), pltpu.VMEM((LEN, depth), BF),
                        pltpu.VMEM((LEN, width), BF), pltpu.VMEM((LEN, depth), BF), pltpu.VMEM((size, depth), BF),
                        pltpu.VMEM((size, depth), F32)] + sums +
                       [pltpu.VMEM((m // 2, depth // m, 4 * width), BF)] +
                       plane_scratch(4 * width) +
                       [pltpu.VMEM((RB, depth), F32), pltpu.VMEM((total, 8, tiles[0]), F32),
                        pltpu.VMEM((total, 8, tiles[0]), F32), pltpu.VMEM((m, 8, tiles[1]), F32),
                        pltpu.VMEM((m, 8, tiles[2]), F32)] + sum_sems +
                       [dma((7,)), dma((m // 2,)), dma((m // 2,)), dma((2, m // 2 - 1)), dma((2, m // 2 - 1))] +
                       [dma((total,))] * 4 + [dma((m,))] * 4,
        compiler_params=params(5), name="input",
    )(grad_qkv, w_qkv, tokens, grad_resid, vectors, vec_two, grad_up_b, attn_in, attn_cot, mixture, normal_one)
    grad_down_w, grad_out_w = grad_down_w.T, grad_out_w.T

    vectors = [vector_grads[k] for k in range(6)]
    grad_up_b, grad_qv_b = grad_up_b[0], grad_qv_b[:2]
    return (layer_out, grad_tokens, vectors[0], vectors[1], grad_qkv_w, grad_qv_b, grad_out_w, vectors[2],
            vectors[3], vectors[4], grad_up_w, grad_up_b, grad_down_w, vectors[5])


def solution(mesh):
    vector, matrix = P(("dp", "tensor")), P(("dp", "tensor"), None)
    in_specs = (matrix, matrix, vector, vector, P(None, "dp", "tensor"), P(None, ("tensor", "dp")), P("tensor", "dp"),
                vector, vector, vector, P("dp", "tensor"), P(("tensor", "dp")), P("tensor", "dp"), vector)
    out_specs = (matrix, matrix, vector, vector, P(None, "dp", "tensor"), P(None, ("tensor", "dp")),
                 P("tensor", "dp"), vector, vector, vector, P("dp", "tensor"), P(("tensor", "dp")), P("tensor", "dp"),
                 vector)
    return jax.shard_map(body, mesh=mesh, in_specs=in_specs, out_specs=out_specs, check_vma=False)
```

```python
import functools

import jax
import jax.numpy as jnp
from jax import lax
from jax.experimental import pallas as pl
from jax.experimental.pallas import tpu as pltpu
from jax.sharding import PartitionSpec as P

HD = 128
LEN = 1024
LANES = 128
EPS = 1e-05
BF = jnp.bfloat16
F32 = jnp.float32
MESH = pl.DeviceIdType.MESH
ANY = pl.BlockSpec(memory_space=pl.ANY)
VM = pl.BlockSpec(memory_space=pltpu.VMEM)
NT = (((1,), (1,)), ((), ()))
TN = (((0,), (0,)), ((), ()))
BIG = 64 * 1024 * 1024 - 65536
RB = 32


def norm_stats(rows):
    mean = jnp.mean(rows, axis=-1, keepdims=True)
    centred = rows - mean
    variance = jnp.mean(centred * centred, axis=-1, keepdims=True)
    inverse = lax.rsqrt(variance + EPS)
    return centred * inverse, inverse


def norm_back(grad_rows, normal_rows, inverse, gain):
    scaled = grad_rows * gain
    first = jnp.mean(scaled, axis=-1, keepdims=True)
    second = jnp.mean(scaled * normal_rows, axis=-1, keepdims=True)
    return inverse * (scaled - first - normal_rows * second)


def loop(count, step):
    def run(i, carry):
        step(i)
        return carry

    lax.fori_loop(0, count, run, 0)


def rows_at(j, size):
    return pl.ds(pl.multiple_of(j * size, size), size)


def remote(src, dst, send, recv, target):
    return pltpu.make_async_remote_copy(src_ref=src, dst_ref=dst, send_sem=send, recv_sem=recv,
                                        device_id={"tensor": target}, device_id_type=MESH)


def greet_neighbours(i, n):
    barrier = pltpu.get_barrier_semaphore()

    @pl.when(i > 0)
    def _():
        pl.semaphore_signal(barrier, inc=1, device_id={"tensor": i - 1}, device_id_type=MESH)

    @pl.when(i < n - 1)
    def _():
        pl.semaphore_signal(barrier, inc=1, device_id={"tensor": i + 1}, device_id_type=MESH)

    pl.semaphore_wait(barrier, jnp.minimum(i, 1) + jnp.minimum(n - 1 - i, 1))


def greet_all(me, n, total):
    barrier = pltpu.get_barrier_semaphore()

    def greet(s):
        other = (me + s + 1) % total
        pl.semaphore_signal(barrier, inc=1, device_id={"dp": other // n, "tensor": other % n}, device_id_type=MESH)

    loop(total - 1, greet)
    pl.semaphore_wait(barrier, total - 1)


def rounds(i, n, line, compute, between=None):
    def round_of(r):
        @pl.when(r > 0)
        def _():
            line.step(r)

        if between is not None:
            between(r)

        def side(s):
            j = jnp.where(s == 0, i - r, i + r)

            @pl.when(jnp.logical_and(jnp.logical_and(j >= 0, j <= n - 1), s * r == s * jnp.maximum(r, 1)))
            def _():
                compute(j)

        loop(2, side)

    loop(n, round_of)


class LineGather:
    PIECES = 2

    def __init__(self, i, n, own, buf, send, recv):
        self.i, self.n, self.own, self.buf, self.send, self.recv = i, n, own, buf, send, recv
        self.size = own.shape[0] // self.PIECES

    def copy(self, src, j, side, s, target):
        here = pl.ds(s * self.size, self.size)
        return remote(src.at[here], self.buf.at[j, here], self.send.at[side, j, s], self.recv.at[j, s], target)

    def start(self):
        i, n = self.i, self.n
        for s in range(self.PIECES):
            @pl.when(i < n - 1)
            def _():
                self.copy(self.own, i, 0, s, i + 1).start()

            @pl.when(i > 0)
            def _():
                self.copy(self.own, i, 1, s, i - 1).start()

    def step(self, r):
        i, n = self.i, self.n
        for s in range(self.PIECES):
            @pl.when(i - r >= 0)
            def _():
                self.copy(self.own, i - r, 0, s, i).wait_recv()

                @pl.when(i < n - 1)
                def _():
                    self.copy(self.buf.at[i - r], i - r, 0, s, i + 1).start()

            @pl.when(i + r <= n - 1)
            def _():
                self.copy(self.own, i + r, 1, s, i).wait_recv()

                @pl.when(i > 0)
                def _():
                    self.copy(self.buf.at[i + r], i + r, 1, s, i - 1).start()

    def finish(self):
        i, n = self.i, self.n

        def one(j):
            for s in range(self.PIECES):
                @pl.when(jnp.logical_and(i < n - 1, j <= i))
                def _():
                    self.copy(self.own, j, 0, s, i + 1).wait_send()

                @pl.when(jnp.logical_and(i > 0, j >= i))
                def _():
                    self.copy(self.own, j, 1, s, i - 1).wait_send()

        loop(n, one)


class LineSum:
    def __init__(self, i, n, part, land, send, recv, pieces):
        self.i, self.n, self.part, self.land, self.send, self.recv = i, n, part, land, send, recv
        self.pieces = pieces
        self.size = part.shape[1] // pieces

    def copy(self, src, d, right, s):
        i, n = self.i, self.n
        target = i + 1 if right else i - 1
        slot = d if right else jnp.where(d == target, n, d)
        here = rows_at(s, self.size)
        return remote(src.at[d, here], self.land.at[slot, here], self.send.at[d, s], self.recv.at[slot, s], target)

    def arrived(self, slot, s):
        here = rows_at(s, self.size)
        remote(self.part.at[0, here], self.land.at[slot, here], self.send.at[0, s], self.recv.at[slot, s],
               self.i).wait_recv()

    def launch(self, d):
        i, n = self.i, self.n

        @pl.when(jnp.logical_and(i == 0, d > 0))
        def _():
            loop(self.pieces, lambda s: self.copy(self.part, d, True, s).start())

        @pl.when(jnp.logical_and(i == n - 1, d < n - 1))
        def _():
            loop(self.pieces, lambda s: self.copy(self.part, d, False, s).start())

    def relay(self, right, left):
        i, n = self.i, self.n

        def move(d, to_right, s):
            self.arrived(d, s)
            here = rows_at(s, self.size)
            total = self.land[d, here, :].astype(F32) + self.part[d, here, :].astype(F32)
            self.land[d, here, :] = total.astype(BF)
            self.copy(self.land, d, to_right, s).start()

        first = jnp.where(i < n // 2, 0, 1)

        def one(s):
            turn, s = (s + first) % 2, s // 2

            @pl.when(jnp.logical_and(turn == 0, jnp.logical_and(i > 0, jnp.logical_and(right > i, right <= n - 1))))
            def _():
                move(right, True, s)

            @pl.when(jnp.logical_and(turn == 1, jnp.logical_and(i < n - 1, jnp.logical_and(left >= 0, left < i))))
            def _():
                move(left, False, s)

        loop(2 * self.pieces, one)

    def own(self, step):
        i, n = self.i, self.n

        def one(s):
            @pl.when(i > 0)
            def _():
                self.arrived(i, s)

            @pl.when(i < n - 1)
            def _():
                self.arrived(n, s)

            loop(self.size // RB, lambda b: step(s * (self.size // RB) + b))

        loop(self.pieces, one)

    def add(self, here, out):
        i, n = self.i, self.n
        out[...] = self.part[i, here, :].astype(F32)

        @pl.when(i > 0)
        def _():
            out[...] += self.land[i, here, :].astype(F32)

        @pl.when(i < n - 1)
        def _():
            out[...] += self.land[n, here, :].astype(F32)

    def finish(self):
        i, n = self.i, self.n

        def one(d):
            @pl.when(jnp.logical_and(i < n - 1, d > i))
            def _():
                loop(self.pieces, lambda s: self.copy(self.part, d, True, s).wait_send())

            @pl.when(jnp.logical_and(i > 0, d < i))
            def _():
                loop(self.pieces, lambda s: self.copy(self.part, d, False, s).wait_send())

        loop(n, one)


def partner(row, bit):
    return row + bit * (1 - 2 * ((row // bit) % 2))


class PlaneGather:
    def __init__(self, row, m, items, send, recv, local):
        self.row, self.m, self.items, self.send, self.recv, self.local = row, m, items, send, recv, local
        bits = [1 << k for k in range(1, m.bit_length() - 1)]
        self.plan = []
        for order in (bits + [1], bits[::-1] + [1]):
            have, at, stages = [0], 0, []
            for bit in order:
                stages.append((bit, [(e, at + k) for k, e in enumerate(have)]))
                at, have = at + len(have), have + [e ^ bit for e in have]
            self.plan.append(stages)
        self.stages = len(bits) + 1

    def owner(self, e):
        d = self.row
        for k in range(self.m.bit_length() - 1):
            if e & (1 << k):
                d = d + (partner(self.row, 1 << k) - self.row)
        return d

    def copies(self, stage):
        for k, (own, whole, own_half, half) in enumerate(self.items):
            for h in range(2):
                bit, moves = self.plan[h][stage]
                for e, at in moves:
                    there = half(whole, self.owner(e), h)
                    src = own_half(own, h) if e == 0 else there
                    yield pltpu.make_async_remote_copy(
                        src_ref=src, dst_ref=there, send_sem=self.send.at[k, h, at], recv_sem=self.recv.at[k, h, e ^ bit],
                        device_id={"dp": partner(self.row, bit)}, device_id_type=MESH)

    def landed(self, stage):
        for k, (own, whole, own_half, half) in enumerate(self.items):
            for h in range(2):
                bit, moves = self.plan[h][stage]
                for e, at in moves:
                    there = half(whole, self.owner(e ^ bit), h)
                    pltpu.make_async_remote_copy(
                        src_ref=there, dst_ref=there, send_sem=self.send.at[k, h, at], recv_sem=self.recv.at[k, h, e ^ bit],
                        device_id={"dp": partner(self.row, bit)}, device_id_type=MESH).wait_recv()

    def locals(self):
        return [pltpu.make_async_copy(own_half(own, h), half(whole, self.row, h), self.local.at[k, h])
                for k, (own, whole, own_half, half) in enumerate(self.items) for h in range(2)]

    def start(self):
        for copy in self.copies(0):
            copy.start()
        for copy in self.locals():
            copy.start()

    def advance(self, stage):
        self.landed(stage - 1)
        for copy in self.copies(stage):
            copy.start()

    def finish(self):
        self.landed(self.stages - 1)
        for stage in range(self.stages):
            for copy in self.copies(stage):
                copy.wait_send()
        for copy in self.locals():
            copy.wait()


def half_rows(own, h):
    size = own.shape[-2] // 2
    return own.at[..., pl.ds(h * size, size), :]


def row_blocks(m):
    def half(whole, d, h):
        size = whole.shape[-2] // m // 2
        return whole.at[..., pl.ds(pl.multiple_of((2 * d + h) * size, size), size), :]

    return half


def column_blocks(m):
    def half(whole, d, h):
        size, width = whole.shape[-2] // 2, whole.shape[-1] // m
        return whole.at[pl.ds(h * size, size), pl.ds(pl.multiple_of(d * width, width), width)]

    return half


def tokens_kernel(n, m, widths, pack_ref, x_ref, wq_ref, wo_ref, a_hbm, n_hbm, affine, qv_bias, up_bias, wq_all, wo_all,
                  vec_ref, buf, a_ref, n_ref, out_sem, w_send, w_recv, w_local, own_sem, send, recv, v_send, v_recv):
    i, row = lax.axis_index("tensor"), lax.axis_index("dp")
    me, total = row * n + i, m * n
    size = x_ref.shape[0]
    greet_all(me, n, total)
    line = LineGather(i, n, x_ref, buf, send, recv)

    def vector(src, other):
        return pltpu.make_async_remote_copy(
            src_ref=pack_ref, dst_ref=vec_ref.at[src], send_sem=v_send.at[other], recv_sem=v_recv.at[src],
            device_id={"dp": other // n, "tensor": other % n}, device_id_type=MESH)

    loop(total - 1, lambda s: vector(me, (me + s + 1) % total).start())
    line.start()
    weights = PlaneGather(row, m, [(wq_ref, wq_all, half_rows, row_blocks(m)), (wo_ref, wo_all, half_rows, column_blocks(m))],
                          w_send, w_recv, w_local)
    weights.start()
    own_copy = pltpu.make_async_copy(x_ref, buf.at[i], own_sem)
    own_copy.start()
    vec_ref[me] = pack_ref[...]
    loop(total - 1, lambda s: vector((me + s + 1) % total, me).wait_recv())
    piece, qv_piece, up_piece = widths

    def assemble(out, piece, first, rows, device):
        group = max(LANES // piece, 1)
        split = max(piece // LANES, 1)
        for tile in range(out.shape[1] // LANES):
            if split > 1:
                at = first + tile % split
                value = vec_ref[device(tile // split), at : at + 1, :].astype(F32)
            else:
                value = vec_ref[device(tile * group), first : first + rows, :].astype(F32)
                for g in range(1, group):
                    value = value + vec_ref[device(tile * group + g), first : first + rows, :].astype(F32)
            out[0:rows, tile * LANES : (tile + 1) * LANES] = value

    assemble(affine, piece, 0, 6, lambda g: g)
    assemble(qv_bias, qv_piece, 6, 2, lambda d: d * n + i)
    assemble(up_bias, up_piece, 8, 1, lambda d: d * n + i)
    own_copy.wait()

    def compute(j):
        def norm(b):
            normal, _ = norm_stats(buf[j, rows_at(b, RB), :].astype(F32))
            here = pl.ds(pl.multiple_of(j * size + b * RB, RB), RB)
            n_ref[here, :] = normal.astype(BF)
            a_ref[here, :] = (normal * affine[0:1, :] + affine[1:2, :]).astype(BF)

        loop(size // RB, norm)
        for copy in leave(j):
            copy.start()

    def leave(j):
        here = rows_at(j, size)
        return [pltpu.make_async_copy(a_ref.at[here], a_hbm.at[here], out_sem.at[0, j]),
                pltpu.make_async_copy(n_ref.at[here], n_hbm.at[here], out_sem.at[1, j])]

    def left(j):
        for copy in leave(j):
            copy.wait()

    def between(r):
        for stage in range(1, weights.stages):
            @pl.when(r == stage)
            def _():
                weights.advance(stage)

    rounds(i, n, line, compute, between)
    line.finish()
    weights.finish()
    loop(n, left)
    loop(total - 1, lambda s: vector(me, (me + s + 1) % total).wait_send())


def attend_kernel(n, m, pieces, a_hbm, wq_hbm, wo_hbm, up_ref, down_ref, x_ref, cot_ref, bias, vec,
                  qkv_hbm, o_hbm, h_ref, c_ref, cot_all, up_all, down_all, w_send, w_recv, w_local, qkv_ref, o_ref, out_sem, a_ref, wq_ref, w_ref, part, land, send, recv, s_send, s_recv, own_sem, a_sem, w_sem):
    i, row = lax.axis_index("tensor"), lax.axis_index("dp")
    size = x_ref.shape[0]
    loads = [pltpu.make_async_copy(a_hbm, a_ref, a_sem)]
    loads += [pltpu.make_async_copy(wq_hbm.at[t], wq_ref.at[t], w_sem.at[t]) for t in range(3)]
    loads += [pltpu.make_async_copy(wo_hbm, w_ref, w_sem.at[3])]
    for load in loads:
        load.start()
    heads = qkv_ref.shape[2] // HD
    depth = w_ref.shape[1]
    greet_cross(i, n, row, m)
    line = LineGather(i, n, cot_ref, cot_all, send, recv)
    line.start()
    weights = PlaneGather(row, m, [(up_ref, up_all, half_rows, row_blocks(m)), (down_ref, down_all, half_rows, column_blocks(m))],
                          w_send, w_recv, w_local)
    weights.start()
    own_copy = pltpu.make_async_copy(cot_ref, cot_all.at[i], own_sem)
    own_copy.start()

    loads[0].wait()
    block = 256
    for t in range(3):
        loads[1 + t].wait()

        def project(b):
            here = rows_at(b, block)
            value = jnp.dot(a_ref[here, :], wq_ref[t], preferred_element_type=F32)
            if t != 1:
                value = value + bias[t // 2 : t // 2 + 1, :]
            qkv_ref[t, here, :] = value.astype(BF)

        loop(LEN // block, project)

    def head(t):
        cols = pl.ds(pl.multiple_of(t * HD, HD), HD)
        for b in range(LEN // block):
            here, keys = slice(b * block, (b + 1) * block), (b + 1) * block
            s = lax.dot_general(qkv_ref[0, here, cols], qkv_ref[1, 0:keys, cols], NT,
                                preferred_element_type=F32) * HD ** (-0.5)
            query = lax.broadcasted_iota(jnp.int32, s.shape, 0) + b * block
            s = jnp.where(query >= lax.broadcasted_iota(jnp.int32, s.shape, 1), s, -1e30)
            e = jnp.exp(s - jnp.max(s, axis=-1, keepdims=True))
            prob = (e / jnp.sum(e, axis=-1, keepdims=True)).astype(BF)
            o_ref[here, cols] = jnp.dot(prob, qkv_ref[2, 0:keys, cols], preferred_element_type=F32).astype(BF)

    loop(heads, head)
    leave = [pltpu.make_async_copy(qkv_ref, qkv_hbm, out_sem.at[0]), pltpu.make_async_copy(o_ref, o_hbm, out_sem.at[1])]
    for copy in leave:
        copy.start()
    loads[4].wait()
    sums = LineSum(i, n, part, land, s_send, s_recv, pieces)
    tile = 512

    def project(t):
        d = jnp.where(i < n // 2, n - 1 - t, t)

        def columns(k):
            cols = rows_at(k, tile)
            part[d, :, cols] = jnp.dot(o_ref[rows_at(d, size), :], w_ref[:, cols], preferred_element_type=F32).astype(BF)

        loop(depth // tile, columns)
        sums.launch(d)

    loop(n, project)
    weights.advance(1)
    for r in range(1, n):
        line.step(r)
        for stage in range(2, weights.stages):
            if r == min(2 * stage - 1, n - 1):
                weights.advance(stage)
        relays(sums, i, n, r)

    def norm(b):
        here = rows_at(b, RB)
        sums.add(here, h_ref.at[here, :])
        rows = h_ref[here, :] + (x_ref[here, :].astype(F32) + vec[2:3, :])
        h_ref[here, :] = rows
        normal, _ = norm_stats(rows)
        c_ref[here, :] = (normal * vec[3:4, :] + vec[4:5, :]).astype(BF)

    sums.own(norm)
    own_copy.wait()
    for copy in leave:
        copy.wait()
    weights.finish()
    line.finish()
    sums.finish()


def hidden_kernel(n, pieces, c_ref, h_ref, cot_hbm, up_hbm, down_hbm, up_bias, vec, c_hbm, g_hbm, du_hbm, mlp_hbm, dh_ref,
                  db_ref, vec_ref, upb_ref, c_all, g_all, du_all, cot_all, up, down, part, land, send, recv, s_send,
                  s_recv, w_sem, cot_sem, own_sem, c_sem, g_sem, du_sem, mlp, mlp_sem):
    i = lax.axis_index("tensor")
    size, depth = c_ref.shape
    units = up.shape[1]
    greet_neighbours(i, n)
    line = LineGather(i, n, c_ref, c_all, send, recv)
    line.start()
    own_copy = pltpu.make_async_copy(c_ref, c_all.at[i], own_sem)
    own_copy.start()
    up_copy = pltpu.make_async_copy(up_hbm, up, w_sem.at[0])
    up_copy.start()
    down_copy = pltpu.make_async_copy(down_hbm, down, w_sem.at[1])
    down_copy.start()
    cot_copy = pltpu.make_async_copy(cot_hbm, cot_all, cot_sem)
    cot_copy.start()
    upb_ref[...] = jnp.zeros_like(upb_ref)
    vec_ref[...] = jnp.zeros_like(vec_ref)
    own_copy.wait()
    up_copy.wait()
    down_copy.wait()
    cot_copy.wait()
    sums = LineSum(i, n, part, land, s_send, s_recv, pieces)
    tile = 256

    def out_copy(src, dst, sem, j):
        return pltpu.make_async_copy(src.at[j], dst.at[j], sem.at[j])

    def compute(j):
        def unit(k):
            cols = rows_at(k, tile)
            u = jnp.dot(c_all[j], up[:, cols], preferred_element_type=F32) + up_bias[0:1, cols]
            dg = lax.dot_general(cot_all[j], down[cols, :], NT, preferred_element_type=F32)
            half = 0.5 + 0.5 * lax.erf(u * (0.5 ** 0.5))
            g_all[j, :, cols] = (u * half).astype(BF)
            slope = half + u * (jnp.exp(u * u * -0.5) * 0.3989422804014327)
            du = (slope * dg).astype(BF)
            du_all[j, :, cols] = du
            upb_ref[0:1, cols] += jnp.sum(du.astype(F32), axis=0, keepdims=True)

        loop(units // tile, unit)

        def back(k):
            cols = rows_at(k, tile)
            part[j, :, cols] = lax.dot_general(du_all[j], up[cols, :], NT, preferred_element_type=F32).astype(BF)

        loop(depth // tile, back)
        sums.launch(j)
        out_copy(g_all, g_hbm, g_sem, j).start()
        out_copy(du_all, du_hbm, du_sem, j).start()
        out_copy(c_all, c_hbm, c_sem, j).start()

    rounds(i, n, line, compute)

    def forward(j):
        def columns(k):
            cols = rows_at(k, tile)
            mlp[j, :, cols] = jnp.dot(g_all[j], down[:, cols], preferred_element_type=F32).astype(BF)

        loop(depth // tile, columns)
        out_copy(mlp, mlp_hbm, mlp_sem, j).start()

    def relay(t):
        early = jnp.where(i < n // 2, 1, 0)
        sums.relay(t + 3 - early - i, 2 * n - 4 - i - t - early)

        @pl.when(t < n // 2)
        def _():
            loop(2, lambda k: forward(2 * t + k))

    loop(2 * n - 3, relay)

    def norm(b):
        here = rows_at(b, RB)
        sums.add(here, dh_ref.at[here, :])
        grad = dh_ref[here, :]
        normal, inverse = norm_stats(h_ref[here, :])
        vec_ref[0:1, :] += jnp.sum(grad * normal, axis=0, keepdims=True)
        vec_ref[1:2, :] += jnp.sum(grad, axis=0, keepdims=True)
        cot = cot_all[i, here, :].astype(F32)
        dh = cot + norm_back(grad, normal, inverse, vec[3:4, :])
        dh_ref[here, :] = dh
        db = dh.astype(BF)
        db_ref[here, :] = db
        vec_ref[2:3, :] += jnp.sum(db.astype(F32), axis=0, keepdims=True)
        vec_ref[3:4, :] += jnp.sum(cot, axis=0, keepdims=True)

    sums.own(norm)

    def done(j):
        out_copy(g_all, g_hbm, g_sem, j).wait()
        out_copy(du_all, du_hbm, du_sem, j).wait()
        out_copy(c_all, c_hbm, c_sem, j).wait()
        out_copy(mlp, mlp_hbm, mlp_sem, j).wait()

    loop(n, done)
    line.finish()
    sums.finish()


def attend_back(b, block, column, heads, put, dk, dv):
    factor = HD ** (-0.5)
    here, keys = slice(b * block, (b + 1) * block), slice(0, (b + 1) * block)

    def head(t):
        q, k, v, do = column(0, here, t), column(1, keys, t), column(2, keys, t), column(3, here, t)
        s = lax.dot_general(q, k, NT, preferred_element_type=F32) * factor
        query = lax.broadcasted_iota(jnp.int32, s.shape, 0) + b * block
        s = jnp.where(query >= lax.broadcasted_iota(jnp.int32, s.shape, 1), s, -1e30)
        e = jnp.exp(s - jnp.max(s, axis=-1, keepdims=True))
        prob = e / jnp.sum(e, axis=-1, keepdims=True)
        dv[t, keys, :] += lax.dot_general(prob.astype(BF), do, TN, preferred_element_type=F32)
        dp = lax.dot_general(do, v, NT, preferred_element_type=F32)
        ds = (prob * (dp - jnp.sum(prob * dp, axis=-1, keepdims=True))).astype(BF)
        put(0, here, t, (jnp.dot(ds, k, preferred_element_type=F32) * factor).astype(BF))
        dk[t, keys, :] += lax.dot_general(ds, q, TN, preferred_element_type=F32)

    loop(heads, head)


class PlaneSum:
    def __init__(self, row, m, out, terms, land, halves, send, recv, h_send, h_recv):
        self.row, self.m, self.out, self.terms, self.land, self.halves = row, m, out, terms, land, halves
        self.send, self.recv, self.h_send, self.h_recv = send, recv, h_send, h_recv
        bits = [1 << k for k in range(1, m.bit_length() - 1)]
        self.plan = []
        for order in (bits, bits[::-1]):
            left, at, stages = [e for e in range(m) if e % 2 == 0], 0, []
            for bit in order:
                out = [e for e in left if e & bit]
                stages.append((bit, [(e, e ^ bit, at + k) for k, e in enumerate(out)]))
                left, at = [e for e in left if not e & bit], at + len(out)
            self.plan.append(stages)
        self.stages = len(bits)

    def owner(self, e):
        d = self.row
        for k in range(self.m.bit_length() - 1):
            if e & (1 << k):
                d = d + (partner(self.row, 1 << k) - self.row)
        return d

    def whole(self, e):
        return pltpu.make_async_remote_copy(
            src_ref=self.out.at[e // 2], dst_ref=self.land.at[e // 2], send_sem=self.send.at[e // 2],
            recv_sem=self.recv.at[e // 2], device_id={"dp": partner(self.row, 1)}, device_id_type=MESH)

    def half(self, h, bit, e, at):
        size = self.halves.shape[2]
        return pltpu.make_async_remote_copy(
            src_ref=self.terms.at[e // 2, pl.ds(h * size, size)], dst_ref=self.halves.at[h, at],
            send_sem=self.h_send.at[h, at], recv_sem=self.h_recv.at[h, at],
            device_id={"dp": partner(self.row, bit)}, device_id_type=MESH)

    def merge(self):
        for e in range(0, self.m, 2):
            self.whole(e + 1).wait_recv()

            def add(b):
                here = rows_at(b, RB)
                total = self.terms[e // 2, here, :].astype(F32) + self.land[e // 2, here, :].astype(F32)
                self.terms[e // 2, here, :] = total.astype(BF)

            loop(self.terms.shape[1] // RB, add)

    def push(self, stage):
        for h in range(2):
            bit, moves = self.plan[h][stage]
            for e, _, at in moves:
                self.half(h, bit, e, at).start()

    def take(self, stage, out=None):
        size = self.halves.shape[2]
        for h in range(2):
            bit, moves = self.plan[h][stage]
            for e, into, at in moves:
                self.half(h, bit, e, at).wait_recv()

                def add(b):
                    here, there = rows_at(b, RB), pl.ds(pl.multiple_of(h * size + b * RB, RB), RB)
                    total = self.terms[into // 2, there, :].astype(F32) + self.halves[h, at, here, :].astype(F32)
                    if out is None:
                        self.terms[into // 2, there, :] = total.astype(BF)
                    else:
                        out(there, total)

                loop(size // RB, add)

    def sent(self):
        for e in range(1, self.m, 2):
            self.whole(e).wait_send()

    def finish(self):
        for h in range(2):
            for bit, moves in self.plan[h]:
                for e, _, at in moves:
                    self.half(h, bit, e, at).wait_send()


class VectorSum:
    def __init__(self, me, count, device, vectors, piece, land, acc, send, recv):
        self.me, self.count, self.device, self.vectors, self.piece = me, count, device, vectors, piece
        self.land, self.acc, self.send, self.recv = land, acc, send, recv

    def lanes(self, owner):
        size = self.land.shape[2]
        return pl.ds(pl.multiple_of(owner * self.piece // size * size, size), size)

    def copy(self, src, other):
        return pltpu.make_async_remote_copy(
            src_ref=self.vectors.at[:, self.lanes(other)], dst_ref=self.land.at[src], send_sem=self.send.at[other],
            recv_sem=self.recv.at[src], device_id=self.device(other), device_id_type=MESH)

    def start(self):
        loop(self.count - 1, lambda s: self.copy(self.me, (self.me + s + 1) % self.count).start())

    def finish(self):
        self.acc[...] = self.vectors[:, self.lanes(self.me)]

        def take(s):
            src = (self.me + s + 1) % self.count
            self.copy(src, self.me).wait_recv()
            self.acc[...] += self.land[src]

        loop(self.count - 1, take)
        loop(self.count - 1, lambda s: self.copy(self.me, (self.me + s + 1) % self.count).wait_send())
        places = self.land.shape[2] // self.piece
        own = self.acc[:, 0 : self.piece]
        for k in range(1, places):
            own = jnp.where(self.me % places == k, self.acc[:, k * self.piece : (k + 1) * self.piece], own)
        return own


def greet_cross(i, n, row, m):
    barrier = pltpu.get_barrier_semaphore()

    @pl.when(i > 0)
    def _():
        pl.semaphore_signal(barrier, inc=1, device_id={"tensor": i - 1}, device_id_type=MESH)

    @pl.when(i < n - 1)
    def _():
        pl.semaphore_signal(barrier, inc=1, device_id={"tensor": i + 1}, device_id_type=MESH)

    bits = [1 << k for k in range(m.bit_length() - 1)]
    for bit in bits:
        pl.semaphore_signal(barrier, inc=1, device_id={"dp": partner(row, bit)}, device_id_type=MESH)
    pl.semaphore_wait(barrier, jnp.minimum(i, 1) + jnp.minimum(n - 1 - i, 1) + len(bits))


def relays(sums, i, n, r):
    sums.relay(n - 1 + i - r, r - (n - 1 - i))


def block_terms(plane, e, pairs):
    size = plane.terms.shape[1]
    cols = rows_at(plane.owner(e), size)
    for lhs, rhs, first in pairs:
        width = rhs.shape[1]
        tile = min(512, width)

        def columns(k):
            there = pl.ds(pl.multiple_of(first + k * tile, tile), tile)
            (plane.out if e % 2 else plane.terms)[e // 2, :, there] = lax.dot_general(
                lhs[:, cols], rhs[:, rows_at(k, tile)], TN, preferred_element_type=F32).astype(BF)

        loop(width // tile, columns)


def branch_kernel(n, m, pieces, db_ref, h_ref, vec, mlp_hbm, g_hbm, cot_hbm, c_hbm, du_hbm, qkv_hbm, wo_hbm,
                  db_all, lo_ref, down_t, up_ref, dqkv_hbm, down_ref, out_sem, lhs, rhs, wo, dk, dv, part, land, out, terms_a, land_a,
                  half_a, terms_b, land_b, half_b, acc, send, recv, s_send, s_recv, own_sem, part_sem, in_sem, qkv_sem,
                  db_sem, p_send, p_recv, h_send, h_recv):
    i, row = lax.axis_index("tensor"), lax.axis_index("dp")
    size = db_ref.shape[0]
    width = wo.shape[0]
    greet_cross(i, n, row, m)
    line = LineGather(i, n, db_ref, db_all, send, recv)
    line.start()
    part_copy = pltpu.make_async_copy(mlp_hbm, part, part_sem)
    part_copy.start()
    own_copy = pltpu.make_async_copy(db_ref, db_all.at[i], own_sem)
    own_copy.start()

    def load(left, right):
        return [pltpu.make_async_copy(left, lhs, in_sem.at[0]), pltpu.make_async_copy(right, rhs, in_sem.at[1])]

    loads = load(cot_hbm, g_hbm)
    for copy in loads:
        copy.start()
    wo_copy = pltpu.make_async_copy(wo_hbm, wo, in_sem.at[2])
    wo_copy.start()
    sums = LineSum(i, n, part, land, s_send, s_recv, pieces)
    part_copy.wait()
    loop(n, lambda t: sums.launch(jnp.where(i < n // 2, n - 1 - t, t)))
    planes = [PlaneSum(row, m, out, terms_a, land_a, half_a, p_send.at[0], p_recv.at[0], h_send.at[0], h_recv.at[0]),
              PlaneSum(row, m, out, terms_b, land_b, half_b, p_send.at[1], p_recv.at[1], h_send.at[1], h_recv.at[1])]
    first, second = planes
    for copy in loads:
        copy.wait()
    left, right = lhs.at[:, 0 : lhs.shape[1]], rhs.at[:, 0 : down_ref.shape[1]]
    for e in range(1, m, 2):
        block_terms(first, e, [(left, right, 0)])
        first.whole(e).start()
    for e in range(m - 2, -1, -2):
        block_terms(first, e, [(left, right, 0)])
    loads = load(c_hbm, du_hbm)
    for copy in loads:
        copy.start()
    first.merge()
    first.push(0)
    first.sent()
    for copy in loads:
        copy.wait()
    for e in range(1, m, 2):
        block_terms(second, e, [(left, right, 0)])
        second.whole(e).start()

    line.step(1)
    for e in range(m - 2, -1, -2):
        block_terms(second, e, [(left, right, 0)])
    qkv_copies = [pltpu.make_async_copy(qkv_hbm.at[p], rhs.at[:, p * width : (p + 1) * width], qkv_sem.at[p])
                  for p in range(3)]
    for copy in qkv_copies:
        copy.start()
    second.merge()
    second.push(0)
    own_copy.wait()
    wo_copy.wait()

    for copy in qkv_copies:
        copy.wait()
    dk[...] = jnp.zeros_like(dk)
    dv[...] = jnp.zeros_like(dv)

    def column(p, here, t):
        return rhs[here, pl.ds(pl.multiple_of(p * width + t * HD, HD), HD)]

    def put(p, here, t, value):
        rhs[here, pl.ds(pl.multiple_of(p * width + t * HD, HD), HD)] = value

    def mixture_back(j):
        here = rows_at(j, size)
        copy = pltpu.make_async_copy(db_all.at[j], lhs.at[here], db_sem.at[j])
        copy.start()
        copy.wait()
        rhs[here, 3 * width : 4 * width] = lax.dot_general(
            lhs[here, :], wo[...], NT, preferred_element_type=F32).astype(BF)
        for b in range(n):
            @pl.when(j == b)
            def _():
                attend_back(b, size, column, width // HD, put, dk, dv)

    def keep(ref):
        def put(here, total):
            ref[here, :] = total

        return put

    def advance(plane, stage, ref):
        if stage < plane.stages - 1:
            plane.take(stage)
            plane.push(stage + 1)
        else:
            plane.take(stage, keep(ref))

    def round_back(r):
        @pl.when(r >= 2)
        def _():
            line.step(r)
            relays(sums, i, n, r - 1)

        def side(s):
            j = jnp.where(s == 0, i - r, i + r)

            @pl.when(jnp.logical_and(jnp.logical_and(j >= 0, j <= n - 1), s * r == s * jnp.maximum(r, 1)))
            def _():
                mixture_back(j)

        loop(2, side)

        @pl.when(r == 1)
        def _():
            advance(first, 0, down_ref)

        @pl.when(r == min(2, n - 1))
        def _():
            advance(second, 0, up_ref)

    loop(n, round_back)
    relays(sums, i, n, n - 1)

    def whole(t):
        put(1, slice(0, LEN), t, (dk[t] * HD ** (-0.5)).astype(BF))
        put(2, slice(0, LEN), t, dv[t].astype(BF))

    loop(width // HD, whole)
    leave = [pltpu.make_async_copy(rhs.at[:, p * width : (p + 1) * width], dqkv_hbm.at[p], out_sem.at[p]) for p in range(3)]
    for copy in leave:
        copy.start()
    for stage in range(1, first.stages):
        advance(first, stage, down_ref)
        advance(second, stage, up_ref)

    def turn(k):
        down_t[rows_at(k, LANES), :] = down_ref[:, rows_at(k, LANES)].T

    loop(down_ref.shape[1] // LANES, turn)

    def output(b):
        here = rows_at(b, RB)
        sums.add(here, acc)
        lo_ref[here, :] = (h_ref[here, :] + (acc[...] + vec[5:6, :])).astype(BF)

    sums.own(output)
    line.finish()
    sums.finish()
    second.sent()
    for plane in planes:
        plane.finish()
    for copy in leave:
        copy.wait()


def input_kernel(n, m, pieces, widths, dqkv_ref, wq_hbm, x_hbm, dh_hbm, vec, early_ref, up_ref, a_hbm, db_hbm, o_hbm,
                 n_hbm, gt_ref, gqkv_ref, gout_t, vec_out, up_out, qv_out, gout_ref, early_acc, late_acc, up_acc, qv_acc, vec_ref, qv_ref, wq, a_ref, db_ref,
                 o_ref, n_ref, x_ref, dh_ref, part, land, out_p, terms, land_p, half_p, acc, early_land, late_land, up_land, qv_land, s_send,
                 s_recv, in_sem, p_send, p_recv, h_send, h_recv, e_send, e_recv, l_send, l_recv, u_send, u_recv, q_send,
                 q_recv):
    i, row = lax.axis_index("tensor"), lax.axis_index("dp")
    me, total_devices = row * n + i, m * n
    size = x_hbm.shape[0]
    width = dqkv_ref.shape[2]
    piece, up_piece, qv_piece = widths
    depth = part.shape[2]
    loads = [pltpu.make_async_copy(src, dst, in_sem.at[k]) for k, (src, dst) in enumerate(
        [(wq_hbm, wq), (a_hbm, a_ref), (db_hbm, db_ref), (o_hbm, o_ref), (n_hbm, n_ref), (x_hbm, x_ref), (dh_hbm, dh_ref)])]
    loads[0].start()
    loads[4].start()
    greet_all(me, n, total_devices)
    every = [VectorSum(me, total_devices, lambda g: {"dp": g // n, "tensor": g % n}, early_ref, piece, early_land, early_acc,
                       e_send, e_recv),
             VectorSum(me, total_devices, lambda g: {"dp": g // n, "tensor": g % n}, vec_ref, piece, late_land, late_acc,
                       l_send, l_recv)]
    column = [VectorSum(row, m, lambda g: {"dp": g}, up_ref, up_piece, up_land, up_acc, u_send, u_recv),
              VectorSum(row, m, lambda g: {"dp": g}, qv_ref, qv_piece, qv_land, qv_acc, q_send, q_recv)]
    every[0].start()
    column[0].start()
    sums = LineSum(i, n, part, land, s_send, s_recv, pieces)
    vec_ref[...] = jnp.zeros_like(vec_ref)
    qv_ref[...] = jnp.zeros_like(qv_ref)
    loads[0].wait()
    loads[4].wait()
    for k in (1, 2, 3, 5, 6):
        loads[k].start()
    tile = 512

    def term(t):
        d = jnp.where(i < n // 2, n - 1 - t, t)
        here = rows_at(d, size)

        def columns(k):
            cols = rows_at(k, tile)
            total = lax.dot_general(dqkv_ref[0, here, :], wq[0, cols, :], NT, preferred_element_type=F32)
            for p in range(1, 3):
                total += lax.dot_general(dqkv_ref[p, here, :], wq[p, cols, :], NT, preferred_element_type=F32)
            part[d, :, cols] = total.astype(BF)
            vec_ref[0:1, cols] += jnp.sum(total * n_ref[here, cols].astype(F32), axis=0, keepdims=True)
            vec_ref[1:2, cols] += jnp.sum(total, axis=0, keepdims=True)

        loop(depth // tile, columns)

        @pl.when(t == 0)
        def _():
            sums.launch(d)

        for p in range(2):
            qv_ref[p : p + 1, :] += jnp.sum(dqkv_ref[2 * p, here, :].astype(F32), axis=0, keepdims=True)

    loop(n, term)
    every[1].start()
    column[1].start()
    loop(n - 1, lambda t: sums.launch(jnp.where(i < n // 2, n - 2 - t, t + 1)))
    for k in (1, 2, 3, 5, 6):
        loads[k].wait()
    plane = PlaneSum(row, m, out_p, terms, land_p, half_p, p_send, p_recv, h_send, h_recv)
    pairs = [(a_ref, dqkv_ref.at[p], p * width) for p in range(3)] + [(db_ref, o_ref, 3 * width)]
    for e in range(1, m, 2):
        block_terms(plane, e, pairs)
        plane.whole(e).start()
    for e in range(m - 2, -1, -2):
        block_terms(plane, e, pairs)
    plane.merge()
    plane.push(0)

    def out(here, total):
        for p in range(3):
            gqkv_ref[p, here, :] = total[:, p * width : (p + 1) * width]
        gout_ref[here, :] = total[:, 3 * width :]

    stage = 0
    for r in range(1, n):
        relays(sums, i, n, r)
        if r > 1 and stage < plane.stages:
            if stage < plane.stages - 1:
                plane.take(stage)
                plane.push(stage + 1)
            else:
                plane.take(stage, out)
            stage += 1

    def norm(b):
        here = rows_at(b, RB)
        sums.add(here, acc)
        grad = acc[...]
        normal, inverse = norm_stats(x_ref[here, :].astype(F32))
        gt_ref[here, :] = (dh_ref[here, :] + norm_back(grad, normal, inverse, vec[0:1, :])).astype(BF)

    while stage < plane.stages:
        if stage < plane.stages - 1:
            plane.take(stage)
            plane.push(stage + 1)
        else:
            plane.take(stage, out)
        stage += 1
    gout_t[...] = gout_ref[...].T
    early, late = every[0].finish(), every[1].finish()
    for k, (rows, at) in enumerate([(late, 0), (late, 1), (early, 2), (early, 0), (early, 1), (early, 3)]):
        vec_out[k : k + 1, :] = rows[at : at + 1, :]
    up_out[...] = column[0].finish()
    qv_out[...] = column[1].finish()
    sums.own(norm)
    sums.finish()
    plane.sent()
    plane.finish()


def params(collective=None):
    if collective is None:
        return pltpu.CompilerParams(vmem_limit_bytes=BIG)
    return pltpu.CompilerParams(vmem_limit_bytes=BIG, collective_id=collective, has_side_effects=True)


def shape(dims, dtype):
    return jax.ShapeDtypeStruct(dims, dtype)


def body(tokens, cotangent, ln1_gain, ln1_bias, qkv_weight, qv_bias, out_weight, out_bias, ln2_gain, ln2_bias,
         up_weight, up_bias, down_weight, down_bias):
    n = lax.axis_size("tensor")
    m = lax.axis_size("dp")
    i, row = lax.axis_index("tensor"), lax.axis_index("dp")
    size, depth = tokens.shape
    width = qkv_weight.shape[2]
    units = up_weight.shape[1]
    piece, qv_piece, up_piece = ln1_gain.shape[0], qv_bias.shape[1], up_bias.shape[0]
    total = m * n

    def lane_rows(value, index):
        count = value.shape[-1]
        if count >= LANES:
            return value.reshape(-1, LANES)
        places = LANES // count
        spread = jnp.tile(value.reshape(-1, count), (1, places))
        return jnp.where((jnp.arange(LANES) // count)[None] == index % places, spread, 0)

    me = row * n + i
    whole = jnp.stack([ln1_gain, ln1_bias, out_bias, ln2_gain, ln2_bias, down_bias])
    pack = jnp.concatenate([lane_rows(whole, me), lane_rows(qv_bias, row), lane_rows(up_bias, row)])
    pack = jnp.pad(pack, ((0, -pack.shape[0] % 16), (0, 0)))
    lanes_up = 8 + max(up_piece // LANES, 1)

    dma = pltpu.SemaphoreType.DMA
    weight_sems = [dma((2, 2, m - 1)), dma((2, 2, m)), dma((2, 2))]
    attn_in, normal_one, vectors, bias_qv, bias_up, w_qkv, w_out = pl.pallas_call(
        functools.partial(tokens_kernel, n, m, (piece, qv_piece, up_piece)),
        out_shape=(shape((LEN, depth), BF), shape((LEN, depth), BF), shape((8, depth), F32), shape((8, width), F32),
                   shape((8, units), F32), shape((3, depth, width), BF), shape((width, depth), BF)),
        in_specs=[VM] * 4, out_specs=(ANY, ANY, VM, VM, VM, ANY, ANY),
        scratch_shapes=[pltpu.VMEM((total,) + pack.shape, BF), pltpu.VMEM((n, size, depth), BF), pltpu.VMEM((LEN, depth), BF),
                        pltpu.VMEM((LEN, depth), BF), dma((2, n))] + weight_sems +
                       [dma, dma((2, n, LineGather.PIECES)), dma((n, LineGather.PIECES)), dma((total,)), dma((total,))],
        compiler_params=params(0), name="gather_tokens",
    )(pack, tokens, qkv_weight, out_weight)

    pieces = 2
    sums = [pltpu.VMEM((n, size, depth), BF), pltpu.VMEM((n + 1, size, depth), BF)]
    qkv, mixture, residual, mlp_own, cot_all, w_up, w_down = pl.pallas_call(
        functools.partial(attend_kernel, n, m, pieces),
        out_shape=(shape((3, LEN, width), BF), shape((LEN, width), BF), shape((size, depth), F32),
                   shape((size, depth), BF), shape((n, size, depth), BF), shape((depth, units), BF), shape((units, depth), BF)),
        in_specs=[ANY] * 3 + [VM] * 6, out_specs=(ANY, ANY, VM, VM, ANY, ANY, ANY),
        scratch_shapes=weight_sems + [pltpu.VMEM((3, LEN, width), BF), pltpu.VMEM((LEN, width), BF), dma((2,)),
                        pltpu.VMEM((LEN, depth), BF), pltpu.VMEM((3, depth, width), BF), pltpu.VMEM((width, depth), BF)] +
                       sums + [dma((2, n, LineGather.PIECES)), dma((n, LineGather.PIECES)), dma((n, pieces)), dma((n + 1, pieces)), dma, dma, dma((4,))],
        compiler_params=params(1), name="attend",
    )(attn_in, w_qkv, w_out, up_weight, down_weight, tokens, cotangent, bias_qv, vectors)

    pieces = min(4, size // RB)
    mlp_in, hidden, grad_pre, mlp_part, grad_resid, branch_cot, vec_two, grad_up_b = pl.pallas_call(
        functools.partial(hidden_kernel, n, pieces),
        out_shape=(shape((n, size, depth), BF), shape((n, size, units), BF), shape((n, size, units), BF),
                   shape((n, size, depth), BF), shape((size, depth), F32), shape((size, depth), BF),
                   shape((8, depth), F32), shape((8, units), F32)),
        in_specs=[VM, VM, ANY, ANY, ANY, VM, VM], out_specs=(ANY, ANY, ANY, ANY, VM, VM, VM, VM),
        scratch_shapes=[pltpu.VMEM((n, size, depth), BF), pltpu.VMEM((n, size, units), BF),
                        pltpu.VMEM((n, size, units), BF), pltpu.VMEM((n, size, depth), BF),
                        pltpu.VMEM((depth, units), BF), pltpu.VMEM((units, depth), BF)] + sums +
                       [dma((2, n, LineGather.PIECES)), dma((n, LineGather.PIECES)), dma((n, pieces)), dma((n + 1, pieces)), dma((2,)), dma, dma,
                        dma((n,)), dma((n,)), dma((n,)), pltpu.VMEM((n, size, depth), BF), dma((n,))],
        compiler_params=params(2), name="hidden",
    )(mlp_own, residual, cot_all, w_up, w_down, bias_up, vectors)
    mlp_in, hidden, grad_pre, cot_rows = [v.reshape(LEN, -1) for v in (mlp_in, hidden, grad_pre, cot_all)]

    def plane_scratch(columns):
        rows = depth // m
        return [pltpu.VMEM((m // 2, rows, columns), BF), pltpu.VMEM((m // 2, rows, columns), BF),
                pltpu.VMEM((2, m // 2 - 1, rows // 2, columns), BF)]

    pieces = 2
    sum_sems = [dma((n, pieces)), dma((n + 1, pieces))]
    attn_cot, layer_out, grad_down_w, grad_up_w, grad_qkv = pl.pallas_call(
        functools.partial(branch_kernel, n, m, pieces),
        out_shape=(shape((n, size, depth), BF), shape((size, depth), BF), shape((units, depth // m), F32),
                   shape((depth // m, units), F32), shape((3, LEN, width), BF)),
        in_specs=[VM] * 3 + [ANY] * 7, out_specs=(ANY, VM, VM, VM, ANY),
        scratch_shapes=[pltpu.VMEM((depth // m, units), F32), dma((3,)), pltpu.VMEM((LEN, depth), BF), pltpu.VMEM((LEN, units), BF), pltpu.VMEM((width, depth), BF),
                        pltpu.VMEM((width // HD, LEN, HD), F32), pltpu.VMEM((width // HD, LEN, HD), F32)] + sums +
                       [pltpu.VMEM((m // 2, depth // m, units), BF)] + plane_scratch(units) * 2 +
                       [pltpu.VMEM((RB, depth), F32), dma((2, n, LineGather.PIECES)), dma((n, LineGather.PIECES))] + sum_sems +
                       [dma, dma, dma((3,)), dma((3,)), dma((n,)), dma((2, m // 2)), dma((2, m // 2)),
                        dma((2, 2, m // 2 - 1)), dma((2, 2, m // 2 - 1))],
        compiler_params=params(4), name="branch",
    )(branch_cot, residual, vectors, mlp_part, hidden, cot_rows, mlp_in, grad_pre, qkv, w_out)
    attn_cot = attn_cot.reshape(LEN, depth)

    tiles = [max(v, LANES) for v in (piece, up_piece, qv_piece)]
    grad_tokens, grad_qkv_w, grad_out_w, vector_grads, grad_up_b, grad_qv_b = pl.pallas_call(
        functools.partial(input_kernel, n, m, pieces, (piece, up_piece, qv_piece)),
        out_shape=(shape((size, depth), BF), shape((3, depth // m, width), F32), shape((width, depth // m), F32),
                   shape((8, piece), F32), shape((8, up_piece), F32), shape((8, qv_piece), F32)),
        in_specs=[VM, ANY, ANY, ANY, VM, VM, VM, ANY, ANY, ANY, ANY], out_specs=(VM,) * 6,
        scratch_shapes=[pltpu.VMEM((depth // m, width), F32)] + [pltpu.VMEM((8, tiles[k]), F32) for k in (0, 0, 1, 2)] + [
                        pltpu.VMEM((8, depth), F32), pltpu.VMEM((8, width), F32),
                        pltpu.VMEM((3, depth, width), BF), pltpu.VMEM((LEN, depth), BF), pltpu.VMEM((LEN, depth), BF),
                        pltpu.VMEM((LEN, width), BF), pltpu.VMEM((LEN, depth), BF), pltpu.VMEM((size, depth), BF),
                        pltpu.VMEM((size, depth), F32)] + sums +
                       [pltpu.VMEM((m // 2, depth // m, 4 * width), BF)] +
                       plane_scratch(4 * width) +
                       [pltpu.VMEM((RB, depth), F32), pltpu.VMEM((total, 8, tiles[0]), F32),
                        pltpu.VMEM((total, 8, tiles[0]), F32), pltpu.VMEM((m, 8, tiles[1]), F32),
                        pltpu.VMEM((m, 8, tiles[2]), F32)] + sum_sems +
                       [dma((7,)), dma((m // 2,)), dma((m // 2,)), dma((2, m // 2 - 1)), dma((2, m // 2 - 1))] +
                       [dma((total,))] * 4 + [dma((m,))] * 4,
        compiler_params=params(5), name="input",
    )(grad_qkv, w_qkv, tokens, grad_resid, vectors, vec_two, grad_up_b, attn_in, attn_cot, mixture, normal_one)

    vectors = [vector_grads[k] for k in range(6)]
    grad_up_b, grad_qv_b = grad_up_b[0], grad_qv_b[:2]
    return (layer_out, grad_tokens, vectors[0], vectors[1], grad_qkv_w, grad_qv_b, grad_out_w, vectors[2],
            vectors[3], vectors[4], grad_up_w, grad_up_b, grad_down_w, vectors[5])


def solution(mesh):
    vector, matrix = P(("dp", "tensor")), P(("dp", "tensor"), None)
    in_specs = (matrix, matrix, vector, vector, P(None, "dp", "tensor"), P(None, ("tensor", "dp")), P("tensor", "dp"),
                vector, vector, vector, P("dp", "tensor"), P(("tensor", "dp")), P("tensor", "dp"), vector)
    out_specs = (matrix, matrix, vector, vector, P(None, "dp", "tensor"), P(None, ("tensor", "dp")),
                 P("tensor", "dp"), vector, vector, vector, P("dp", "tensor"), P(("tensor", "dp")), P("tensor", "dp"),
                 vector)
    return jax.shard_map(body, mesh=mesh, in_specs=in_specs, out_specs=out_specs, check_vma=False)
```

```python
import functools

import jax
import jax.numpy as jnp
from jax import lax
from jax.experimental import pallas as pl
from jax.experimental.pallas import tpu as pltpu
from jax.sharding import PartitionSpec as P

HD = 128
LEN = 1024
LANES = 128
EPS = 1e-05
BF = jnp.bfloat16
F32 = jnp.float32
MESH = pl.DeviceIdType.MESH
ANY = pl.BlockSpec(memory_space=pl.ANY)
VM = pl.BlockSpec(memory_space=pltpu.VMEM)
NT = (((1,), (1,)), ((), ()))
TN = (((0,), (0,)), ((), ()))
BIG = 64 * 1024 * 1024 - 65536
RB = 32


def norm_stats(rows):
    mean = jnp.mean(rows, axis=-1, keepdims=True)
    centred = rows - mean
    variance = jnp.mean(centred * centred, axis=-1, keepdims=True)
    inverse = lax.rsqrt(variance + EPS)
    return centred * inverse, inverse


def norm_back(grad_rows, normal_rows, inverse, gain):
    scaled = grad_rows * gain
    first = jnp.mean(scaled, axis=-1, keepdims=True)
    second = jnp.mean(scaled * normal_rows, axis=-1, keepdims=True)
    return inverse * (scaled - first - normal_rows * second)


def loop(count, step):
    def run(i, carry):
        step(i)
        return carry

    lax.fori_loop(0, count, run, 0)


def rows_at(j, size):
    return pl.ds(pl.multiple_of(j * size, size), size)


def remote(src, dst, send, recv, target):
    return pltpu.make_async_remote_copy(src_ref=src, dst_ref=dst, send_sem=send, recv_sem=recv,
                                        device_id={"tensor": target}, device_id_type=MESH)


def greet_neighbours(i, n):
    barrier = pltpu.get_barrier_semaphore()

    @pl.when(i > 0)
    def _():
        pl.semaphore_signal(barrier, inc=1, device_id={"tensor": i - 1}, device_id_type=MESH)

    @pl.when(i < n - 1)
    def _():
        pl.semaphore_signal(barrier, inc=1, device_id={"tensor": i + 1}, device_id_type=MESH)

    pl.semaphore_wait(barrier, jnp.minimum(i, 1) + jnp.minimum(n - 1 - i, 1))


def greet_all(me, n, total):
    barrier = pltpu.get_barrier_semaphore()

    def greet(s):
        other = (me + s + 1) % total
        pl.semaphore_signal(barrier, inc=1, device_id={"dp": other // n, "tensor": other % n}, device_id_type=MESH)

    loop(total - 1, greet)
    pl.semaphore_wait(barrier, total - 1)


def rounds(i, n, line, compute, between=None):
    def round_of(r):
        @pl.when(r > 0)
        def _():
            line.step(r)

        if between is not None:
            between(r)

        def side(s):
            j = jnp.where(s == 0, i - r, i + r)

            @pl.when(jnp.logical_and(jnp.logical_and(j >= 0, j <= n - 1), s * r == s * jnp.maximum(r, 1)))
            def _():
                compute(j)

        loop(2, side)

    loop(n, round_of)


class LineGather:
    PIECES = 2

    def __init__(self, i, n, own, buf, send, recv):
        self.i, self.n, self.own, self.buf, self.send, self.recv = i, n, own, buf, send, recv
        self.size = own.shape[0] // self.PIECES

    def copy(self, src, j, side, s, target):
        here = pl.ds(s * self.size, self.size)
        return remote(src.at[here], self.buf.at[j, here], self.send.at[side, j, s], self.recv.at[j, s], target)

    def start(self):
        i, n = self.i, self.n
        for s in range(self.PIECES):
            @pl.when(i < n - 1)
            def _():
                self.copy(self.own, i, 0, s, i + 1).start()

            @pl.when(i > 0)
            def _():
                self.copy(self.own, i, 1, s, i - 1).start()

    def step(self, r):
        i, n = self.i, self.n
        for s in range(self.PIECES):
            @pl.when(i - r >= 0)
            def _():
                self.copy(self.own, i - r, 0, s, i).wait_recv()

                @pl.when(i < n - 1)
                def _():
                    self.copy(self.buf.at[i - r], i - r, 0, s, i + 1).start()

            @pl.when(i + r <= n - 1)
            def _():
                self.copy(self.own, i + r, 1, s, i).wait_recv()

                @pl.when(i > 0)
                def _():
                    self.copy(self.buf.at[i + r], i + r, 1, s, i - 1).start()

    def finish(self):
        i, n = self.i, self.n

        def one(j):
            for s in range(self.PIECES):
                @pl.when(jnp.logical_and(i < n - 1, j <= i))
                def _():
                    self.copy(self.own, j, 0, s, i + 1).wait_send()

                @pl.when(jnp.logical_and(i > 0, j >= i))
                def _():
                    self.copy(self.own, j, 1, s, i - 1).wait_send()

        loop(n, one)


class LineSum:
    def __init__(self, i, n, part, land, send, recv, pieces):
        self.i, self.n, self.part, self.land, self.send, self.recv = i, n, part, land, send, recv
        self.pieces = pieces
        self.size = part.shape[1] // pieces

    def copy(self, src, d, right, s):
        i, n = self.i, self.n
        target = i + 1 if right else i - 1
        slot = d if right else jnp.where(d == target, n, d)
        here = rows_at(s, self.size)
        return remote(src.at[d, here], self.land.at[slot, here], self.send.at[d, s], self.recv.at[slot, s], target)

    def arrived(self, slot, s):
        here = rows_at(s, self.size)
        remote(self.part.at[0, here], self.land.at[slot, here], self.send.at[0, s], self.recv.at[slot, s],
               self.i).wait_recv()

    def launch(self, d):
        i, n = self.i, self.n

        @pl.when(jnp.logical_and(i == 0, d > 0))
        def _():
            loop(self.pieces, lambda s: self.copy(self.part, d, True, s).start())

        @pl.when(jnp.logical_and(i == n - 1, d < n - 1))
        def _():
            loop(self.pieces, lambda s: self.copy(self.part, d, False, s).start())

    def relay(self, right, left):
        i, n = self.i, self.n

        def move(d, to_right, s):
            self.arrived(d, s)
            here = rows_at(s, self.size)
            total = self.land[d, here, :].astype(F32) + self.part[d, here, :].astype(F32)
            self.land[d, here, :] = total.astype(BF)
            self.copy(self.land, d, to_right, s).start()

        first = jnp.where(i < n // 2, 0, 1)

        def one(s):
            turn, s = (s + first) % 2, s // 2

            @pl.when(jnp.logical_and(turn == 0, jnp.logical_and(i > 0, jnp.logical_and(right > i, right <= n - 1))))
            def _():
                move(right, True, s)

            @pl.when(jnp.logical_and(turn == 1, jnp.logical_and(i < n - 1, jnp.logical_and(left >= 0, left < i))))
            def _():
                move(left, False, s)

        loop(2 * self.pieces, one)

    def own(self, step):
        i, n = self.i, self.n

        def one(s):
            @pl.when(i > 0)
            def _():
                self.arrived(i, s)

            @pl.when(i < n - 1)
            def _():
                self.arrived(n, s)

            loop(self.size // RB, lambda b: step(s * (self.size // RB) + b))

        loop(self.pieces, one)

    def add(self, here, out):
        i, n = self.i, self.n
        out[...] = self.part[i, here, :].astype(F32)

        @pl.when(i > 0)
        def _():
            out[...] += self.land[i, here, :].astype(F32)

        @pl.when(i < n - 1)
        def _():
            out[...] += self.land[n, here, :].astype(F32)

    def finish(self):
        i, n = self.i, self.n

        def one(d):
            @pl.when(jnp.logical_and(i < n - 1, d > i))
            def _():
                loop(self.pieces, lambda s: self.copy(self.part, d, True, s).wait_send())

            @pl.when(jnp.logical_and(i > 0, d < i))
            def _():
                loop(self.pieces, lambda s: self.copy(self.part, d, False, s).wait_send())

        loop(n, one)


def partner(row, bit):
    return row + bit * (1 - 2 * ((row // bit) % 2))


class PlaneGather:
    def __init__(self, row, m, items, send, recv, local):
        self.row, self.m, self.items, self.send, self.recv, self.local = row, m, items, send, recv, local
        bits = [1 << k for k in range(1, m.bit_length() - 1)]
        self.plan = []
        for order in (bits + [1], bits[::-1] + [1]):
            have, at, stages = [0], 0, []
            for bit in order:
                stages.append((bit, [(e, at + k) for k, e in enumerate(have)]))
                at, have = at + len(have), have + [e ^ bit for e in have]
            self.plan.append(stages)
        self.stages = len(bits) + 1

    def owner(self, e):
        d = self.row
        for k in range(self.m.bit_length() - 1):
            if e & (1 << k):
                d = d + (partner(self.row, 1 << k) - self.row)
        return d

    def copies(self, stage):
        for k, (own, whole, own_half, half) in enumerate(self.items):
            for h in range(2):
                bit, moves = self.plan[h][stage]
                for e, at in moves:
                    there = half(whole, self.owner(e), h)
                    src = own_half(own, h) if e == 0 else there
                    yield pltpu.make_async_remote_copy(
                        src_ref=src, dst_ref=there, send_sem=self.send.at[k, h, at], recv_sem=self.recv.at[k, h, e ^ bit],
                        device_id={"dp": partner(self.row, bit)}, device_id_type=MESH)

    def landed(self, stage):
        for k, (own, whole, own_half, half) in enumerate(self.items):
            for h in range(2):
                bit, moves = self.plan[h][stage]
                for e, at in moves:
                    there = half(whole, self.owner(e ^ bit), h)
                    pltpu.make_async_remote_copy(
                        src_ref=there, dst_ref=there, send_sem=self.send.at[k, h, at], recv_sem=self.recv.at[k, h, e ^ bit],
                        device_id={"dp": partner(self.row, bit)}, device_id_type=MESH).wait_recv()

    def locals(self):
        return [pltpu.make_async_copy(own_half(own, h), half(whole, self.row, h), self.local.at[k, h])
                for k, (own, whole, own_half, half) in enumerate(self.items) for h in range(2)]

    def start(self):
        for copy in self.copies(0):
            copy.start()
        for copy in self.locals():
            copy.start()

    def advance(self, stage):
        self.landed(stage - 1)
        for copy in self.copies(stage):
            copy.start()

    def finish(self):
        self.landed(self.stages - 1)
        for stage in range(self.stages):
            for copy in self.copies(stage):
                copy.wait_send()
        for copy in self.locals():
            copy.wait()


def half_rows(own, h):
    size = own.shape[-2] // 2
    return own.at[..., pl.ds(h * size, size), :]


def row_blocks(m):
    def half(whole, d, h):
        size = whole.shape[-2] // m // 2
        return whole.at[..., pl.ds(pl.multiple_of((2 * d + h) * size, size), size), :]

    return half


def column_blocks(m):
    def half(whole, d, h):
        size, width = whole.shape[-2] // 2, whole.shape[-1] // m
        return whole.at[pl.ds(h * size, size), pl.ds(pl.multiple_of(d * width, width), width)]

    return half


def tokens_kernel(n, m, widths, pack_ref, x_ref, wq_ref, wo_ref, a_hbm, n_hbm, affine, qv_bias, up_bias, wq_all, wo_all,
                  vec_ref, buf, a_ref, n_ref, out_sem, w_send, w_recv, w_local, own_sem, send, recv, v_send, v_recv):
    i, row = lax.axis_index("tensor"), lax.axis_index("dp")
    me, total = row * n + i, m * n
    size = x_ref.shape[0]
    greet_all(me, n, total)
    line = LineGather(i, n, x_ref, buf, send, recv)

    def vector(src, other):
        return pltpu.make_async_remote_copy(
            src_ref=pack_ref, dst_ref=vec_ref.at[src], send_sem=v_send.at[other], recv_sem=v_recv.at[src],
            device_id={"dp": other // n, "tensor": other % n}, device_id_type=MESH)

    loop(total - 1, lambda s: vector(me, (me + s + 1) % total).start())
    line.start()
    weights = PlaneGather(row, m, [(wq_ref, wq_all, half_rows, row_blocks(m)), (wo_ref, wo_all, half_rows, column_blocks(m))],
                          w_send, w_recv, w_local)
    weights.start()
    own_copy = pltpu.make_async_copy(x_ref, buf.at[i], own_sem)
    own_copy.start()
    vec_ref[me] = pack_ref[...]
    loop(total - 1, lambda s: vector((me + s + 1) % total, me).wait_recv())
    piece, qv_piece, up_piece = widths

    def assemble(out, piece, first, rows, device):
        group = max(LANES // piece, 1)
        split = max(piece // LANES, 1)
        for tile in range(out.shape[1] // LANES):
            if split > 1:
                at = first + tile % split
                value = vec_ref[device(tile // split), at : at + 1, :].astype(F32)
            else:
                value = vec_ref[device(tile * group), first : first + rows, :].astype(F32)
                for g in range(1, group):
                    value = value + vec_ref[device(tile * group + g), first : first + rows, :].astype(F32)
            out[0:rows, tile * LANES : (tile + 1) * LANES] = value

    assemble(affine, piece, 0, 6, lambda g: g)
    assemble(qv_bias, qv_piece, 6, 2, lambda d: d * n + i)
    assemble(up_bias, up_piece, 8, 1, lambda d: d * n + i)
    own_copy.wait()

    def compute(j):
        def norm(b):
            normal, _ = norm_stats(buf[j, rows_at(b, RB), :].astype(F32))
            here = pl.ds(pl.multiple_of(j * size + b * RB, RB), RB)
            n_ref[here, :] = normal.astype(BF)
            a_ref[here, :] = (normal * affine[0:1, :] + affine[1:2, :]).astype(BF)

        loop(size // RB, norm)
        for copy in leave(j):
            copy.start()

    def leave(j):
        here = rows_at(j, size)
        return [pltpu.make_async_copy(a_ref.at[here], a_hbm.at[here], out_sem.at[0, j]),
                pltpu.make_async_copy(n_ref.at[here], n_hbm.at[here], out_sem.at[1, j])]

    def left(j):
        for copy in leave(j):
            copy.wait()

    def between(r):
        for stage in range(1, weights.stages):
            @pl.when(r == stage)
            def _():
                weights.advance(stage)

    rounds(i, n, line, compute, between)
    line.finish()
    weights.finish()
    loop(n, left)
    loop(total - 1, lambda s: vector(me, (me + s + 1) % total).wait_send())


def attend_kernel(n, m, pieces, a_hbm, wq_hbm, wo_hbm, up_ref, down_ref, x_ref, cot_ref, bias, vec,
                  qkv_hbm, o_hbm, h_ref, c_ref, cot_all, up_all, down_all, w_send, w_recv, w_local, qkv_ref, o_ref, out_sem, a_ref, wq_ref, w_ref, part, land, send, recv, s_send, s_recv, own_sem, a_sem, w_sem):
    i, row = lax.axis_index("tensor"), lax.axis_index("dp")
    size = x_ref.shape[0]
    loads = [pltpu.make_async_copy(a_hbm, a_ref, a_sem)]
    loads += [pltpu.make_async_copy(wq_hbm.at[t], wq_ref.at[t], w_sem.at[t]) for t in range(3)]
    loads += [pltpu.make_async_copy(wo_hbm, w_ref, w_sem.at[3])]
    for load in loads:
        load.start()
    heads = qkv_ref.shape[2] // HD
    depth = w_ref.shape[1]
    greet_cross(i, n, row, m)
    line = LineGather(i, n, cot_ref, cot_all, send, recv)
    line.start()
    weights = PlaneGather(row, m, [(up_ref, up_all, half_rows, row_blocks(m)), (down_ref, down_all, half_rows, column_blocks(m))],
                          w_send, w_recv, w_local)
    weights.start()
    own_copy = pltpu.make_async_copy(cot_ref, cot_all.at[i], own_sem)
    own_copy.start()

    loads[0].wait()
    block = 256
    for t in range(3):
        loads[1 + t].wait()

        def project(b):
            here = rows_at(b, block)
            value = jnp.dot(a_ref[here, :], wq_ref[t], preferred_element_type=F32)
            if t != 1:
                value = value + bias[t // 2 : t // 2 + 1, :]
            qkv_ref[t, here, :] = value.astype(BF)

        loop(LEN // block, project)

    def head(t):
        cols = pl.ds(pl.multiple_of(t * HD, HD), HD)
        for b in range(LEN // block):
            here, keys = slice(b * block, (b + 1) * block), (b + 1) * block
            s = lax.dot_general(qkv_ref[0, here, cols], qkv_ref[1, 0:keys, cols], NT,
                                preferred_element_type=F32) * HD ** (-0.5)
            query = lax.broadcasted_iota(jnp.int32, s.shape, 0) + b * block
            s = jnp.where(query >= lax.broadcasted_iota(jnp.int32, s.shape, 1), s, -1e30)
            e = jnp.exp(s - jnp.max(s, axis=-1, keepdims=True))
            prob = (e / jnp.sum(e, axis=-1, keepdims=True)).astype(BF)
            o_ref[here, cols] = jnp.dot(prob, qkv_ref[2, 0:keys, cols], preferred_element_type=F32).astype(BF)

    loop(heads, head)
    leave = [pltpu.make_async_copy(qkv_ref, qkv_hbm, out_sem.at[0]), pltpu.make_async_copy(o_ref, o_hbm, out_sem.at[1])]
    for copy in leave:
        copy.start()
    loads[4].wait()
    sums = LineSum(i, n, part, land, s_send, s_recv, pieces)
    tile = 512

    def project(t):
        d = jnp.where(i < n // 2, n - 1 - t, t)

        def columns(k):
            cols = rows_at(k, tile)
            part[d, :, cols] = jnp.dot(o_ref[rows_at(d, size), :], w_ref[:, cols], preferred_element_type=F32).astype(BF)

        loop(depth // tile, columns)
        sums.launch(d)

    loop(n, project)
    weights.advance(1)
    for r in range(1, n):
        line.step(r)
        for stage in range(2, weights.stages):
            if r == min(2 * stage - 1, n - 1):
                weights.advance(stage)
        relays(sums, i, n, r)

    def norm(b):
        here = rows_at(b, RB)
        sums.add(here, h_ref.at[here, :])
        rows = h_ref[here, :] + (x_ref[here, :].astype(F32) + vec[2:3, :])
        h_ref[here, :] = rows
        normal, _ = norm_stats(rows)
        c_ref[here, :] = (normal * vec[3:4, :] + vec[4:5, :]).astype(BF)

    sums.own(norm)
    own_copy.wait()
    for copy in leave:
        copy.wait()
    weights.finish()
    line.finish()
    sums.finish()


def hidden_kernel(n, pieces, c_ref, h_ref, cot_hbm, up_hbm, down_hbm, up_bias, vec, c_hbm, g_hbm, du_hbm, mlp_hbm, dh_ref,
                  db_ref, vec_ref, upb_ref, c_all, g_all, du_all, cot_all, up, down, part, land, send, recv, s_send,
                  s_recv, w_sem, cot_sem, own_sem, c_sem, g_sem, du_sem, mlp, mlp_sem):
    i = lax.axis_index("tensor")
    size, depth = c_ref.shape
    units = up.shape[1]
    greet_neighbours(i, n)
    line = LineGather(i, n, c_ref, c_all, send, recv)
    line.start()
    own_copy = pltpu.make_async_copy(c_ref, c_all.at[i], own_sem)
    own_copy.start()
    up_copy = pltpu.make_async_copy(up_hbm, up, w_sem.at[0])
    up_copy.start()
    down_copy = pltpu.make_async_copy(down_hbm, down, w_sem.at[1])
    down_copy.start()
    cot_copy = pltpu.make_async_copy(cot_hbm, cot_all, cot_sem)
    cot_copy.start()
    upb_ref[...] = jnp.zeros_like(upb_ref)
    vec_ref[...] = jnp.zeros_like(vec_ref)
    own_copy.wait()
    up_copy.wait()
    down_copy.wait()
    cot_copy.wait()
    sums = LineSum(i, n, part, land, s_send, s_recv, pieces)
    tile = 256

    def out_copy(src, dst, sem, j):
        return pltpu.make_async_copy(src.at[j], dst.at[j], sem.at[j])

    def compute(j):
        def unit(k):
            cols = rows_at(k, tile)
            u = jnp.dot(c_all[j], up[:, cols], preferred_element_type=F32) + up_bias[0:1, cols]
            dg = lax.dot_general(cot_all[j], down[cols, :], NT, preferred_element_type=F32)
            half = 0.5 + 0.5 * lax.erf(u * (0.5 ** 0.5))
            g_all[j, :, cols] = (u * half).astype(BF)
            slope = half + u * (jnp.exp(u * u * -0.5) * 0.3989422804014327)
            du = (slope * dg).astype(BF)
            du_all[j, :, cols] = du
            upb_ref[0:1, cols] += jnp.sum(du.astype(F32), axis=0, keepdims=True)

        loop(units // tile, unit)

        def back(k):
            cols = rows_at(k, tile)
            part[j, :, cols] = lax.dot_general(du_all[j], up[cols, :], NT, preferred_element_type=F32).astype(BF)

        loop(depth // tile, back)
        sums.launch(j)
        out_copy(g_all, g_hbm, g_sem, j).start()
        out_copy(du_all, du_hbm, du_sem, j).start()
        out_copy(c_all, c_hbm, c_sem, j).start()

    rounds(i, n, line, compute)

    def forward(j):
        def columns(k):
            cols = rows_at(k, tile)
            mlp[j, :, cols] = jnp.dot(g_all[j], down[:, cols], preferred_element_type=F32).astype(BF)

        loop(depth // tile, columns)
        out_copy(mlp, mlp_hbm, mlp_sem, j).start()

    def relay(t):
        early = jnp.where(i < n // 2, 1, 0)
        sums.relay(t + 3 - early - i, 2 * n - 4 - i - t - early)

        @pl.when(t < n // 2)
        def _():
            loop(2, lambda k: forward(2 * t + k))

    loop(2 * n - 3, relay)

    def norm(b):
        here = rows_at(b, RB)
        sums.add(here, dh_ref.at[here, :])
        grad = dh_ref[here, :]
        normal, inverse = norm_stats(h_ref[here, :])
        vec_ref[0:1, :] += jnp.sum(grad * normal, axis=0, keepdims=True)
        vec_ref[1:2, :] += jnp.sum(grad, axis=0, keepdims=True)
        cot = cot_all[i, here, :].astype(F32)
        dh = cot + norm_back(grad, normal, inverse, vec[3:4, :])
        dh_ref[here, :] = dh
        db = dh.astype(BF)
        db_ref[here, :] = db
        vec_ref[2:3, :] += jnp.sum(db.astype(F32), axis=0, keepdims=True)
        vec_ref[3:4, :] += jnp.sum(cot, axis=0, keepdims=True)

    sums.own(norm)

    def done(j):
        out_copy(g_all, g_hbm, g_sem, j).wait()
        out_copy(du_all, du_hbm, du_sem, j).wait()
        out_copy(c_all, c_hbm, c_sem, j).wait()
        out_copy(mlp, mlp_hbm, mlp_sem, j).wait()

    loop(n, done)
    line.finish()
    sums.finish()


def attend_back(b, block, column, heads, put, dk, dv):
    factor = HD ** (-0.5)
    here, keys = slice(b * block, (b + 1) * block), slice(0, (b + 1) * block)

    def head(t):
        q, k, v, do = column(0, here, t), column(1, keys, t), column(2, keys, t), column(3, here, t)
        s = lax.dot_general(q, k, NT, preferred_element_type=F32) * factor
        query = lax.broadcasted_iota(jnp.int32, s.shape, 0) + b * block
        s = jnp.where(query >= lax.broadcasted_iota(jnp.int32, s.shape, 1), s, -1e30)
        e = jnp.exp(s - jnp.max(s, axis=-1, keepdims=True))
        prob = e / jnp.sum(e, axis=-1, keepdims=True)
        dv[t, keys, :] += lax.dot_general(prob.astype(BF), do, TN, preferred_element_type=F32)
        dp = lax.dot_general(do, v, NT, preferred_element_type=F32)
        ds = (prob * (dp - jnp.sum(prob * dp, axis=-1, keepdims=True))).astype(BF)
        put(0, here, t, (jnp.dot(ds, k, preferred_element_type=F32) * factor).astype(BF))
        dk[t, keys, :] += lax.dot_general(ds, q, TN, preferred_element_type=F32)

    loop(heads, head)


class PlaneSum:
    def __init__(self, row, m, out, terms, land, halves, send, recv, h_send, h_recv):
        self.row, self.m, self.out, self.terms, self.land, self.halves = row, m, out, terms, land, halves
        self.send, self.recv, self.h_send, self.h_recv = send, recv, h_send, h_recv
        bits = [1 << k for k in range(1, m.bit_length() - 1)]
        self.plan = []
        for order in (bits, bits[::-1]):
            left, at, stages = [e for e in range(m) if e % 2 == 0], 0, []
            for bit in order:
                out = [e for e in left if e & bit]
                stages.append((bit, [(e, e ^ bit, at + k) for k, e in enumerate(out)]))
                left, at = [e for e in left if not e & bit], at + len(out)
            self.plan.append(stages)
        self.stages = len(bits)

    def owner(self, e):
        d = self.row
        for k in range(self.m.bit_length() - 1):
            if e & (1 << k):
                d = d + (partner(self.row, 1 << k) - self.row)
        return d

    def whole(self, e):
        return pltpu.make_async_remote_copy(
            src_ref=self.out.at[e // 2], dst_ref=self.land.at[e // 2], send_sem=self.send.at[e // 2],
            recv_sem=self.recv.at[e // 2], device_id={"dp": partner(self.row, 1)}, device_id_type=MESH)

    def half(self, h, bit, e, at):
        size = self.halves.shape[2]
        return pltpu.make_async_remote_copy(
            src_ref=self.terms.at[e // 2, pl.ds(h * size, size)], dst_ref=self.halves.at[h, at],
            send_sem=self.h_send.at[h, at], recv_sem=self.h_recv.at[h, at],
            device_id={"dp": partner(self.row, bit)}, device_id_type=MESH)

    def merge(self):
        for e in range(0, self.m, 2):
            self.whole(e + 1).wait_recv()

            def add(b):
                here = rows_at(b, RB)
                total = self.terms[e // 2, here, :].astype(F32) + self.land[e // 2, here, :].astype(F32)
                self.terms[e // 2, here, :] = total.astype(BF)

            loop(self.terms.shape[1] // RB, add)

    def push(self, stage):
        for h in range(2):
            bit, moves = self.plan[h][stage]
            for e, _, at in moves:
                self.half(h, bit, e, at).start()

    def take(self, stage, out=None):
        size = self.halves.shape[2]
        for h in range(2):
            bit, moves = self.plan[h][stage]
            for e, into, at in moves:
                self.half(h, bit, e, at).wait_recv()

                def add(b):
                    here, there = rows_at(b, RB), pl.ds(pl.multiple_of(h * size + b * RB, RB), RB)
                    total = self.terms[into // 2, there, :].astype(F32) + self.halves[h, at, here, :].astype(F32)
                    if out is None:
                        self.terms[into // 2, there, :] = total.astype(BF)
                    else:
                        out(there, total)

                loop(size // RB, add)

    def sent(self):
        for e in range(1, self.m, 2):
            self.whole(e).wait_send()

    def finish(self):
        for h in range(2):
            for bit, moves in self.plan[h]:
                for e, _, at in moves:
                    self.half(h, bit, e, at).wait_send()


class VectorSum:
    def __init__(self, me, count, device, vectors, piece, land, acc, send, recv):
        self.me, self.count, self.device, self.vectors, self.piece = me, count, device, vectors, piece
        self.land, self.acc, self.send, self.recv = land, acc, send, recv

    def lanes(self, owner):
        size = self.land.shape[2]
        return pl.ds(pl.multiple_of(owner * self.piece // size * size, size), size)

    def copy(self, src, other):
        return pltpu.make_async_remote_copy(
            src_ref=self.vectors.at[:, self.lanes(other)], dst_ref=self.land.at[src], send_sem=self.send.at[other],
            recv_sem=self.recv.at[src], device_id=self.device(other), device_id_type=MESH)

    def start(self):
        loop(self.count - 1, lambda s: self.copy(self.me, (self.me + s + 1) % self.count).start())

    def finish(self):
        self.acc[...] = self.vectors[:, self.lanes(self.me)]

        def take(s):
            src = (self.me + s + 1) % self.count
            self.copy(src, self.me).wait_recv()
            self.acc[...] += self.land[src]

        loop(self.count - 1, take)
        loop(self.count - 1, lambda s: self.copy(self.me, (self.me + s + 1) % self.count).wait_send())
        places = self.land.shape[2] // self.piece
        own = self.acc[:, 0 : self.piece]
        for k in range(1, places):
            own = jnp.where(self.me % places == k, self.acc[:, k * self.piece : (k + 1) * self.piece], own)
        return own


def greet_cross(i, n, row, m):
    barrier = pltpu.get_barrier_semaphore()

    @pl.when(i > 0)
    def _():
        pl.semaphore_signal(barrier, inc=1, device_id={"tensor": i - 1}, device_id_type=MESH)

    @pl.when(i < n - 1)
    def _():
        pl.semaphore_signal(barrier, inc=1, device_id={"tensor": i + 1}, device_id_type=MESH)

    bits = [1 << k for k in range(m.bit_length() - 1)]
    for bit in bits:
        pl.semaphore_signal(barrier, inc=1, device_id={"dp": partner(row, bit)}, device_id_type=MESH)
    pl.semaphore_wait(barrier, jnp.minimum(i, 1) + jnp.minimum(n - 1 - i, 1) + len(bits))


def relays(sums, i, n, r):
    sums.relay(n - 1 + i - r, r - (n - 1 - i))


def block_terms(plane, e, pairs):
    size = plane.terms.shape[1]
    cols = rows_at(plane.owner(e), size)
    for lhs, rhs, first in pairs:
        width = rhs.shape[1]
        tile = min(512, width)

        def columns(k):
            there = pl.ds(pl.multiple_of(first + k * tile, tile), tile)
            (plane.out if e % 2 else plane.terms)[e // 2, :, there] = lax.dot_general(
                lhs[:, cols], rhs[:, rows_at(k, tile)], TN, preferred_element_type=F32).astype(BF)

        loop(width // tile, columns)


def branch_kernel(n, m, pieces, db_ref, h_ref, vec, mlp_hbm, g_hbm, cot_hbm, c_hbm, du_hbm, qkv_hbm, wo_hbm,
                  db_all, lo_ref, down_t, up_ref, dqkv_hbm, down_ref, out_sem, lhs, rhs, wo, dk, dv, part, land, out, terms_a, land_a,
                  half_a, terms_b, land_b, half_b, acc, send, recv, s_send, s_recv, own_sem, part_sem, in_sem, qkv_sem,
                  db_sem, p_send, p_recv, h_send, h_recv):
    i, row = lax.axis_index("tensor"), lax.axis_index("dp")
    size = db_ref.shape[0]
    width = wo.shape[0]
    greet_cross(i, n, row, m)
    line = LineGather(i, n, db_ref, db_all, send, recv)
    line.start()
    part_copy = pltpu.make_async_copy(mlp_hbm, part, part_sem)
    part_copy.start()
    own_copy = pltpu.make_async_copy(db_ref, db_all.at[i], own_sem)
    own_copy.start()

    def load(left, right):
        return [pltpu.make_async_copy(left, lhs, in_sem.at[0]), pltpu.make_async_copy(right, rhs, in_sem.at[1])]

    loads = load(cot_hbm, g_hbm)
    for copy in loads:
        copy.start()
    wo_copy = pltpu.make_async_copy(wo_hbm, wo, in_sem.at[2])
    wo_copy.start()
    sums = LineSum(i, n, part, land, s_send, s_recv, pieces)
    part_copy.wait()
    loop(n, lambda t: sums.launch(jnp.where(i < n // 2, n - 1 - t, t)))
    planes = [PlaneSum(row, m, out, terms_a, land_a, half_a, p_send.at[0], p_recv.at[0], h_send.at[0], h_recv.at[0]),
              PlaneSum(row, m, out, terms_b, land_b, half_b, p_send.at[1], p_recv.at[1], h_send.at[1], h_recv.at[1])]
    first, second = planes
    for copy in loads:
        copy.wait()
    left, right = lhs.at[:, 0 : lhs.shape[1]], rhs.at[:, 0 : down_ref.shape[1]]
    for e in range(1, m, 2):
        block_terms(first, e, [(left, right, 0)])
        first.whole(e).start()
    for e in range(m - 2, -1, -2):
        block_terms(first, e, [(left, right, 0)])
    loads = load(c_hbm, du_hbm)
    for copy in loads:
        copy.start()
    first.merge()
    first.push(0)
    first.sent()
    for copy in loads:
        copy.wait()
    for e in range(1, m, 2):
        block_terms(second, e, [(left, right, 0)])
        second.whole(e).start()

    line.step(1)
    for e in range(m - 2, -1, -2):
        block_terms(second, e, [(left, right, 0)])
    qkv_copies = [pltpu.make_async_copy(qkv_hbm.at[p], rhs.at[:, p * width : (p + 1) * width], qkv_sem.at[p])
                  for p in range(3)]
    for copy in qkv_copies:
        copy.start()
    second.merge()
    second.push(0)
    own_copy.wait()
    wo_copy.wait()

    for copy in qkv_copies:
        copy.wait()
    dk[...] = jnp.zeros_like(dk)
    dv[...] = jnp.zeros_like(dv)

    def column(p, here, t):
        return rhs[here, pl.ds(pl.multiple_of(p * width + t * HD, HD), HD)]

    def put(p, here, t, value):
        rhs[here, pl.ds(pl.multiple_of(p * width + t * HD, HD), HD)] = value

    def mixture_back(j):
        here = rows_at(j, size)
        copy = pltpu.make_async_copy(db_all.at[j], lhs.at[here], db_sem.at[j])
        copy.start()
        copy.wait()
        rhs[here, 3 * width : 4 * width] = lax.dot_general(
            lhs[here, :], wo[...], NT, preferred_element_type=F32).astype(BF)
        for b in range(n):
            @pl.when(j == b)
            def _():
                attend_back(b, size, column, width // HD, put, dk, dv)

    def keep(ref):
        def put(here, total):
            ref[here, :] = total

        return put

    def advance(plane, stage, ref):
        if stage < plane.stages - 1:
            plane.take(stage)
            plane.push(stage + 1)
        else:
            plane.take(stage, keep(ref))

    def round_back(r):
        @pl.when(jnp.logical_and(r >= 1, r <= n - 2))
        def _():
            line.step(r + 1)
            relays(sums, i, n, r)

        def side(s):
            j = jnp.where(s == 0, i - r, i + r)

            @pl.when(jnp.logical_and(jnp.logical_and(j >= 0, j <= n - 1), s * r == s * jnp.maximum(r, 1)))
            def _():
                mixture_back(j)

        loop(2, side)

        @pl.when(r == 1)
        def _():
            advance(first, 0, down_ref)

        @pl.when(r == min(2, n - 1))
        def _():
            advance(second, 0, up_ref)

    loop(n, round_back)
    relays(sums, i, n, n - 1)

    def whole(t):
        put(1, slice(0, LEN), t, (dk[t] * HD ** (-0.5)).astype(BF))
        put(2, slice(0, LEN), t, dv[t].astype(BF))

    loop(width // HD, whole)
    leave = [pltpu.make_async_copy(rhs.at[:, p * width : (p + 1) * width], dqkv_hbm.at[p], out_sem.at[p]) for p in range(3)]
    for copy in leave:
        copy.start()
    for stage in range(1, first.stages):
        advance(first, stage, down_ref)
        advance(second, stage, up_ref)

    def turn(k):
        down_t[rows_at(k, LANES), :] = down_ref[:, rows_at(k, LANES)].T

    loop(down_ref.shape[1] // LANES, turn)

    def output(b):
        here = rows_at(b, RB)
        sums.add(here, acc)
        lo_ref[here, :] = (h_ref[here, :] + (acc[...] + vec[5:6, :])).astype(BF)

    sums.own(output)
    line.finish()
    sums.finish()
    second.sent()
    for plane in planes:
        plane.finish()
    for copy in leave:
        copy.wait()


def input_kernel(n, m, pieces, widths, dqkv_ref, wq_hbm, x_hbm, dh_hbm, vec, early_ref, up_ref, a_hbm, db_hbm, o_hbm,
                 n_hbm, gt_ref, gqkv_ref, gout_t, vec_out, up_out, qv_out, gout_ref, early_acc, late_acc, up_acc, qv_acc, vec_ref, qv_ref, wq, a_ref, db_ref,
                 o_ref, n_ref, x_ref, dh_ref, part, land, out_p, terms, land_p, half_p, acc, early_land, late_land, up_land, qv_land, s_send,
                 s_recv, in_sem, p_send, p_recv, h_send, h_recv, e_send, e_recv, l_send, l_recv, u_send, u_recv, q_send,
                 q_recv):
    i, row = lax.axis_index("tensor"), lax.axis_index("dp")
    me, total_devices = row * n + i, m * n
    size = x_hbm.shape[0]
    width = dqkv_ref.shape[2]
    piece, up_piece, qv_piece = widths
    depth = part.shape[2]
    loads = [pltpu.make_async_copy(src, dst, in_sem.at[k]) for k, (src, dst) in enumerate(
        [(wq_hbm, wq), (a_hbm, a_ref), (db_hbm, db_ref), (o_hbm, o_ref), (n_hbm, n_ref), (x_hbm, x_ref), (dh_hbm, dh_ref)])]
    loads[0].start()
    loads[4].start()
    greet_all(me, n, total_devices)
    every = [VectorSum(me, total_devices, lambda g: {"dp": g // n, "tensor": g % n}, early_ref, piece, early_land, early_acc,
                       e_send, e_recv),
             VectorSum(me, total_devices, lambda g: {"dp": g // n, "tensor": g % n}, vec_ref, piece, late_land, late_acc,
                       l_send, l_recv)]
    column = [VectorSum(row, m, lambda g: {"dp": g}, up_ref, up_piece, up_land, up_acc, u_send, u_recv),
              VectorSum(row, m, lambda g: {"dp": g}, qv_ref, qv_piece, qv_land, qv_acc, q_send, q_recv)]
    every[0].start()
    column[0].start()
    sums = LineSum(i, n, part, land, s_send, s_recv, pieces)
    vec_ref[...] = jnp.zeros_like(vec_ref)
    qv_ref[...] = jnp.zeros_like(qv_ref)
    loads[0].wait()
    loads[4].wait()
    for k in (1, 2, 3, 5, 6):
        loads[k].start()
    tile = 512

    def term(t):
        d = jnp.where(i < n // 2, n - 1 - t, t)
        here = rows_at(d, size)

        def columns(k):
            cols = rows_at(k, tile)
            total = lax.dot_general(dqkv_ref[0, here, :], wq[0, cols, :], NT, preferred_element_type=F32)
            for p in range(1, 3):
                total += lax.dot_general(dqkv_ref[p, here, :], wq[p, cols, :], NT, preferred_element_type=F32)
            part[d, :, cols] = total.astype(BF)
            vec_ref[0:1, cols] += jnp.sum(total * n_ref[here, cols].astype(F32), axis=0, keepdims=True)
            vec_ref[1:2, cols] += jnp.sum(total, axis=0, keepdims=True)

        loop(depth // tile, columns)

        @pl.when(t == 0)
        def _():
            sums.launch(d)

        for p in range(2):
            qv_ref[p : p + 1, :] += jnp.sum(dqkv_ref[2 * p, here, :].astype(F32), axis=0, keepdims=True)

    loop(n, term)
    every[1].start()
    column[1].start()
    loop(n - 1, lambda t: sums.launch(jnp.where(i < n // 2, n - 2 - t, t + 1)))
    for k in (1, 2, 3, 5, 6):
        loads[k].wait()
    plane = PlaneSum(row, m, out_p, terms, land_p, half_p, p_send, p_recv, h_send, h_recv)
    pairs = [(a_ref, dqkv_ref.at[p], p * width) for p in range(3)] + [(db_ref, o_ref, 3 * width)]
    for e in range(1, m, 2):
        block_terms(plane, e, pairs)
        plane.whole(e).start()
    for e in range(m - 2, -1, -2):
        block_terms(plane, e, pairs)
    plane.merge()
    plane.push(0)

    def out(here, total):
        for p in range(3):
            gqkv_ref[p, here, :] = total[:, p * width : (p + 1) * width]
        gout_ref[here, :] = total[:, 3 * width :]

    stage = 0
    for r in range(1, n):
        relays(sums, i, n, r)
        if r > 1 and stage < plane.stages:
            if stage < plane.stages - 1:
                plane.take(stage)
                plane.push(stage + 1)
            else:
                plane.take(stage, out)
            stage += 1

    def norm(b):
        here = rows_at(b, RB)
        sums.add(here, acc)
        grad = acc[...]
        normal, inverse = norm_stats(x_ref[here, :].astype(F32))
        gt_ref[here, :] = (dh_ref[here, :] + norm_back(grad, normal, inverse, vec[0:1, :])).astype(BF)

    while stage < plane.stages:
        if stage < plane.stages - 1:
            plane.take(stage)
            plane.push(stage + 1)
        else:
            plane.take(stage, out)
        stage += 1
    gout_t[...] = gout_ref[...].T
    early, late = every[0].finish(), every[1].finish()
    for k, (rows, at) in enumerate([(late, 0), (late, 1), (early, 2), (early, 0), (early, 1), (early, 3)]):
        vec_out[k : k + 1, :] = rows[at : at + 1, :]
    up_out[...] = column[0].finish()
    qv_out[...] = column[1].finish()
    sums.own(norm)
    sums.finish()
    plane.sent()
    plane.finish()


def params(collective=None):
    if collective is None:
        return pltpu.CompilerParams(vmem_limit_bytes=BIG)
    return pltpu.CompilerParams(vmem_limit_bytes=BIG, collective_id=collective, has_side_effects=True)


def shape(dims, dtype):
    return jax.ShapeDtypeStruct(dims, dtype)


def body(tokens, cotangent, ln1_gain, ln1_bias, qkv_weight, qv_bias, out_weight, out_bias, ln2_gain, ln2_bias,
         up_weight, up_bias, down_weight, down_bias):
    n = lax.axis_size("tensor")
    m = lax.axis_size("dp")
    i, row = lax.axis_index("tensor"), lax.axis_index("dp")
    size, depth = tokens.shape
    width = qkv_weight.shape[2]
    units = up_weight.shape[1]
    piece, qv_piece, up_piece = ln1_gain.shape[0], qv_bias.shape[1], up_bias.shape[0]
    total = m * n

    def lane_rows(value, index):
        count = value.shape[-1]
        if count >= LANES:
            return value.reshape(-1, LANES)
        places = LANES // count
        spread = jnp.tile(value.reshape(-1, count), (1, places))
        return jnp.where((jnp.arange(LANES) // count)[None] == index % places, spread, 0)

    me = row * n + i
    whole = jnp.stack([ln1_gain, ln1_bias, out_bias, ln2_gain, ln2_bias, down_bias])
    pack = jnp.concatenate([lane_rows(whole, me), lane_rows(qv_bias, row), lane_rows(up_bias, row)])
    pack = jnp.pad(pack, ((0, -pack.shape[0] % 16), (0, 0)))
    lanes_up = 8 + max(up_piece // LANES, 1)

    dma = pltpu.SemaphoreType.DMA
    weight_sems = [dma((2, 2, m - 1)), dma((2, 2, m)), dma((2, 2))]
    attn_in, normal_one, vectors, bias_qv, bias_up, w_qkv, w_out = pl.pallas_call(
        functools.partial(tokens_kernel, n, m, (piece, qv_piece, up_piece)),
        out_shape=(shape((LEN, depth), BF), shape((LEN, depth), BF), shape((8, depth), F32), shape((8, width), F32),
                   shape((8, units), F32), shape((3, depth, width), BF), shape((width, depth), BF)),
        in_specs=[VM] * 4, out_specs=(ANY, ANY, VM, VM, VM, ANY, ANY),
        scratch_shapes=[pltpu.VMEM((total,) + pack.shape, BF), pltpu.VMEM((n, size, depth), BF), pltpu.VMEM((LEN, depth), BF),
                        pltpu.VMEM((LEN, depth), BF), dma((2, n))] + weight_sems +
                       [dma, dma((2, n, LineGather.PIECES)), dma((n, LineGather.PIECES)), dma((total,)), dma((total,))],
        compiler_params=params(0), name="gather_tokens",
    )(pack, tokens, qkv_weight, out_weight)

    pieces = 2
    sums = [pltpu.VMEM((n, size, depth), BF), pltpu.VMEM((n + 1, size, depth), BF)]
    qkv, mixture, residual, mlp_own, cot_all, w_up, w_down = pl.pallas_call(
        functools.partial(attend_kernel, n, m, pieces),
        out_shape=(shape((3, LEN, width), BF), shape((LEN, width), BF), shape((size, depth), F32),
                   shape((size, depth), BF), shape((n, size, depth), BF), shape((depth, units), BF), shape((units, depth), BF)),
        in_specs=[ANY] * 3 + [VM] * 6, out_specs=(ANY, ANY, VM, VM, ANY, ANY, ANY),
        scratch_shapes=weight_sems + [pltpu.VMEM((3, LEN, width), BF), pltpu.VMEM((LEN, width), BF), dma((2,)),
                        pltpu.VMEM((LEN, depth), BF), pltpu.VMEM((3, depth, width), BF), pltpu.VMEM((width, depth), BF)] +
                       sums + [dma((2, n, LineGather.PIECES)), dma((n, LineGather.PIECES)), dma((n, pieces)), dma((n + 1, pieces)), dma, dma, dma((4,))],
        compiler_params=params(1), name="attend",
    )(attn_in, w_qkv, w_out, up_weight, down_weight, tokens, cotangent, bias_qv, vectors)

    pieces = min(4, size // RB)
    mlp_in, hidden, grad_pre, mlp_part, grad_resid, branch_cot, vec_two, grad_up_b = pl.pallas_call(
        functools.partial(hidden_kernel, n, pieces),
        out_shape=(shape((n, size, depth), BF), shape((n, size, units), BF), shape((n, size, units), BF),
                   shape((n, size, depth), BF), shape((size, depth), F32), shape((size, depth), BF),
                   shape((8, depth), F32), shape((8, units), F32)),
        in_specs=[VM, VM, ANY, ANY, ANY, VM, VM], out_specs=(ANY, ANY, ANY, ANY, VM, VM, VM, VM),
        scratch_shapes=[pltpu.VMEM((n, size, depth), BF), pltpu.VMEM((n, size, units), BF),
                        pltpu.VMEM((n, size, units), BF), pltpu.VMEM((n, size, depth), BF),
                        pltpu.VMEM((depth, units), BF), pltpu.VMEM((units, depth), BF)] + sums +
                       [dma((2, n, LineGather.PIECES)), dma((n, LineGather.PIECES)), dma((n, pieces)), dma((n + 1, pieces)), dma((2,)), dma, dma,
                        dma((n,)), dma((n,)), dma((n,)), pltpu.VMEM((n, size, depth), BF), dma((n,))],
        compiler_params=params(2), name="hidden",
    )(mlp_own, residual, cot_all, w_up, w_down, bias_up, vectors)
    mlp_in, hidden, grad_pre, cot_rows = [v.reshape(LEN, -1) for v in (mlp_in, hidden, grad_pre, cot_all)]

    def plane_scratch(columns):
        rows = depth // m
        return [pltpu.VMEM((m // 2, rows, columns), BF), pltpu.VMEM((m // 2, rows, columns), BF),
                pltpu.VMEM((2, m // 2 - 1, rows // 2, columns), BF)]

    pieces = 2
    sum_sems = [dma((n, pieces)), dma((n + 1, pieces))]
    attn_cot, layer_out, grad_down_w, grad_up_w, grad_qkv = pl.pallas_call(
        functools.partial(branch_kernel, n, m, pieces),
        out_shape=(shape((n, size, depth), BF), shape((size, depth), BF), shape((units, depth // m), F32),
                   shape((depth // m, units), F32), shape((3, LEN, width), BF)),
        in_specs=[VM] * 3 + [ANY] * 7, out_specs=(ANY, VM, VM, VM, ANY),
        scratch_shapes=[pltpu.VMEM((depth // m, units), F32), dma((3,)), pltpu.VMEM((LEN, depth), BF), pltpu.VMEM((LEN, units), BF), pltpu.VMEM((width, depth), BF),
                        pltpu.VMEM((width // HD, LEN, HD), F32), pltpu.VMEM((width // HD, LEN, HD), F32)] + sums +
                       [pltpu.VMEM((m // 2, depth // m, units), BF)] + plane_scratch(units) * 2 +
                       [pltpu.VMEM((RB, depth), F32), dma((2, n, LineGather.PIECES)), dma((n, LineGather.PIECES))] + sum_sems +
                       [dma, dma, dma((3,)), dma((3,)), dma((n,)), dma((2, m // 2)), dma((2, m // 2)),
                        dma((2, 2, m // 2 - 1)), dma((2, 2, m // 2 - 1))],
        compiler_params=params(4), name="branch",
    )(branch_cot, residual, vectors, mlp_part, hidden, cot_rows, mlp_in, grad_pre, qkv, w_out)
    attn_cot = attn_cot.reshape(LEN, depth)

    tiles = [max(v, LANES) for v in (piece, up_piece, qv_piece)]
    grad_tokens, grad_qkv_w, grad_out_w, vector_grads, grad_up_b, grad_qv_b = pl.pallas_call(
        functools.partial(input_kernel, n, m, pieces, (piece, up_piece, qv_piece)),
        out_shape=(shape((size, depth), BF), shape((3, depth // m, width), F32), shape((width, depth // m), F32),
                   shape((8, piece), F32), shape((8, up_piece), F32), shape((8, qv_piece), F32)),
        in_specs=[VM, ANY, ANY, ANY, VM, VM, VM, ANY, ANY, ANY, ANY], out_specs=(VM,) * 6,
        scratch_shapes=[pltpu.VMEM((depth // m, width), F32)] + [pltpu.VMEM((8, tiles[k]), F32) for k in (0, 0, 1, 2)] + [
                        pltpu.VMEM((8, depth), F32), pltpu.VMEM((8, width), F32),
                        pltpu.VMEM((3, depth, width), BF), pltpu.VMEM((LEN, depth), BF), pltpu.VMEM((LEN, depth), BF),
                        pltpu.VMEM((LEN, width), BF), pltpu.VMEM((LEN, depth), BF), pltpu.VMEM((size, depth), BF),
                        pltpu.VMEM((size, depth), F32)] + sums +
                       [pltpu.VMEM((m // 2, depth // m, 4 * width), BF)] +
                       plane_scratch(4 * width) +
                       [pltpu.VMEM((RB, depth), F32), pltpu.VMEM((total, 8, tiles[0]), F32),
                        pltpu.VMEM((total, 8, tiles[0]), F32), pltpu.VMEM((m, 8, tiles[1]), F32),
                        pltpu.VMEM((m, 8, tiles[2]), F32)] + sum_sems +
                       [dma((7,)), dma((m // 2,)), dma((m // 2,)), dma((2, m // 2 - 1)), dma((2, m // 2 - 1))] +
                       [dma((total,))] * 4 + [dma((m,))] * 4,
        compiler_params=params(5), name="input",
    )(grad_qkv, w_qkv, tokens, grad_resid, vectors, vec_two, grad_up_b, attn_in, attn_cot, mixture, normal_one)

    vectors = [vector_grads[k] for k in range(6)]
    grad_up_b, grad_qv_b = grad_up_b[0], grad_qv_b[:2]
    return (layer_out, grad_tokens, vectors[0], vectors[1], grad_qkv_w, grad_qv_b, grad_out_w, vectors[2],
            vectors[3], vectors[4], grad_up_w, grad_up_b, grad_down_w, vectors[5])


def solution(mesh):
    vector, matrix = P(("dp", "tensor")), P(("dp", "tensor"), None)
    in_specs = (matrix, matrix, vector, vector, P(None, "dp", "tensor"), P(None, ("tensor", "dp")), P("tensor", "dp"),
                vector, vector, vector, P("dp", "tensor"), P(("tensor", "dp")), P("tensor", "dp"), vector)
    out_specs = (matrix, matrix, vector, vector, P(None, "dp", "tensor"), P(None, ("tensor", "dp")),
                 P("tensor", "dp"), vector, vector, vector, P("dp", "tensor"), P(("tensor", "dp")), P("tensor", "dp"),
                 vector)
    return jax.shard_map(body, mesh=mesh, in_specs=in_specs, out_specs=out_specs, check_vma=False)
```

```python
import functools

import jax
import jax.numpy as jnp
from jax import lax
from jax.experimental import pallas as pl
from jax.experimental.pallas import tpu as pltpu
from jax.sharding import PartitionSpec as P

HD = 128
LEN = 1024
LANES = 128
EPS = 1e-05
BF = jnp.bfloat16
F32 = jnp.float32
MESH = pl.DeviceIdType.MESH
ANY = pl.BlockSpec(memory_space=pl.ANY)
VM = pl.BlockSpec(memory_space=pltpu.VMEM)
NT = (((1,), (1,)), ((), ()))
TN = (((0,), (0,)), ((), ()))
BIG = 64 * 1024 * 1024 - 65536
RB = 32


def norm_stats(rows):
    mean = jnp.mean(rows, axis=-1, keepdims=True)
    centred = rows - mean
    variance = jnp.mean(centred * centred, axis=-1, keepdims=True)
    inverse = lax.rsqrt(variance + EPS)
    return centred * inverse, inverse


def norm_back(grad_rows, normal_rows, inverse, gain):
    scaled = grad_rows * gain
    first = jnp.mean(scaled, axis=-1, keepdims=True)
    second = jnp.mean(scaled * normal_rows, axis=-1, keepdims=True)
    return inverse * (scaled - first - normal_rows * second)


def loop(count, step):
    def run(i, carry):
        step(i)
        return carry

    lax.fori_loop(0, count, run, 0)


def rows_at(j, size):
    return pl.ds(pl.multiple_of(j * size, size), size)


def remote(src, dst, send, recv, target):
    return pltpu.make_async_remote_copy(src_ref=src, dst_ref=dst, send_sem=send, recv_sem=recv,
                                        device_id={"tensor": target}, device_id_type=MESH)


def greet_neighbours(i, n):
    barrier = pltpu.get_barrier_semaphore()

    @pl.when(i > 0)
    def _():
        pl.semaphore_signal(barrier, inc=1, device_id={"tensor": i - 1}, device_id_type=MESH)

    @pl.when(i < n - 1)
    def _():
        pl.semaphore_signal(barrier, inc=1, device_id={"tensor": i + 1}, device_id_type=MESH)

    pl.semaphore_wait(barrier, jnp.minimum(i, 1) + jnp.minimum(n - 1 - i, 1))


def greet_all(me, n, total):
    barrier = pltpu.get_barrier_semaphore()

    def greet(s):
        other = (me + s + 1) % total
        pl.semaphore_signal(barrier, inc=1, device_id={"dp": other // n, "tensor": other % n}, device_id_type=MESH)

    loop(total - 1, greet)
    pl.semaphore_wait(barrier, total - 1)


def rounds(i, n, line, compute, between=None):
    def round_of(r):
        @pl.when(r > 0)
        def _():
            line.step(r)

        if between is not None:
            between(r)

        def side(s):
            j = jnp.where(s == 0, i - r, i + r)

            @pl.when(jnp.logical_and(jnp.logical_and(j >= 0, j <= n - 1), s * r == s * jnp.maximum(r, 1)))
            def _():
                compute(j)

        loop(2, side)

    loop(n, round_of)


class LineGather:
    PIECES = 2

    def __init__(self, i, n, own, buf, send, recv):
        self.i, self.n, self.own, self.buf, self.send, self.recv = i, n, own, buf, send, recv
        self.size = own.shape[0] // self.PIECES

    def copy(self, src, j, side, s, target):
        here = pl.ds(s * self.size, self.size)
        return remote(src.at[here], self.buf.at[j, here], self.send.at[side, j, s], self.recv.at[j, s], target)

    def start(self):
        i, n = self.i, self.n
        for s in range(self.PIECES):
            @pl.when(i < n - 1)
            def _():
                self.copy(self.own, i, 0, s, i + 1).start()

            @pl.when(i > 0)
            def _():
                self.copy(self.own, i, 1, s, i - 1).start()

    def step(self, r):
        i, n = self.i, self.n
        for s in range(self.PIECES):
            @pl.when(i - r >= 0)
            def _():
                self.copy(self.own, i - r, 0, s, i).wait_recv()

                @pl.when(i < n - 1)
                def _():
                    self.copy(self.buf.at[i - r], i - r, 0, s, i + 1).start()

            @pl.when(i + r <= n - 1)
            def _():
                self.copy(self.own, i + r, 1, s, i).wait_recv()

                @pl.when(i > 0)
                def _():
                    self.copy(self.buf.at[i + r], i + r, 1, s, i - 1).start()

    def finish(self):
        i, n = self.i, self.n

        def one(j):
            for s in range(self.PIECES):
                @pl.when(jnp.logical_and(i < n - 1, j <= i))
                def _():
                    self.copy(self.own, j, 0, s, i + 1).wait_send()

                @pl.when(jnp.logical_and(i > 0, j >= i))
                def _():
                    self.copy(self.own, j, 1, s, i - 1).wait_send()

        loop(n, one)


class LineSum:
    def __init__(self, i, n, part, land, send, recv, pieces):
        self.i, self.n, self.part, self.land, self.send, self.recv = i, n, part, land, send, recv
        self.pieces = pieces
        self.size = part.shape[1] // pieces

    def copy(self, src, d, right, s):
        i, n = self.i, self.n
        target = i + 1 if right else i - 1
        slot = d if right else jnp.where(d == target, n, d)
        here = rows_at(s, self.size)
        return remote(src.at[d, here], self.land.at[slot, here], self.send.at[d, s], self.recv.at[slot, s], target)

    def arrived(self, slot, s):
        here = rows_at(s, self.size)
        remote(self.part.at[0, here], self.land.at[slot, here], self.send.at[0, s], self.recv.at[slot, s],
               self.i).wait_recv()

    def launch(self, d):
        i, n = self.i, self.n

        @pl.when(jnp.logical_and(i == 0, d > 0))
        def _():
            loop(self.pieces, lambda s: self.copy(self.part, d, True, s).start())

        @pl.when(jnp.logical_and(i == n - 1, d < n - 1))
        def _():
            loop(self.pieces, lambda s: self.copy(self.part, d, False, s).start())

    def relay(self, right, left):
        i, n = self.i, self.n

        def move(d, to_right, s):
            self.arrived(d, s)
            here = rows_at(s, self.size)
            total = self.land[d, here, :].astype(F32) + self.part[d, here, :].astype(F32)
            self.land[d, here, :] = total.astype(BF)
            self.copy(self.land, d, to_right, s).start()

        first = jnp.where(i < n // 2, 0, 1)

        def one(s):
            turn, s = (s + first) % 2, s // 2

            @pl.when(jnp.logical_and(turn == 0, jnp.logical_and(i > 0, jnp.logical_and(right > i, right <= n - 1))))
            def _():
                move(right, True, s)

            @pl.when(jnp.logical_and(turn == 1, jnp.logical_and(i < n - 1, jnp.logical_and(left >= 0, left < i))))
            def _():
                move(left, False, s)

        loop(2 * self.pieces, one)

    def own(self, step):
        i, n = self.i, self.n

        def one(s):
            @pl.when(i > 0)
            def _():
                self.arrived(i, s)

            @pl.when(i < n - 1)
            def _():
                self.arrived(n, s)

            loop(self.size // RB, lambda b: step(s * (self.size // RB) + b))

        loop(self.pieces, one)

    def add(self, here, out):
        i, n = self.i, self.n
        out[...] = self.part[i, here, :].astype(F32)

        @pl.when(i > 0)
        def _():
            out[...] += self.land[i, here, :].astype(F32)

        @pl.when(i < n - 1)
        def _():
            out[...] += self.land[n, here, :].astype(F32)

    def finish(self):
        i, n = self.i, self.n

        def one(d):
            @pl.when(jnp.logical_and(i < n - 1, d > i))
            def _():
                loop(self.pieces, lambda s: self.copy(self.part, d, True, s).wait_send())

            @pl.when(jnp.logical_and(i > 0, d < i))
            def _():
                loop(self.pieces, lambda s: self.copy(self.part, d, False, s).wait_send())

        loop(n, one)


def partner(row, bit):
    return row + bit * (1 - 2 * ((row // bit) % 2))


class PlaneGather:
    def __init__(self, row, m, items, send, recv, local):
        self.row, self.m, self.items, self.send, self.recv, self.local = row, m, items, send, recv, local
        bits = [1 << k for k in range(1, m.bit_length() - 1)]
        self.plan = []
        for order in (bits + [1], bits[::-1] + [1]):
            have, at, stages = [0], 0, []
            for bit in order:
                stages.append((bit, [(e, at + k) for k, e in enumerate(have)]))
                at, have = at + len(have), have + [e ^ bit for e in have]
            self.plan.append(stages)
        self.stages = len(bits) + 1

    def owner(self, e):
        d = self.row
        for k in range(self.m.bit_length() - 1):
            if e & (1 << k):
                d = d + (partner(self.row, 1 << k) - self.row)
        return d

    def copies(self, stage):
        for k, (own, whole, own_half, half) in enumerate(self.items):
            for h in range(2):
                bit, moves = self.plan[h][stage]
                for e, at in moves:
                    there = half(whole, self.owner(e), h)
                    src = own_half(own, h) if e == 0 else there
                    yield pltpu.make_async_remote_copy(
                        src_ref=src, dst_ref=there, send_sem=self.send.at[k, h, at], recv_sem=self.recv.at[k, h, e ^ bit],
                        device_id={"dp": partner(self.row, bit)}, device_id_type=MESH)

    def landed(self, stage):
        for k, (own, whole, own_half, half) in enumerate(self.items):
            for h in range(2):
                bit, moves = self.plan[h][stage]
                for e, at in moves:
                    there = half(whole, self.owner(e ^ bit), h)
                    pltpu.make_async_remote_copy(
                        src_ref=there, dst_ref=there, send_sem=self.send.at[k, h, at], recv_sem=self.recv.at[k, h, e ^ bit],
                        device_id={"dp": partner(self.row, bit)}, device_id_type=MESH).wait_recv()

    def locals(self):
        return [pltpu.make_async_copy(own_half(own, h), half(whole, self.row, h), self.local.at[k, h])
                for k, (own, whole, own_half, half) in enumerate(self.items) for h in range(2)]

    def start(self):
        for copy in self.copies(0):
            copy.start()
        for copy in self.locals():
            copy.start()

    def advance(self, stage):
        self.landed(stage - 1)
        for copy in self.copies(stage):
            copy.start()

    def finish(self):
        self.landed(self.stages - 1)
        for stage in range(self.stages):
            for copy in self.copies(stage):
                copy.wait_send()
        for copy in self.locals():
            copy.wait()


def half_rows(own, h):
    size = own.shape[-2] // 2
    return own.at[..., pl.ds(h * size, size), :]


def row_blocks(m):
    def half(whole, d, h):
        size = whole.shape[-2] // m // 2
        return whole.at[..., pl.ds(pl.multiple_of((2 * d + h) * size, size), size), :]

    return half


def column_blocks(m):
    def half(whole, d, h):
        size, width = whole.shape[-2] // 2, whole.shape[-1] // m
        return whole.at[pl.ds(h * size, size), pl.ds(pl.multiple_of(d * width, width), width)]

    return half


def tokens_kernel(n, m, widths, pack_ref, x_ref, wq_ref, wo_ref, a_hbm, n_hbm, affine, qv_bias, up_bias, wq_all, wo_all,
                  vec_ref, buf, a_ref, n_ref, out_sem, w_send, w_recv, w_local, own_sem, send, recv, v_send, v_recv):
    i, row = lax.axis_index("tensor"), lax.axis_index("dp")
    me, total = row * n + i, m * n
    size = x_ref.shape[0]
    greet_all(me, n, total)
    line = LineGather(i, n, x_ref, buf, send, recv)

    def vector(src, other):
        return pltpu.make_async_remote_copy(
            src_ref=pack_ref, dst_ref=vec_ref.at[src], send_sem=v_send.at[other], recv_sem=v_recv.at[src],
            device_id={"dp": other // n, "tensor": other % n}, device_id_type=MESH)

    loop(total - 1, lambda s: vector(me, (me + s + 1) % total).start())
    line.start()
    weights = PlaneGather(row, m, [(wq_ref, wq_all, half_rows, row_blocks(m)), (wo_ref, wo_all, half_rows, column_blocks(m))],
                          w_send, w_recv, w_local)
    weights.start()
    own_copy = pltpu.make_async_copy(x_ref, buf.at[i], own_sem)
    own_copy.start()
    vec_ref[me] = pack_ref[...]
    loop(total - 1, lambda s: vector((me + s + 1) % total, me).wait_recv())
    piece, qv_piece, up_piece = widths

    def assemble(out, piece, first, rows, device):
        group = max(LANES // piece, 1)
        split = max(piece // LANES, 1)
        for tile in range(out.shape[1] // LANES):
            if split > 1:
                at = first + tile % split
                value = vec_ref[device(tile // split), at : at + 1, :].astype(F32)
            else:
                value = vec_ref[device(tile * group), first : first + rows, :].astype(F32)
                for g in range(1, group):
                    value = value + vec_ref[device(tile * group + g), first : first + rows, :].astype(F32)
            out[0:rows, tile * LANES : (tile + 1) * LANES] = value

    assemble(affine, piece, 0, 6, lambda g: g)
    assemble(qv_bias, qv_piece, 6, 2, lambda d: d * n + i)
    assemble(up_bias, up_piece, 8, 1, lambda d: d * n + i)
    own_copy.wait()

    def compute(j):
        def norm(b):
            normal, _ = norm_stats(buf[j, rows_at(b, RB), :].astype(F32))
            here = pl.ds(pl.multiple_of(j * size + b * RB, RB), RB)
            n_ref[here, :] = normal.astype(BF)
            a_ref[here, :] = (normal * affine[0:1, :] + affine[1:2, :]).astype(BF)

        loop(size // RB, norm)
        for copy in leave(j):
            copy.start()

    def leave(j):
        here = rows_at(j, size)
        return [pltpu.make_async_copy(a_ref.at[here], a_hbm.at[here], out_sem.at[0, j]),
                pltpu.make_async_copy(n_ref.at[here], n_hbm.at[here], out_sem.at[1, j])]

    def left(j):
        for copy in leave(j):
            copy.wait()

    def between(r):
        for stage in range(1, weights.stages):
            @pl.when(r == stage)
            def _():
                weights.advance(stage)

    rounds(i, n, line, compute, between)
    line.finish()
    weights.finish()
    loop(n, left)
    loop(total - 1, lambda s: vector(me, (me + s + 1) % total).wait_send())


def attend_kernel(n, m, pieces, a_hbm, wq_hbm, wo_hbm, up_ref, down_ref, x_ref, cot_ref, bias, vec,
                  qkv_hbm, o_hbm, h_ref, c_ref, cot_all, up_all, down_all, w_send, w_recv, w_local, qkv_ref, o_ref, out_sem, a_ref, wq_ref, w_ref, part, land, send, recv, s_send, s_recv, own_sem, a_sem, w_sem):
    i, row = lax.axis_index("tensor"), lax.axis_index("dp")
    size = x_ref.shape[0]
    loads = [pltpu.make_async_copy(a_hbm, a_ref, a_sem)]
    loads += [pltpu.make_async_copy(wq_hbm.at[t], wq_ref.at[t], w_sem.at[t]) for t in range(3)]
    loads += [pltpu.make_async_copy(wo_hbm, w_ref, w_sem.at[3])]
    for load in loads:
        load.start()
    heads = qkv_ref.shape[2] // HD
    depth = w_ref.shape[1]
    greet_cross(i, n, row, m)
    line = LineGather(i, n, cot_ref, cot_all, send, recv)
    line.start()
    weights = PlaneGather(row, m, [(up_ref, up_all, half_rows, row_blocks(m)), (down_ref, down_all, half_rows, column_blocks(m))],
                          w_send, w_recv, w_local)
    weights.start()
    own_copy = pltpu.make_async_copy(cot_ref, cot_all.at[i], own_sem)
    own_copy.start()

    loads[0].wait()
    block = 256
    for t in range(3):
        loads[1 + t].wait()

        def project(b):
            here = rows_at(b, block)
            value = jnp.dot(a_ref[here, :], wq_ref[t], preferred_element_type=F32)
            if t != 1:
                value = value + bias[t // 2 : t // 2 + 1, :]
            qkv_ref[t, here, :] = value.astype(BF)

        loop(LEN // block, project)

    def head(t):
        cols = pl.ds(pl.multiple_of(t * HD, HD), HD)
        for b in range(LEN // block):
            here, keys = slice(b * block, (b + 1) * block), (b + 1) * block
            s = lax.dot_general(qkv_ref[0, here, cols], qkv_ref[1, 0:keys, cols], NT,
                                preferred_element_type=F32) * HD ** (-0.5)
            query = lax.broadcasted_iota(jnp.int32, s.shape, 0) + b * block
            s = jnp.where(query >= lax.broadcasted_iota(jnp.int32, s.shape, 1), s, -1e30)
            e = jnp.exp(s - jnp.max(s, axis=-1, keepdims=True))
            prob = (e / jnp.sum(e, axis=-1, keepdims=True)).astype(BF)
            o_ref[here, cols] = jnp.dot(prob, qkv_ref[2, 0:keys, cols], preferred_element_type=F32).astype(BF)

    loop(heads, head)
    leave = [pltpu.make_async_copy(qkv_ref, qkv_hbm, out_sem.at[0]), pltpu.make_async_copy(o_ref, o_hbm, out_sem.at[1])]
    for copy in leave:
        copy.start()
    loads[4].wait()
    sums = LineSum(i, n, part, land, s_send, s_recv, pieces)
    tile = 512

    def project(t):
        d = jnp.where(i < n // 2, n - 1 - t, t)

        def columns(k):
            cols = rows_at(k, tile)
            part[d, :, cols] = jnp.dot(o_ref[rows_at(d, size), :], w_ref[:, cols], preferred_element_type=F32).astype(BF)

        loop(depth // tile, columns)
        sums.launch(d)

    loop(n, project)
    weights.advance(1)
    for r in range(1, n):
        line.step(r)
        for stage in range(2, weights.stages):
            if r == min(2 * stage - 1, n - 1):
                weights.advance(stage)
        relays(sums, i, n, r)

    def norm(b):
        here = rows_at(b, RB)
        sums.add(here, h_ref.at[here, :])
        rows = h_ref[here, :] + (x_ref[here, :].astype(F32) + vec[2:3, :])
        h_ref[here, :] = rows
        normal, _ = norm_stats(rows)
        c_ref[here, :] = (normal * vec[3:4, :] + vec[4:5, :]).astype(BF)

    sums.own(norm)
    own_copy.wait()
    for copy in leave:
        copy.wait()
    weights.finish()
    line.finish()
    sums.finish()


def hidden_kernel(n, pieces, c_ref, h_ref, cot_hbm, up_hbm, down_hbm, up_bias, vec, c_hbm, g_hbm, du_hbm, mlp_hbm, dh_ref,
                  db_ref, vec_ref, upb_ref, c_all, g_all, du_all, cot_all, up, down, part, land, send, recv, s_send,
                  s_recv, w_sem, cot_sem, own_sem, c_sem, g_sem, du_sem, mlp, mlp_sem, ahead):
    i = lax.axis_index("tensor")
    size, depth = c_ref.shape
    units = up.shape[1]
    greet_neighbours(i, n)
    line = LineGather(i, n, c_ref, c_all, send, recv)
    line.start()
    own_copy = pltpu.make_async_copy(c_ref, c_all.at[i], own_sem)
    own_copy.start()
    up_copy = pltpu.make_async_copy(up_hbm, up, w_sem.at[0])
    up_copy.start()
    down_copy = pltpu.make_async_copy(down_hbm, down, w_sem.at[1])
    down_copy.start()
    cot_copy = pltpu.make_async_copy(cot_hbm, cot_all, cot_sem)
    cot_copy.start()
    upb_ref[...] = jnp.zeros_like(upb_ref)
    vec_ref[...] = jnp.zeros_like(vec_ref)
    own_copy.wait()
    up_copy.wait()
    down_copy.wait()
    cot_copy.wait()
    sums = LineSum(i, n, part, land, s_send, s_recv, pieces)
    tile = 256

    far = jnp.where(i < n // 2, n - 1, 0)

    def before(k):
        cols = rows_at(k, tile)
        ahead[1, :, cols] = lax.dot_general(cot_all[far], down[cols, :], NT, preferred_element_type=F32)

    loop(units // tile, before)

    def out_copy(src, dst, sem, j):
        return pltpu.make_async_copy(src.at[j], dst.at[j], sem.at[j])

    def compute(j):
        def unit(k):
            cols = rows_at(k, tile)
            u = jnp.dot(c_all[j], up[:, cols], preferred_element_type=F32) + up_bias[0:1, cols]

            @pl.when(j != far)
            def _():
                ahead[0, :, cols] = lax.dot_general(cot_all[j], down[cols, :], NT, preferred_element_type=F32)

            dg = ahead[jnp.where(j == far, 1, 0), :, cols]
            half = 0.5 + 0.5 * lax.erf(u * (0.5 ** 0.5))
            g_all[j, :, cols] = (u * half).astype(BF)
            slope = half + u * (jnp.exp(u * u * -0.5) * 0.3989422804014327)
            du = (slope * dg).astype(BF)
            du_all[j, :, cols] = du
            upb_ref[0:1, cols] += jnp.sum(du.astype(F32), axis=0, keepdims=True)

        loop(units // tile, unit)

        def back(k):
            cols = rows_at(k, tile)
            part[j, :, cols] = lax.dot_general(du_all[j], up[cols, :], NT, preferred_element_type=F32).astype(BF)

        loop(depth // tile, back)
        sums.launch(j)
        out_copy(g_all, g_hbm, g_sem, j).start()
        out_copy(du_all, du_hbm, du_sem, j).start()
        out_copy(c_all, c_hbm, c_sem, j).start()

    rounds(i, n, line, compute)

    def forward(j):
        def columns(k):
            cols = rows_at(k, tile)
            mlp[j, :, cols] = jnp.dot(g_all[j], down[:, cols], preferred_element_type=F32).astype(BF)

        loop(depth // tile, columns)
        out_copy(mlp, mlp_hbm, mlp_sem, j).start()

    def relay(t):
        early = jnp.where(i < n // 2, 1, 0)
        sums.relay(t + 3 - early - i, 2 * n - 4 - i - t - early)

        @pl.when(t < n // 2)
        def _():
            loop(2, lambda k: forward(2 * t + k))

    loop(2 * n - 3, relay)

    def norm(b):
        here = rows_at(b, RB)
        sums.add(here, dh_ref.at[here, :])
        grad = dh_ref[here, :]
        normal, inverse = norm_stats(h_ref[here, :])
        vec_ref[0:1, :] += jnp.sum(grad * normal, axis=0, keepdims=True)
        vec_ref[1:2, :] += jnp.sum(grad, axis=0, keepdims=True)
        cot = cot_all[i, here, :].astype(F32)
        dh = cot + norm_back(grad, normal, inverse, vec[3:4, :])
        dh_ref[here, :] = dh
        db = dh.astype(BF)
        db_ref[here, :] = db
        vec_ref[2:3, :] += jnp.sum(db.astype(F32), axis=0, keepdims=True)
        vec_ref[3:4, :] += jnp.sum(cot, axis=0, keepdims=True)

    sums.own(norm)

    def done(j):
        out_copy(g_all, g_hbm, g_sem, j).wait()
        out_copy(du_all, du_hbm, du_sem, j).wait()
        out_copy(c_all, c_hbm, c_sem, j).wait()
        out_copy(mlp, mlp_hbm, mlp_sem, j).wait()

    loop(n, done)
    line.finish()
    sums.finish()


def attend_back(b, block, column, heads, put, dk, dv):
    factor = HD ** (-0.5)
    here, keys = slice(b * block, (b + 1) * block), slice(0, (b + 1) * block)

    def head(t):
        q, k, v, do = column(0, here, t), column(1, keys, t), column(2, keys, t), column(3, here, t)
        s = lax.dot_general(q, k, NT, preferred_element_type=F32) * factor
        query = lax.broadcasted_iota(jnp.int32, s.shape, 0) + b * block
        s = jnp.where(query >= lax.broadcasted_iota(jnp.int32, s.shape, 1), s, -1e30)
        e = jnp.exp(s - jnp.max(s, axis=-1, keepdims=True))
        prob = e / jnp.sum(e, axis=-1, keepdims=True)
        dv[t, keys, :] += lax.dot_general(prob.astype(BF), do, TN, preferred_element_type=F32)
        dp = lax.dot_general(do, v, NT, preferred_element_type=F32)
        ds = (prob * (dp - jnp.sum(prob * dp, axis=-1, keepdims=True))).astype(BF)
        put(0, here, t, (jnp.dot(ds, k, preferred_element_type=F32) * factor).astype(BF))
        dk[t, keys, :] += lax.dot_general(ds, q, TN, preferred_element_type=F32)

    loop(heads, head)


class PlaneSum:
    def __init__(self, row, m, out, terms, land, halves, send, recv, h_send, h_recv):
        self.row, self.m, self.out, self.terms, self.land, self.halves = row, m, out, terms, land, halves
        self.send, self.recv, self.h_send, self.h_recv = send, recv, h_send, h_recv
        bits = [1 << k for k in range(1, m.bit_length() - 1)]
        self.plan = []
        for order in (bits, bits[::-1]):
            left, at, stages = [e for e in range(m) if e % 2 == 0], 0, []
            for bit in order:
                out = [e for e in left if e & bit]
                stages.append((bit, [(e, e ^ bit, at + k) for k, e in enumerate(out)]))
                left, at = [e for e in left if not e & bit], at + len(out)
            self.plan.append(stages)
        self.stages = len(bits)

    def owner(self, e):
        d = self.row
        for k in range(self.m.bit_length() - 1):
            if e & (1 << k):
                d = d + (partner(self.row, 1 << k) - self.row)
        return d

    def whole(self, e):
        return pltpu.make_async_remote_copy(
            src_ref=self.out.at[e // 2], dst_ref=self.land.at[e // 2], send_sem=self.send.at[e // 2],
            recv_sem=self.recv.at[e // 2], device_id={"dp": partner(self.row, 1)}, device_id_type=MESH)

    def half(self, h, bit, e, at):
        size = self.halves.shape[2]
        return pltpu.make_async_remote_copy(
            src_ref=self.terms.at[e // 2, pl.ds(h * size, size)], dst_ref=self.halves.at[h, at],
            send_sem=self.h_send.at[h, at], recv_sem=self.h_recv.at[h, at],
            device_id={"dp": partner(self.row, bit)}, device_id_type=MESH)

    def merge(self):
        for e in range(0, self.m, 2):
            self.whole(e + 1).wait_recv()

            def add(b):
                here = rows_at(b, RB)
                total = self.terms[e // 2, here, :].astype(F32) + self.land[e // 2, here, :].astype(F32)
                self.terms[e // 2, here, :] = total.astype(BF)

            loop(self.terms.shape[1] // RB, add)

    def push(self, stage):
        for h in range(2):
            bit, moves = self.plan[h][stage]
            for e, _, at in moves:
                self.half(h, bit, e, at).start()

    def take(self, stage, out=None):
        size = self.halves.shape[2]
        for h in range(2):
            bit, moves = self.plan[h][stage]
            for e, into, at in moves:
                self.half(h, bit, e, at).wait_recv()

                def add(b):
                    here, there = rows_at(b, RB), pl.ds(pl.multiple_of(h * size + b * RB, RB), RB)
                    total = self.terms[into // 2, there, :].astype(F32) + self.halves[h, at, here, :].astype(F32)
                    if out is None:
                        self.terms[into // 2, there, :] = total.astype(BF)
                    else:
                        out(there, total)

                loop(size // RB, add)

    def sent(self):
        for e in range(1, self.m, 2):
            self.whole(e).wait_send()

    def finish(self):
        for h in range(2):
            for bit, moves in self.plan[h]:
                for e, _, at in moves:
                    self.half(h, bit, e, at).wait_send()


class VectorSum:
    def __init__(self, me, count, device, vectors, piece, land, acc, send, recv):
        self.me, self.count, self.device, self.vectors, self.piece = me, count, device, vectors, piece
        self.land, self.acc, self.send, self.recv = land, acc, send, recv

    def lanes(self, owner):
        size = self.land.shape[2]
        return pl.ds(pl.multiple_of(owner * self.piece // size * size, size), size)

    def copy(self, src, other):
        return pltpu.make_async_remote_copy(
            src_ref=self.vectors.at[:, self.lanes(other)], dst_ref=self.land.at[src], send_sem=self.send.at[other],
            recv_sem=self.recv.at[src], device_id=self.device(other), device_id_type=MESH)

    def start(self):
        loop(self.count - 1, lambda s: self.copy(self.me, (self.me + s + 1) % self.count).start())

    def finish(self):
        self.acc[...] = self.vectors[:, self.lanes(self.me)]

        def take(s):
            src = (self.me + s + 1) % self.count
            self.copy(src, self.me).wait_recv()
            self.acc[...] += self.land[src]

        loop(self.count - 1, take)
        loop(self.count - 1, lambda s: self.copy(self.me, (self.me + s + 1) % self.count).wait_send())
        places = self.land.shape[2] // self.piece
        own = self.acc[:, 0 : self.piece]
        for k in range(1, places):
            own = jnp.where(self.me % places == k, self.acc[:, k * self.piece : (k + 1) * self.piece], own)
        return own


def greet_cross(i, n, row, m):
    barrier = pltpu.get_barrier_semaphore()

    @pl.when(i > 0)
    def _():
        pl.semaphore_signal(barrier, inc=1, device_id={"tensor": i - 1}, device_id_type=MESH)

    @pl.when(i < n - 1)
    def _():
        pl.semaphore_signal(barrier, inc=1, device_id={"tensor": i + 1}, device_id_type=MESH)

    bits = [1 << k for k in range(m.bit_length() - 1)]
    for bit in bits:
        pl.semaphore_signal(barrier, inc=1, device_id={"dp": partner(row, bit)}, device_id_type=MESH)
    pl.semaphore_wait(barrier, jnp.minimum(i, 1) + jnp.minimum(n - 1 - i, 1) + len(bits))


def relays(sums, i, n, r):
    sums.relay(n - 1 + i - r, r - (n - 1 - i))


def block_terms(plane, e, pairs):
    size = plane.terms.shape[1]
    cols = rows_at(plane.owner(e), size)
    for lhs, rhs, first in pairs:
        width = rhs.shape[1]
        tile = min(512, width)

        def columns(k):
            there = pl.ds(pl.multiple_of(first + k * tile, tile), tile)
            (plane.out if e % 2 else plane.terms)[e // 2, :, there] = lax.dot_general(
                lhs[:, cols], rhs[:, rows_at(k, tile)], TN, preferred_element_type=F32).astype(BF)

        loop(width // tile, columns)


def branch_kernel(n, m, pieces, db_ref, h_ref, vec, mlp_hbm, g_hbm, cot_hbm, c_hbm, du_hbm, qkv_hbm, wo_hbm,
                  db_all, lo_ref, down_out, up_out, dqkv_hbm, down_t, up_ref, down_ref, out_sem, lhs, rhs, wo, dk, dv, part, land, out, terms_a, land_a,
                  half_a, terms_b, land_b, half_b, acc, send, recv, s_send, s_recv, own_sem, part_sem, in_sem, qkv_sem,
                  db_sem, p_send, p_recv, h_send, h_recv):
    i, row = lax.axis_index("tensor"), lax.axis_index("dp")
    size = db_ref.shape[0]
    width = wo.shape[0]
    greet_cross(i, n, row, m)
    line = LineGather(i, n, db_ref, db_all, send, recv)
    line.start()
    part_copy = pltpu.make_async_copy(mlp_hbm, part, part_sem)
    part_copy.start()
    own_copy = pltpu.make_async_copy(db_ref, db_all.at[i], own_sem)
    own_copy.start()

    def load(left, right):
        return [pltpu.make_async_copy(left, lhs, in_sem.at[0]), pltpu.make_async_copy(right, rhs, in_sem.at[1])]

    loads = load(cot_hbm, g_hbm)
    for copy in loads:
        copy.start()
    wo_copy = pltpu.make_async_copy(wo_hbm, wo, in_sem.at[2])
    wo_copy.start()
    sums = LineSum(i, n, part, land, s_send, s_recv, pieces)
    part_copy.wait()
    loop(n, lambda t: sums.launch(jnp.where(i < n // 2, n - 1 - t, t)))
    planes = [PlaneSum(row, m, out, terms_a, land_a, half_a, p_send.at[0], p_recv.at[0], h_send.at[0], h_recv.at[0]),
              PlaneSum(row, m, out, terms_b, land_b, half_b, p_send.at[1], p_recv.at[1], h_send.at[1], h_recv.at[1])]
    first, second = planes
    for copy in loads:
        copy.wait()
    left, right = lhs.at[:, 0 : lhs.shape[1]], rhs.at[:, 0 : down_ref.shape[1]]
    for e in range(1, m, 2):
        block_terms(first, e, [(left, right, 0)])
        first.whole(e).start()
    for e in range(m - 2, -1, -2):
        block_terms(first, e, [(left, right, 0)])
    loads = load(c_hbm, du_hbm)
    for copy in loads:
        copy.start()
    first.merge()
    first.push(0)
    first.sent()
    for copy in loads:
        copy.wait()
    for e in range(1, m, 2):
        block_terms(second, e, [(left, right, 0)])
        second.whole(e).start()

    line.step(1)
    for e in range(m - 2, -1, -2):
        block_terms(second, e, [(left, right, 0)])
    qkv_copies = [pltpu.make_async_copy(qkv_hbm.at[p], rhs.at[:, p * width : (p + 1) * width], qkv_sem.at[p])
                  for p in range(3)]
    for copy in qkv_copies:
        copy.start()
    second.merge()
    second.push(0)
    own_copy.wait()
    wo_copy.wait()

    for copy in qkv_copies:
        copy.wait()
    dk[...] = jnp.zeros_like(dk)
    dv[...] = jnp.zeros_like(dv)

    def column(p, here, t):
        return rhs[here, pl.ds(pl.multiple_of(p * width + t * HD, HD), HD)]

    def put(p, here, t, value):
        rhs[here, pl.ds(pl.multiple_of(p * width + t * HD, HD), HD)] = value

    def mixture_back(j):
        here = rows_at(j, size)
        copy = pltpu.make_async_copy(db_all.at[j], lhs.at[here], db_sem.at[j])
        copy.start()
        copy.wait()
        rhs[here, 3 * width : 4 * width] = lax.dot_general(
            lhs[here, :], wo[...], NT, preferred_element_type=F32).astype(BF)
        for b in range(n):
            @pl.when(j == b)
            def _():
                attend_back(b, size, column, width // HD, put, dk, dv)

    def keep(ref):
        def put(here, total):
            ref[here, :] = total

        return put

    def advance(plane, stage, ref):
        if stage < plane.stages - 1:
            plane.take(stage)
            plane.push(stage + 1)
        else:
            plane.take(stage, keep(ref))

    def round_back(r):
        @pl.when(jnp.logical_and(r >= 1, r <= n - 2))
        def _():
            line.step(r + 1)
            relays(sums, i, n, r)

        def side(s):
            j = jnp.where(s == 0, i - r, i + r)

            @pl.when(jnp.logical_and(jnp.logical_and(j >= 0, j <= n - 1), s * r == s * jnp.maximum(r, 1)))
            def _():
                mixture_back(j)

        loop(2, side)

        @pl.when(r == 1)
        def _():
            advance(first, 0, down_ref)

        @pl.when(r == min(2, n - 1))
        def _():
            advance(second, 0, up_ref)

    loop(n, round_back)
    relays(sums, i, n, n - 1)

    def whole(t):
        put(1, slice(0, LEN), t, (dk[t] * HD ** (-0.5)).astype(BF))
        put(2, slice(0, LEN), t, dv[t].astype(BF))

    loop(width // HD, whole)
    leave = [pltpu.make_async_copy(rhs.at[:, p * width : (p + 1) * width], dqkv_hbm.at[p], out_sem.at[p]) for p in range(3)]
    for copy in leave:
        copy.start()
    for stage in range(1, first.stages):
        advance(first, stage, down_ref)
        advance(second, stage, up_ref)

    def turn(k):
        down_t[rows_at(k, LANES), :] = down_ref[:, rows_at(k, LANES)].T

    loop(down_ref.shape[1] // LANES, turn)
    leave += [pltpu.make_async_copy(down_t, down_out, out_sem.at[3]), pltpu.make_async_copy(up_ref, up_out, out_sem.at[4])]
    for copy in leave[3:]:
        copy.start()

    def output(b):
        here = rows_at(b, RB)
        sums.add(here, acc)
        lo_ref[here, :] = (h_ref[here, :] + (acc[...] + vec[5:6, :])).astype(BF)

    sums.own(output)
    line.finish()
    sums.finish()
    second.sent()
    for plane in planes:
        plane.finish()
    for copy in leave:
        copy.wait()


def input_kernel(n, m, pieces, widths, dqkv_ref, wq_hbm, x_hbm, dh_hbm, vec, early_ref, up_ref, a_hbm, db_hbm, o_hbm,
                 n_hbm, gt_ref, gqkv_out, gout_out, vec_out, up_out, qv_out, gqkv_ref, gout_t, out_sem, gout_ref, early_acc, late_acc, up_acc, qv_acc, vec_ref, qv_ref, wq, a_ref, db_ref,
                 o_ref, n_ref, x_ref, dh_ref, part, land, out_p, terms, land_p, half_p, acc, early_land, late_land, up_land, qv_land, s_send,
                 s_recv, in_sem, p_send, p_recv, h_send, h_recv, e_send, e_recv, l_send, l_recv, u_send, u_recv, q_send,
                 q_recv):
    i, row = lax.axis_index("tensor"), lax.axis_index("dp")
    me, total_devices = row * n + i, m * n
    size = x_hbm.shape[0]
    width = dqkv_ref.shape[2]
    piece, up_piece, qv_piece = widths
    depth = part.shape[2]
    loads = [pltpu.make_async_copy(src, dst, in_sem.at[k]) for k, (src, dst) in enumerate(
        [(wq_hbm, wq), (a_hbm, a_ref), (db_hbm, db_ref), (o_hbm, o_ref), (n_hbm, n_ref), (x_hbm, x_ref), (dh_hbm, dh_ref)])]
    loads[0].start()
    loads[4].start()
    greet_all(me, n, total_devices)
    every = [VectorSum(me, total_devices, lambda g: {"dp": g // n, "tensor": g % n}, early_ref, piece, early_land, early_acc,
                       e_send, e_recv),
             VectorSum(me, total_devices, lambda g: {"dp": g // n, "tensor": g % n}, vec_ref, piece, late_land, late_acc,
                       l_send, l_recv)]
    column = [VectorSum(row, m, lambda g: {"dp": g}, up_ref, up_piece, up_land, up_acc, u_send, u_recv),
              VectorSum(row, m, lambda g: {"dp": g}, qv_ref, qv_piece, qv_land, qv_acc, q_send, q_recv)]
    every[0].start()
    column[0].start()
    sums = LineSum(i, n, part, land, s_send, s_recv, pieces)
    vec_ref[...] = jnp.zeros_like(vec_ref)
    qv_ref[...] = jnp.zeros_like(qv_ref)
    loads[0].wait()
    loads[4].wait()
    for k in (1, 2, 3, 5, 6):
        loads[k].start()
    tile = 512

    def term(t):
        d = jnp.where(i < n // 2, n - 1 - t, t)
        here = rows_at(d, size)

        def columns(k):
            cols = rows_at(k, tile)
            total = lax.dot_general(dqkv_ref[0, here, :], wq[0, cols, :], NT, preferred_element_type=F32)
            for p in range(1, 3):
                total += lax.dot_general(dqkv_ref[p, here, :], wq[p, cols, :], NT, preferred_element_type=F32)
            part[d, :, cols] = total.astype(BF)
            vec_ref[0:1, cols] += jnp.sum(total * n_ref[here, cols].astype(F32), axis=0, keepdims=True)
            vec_ref[1:2, cols] += jnp.sum(total, axis=0, keepdims=True)

        loop(depth // tile, columns)

        @pl.when(t == 0)
        def _():
            sums.launch(d)

        for p in range(2):
            qv_ref[p : p + 1, :] += jnp.sum(dqkv_ref[2 * p, here, :].astype(F32), axis=0, keepdims=True)

    loop(n, term)
    every[1].start()
    column[1].start()
    loop(n - 1, lambda t: sums.launch(jnp.where(i < n // 2, n - 2 - t, t + 1)))
    for k in (1, 2, 3, 5, 6):
        loads[k].wait()
    plane = PlaneSum(row, m, out_p, terms, land_p, half_p, p_send, p_recv, h_send, h_recv)
    pairs = [(a_ref, dqkv_ref.at[p], p * width) for p in range(3)] + [(db_ref, o_ref, 3 * width)]
    for e in range(1, m, 2):
        block_terms(plane, e, pairs)
        plane.whole(e).start()
    for e in range(m - 2, -1, -2):
        block_terms(plane, e, pairs)
    plane.merge()
    plane.push(0)

    def out(here, total):
        for p in range(3):
            gqkv_ref[p, here, :] = total[:, p * width : (p + 1) * width]
        gout_ref[here, :] = total[:, 3 * width :]

    stage = 0
    for r in range(1, n):
        relays(sums, i, n, r)
        if r > 1 and stage < plane.stages:
            if stage < plane.stages - 1:
                plane.take(stage)
                plane.push(stage + 1)
            else:
                plane.take(stage, out)
            stage += 1

    def norm(b):
        here = rows_at(b, RB)
        sums.add(here, acc)
        grad = acc[...]
        normal, inverse = norm_stats(x_ref[here, :].astype(F32))
        gt_ref[here, :] = (dh_ref[here, :] + norm_back(grad, normal, inverse, vec[0:1, :])).astype(BF)

    while stage < plane.stages:
        if stage < plane.stages - 1:
            plane.take(stage)
            plane.push(stage + 1)
        else:
            plane.take(stage, out)
        stage += 1
    gout_t[...] = gout_ref[...].T
    leave = [pltpu.make_async_copy(gqkv_ref, gqkv_out, out_sem.at[0]), pltpu.make_async_copy(gout_t, gout_out, out_sem.at[1])]
    for copy in leave:
        copy.start()
    early, late = every[0].finish(), every[1].finish()
    for k, (rows, at) in enumerate([(late, 0), (late, 1), (early, 2), (early, 0), (early, 1), (early, 3)]):
        vec_out[k : k + 1, :] = rows[at : at + 1, :]
    up_out[...] = column[0].finish()
    qv_out[...] = column[1].finish()
    sums.own(norm)
    for copy in leave:
        copy.wait()
    sums.finish()
    plane.sent()
    plane.finish()


def params(collective=None):
    if collective is None:
        return pltpu.CompilerParams(vmem_limit_bytes=BIG)
    return pltpu.CompilerParams(vmem_limit_bytes=BIG, collective_id=collective, has_side_effects=True)


def shape(dims, dtype):
    return jax.ShapeDtypeStruct(dims, dtype)


def body(tokens, cotangent, ln1_gain, ln1_bias, qkv_weight, qv_bias, out_weight, out_bias, ln2_gain, ln2_bias,
         up_weight, up_bias, down_weight, down_bias):
    n = lax.axis_size("tensor")
    m = lax.axis_size("dp")
    i, row = lax.axis_index("tensor"), lax.axis_index("dp")
    size, depth = tokens.shape
    width = qkv_weight.shape[2]
    units = up_weight.shape[1]
    piece, qv_piece, up_piece = ln1_gain.shape[0], qv_bias.shape[1], up_bias.shape[0]
    total = m * n

    def lane_rows(value, index):
        count = value.shape[-1]
        if count >= LANES:
            return value.reshape(-1, LANES)
        places = LANES // count
        spread = jnp.concatenate([value.reshape(-1, count)] * places, axis=1)
        return jnp.where((jnp.arange(LANES) // count)[None] == index % places, spread, 0)

    me = row * n + i
    whole = jnp.stack([ln1_gain, ln1_bias, out_bias, ln2_gain, ln2_bias, down_bias])
    pack = jnp.concatenate([lane_rows(whole, me), lane_rows(qv_bias, row), lane_rows(up_bias, row)])
    pack = jnp.pad(pack, ((0, -pack.shape[0] % 16), (0, 0)))
    lanes_up = 8 + max(up_piece // LANES, 1)

    dma = pltpu.SemaphoreType.DMA
    weight_sems = [dma((2, 2, m - 1)), dma((2, 2, m)), dma((2, 2))]
    attn_in, normal_one, vectors, bias_qv, bias_up, w_qkv, w_out = pl.pallas_call(
        functools.partial(tokens_kernel, n, m, (piece, qv_piece, up_piece)),
        out_shape=(shape((LEN, depth), BF), shape((LEN, depth), BF), shape((8, depth), F32), shape((8, width), F32),
                   shape((8, units), F32), shape((3, depth, width), BF), shape((width, depth), BF)),
        in_specs=[VM] * 4, out_specs=(ANY, ANY, VM, VM, VM, ANY, ANY),
        scratch_shapes=[pltpu.VMEM((total,) + pack.shape, BF), pltpu.VMEM((n, size, depth), BF), pltpu.VMEM((LEN, depth), BF),
                        pltpu.VMEM((LEN, depth), BF), dma((2, n))] + weight_sems +
                       [dma, dma((2, n, LineGather.PIECES)), dma((n, LineGather.PIECES)), dma((total,)), dma((total,))],
        compiler_params=params(0), name="gather_tokens",
    )(pack, tokens, qkv_weight, out_weight)

    pieces = 2
    sums = [pltpu.VMEM((n, size, depth), BF), pltpu.VMEM((n + 1, size, depth), BF)]
    qkv, mixture, residual, mlp_own, cot_all, w_up, w_down = pl.pallas_call(
        functools.partial(attend_kernel, n, m, pieces),
        out_shape=(shape((3, LEN, width), BF), shape((LEN, width), BF), shape((size, depth), F32),
                   shape((size, depth), BF), shape((n, size, depth), BF), shape((depth, units), BF), shape((units, depth), BF)),
        in_specs=[ANY] * 3 + [VM] * 6, out_specs=(ANY, ANY, VM, VM, ANY, ANY, ANY),
        scratch_shapes=weight_sems + [pltpu.VMEM((3, LEN, width), BF), pltpu.VMEM((LEN, width), BF), dma((2,)),
                        pltpu.VMEM((LEN, depth), BF), pltpu.VMEM((3, depth, width), BF), pltpu.VMEM((width, depth), BF)] +
                       sums + [dma((2, n, LineGather.PIECES)), dma((n, LineGather.PIECES)), dma((n, pieces)), dma((n + 1, pieces)), dma, dma, dma((4,))],
        compiler_params=params(1), name="attend",
    )(attn_in, w_qkv, w_out, up_weight, down_weight, tokens, cotangent, bias_qv, vectors)

    pieces = min(4, size // RB)
    mlp_in, hidden, grad_pre, mlp_part, grad_resid, branch_cot, vec_two, grad_up_b = pl.pallas_call(
        functools.partial(hidden_kernel, n, pieces),
        out_shape=(shape((n, size, depth), BF), shape((n, size, units), BF), shape((n, size, units), BF),
                   shape((n, size, depth), BF), shape((size, depth), F32), shape((size, depth), BF),
                   shape((8, depth), F32), shape((8, units), F32)),
        in_specs=[VM, VM, ANY, ANY, ANY, VM, VM], out_specs=(ANY, ANY, ANY, ANY, VM, VM, VM, VM),
        scratch_shapes=[pltpu.VMEM((n, size, depth), BF), pltpu.VMEM((n, size, units), BF),
                        pltpu.VMEM((n, size, units), BF), pltpu.VMEM((n, size, depth), BF),
                        pltpu.VMEM((depth, units), BF), pltpu.VMEM((units, depth), BF)] + sums +
                       [dma((2, n, LineGather.PIECES)), dma((n, LineGather.PIECES)), dma((n, pieces)), dma((n + 1, pieces)), dma((2,)), dma, dma,
                        dma((n,)), dma((n,)), dma((n,)), pltpu.VMEM((n, size, depth), BF), dma((n,)), pltpu.VMEM((2, size, units), F32)],
        compiler_params=params(2), name="hidden",
    )(mlp_own, residual, cot_all, w_up, w_down, bias_up, vectors)
    mlp_in, hidden, grad_pre, cot_rows = [v.reshape(LEN, -1) for v in (mlp_in, hidden, grad_pre, cot_all)]

    def plane_scratch(columns):
        rows = depth // m
        return [pltpu.VMEM((m // 2, rows, columns), BF), pltpu.VMEM((m // 2, rows, columns), BF),
                pltpu.VMEM((2, m // 2 - 1, rows // 2, columns), BF)]

    pieces = 2
    sum_sems = [dma((n, pieces)), dma((n + 1, pieces))]
    attn_cot, layer_out, grad_down_w, grad_up_w, grad_qkv = pl.pallas_call(
        functools.partial(branch_kernel, n, m, pieces),
        out_shape=(shape((n, size, depth), BF), shape((size, depth), BF), shape((units, depth // m), F32),
                   shape((depth // m, units), F32), shape((3, LEN, width), BF)),
        in_specs=[VM] * 3 + [ANY] * 7, out_specs=(ANY, VM, ANY, ANY, ANY),
        scratch_shapes=[pltpu.VMEM((units, depth // m), F32), pltpu.VMEM((depth // m, units), F32),
                        pltpu.VMEM((depth // m, units), F32), dma((5,)), pltpu.VMEM((LEN, depth), BF), pltpu.VMEM((LEN, units), BF), pltpu.VMEM((width, depth), BF),
                        pltpu.VMEM((width // HD, LEN, HD), F32), pltpu.VMEM((width // HD, LEN, HD), F32)] + sums +
                       [pltpu.VMEM((m // 2, depth // m, units), BF)] + plane_scratch(units) * 2 +
                       [pltpu.VMEM((RB, depth), F32), dma((2, n, LineGather.PIECES)), dma((n, LineGather.PIECES))] + sum_sems +
                       [dma, dma, dma((3,)), dma((3,)), dma((n,)), dma((2, m // 2)), dma((2, m // 2)),
                        dma((2, 2, m // 2 - 1)), dma((2, 2, m // 2 - 1))],
        compiler_params=params(4), name="branch",
    )(branch_cot, residual, vectors, mlp_part, hidden, cot_rows, mlp_in, grad_pre, qkv, w_out)
    attn_cot = attn_cot.reshape(LEN, depth)

    tiles = [max(v, LANES) for v in (piece, up_piece, qv_piece)]
    grad_tokens, grad_qkv_w, grad_out_w, vector_grads, grad_up_b, grad_qv_b = pl.pallas_call(
        functools.partial(input_kernel, n, m, pieces, (piece, up_piece, qv_piece)),
        out_shape=(shape((size, depth), BF), shape((3, depth // m, width), F32), shape((width, depth // m), F32),
                   shape((8, piece), F32), shape((8, up_piece), F32), shape((8, qv_piece), F32)),
        in_specs=[VM, ANY, ANY, ANY, VM, VM, VM, ANY, ANY, ANY, ANY], out_specs=(VM, ANY, ANY, VM, VM, VM),
        scratch_shapes=[pltpu.VMEM((3, depth // m, width), F32), pltpu.VMEM((width, depth // m), F32), dma((2,)),
                        pltpu.VMEM((depth // m, width), F32)] + [pltpu.VMEM((8, tiles[k]), F32) for k in (0, 0, 1, 2)] + [
                        pltpu.VMEM((8, depth), F32), pltpu.VMEM((8, width), F32),
                        pltpu.VMEM((3, depth, width), BF), pltpu.VMEM((LEN, depth), BF), pltpu.VMEM((LEN, depth), BF),
                        pltpu.VMEM((LEN, width), BF), pltpu.VMEM((LEN, depth), BF), pltpu.VMEM((size, depth), BF),
                        pltpu.VMEM((size, depth), F32)] + sums +
                       [pltpu.VMEM((m // 2, depth // m, 4 * width), BF)] +
                       plane_scratch(4 * width) +
                       [pltpu.VMEM((RB, depth), F32), pltpu.VMEM((total, 8, tiles[0]), F32),
                        pltpu.VMEM((total, 8, tiles[0]), F32), pltpu.VMEM((m, 8, tiles[1]), F32),
                        pltpu.VMEM((m, 8, tiles[2]), F32)] + sum_sems +
                       [dma((7,)), dma((m // 2,)), dma((m // 2,)), dma((2, m // 2 - 1)), dma((2, m // 2 - 1))] +
                       [dma((total,))] * 4 + [dma((m,))] * 4,
        compiler_params=params(5), name="input",
    )(grad_qkv, w_qkv, tokens, grad_resid, vectors, vec_two, grad_up_b, attn_in, attn_cot, mixture, normal_one)

    vectors = [vector_grads[k] for k in range(6)]
    grad_up_b, grad_qv_b = grad_up_b[0], grad_qv_b[:2]
    return (layer_out, grad_tokens, vectors[0], vectors[1], grad_qkv_w, grad_qv_b, grad_out_w, vectors[2],
            vectors[3], vectors[4], grad_up_w, grad_up_b, grad_down_w, vectors[5])


def solution(mesh):
    vector, matrix = P(("dp", "tensor")), P(("dp", "tensor"), None)
    in_specs = (matrix, matrix, vector, vector, P(None, "dp", "tensor"), P(None, ("tensor", "dp")), P("tensor", "dp"),
                vector, vector, vector, P("dp", "tensor"), P(("tensor", "dp")), P("tensor", "dp"), vector)
    out_specs = (matrix, matrix, vector, vector, P(None, "dp", "tensor"), P(None, ("tensor", "dp")),
                 P("tensor", "dp"), vector, vector, vector, P("dp", "tensor"), P(("tensor", "dp")), P("tensor", "dp"),
                 vector)
    return jax.shard_map(body, mesh=mesh, in_specs=in_specs, out_specs=out_specs, check_vma=False)
```

```python
import functools

import jax
import jax.numpy as jnp
from jax import lax
from jax.experimental import pallas as pl
from jax.experimental.pallas import tpu as pltpu
from jax.sharding import PartitionSpec as P

HD = 128
LEN = 1024
LANES = 128
EPS = 1e-05
BF = jnp.bfloat16
F32 = jnp.float32
MESH = pl.DeviceIdType.MESH
ANY = pl.BlockSpec(memory_space=pl.ANY)
VM = pl.BlockSpec(memory_space=pltpu.VMEM)
NT = (((1,), (1,)), ((), ()))
TN = (((0,), (0,)), ((), ()))
BIG = 64 * 1024 * 1024 - 65536
RB = 32


def norm_stats(rows):
    mean = jnp.mean(rows, axis=-1, keepdims=True)
    centred = rows - mean
    variance = jnp.mean(centred * centred, axis=-1, keepdims=True)
    inverse = lax.rsqrt(variance + EPS)
    return centred * inverse, inverse


def norm_back(grad_rows, normal_rows, inverse, gain):
    scaled = grad_rows * gain
    first = jnp.mean(scaled, axis=-1, keepdims=True)
    second = jnp.mean(scaled * normal_rows, axis=-1, keepdims=True)
    return inverse * (scaled - first - normal_rows * second)


def loop(count, step):
    def run(i, carry):
        step(i)
        return carry

    lax.fori_loop(0, count, run, 0)


def rows_at(j, size):
    return pl.ds(pl.multiple_of(j * size, size), size)


def remote(src, dst, send, recv, target):
    return pltpu.make_async_remote_copy(src_ref=src, dst_ref=dst, send_sem=send, recv_sem=recv,
                                        device_id={"tensor": target}, device_id_type=MESH)


def greet_neighbours(i, n):
    barrier = pltpu.get_barrier_semaphore()

    @pl.when(i > 0)
    def _():
        pl.semaphore_signal(barrier, inc=1, device_id={"tensor": i - 1}, device_id_type=MESH)

    @pl.when(i < n - 1)
    def _():
        pl.semaphore_signal(barrier, inc=1, device_id={"tensor": i + 1}, device_id_type=MESH)

    pl.semaphore_wait(barrier, jnp.minimum(i, 1) + jnp.minimum(n - 1 - i, 1))


def greet_all(me, n, total):
    barrier = pltpu.get_barrier_semaphore()

    def greet(s):
        other = (me + s + 1) % total
        pl.semaphore_signal(barrier, inc=1, device_id={"dp": other // n, "tensor": other % n}, device_id_type=MESH)

    loop(total - 1, greet)
    pl.semaphore_wait(barrier, total - 1)


def rounds(i, n, line, compute, between=None):
    def round_of(r):
        @pl.when(r > 0)
        def _():
            line.step(r)

        if between is not None:
            between(r)

        def side(s):
            j = jnp.where(s == 0, i - r, i + r)

            @pl.when(jnp.logical_and(jnp.logical_and(j >= 0, j <= n - 1), s * r == s * jnp.maximum(r, 1)))
            def _():
                compute(j)

        loop(2, side)

    loop(n, round_of)


class LineGather:
    PIECES = 2

    def __init__(self, i, n, own, buf, send, recv):
        self.i, self.n, self.own, self.buf, self.send, self.recv = i, n, own, buf, send, recv
        self.size = own.shape[0] // self.PIECES

    def copy(self, src, j, side, s, target):
        here = pl.ds(s * self.size, self.size)
        return remote(src.at[here], self.buf.at[j, here], self.send.at[side, j, s], self.recv.at[j, s], target)

    def start(self):
        i, n = self.i, self.n
        for s in range(self.PIECES):
            @pl.when(i < n - 1)
            def _():
                self.copy(self.own, i, 0, s, i + 1).start()

            @pl.when(i > 0)
            def _():
                self.copy(self.own, i, 1, s, i - 1).start()

    def step(self, r):
        i, n = self.i, self.n
        for s in range(self.PIECES):
            @pl.when(i - r >= 0)
            def _():
                self.copy(self.own, i - r, 0, s, i).wait_recv()

                @pl.when(i < n - 1)
                def _():
                    self.copy(self.buf.at[i - r], i - r, 0, s, i + 1).start()

            @pl.when(i + r <= n - 1)
            def _():
                self.copy(self.own, i + r, 1, s, i).wait_recv()

                @pl.when(i > 0)
                def _():
                    self.copy(self.buf.at[i + r], i + r, 1, s, i - 1).start()

    def finish(self):
        i, n = self.i, self.n

        def one(j):
            for s in range(self.PIECES):
                @pl.when(jnp.logical_and(i < n - 1, j <= i))
                def _():
                    self.copy(self.own, j, 0, s, i + 1).wait_send()

                @pl.when(jnp.logical_and(i > 0, j >= i))
                def _():
                    self.copy(self.own, j, 1, s, i - 1).wait_send()

        loop(n, one)


class LineSum:
    def __init__(self, i, n, part, land, send, recv, pieces):
        self.i, self.n, self.part, self.land, self.send, self.recv = i, n, part, land, send, recv
        self.pieces = pieces
        self.size = part.shape[1] // pieces

    def copy(self, src, d, right, s):
        i, n = self.i, self.n
        target = i + 1 if right else i - 1
        slot = d if right else jnp.where(d == target, n, d)
        here = rows_at(s, self.size)
        return remote(src.at[d, here], self.land.at[slot, here], self.send.at[d, s], self.recv.at[slot, s], target)

    def arrived(self, slot, s):
        here = rows_at(s, self.size)
        remote(self.part.at[0, here], self.land.at[slot, here], self.send.at[0, s], self.recv.at[slot, s],
               self.i).wait_recv()

    def launch(self, d):
        i, n = self.i, self.n

        @pl.when(jnp.logical_and(i == 0, d > 0))
        def _():
            loop(self.pieces, lambda s: self.copy(self.part, d, True, s).start())

        @pl.when(jnp.logical_and(i == n - 1, d < n - 1))
        def _():
            loop(self.pieces, lambda s: self.copy(self.part, d, False, s).start())

    def relay(self, right, left):
        i, n = self.i, self.n

        def move(d, to_right, s):
            self.arrived(d, s)
            here = rows_at(s, self.size)
            total = self.land[d, here, :].astype(F32) + self.part[d, here, :].astype(F32)
            self.land[d, here, :] = total.astype(BF)
            self.copy(self.land, d, to_right, s).start()

        first = jnp.where(i < n // 2, 0, 1)

        def one(s):
            turn, s = (s + first) % 2, s // 2

            @pl.when(jnp.logical_and(turn == 0, jnp.logical_and(i > 0, jnp.logical_and(right > i, right <= n - 1))))
            def _():
                move(right, True, s)

            @pl.when(jnp.logical_and(turn == 1, jnp.logical_and(i < n - 1, jnp.logical_and(left >= 0, left < i))))
            def _():
                move(left, False, s)

        loop(2 * self.pieces, one)

    def own(self, step):
        i, n = self.i, self.n

        def one(s):
            @pl.when(i > 0)
            def _():
                self.arrived(i, s)

            @pl.when(i < n - 1)
            def _():
                self.arrived(n, s)

            loop(self.size // RB, lambda b: step(s * (self.size // RB) + b))

        loop(self.pieces, one)

    def add(self, here, out):
        i, n = self.i, self.n
        out[...] = self.part[i, here, :].astype(F32)

        @pl.when(i > 0)
        def _():
            out[...] += self.land[i, here, :].astype(F32)

        @pl.when(i < n - 1)
        def _():
            out[...] += self.land[n, here, :].astype(F32)

    def finish(self):
        i, n = self.i, self.n

        def one(d):
            @pl.when(jnp.logical_and(i < n - 1, d > i))
            def _():
                loop(self.pieces, lambda s: self.copy(self.part, d, True, s).wait_send())

            @pl.when(jnp.logical_and(i > 0, d < i))
            def _():
                loop(self.pieces, lambda s: self.copy(self.part, d, False, s).wait_send())

        loop(n, one)


def partner(row, bit):
    return row + bit * (1 - 2 * ((row // bit) % 2))


class PlaneGather:
    def __init__(self, row, m, items, send, recv, local):
        self.row, self.m, self.items, self.send, self.recv, self.local = row, m, items, send, recv, local
        bits = [1 << k for k in range(1, m.bit_length() - 1)]
        self.plan = []
        for order in (bits + [1], bits[::-1] + [1]):
            have, at, stages = [0], 0, []
            for bit in order:
                stages.append((bit, [(e, at + k) for k, e in enumerate(have)]))
                at, have = at + len(have), have + [e ^ bit for e in have]
            self.plan.append(stages)
        self.stages = len(bits) + 1

    def owner(self, e):
        d = self.row
        for k in range(self.m.bit_length() - 1):
            if e & (1 << k):
                d = d + (partner(self.row, 1 << k) - self.row)
        return d

    def copies(self, stage):
        for k, (own, whole, own_half, half) in enumerate(self.items):
            for h in range(2):
                bit, moves = self.plan[h][stage]
                for e, at in moves:
                    there = half(whole, self.owner(e), h)
                    src = own_half(own, h) if e == 0 else there
                    yield pltpu.make_async_remote_copy(
                        src_ref=src, dst_ref=there, send_sem=self.send.at[k, h, at], recv_sem=self.recv.at[k, h, e ^ bit],
                        device_id={"dp": partner(self.row, bit)}, device_id_type=MESH)

    def landed(self, stage):
        for k, (own, whole, own_half, half) in enumerate(self.items):
            for h in range(2):
                bit, moves = self.plan[h][stage]
                for e, at in moves:
                    there = half(whole, self.owner(e ^ bit), h)
                    pltpu.make_async_remote_copy(
                        src_ref=there, dst_ref=there, send_sem=self.send.at[k, h, at], recv_sem=self.recv.at[k, h, e ^ bit],
                        device_id={"dp": partner(self.row, bit)}, device_id_type=MESH).wait_recv()

    def locals(self):
        return [pltpu.make_async_copy(own_half(own, h), half(whole, self.row, h), self.local.at[k, h])
                for k, (own, whole, own_half, half) in enumerate(self.items) for h in range(2)]

    def start(self):
        for copy in self.copies(0):
            copy.start()
        for copy in self.locals():
            copy.start()

    def advance(self, stage):
        self.landed(stage - 1)
        for copy in self.copies(stage):
            copy.start()

    def finish(self):
        self.landed(self.stages - 1)
        for stage in range(self.stages):
            for copy in self.copies(stage):
                copy.wait_send()
        for copy in self.locals():
            copy.wait()


def half_rows(own, h):
    size = own.shape[-2] // 2
    return own.at[..., pl.ds(h * size, size), :]


def row_blocks(m):
    def half(whole, d, h):
        size = whole.shape[-2] // m // 2
        return whole.at[..., pl.ds(pl.multiple_of((2 * d + h) * size, size), size), :]

    return half


def column_blocks(m):
    def half(whole, d, h):
        size, width = whole.shape[-2] // 2, whole.shape[-1] // m
        return whole.at[pl.ds(h * size, size), pl.ds(pl.multiple_of(d * width, width), width)]

    return half


def tokens_kernel(n, m, widths, pack_ref, x_ref, wq_ref, wo_ref, a_hbm, n_hbm, affine, qv_bias, up_bias, wq_all, wo_all,
                  vec_ref, buf, a_ref, n_ref, out_sem, w_send, w_recv, w_local, own_sem, send, recv, v_send, v_recv):
    i, row = lax.axis_index("tensor"), lax.axis_index("dp")
    me, total = row * n + i, m * n
    size = x_ref.shape[0]
    greet_all(me, n, total)
    line = LineGather(i, n, x_ref, buf, send, recv)

    def vector(src, other):
        return pltpu.make_async_remote_copy(
            src_ref=pack_ref, dst_ref=vec_ref.at[src], send_sem=v_send.at[other], recv_sem=v_recv.at[src],
            device_id={"dp": other // n, "tensor": other % n}, device_id_type=MESH)

    loop(total - 1, lambda s: vector(me, (me + s + 1) % total).start())
    line.start()
    weights = PlaneGather(row, m, [(wq_ref, wq_all, half_rows, row_blocks(m)), (wo_ref, wo_all, half_rows, column_blocks(m))],
                          w_send, w_recv, w_local)
    weights.start()
    own_copy = pltpu.make_async_copy(x_ref, buf.at[i], own_sem)
    own_copy.start()
    vec_ref[me] = pack_ref[...]
    loop(total - 1, lambda s: vector((me + s + 1) % total, me).wait_recv())
    piece, qv_piece, up_piece = widths

    def assemble(out, piece, first, rows, device):
        group = max(LANES // piece, 1)
        split = max(piece // LANES, 1)
        for tile in range(out.shape[1] // LANES):
            if split > 1:
                at = first + tile % split
                value = vec_ref[device(tile // split), at : at + 1, :].astype(F32)
            else:
                value = vec_ref[device(tile * group), first : first + rows, :].astype(F32)
                for g in range(1, group):
                    value = value + vec_ref[device(tile * group + g), first : first + rows, :].astype(F32)
            out[0:rows, tile * LANES : (tile + 1) * LANES] = value

    assemble(affine, piece, 0, 6, lambda g: g)
    assemble(qv_bias, qv_piece, 6, 2, lambda d: d * n + i)
    assemble(up_bias, up_piece, 8, 1, lambda d: d * n + i)
    own_copy.wait()

    def compute(j):
        def norm(b):
            normal, _ = norm_stats(buf[j, rows_at(b, RB), :].astype(F32))
            here = pl.ds(pl.multiple_of(j * size + b * RB, RB), RB)
            n_ref[here, :] = normal.astype(BF)
            a_ref[here, :] = (normal * affine[0:1, :] + affine[1:2, :]).astype(BF)

        loop(size // RB, norm)
        for copy in leave(j):
            copy.start()

    def leave(j):
        here = rows_at(j, size)
        return [pltpu.make_async_copy(a_ref.at[here], a_hbm.at[here], out_sem.at[0, j]),
                pltpu.make_async_copy(n_ref.at[here], n_hbm.at[here], out_sem.at[1, j])]

    def left(j):
        for copy in leave(j):
            copy.wait()

    def between(r):
        for stage in range(1, weights.stages):
            @pl.when(r == stage)
            def _():
                weights.advance(stage)

    rounds(i, n, line, compute, between)
    line.finish()
    weights.finish()
    loop(n, left)
    loop(total - 1, lambda s: vector(me, (me + s + 1) % total).wait_send())


def attend_kernel(n, m, pieces, a_hbm, wq_hbm, wo_hbm, up_ref, down_ref, x_ref, cot_ref, bias, vec,
                  qkv_hbm, o_hbm, h_ref, c_ref, cot_all, up_all, down_all, w_send, w_recv, w_local, qkv_ref, o_ref, out_sem, a_ref, wq_ref, w_ref, part, land, send, recv, s_send, s_recv, own_sem, a_sem, w_sem):
    i, row = lax.axis_index("tensor"), lax.axis_index("dp")
    size = x_ref.shape[0]
    loads = [pltpu.make_async_copy(a_hbm, a_ref, a_sem)]
    loads += [pltpu.make_async_copy(wq_hbm.at[t], wq_ref.at[t], w_sem.at[t]) for t in range(3)]
    loads += [pltpu.make_async_copy(wo_hbm, w_ref, w_sem.at[3])]
    for load in loads:
        load.start()
    heads = qkv_ref.shape[2] // HD
    depth = w_ref.shape[1]
    greet_cross(i, n, row, m)
    line = LineGather(i, n, cot_ref, cot_all, send, recv)
    line.start()
    weights = PlaneGather(row, m, [(up_ref, up_all, half_rows, row_blocks(m)), (down_ref, down_all, half_rows, column_blocks(m))],
                          w_send, w_recv, w_local)
    weights.start()
    own_copy = pltpu.make_async_copy(cot_ref, cot_all.at[i], own_sem)
    own_copy.start()

    loads[0].wait()
    block = 256
    for t in range(3):
        loads[1 + t].wait()

        def project(b):
            here = rows_at(b, block)
            value = jnp.dot(a_ref[here, :], wq_ref[t], preferred_element_type=F32)
            if t != 1:
                value = value + bias[t // 2 : t // 2 + 1, :]
            qkv_ref[t, here, :] = value.astype(BF)

        loop(LEN // block, project)

    def head(t):
        cols = pl.ds(pl.multiple_of(t * HD, HD), HD)
        for b in range(LEN // block):
            here, keys = slice(b * block, (b + 1) * block), (b + 1) * block
            s = lax.dot_general(qkv_ref[0, here, cols], qkv_ref[1, 0:keys, cols], NT,
                                preferred_element_type=F32) * HD ** (-0.5)
            query = lax.broadcasted_iota(jnp.int32, s.shape, 0) + b * block
            s = jnp.where(query >= lax.broadcasted_iota(jnp.int32, s.shape, 1), s, -1e30)
            e = jnp.exp(s - jnp.max(s, axis=-1, keepdims=True))
            prob = (e / jnp.sum(e, axis=-1, keepdims=True)).astype(BF)
            o_ref[here, cols] = jnp.dot(prob, qkv_ref[2, 0:keys, cols], preferred_element_type=F32).astype(BF)

    loop(heads, head)
    leave = [pltpu.make_async_copy(qkv_ref, qkv_hbm, out_sem.at[0]), pltpu.make_async_copy(o_ref, o_hbm, out_sem.at[1])]
    for copy in leave:
        copy.start()
    loads[4].wait()
    sums = LineSum(i, n, part, land, s_send, s_recv, pieces)
    tile = 512

    def project(t):
        d = jnp.where(i < n // 2, n - 1 - t, t)

        def columns(k):
            cols = rows_at(k, tile)
            part[d, :, cols] = jnp.dot(o_ref[rows_at(d, size), :], w_ref[:, cols], preferred_element_type=F32).astype(BF)

        loop(depth // tile, columns)
        sums.launch(d)

    loop(n, project)
    weights.advance(1)
    for r in range(1, n):
        line.step(r)
        for stage in range(2, weights.stages):
            if r == min(2 * stage - 1, n - 1):
                weights.advance(stage)
        relays(sums, i, n, r)

    def norm(b):
        here = rows_at(b, RB)
        sums.add(here, h_ref.at[here, :])
        rows = h_ref[here, :] + (x_ref[here, :].astype(F32) + vec[2:3, :])
        h_ref[here, :] = rows
        normal, _ = norm_stats(rows)
        c_ref[here, :] = (normal * vec[3:4, :] + vec[4:5, :]).astype(BF)

    sums.own(norm)
    own_copy.wait()
    for copy in leave:
        copy.wait()
    weights.finish()
    line.finish()
    sums.finish()


def hidden_kernel(n, pieces, c_ref, h_ref, cot_hbm, up_hbm, down_hbm, up_bias, vec, c_hbm, g_hbm, du_hbm, mlp_hbm, dh_ref,
                  db_ref, vec_ref, upb_ref, c_all, g_all, du_all, cot_all, up, down, part, land, send, recv, s_send,
                  s_recv, w_sem, cot_sem, own_sem, c_sem, g_sem, du_sem, mlp, mlp_sem):
    i = lax.axis_index("tensor")
    size, depth = c_ref.shape
    units = up.shape[1]
    greet_neighbours(i, n)
    line = LineGather(i, n, c_ref, c_all, send, recv)
    line.start()
    own_copy = pltpu.make_async_copy(c_ref, c_all.at[i], own_sem)
    own_copy.start()
    up_copy = pltpu.make_async_copy(up_hbm, up, w_sem.at[0])
    up_copy.start()
    down_copy = pltpu.make_async_copy(down_hbm, down, w_sem.at[1])
    down_copy.start()
    cot_copy = pltpu.make_async_copy(cot_hbm, cot_all, cot_sem)
    cot_copy.start()
    upb_ref[...] = jnp.zeros_like(upb_ref)
    vec_ref[...] = jnp.zeros_like(vec_ref)
    own_copy.wait()
    up_copy.wait()
    down_copy.wait()
    cot_copy.wait()
    sums = LineSum(i, n, part, land, s_send, s_recv, pieces)
    tile = 256

    def out_copy(src, dst, sem, j):
        return pltpu.make_async_copy(src.at[j], dst.at[j], sem.at[j])

    def compute(j):
        def unit(k):
            cols = rows_at(k, tile)
            u = jnp.dot(c_all[j], up[:, cols], preferred_element_type=F32) + up_bias[0:1, cols]
            dg = lax.dot_general(cot_all[j], down[cols, :], NT, preferred_element_type=F32)
            half = 0.5 + 0.5 * lax.erf(u * (0.5 ** 0.5))
            g_all[j, :, cols] = (u * half).astype(BF)
            slope = half + u * (jnp.exp(u * u * -0.5) * 0.3989422804014327)
            du = (slope * dg).astype(BF)
            du_all[j, :, cols] = du
            upb_ref[0:1, cols] += jnp.sum(du.astype(F32), axis=0, keepdims=True)

        loop(units // tile, unit)

        def back(k):
            cols = rows_at(k, tile)
            part[j, :, cols] = lax.dot_general(du_all[j], up[cols, :], NT, preferred_element_type=F32).astype(BF)

        loop(depth // tile, back)
        sums.launch(j)
        out_copy(g_all, g_hbm, g_sem, j).start()
        out_copy(du_all, du_hbm, du_sem, j).start()
        out_copy(c_all, c_hbm, c_sem, j).start()

    rounds(i, n, line, compute)

    def forward(j):
        def columns(k):
            cols = rows_at(k, tile)
            mlp[j, :, cols] = jnp.dot(g_all[j], down[:, cols], preferred_element_type=F32).astype(BF)

        loop(depth // tile, columns)
        out_copy(mlp, mlp_hbm, mlp_sem, j).start()

    def relay(t):
        early = jnp.where(i < n // 2, 1, 0)
        sums.relay(t + 3 - early - i, 2 * n - 4 - i - t - early)

        @pl.when(t < n // 2)
        def _():
            loop(2, lambda k: forward(2 * t + k))

    loop(2 * n - 3, relay)

    def norm(b):
        here = rows_at(b, RB)
        sums.add(here, dh_ref.at[here, :])
        grad = dh_ref[here, :]
        normal, inverse = norm_stats(h_ref[here, :])
        vec_ref[0:1, :] += jnp.sum(grad * normal, axis=0, keepdims=True)
        vec_ref[1:2, :] += jnp.sum(grad, axis=0, keepdims=True)
        cot = cot_all[i, here, :].astype(F32)
        dh = cot + norm_back(grad, normal, inverse, vec[3:4, :])
        dh_ref[here, :] = dh
        db = dh.astype(BF)
        db_ref[here, :] = db
        vec_ref[2:3, :] += jnp.sum(db.astype(F32), axis=0, keepdims=True)
        vec_ref[3:4, :] += jnp.sum(cot, axis=0, keepdims=True)

    sums.own(norm)

    def done(j):
        out_copy(g_all, g_hbm, g_sem, j).wait()
        out_copy(du_all, du_hbm, du_sem, j).wait()
        out_copy(c_all, c_hbm, c_sem, j).wait()
        out_copy(mlp, mlp_hbm, mlp_sem, j).wait()

    loop(n, done)
    line.finish()
    sums.finish()


def attend_back(b, block, column, heads, put, dk, dv):
    factor = HD ** (-0.5)
    here, keys = slice(b * block, (b + 1) * block), slice(0, (b + 1) * block)

    def head(t):
        q, k, v, do = column(0, here, t), column(1, keys, t), column(2, keys, t), column(3, here, t)
        s = lax.dot_general(q, k, NT, preferred_element_type=F32) * factor
        query = lax.broadcasted_iota(jnp.int32, s.shape, 0) + b * block
        s = jnp.where(query >= lax.broadcasted_iota(jnp.int32, s.shape, 1), s, -1e30)
        e = jnp.exp(s - jnp.max(s, axis=-1, keepdims=True))
        prob = e / jnp.sum(e, axis=-1, keepdims=True)
        dv[t, keys, :] += lax.dot_general(prob.astype(BF), do, TN, preferred_element_type=F32)
        dp = lax.dot_general(do, v, NT, preferred_element_type=F32)
        ds = (prob * (dp - jnp.sum(prob * dp, axis=-1, keepdims=True))).astype(BF)
        put(0, here, t, (jnp.dot(ds, k, preferred_element_type=F32) * factor).astype(BF))
        dk[t, keys, :] += lax.dot_general(ds, q, TN, preferred_element_type=F32)

    loop(heads, head)


class PlaneSum:
    def __init__(self, row, m, out, terms, land, halves, send, recv, h_send, h_recv):
        self.row, self.m, self.out, self.terms, self.land, self.halves = row, m, out, terms, land, halves
        self.send, self.recv, self.h_send, self.h_recv = send, recv, h_send, h_recv
        bits = [1 << k for k in range(1, m.bit_length() - 1)]
        self.plan = []
        for order in (bits, bits[::-1]):
            left, at, stages = [e for e in range(m) if e % 2 == 0], 0, []
            for bit in order:
                out = [e for e in left if e & bit]
                stages.append((bit, [(e, e ^ bit, at + k) for k, e in enumerate(out)]))
                left, at = [e for e in left if not e & bit], at + len(out)
            self.plan.append(stages)
        self.stages = len(bits)

    def owner(self, e):
        d = self.row
        for k in range(self.m.bit_length() - 1):
            if e & (1 << k):
                d = d + (partner(self.row, 1 << k) - self.row)
        return d

    def whole(self, e):
        return pltpu.make_async_remote_copy(
            src_ref=self.out.at[e // 2], dst_ref=self.land.at[e // 2], send_sem=self.send.at[e // 2],
            recv_sem=self.recv.at[e // 2], device_id={"dp": partner(self.row, 1)}, device_id_type=MESH)

    def half(self, h, bit, e, at):
        size = self.halves.shape[2]
        return pltpu.make_async_remote_copy(
            src_ref=self.terms.at[e // 2, pl.ds(h * size, size)], dst_ref=self.halves.at[h, at],
            send_sem=self.h_send.at[h, at], recv_sem=self.h_recv.at[h, at],
            device_id={"dp": partner(self.row, bit)}, device_id_type=MESH)

    def merge(self):
        for e in range(0, self.m, 2):
            self.whole(e + 1).wait_recv()

            def add(b):
                here = rows_at(b, RB)
                total = self.terms[e // 2, here, :].astype(F32) + self.land[e // 2, here, :].astype(F32)
                self.terms[e // 2, here, :] = total.astype(BF)

            loop(self.terms.shape[1] // RB, add)

    def push(self, stage):
        for h in range(2):
            bit, moves = self.plan[h][stage]
            for e, _, at in moves:
                self.half(h, bit, e, at).start()

    def take(self, stage, out=None):
        size = self.halves.shape[2]
        for h in range(2):
            bit, moves = self.plan[h][stage]
            for e, into, at in moves:
                self.half(h, bit, e, at).wait_recv()

                def add(b):
                    here, there = rows_at(b, RB), pl.ds(pl.multiple_of(h * size + b * RB, RB), RB)
                    total = self.terms[into // 2, there, :].astype(F32) + self.halves[h, at, here, :].astype(F32)
                    if out is None:
                        self.terms[into // 2, there, :] = total.astype(BF)
                    else:
                        out(there, total)

                loop(size // RB, add)

    def sent(self):
        for e in range(1, self.m, 2):
            self.whole(e).wait_send()

    def finish(self):
        for h in range(2):
            for bit, moves in self.plan[h]:
                for e, _, at in moves:
                    self.half(h, bit, e, at).wait_send()


class VectorSum:
    def __init__(self, me, count, device, vectors, piece, land, acc, send, recv):
        self.me, self.count, self.device, self.vectors, self.piece = me, count, device, vectors, piece
        self.land, self.acc, self.send, self.recv = land, acc, send, recv

    def lanes(self, owner):
        size = self.land.shape[2]
        return pl.ds(pl.multiple_of(owner * self.piece // size * size, size), size)

    def copy(self, src, other):
        return pltpu.make_async_remote_copy(
            src_ref=self.vectors.at[:, self.lanes(other)], dst_ref=self.land.at[src], send_sem=self.send.at[other],
            recv_sem=self.recv.at[src], device_id=self.device(other), device_id_type=MESH)

    def start(self):
        loop(self.count - 1, lambda s: self.copy(self.me, (self.me + s + 1) % self.count).start())

    def finish(self):
        self.acc[...] = self.vectors[:, self.lanes(self.me)]

        def take(s):
            src = (self.me + s + 1) % self.count
            self.copy(src, self.me).wait_recv()
            self.acc[...] += self.land[src]

        loop(self.count - 1, take)
        loop(self.count - 1, lambda s: self.copy(self.me, (self.me + s + 1) % self.count).wait_send())
        places = self.land.shape[2] // self.piece
        own = self.acc[:, 0 : self.piece]
        for k in range(1, places):
            own = jnp.where(self.me % places == k, self.acc[:, k * self.piece : (k + 1) * self.piece], own)
        return own


def greet_cross(i, n, row, m):
    barrier = pltpu.get_barrier_semaphore()

    @pl.when(i > 0)
    def _():
        pl.semaphore_signal(barrier, inc=1, device_id={"tensor": i - 1}, device_id_type=MESH)

    @pl.when(i < n - 1)
    def _():
        pl.semaphore_signal(barrier, inc=1, device_id={"tensor": i + 1}, device_id_type=MESH)

    bits = [1 << k for k in range(m.bit_length() - 1)]
    for bit in bits:
        pl.semaphore_signal(barrier, inc=1, device_id={"dp": partner(row, bit)}, device_id_type=MESH)
    pl.semaphore_wait(barrier, jnp.minimum(i, 1) + jnp.minimum(n - 1 - i, 1) + len(bits))


def relays(sums, i, n, r):
    sums.relay(n - 1 + i - r, r - (n - 1 - i))


def block_terms(plane, e, pairs):
    size = plane.terms.shape[1]
    cols = rows_at(plane.owner(e), size)
    for lhs, rhs, first in pairs:
        width = rhs.shape[1]
        tile = min(512, width)

        def columns(k):
            there = pl.ds(pl.multiple_of(first + k * tile, tile), tile)
            (plane.out if e % 2 else plane.terms)[e // 2, :, there] = lax.dot_general(
                lhs[:, cols], rhs[:, rows_at(k, tile)], TN, preferred_element_type=F32).astype(BF)

        loop(width // tile, columns)


def branch_kernel(n, m, pieces, db_ref, h_ref, vec, mlp_hbm, g_hbm, cot_hbm, c_hbm, du_hbm, qkv_hbm, wo_hbm,
                  db_all, lo_ref, down_t, up_ref, dqkv_hbm, down_ref, out_sem, lhs, rhs, wo, dk, dv, part, land, out, terms_a, land_a,
                  half_a, terms_b, land_b, half_b, acc, send, recv, s_send, s_recv, own_sem, part_sem, in_sem, qkv_sem,
                  db_sem, p_send, p_recv, h_send, h_recv):
    i, row = lax.axis_index("tensor"), lax.axis_index("dp")
    size = db_ref.shape[0]
    width = wo.shape[0]
    greet_cross(i, n, row, m)
    line = LineGather(i, n, db_ref, db_all, send, recv)
    line.start()
    part_copy = pltpu.make_async_copy(mlp_hbm, part, part_sem)
    part_copy.start()
    own_copy = pltpu.make_async_copy(db_ref, db_all.at[i], own_sem)
    own_copy.start()

    def load(left, right):
        return [pltpu.make_async_copy(left, lhs, in_sem.at[0]), pltpu.make_async_copy(right, rhs, in_sem.at[1])]

    loads = load(cot_hbm, g_hbm)
    for copy in loads:
        copy.start()
    wo_copy = pltpu.make_async_copy(wo_hbm, wo, in_sem.at[2])
    wo_copy.start()
    sums = LineSum(i, n, part, land, s_send, s_recv, pieces)
    part_copy.wait()
    loop(n, lambda t: sums.launch(jnp.where(i < n // 2, n - 1 - t, t)))
    planes = [PlaneSum(row, m, out, terms_a, land_a, half_a, p_send.at[0], p_recv.at[0], h_send.at[0], h_recv.at[0]),
              PlaneSum(row, m, out, terms_b, land_b, half_b, p_send.at[1], p_recv.at[1], h_send.at[1], h_recv.at[1])]
    first, second = planes
    for copy in loads:
        copy.wait()
    left, right = lhs.at[:, 0 : lhs.shape[1]], rhs.at[:, 0 : down_ref.shape[1]]
    for e in range(1, m, 2):
        block_terms(first, e, [(left, right, 0)])
        first.whole(e).start()
    for e in range(m - 2, -1, -2):
        block_terms(first, e, [(left, right, 0)])
    loads = load(c_hbm, du_hbm)
    for copy in loads:
        copy.start()
    first.merge()
    first.push(0)
    first.sent()
    for copy in loads:
        copy.wait()
    for e in range(1, m, 2):
        block_terms(second, e, [(left, right, 0)])
        second.whole(e).start()

    line.step(1)
    for e in range(m - 2, -1, -2):
        block_terms(second, e, [(left, right, 0)])
    qkv_copies = [pltpu.make_async_copy(qkv_hbm.at[p], rhs.at[:, p * width : (p + 1) * width], qkv_sem.at[p])
                  for p in range(3)]
    for copy in qkv_copies:
        copy.start()
    second.merge()
    second.push(0)
    own_copy.wait()
    wo_copy.wait()

    for copy in qkv_copies:
        copy.wait()
    dk[...] = jnp.zeros_like(dk)
    dv[...] = jnp.zeros_like(dv)

    def column(p, here, t):
        return rhs[here, pl.ds(pl.multiple_of(p * width + t * HD, HD), HD)]

    def put(p, here, t, value):
        rhs[here, pl.ds(pl.multiple_of(p * width + t * HD, HD), HD)] = value

    def mixture_back(j):
        here = rows_at(j, size)
        copy = pltpu.make_async_copy(db_all.at[j], lhs.at[here], db_sem.at[j])
        copy.start()
        copy.wait()
        rhs[here, 3 * width : 4 * width] = lax.dot_general(
            lhs[here, :], wo[...], NT, preferred_element_type=F32).astype(BF)
        for b in range(n):
            @pl.when(j == b)
            def _():
                attend_back(b, size, column, width // HD, put, dk, dv)

    def keep(ref):
        def put(here, total):
            ref[here, :] = total

        return put

    def advance(plane, stage, ref):
        if stage < plane.stages - 1:
            plane.take(stage)
            plane.push(stage + 1)
        else:
            plane.take(stage, keep(ref))

    def round_back(r):
        @pl.when(jnp.logical_and(r >= 1, r <= n - 2))
        def _():
            line.step(r + 1)
            relays(sums, i, n, r)

        def side(s):
            j = jnp.where(s == 0, i - r, i + r)

            @pl.when(jnp.logical_and(jnp.logical_and(j >= 0, j <= n - 1), s * r == s * jnp.maximum(r, 1)))
            def _():
                mixture_back(j)

        loop(2, side)

        @pl.when(r == 1)
        def _():
            advance(first, 0, down_ref)

        @pl.when(r == min(2, n - 1))
        def _():
            advance(second, 0, up_ref)

    loop(n, round_back)
    relays(sums, i, n, n - 1)

    def whole(t):
        put(1, slice(0, LEN), t, (dk[t] * HD ** (-0.5)).astype(BF))
        put(2, slice(0, LEN), t, dv[t].astype(BF))

    loop(width // HD, whole)
    leave = [pltpu.make_async_copy(rhs.at[:, p * width : (p + 1) * width], dqkv_hbm.at[p], out_sem.at[p]) for p in range(3)]
    for copy in leave:
        copy.start()
    for stage in range(1, first.stages):
        advance(first, stage, down_ref)
        advance(second, stage, up_ref)

    def turn(k):
        down_t[rows_at(k, LANES), :] = down_ref[:, rows_at(k, LANES)].T

    loop(down_ref.shape[1] // LANES, turn)

    def output(b):
        here = rows_at(b, RB)
        sums.add(here, acc)
        lo_ref[here, :] = (h_ref[here, :] + (acc[...] + vec[5:6, :])).astype(BF)

    sums.own(output)
    line.finish()
    sums.finish()
    second.sent()
    for plane in planes:
        plane.finish()
    for copy in leave:
        copy.wait()


def input_kernel(n, m, pieces, widths, dqkv_ref, wq_hbm, x_hbm, dh_hbm, vec, early_ref, up_ref, a_hbm, db_hbm, o_hbm,
                 n_hbm, gt_ref, gqkv_ref, gout_t, vec_out, up_out, qv_out, gout_ref, late_acc, up_acc, qv_acc, vec_ref, qv_ref, wq, a_ref, db_ref,
                 o_ref, n_ref, x_ref, dh_ref, part, land, out_p, terms, land_p, half_p, acc, late_land, up_land, qv_land, s_send,
                 s_recv, in_sem, p_send, p_recv, h_send, h_recv, l_send, l_recv, u_send, u_recv, q_send,
                 q_recv):
    i, row = lax.axis_index("tensor"), lax.axis_index("dp")
    me, total_devices = row * n + i, m * n
    size = x_hbm.shape[0]
    width = dqkv_ref.shape[2]
    piece, up_piece, qv_piece = widths
    depth = part.shape[2]
    loads = [pltpu.make_async_copy(src, dst, in_sem.at[k]) for k, (src, dst) in enumerate(
        [(wq_hbm, wq), (a_hbm, a_ref), (db_hbm, db_ref), (o_hbm, o_ref), (n_hbm, n_ref), (x_hbm, x_ref), (dh_hbm, dh_ref)])]
    loads[0].start()
    loads[4].start()
    greet_all(me, n, total_devices)
    every = VectorSum(me, total_devices, lambda g: {"dp": g // n, "tensor": g % n}, vec_ref, piece, late_land, late_acc,
                      l_send, l_recv)
    column = [VectorSum(row, m, lambda g: {"dp": g}, up_ref, up_piece, up_land, up_acc, u_send, u_recv),
              VectorSum(row, m, lambda g: {"dp": g}, qv_ref, qv_piece, qv_land, qv_acc, q_send, q_recv)]
    column[0].start()
    sums = LineSum(i, n, part, land, s_send, s_recv, pieces)
    vec_ref[...] = jnp.zeros_like(vec_ref)
    vec_ref[2:6, :] = early_ref[0:4, :]
    qv_ref[...] = jnp.zeros_like(qv_ref)
    loads[0].wait()
    loads[4].wait()
    for k in (1, 2, 3, 5, 6):
        loads[k].start()
    tile = 512

    def term(t):
        d = jnp.where(i < n // 2, n - 1 - t, t)
        here = rows_at(d, size)

        def columns(k):
            cols = rows_at(k, tile)
            total = lax.dot_general(dqkv_ref[0, here, :], wq[0, cols, :], NT, preferred_element_type=F32)
            for p in range(1, 3):
                total += lax.dot_general(dqkv_ref[p, here, :], wq[p, cols, :], NT, preferred_element_type=F32)
            part[d, :, cols] = total.astype(BF)
            vec_ref[0:1, cols] += jnp.sum(total * n_ref[here, cols].astype(F32), axis=0, keepdims=True)
            vec_ref[1:2, cols] += jnp.sum(total, axis=0, keepdims=True)

        loop(depth // tile, columns)

        @pl.when(t == 0)
        def _():
            sums.launch(d)

        for p in range(2):
            qv_ref[p : p + 1, :] += jnp.sum(dqkv_ref[2 * p, here, :].astype(F32), axis=0, keepdims=True)

    loop(n, term)
    every.start()
    column[1].start()
    loop(n - 1, lambda t: sums.launch(jnp.where(i < n // 2, n - 2 - t, t + 1)))
    for k in (1, 2, 3, 5, 6):
        loads[k].wait()
    plane = PlaneSum(row, m, out_p, terms, land_p, half_p, p_send, p_recv, h_send, h_recv)
    pairs = [(a_ref, dqkv_ref.at[p], p * width) for p in range(3)] + [(db_ref, o_ref, 3 * width)]
    for e in range(1, m, 2):
        block_terms(plane, e, pairs)
        plane.whole(e).start()
    for e in range(m - 2, -1, -2):
        block_terms(plane, e, pairs)
    plane.merge()
    plane.push(0)

    def out(here, total):
        for p in range(3):
            gqkv_ref[p, here, :] = total[:, p * width : (p + 1) * width]
        gout_ref[here, :] = total[:, 3 * width :]

    stage = 0
    for r in range(1, n):
        relays(sums, i, n, r)
        if r > 1 and stage < plane.stages:
            if stage < plane.stages - 1:
                plane.take(stage)
                plane.push(stage + 1)
            else:
                plane.take(stage, out)
            stage += 1

    def norm(b):
        here = rows_at(b, RB)
        sums.add(here, acc)
        grad = acc[...]
        normal, inverse = norm_stats(x_ref[here, :].astype(F32))
        gt_ref[here, :] = (dh_ref[here, :] + norm_back(grad, normal, inverse, vec[0:1, :])).astype(BF)

    while stage < plane.stages:
        if stage < plane.stages - 1:
            plane.take(stage)
            plane.push(stage + 1)
        else:
            plane.take(stage, out)
        stage += 1
    gout_t[...] = gout_ref[...].T
    rows = every.finish()
    for k, at in enumerate([0, 1, 4, 2, 3, 5]):
        vec_out[k : k + 1, :] = rows[at : at + 1, :]
    up_out[...] = column[0].finish()
    qv_out[...] = column[1].finish()
    sums.own(norm)
    sums.finish()
    plane.sent()
    plane.finish()


def params(collective=None):
    if collective is None:
        return pltpu.CompilerParams(vmem_limit_bytes=BIG)
    return pltpu.CompilerParams(vmem_limit_bytes=BIG, collective_id=collective, has_side_effects=True)


def shape(dims, dtype):
    return jax.ShapeDtypeStruct(dims, dtype)


def body(tokens, cotangent, ln1_gain, ln1_bias, qkv_weight, qv_bias, out_weight, out_bias, ln2_gain, ln2_bias,
         up_weight, up_bias, down_weight, down_bias):
    n = lax.axis_size("tensor")
    m = lax.axis_size("dp")
    i, row = lax.axis_index("tensor"), lax.axis_index("dp")
    size, depth = tokens.shape
    width = qkv_weight.shape[2]
    units = up_weight.shape[1]
    piece, qv_piece, up_piece = ln1_gain.shape[0], qv_bias.shape[1], up_bias.shape[0]
    total = m * n

    def lane_rows(value, index):
        count = value.shape[-1]
        if count >= LANES:
            return value.reshape(-1, LANES)
        places = LANES // count
        spread = jnp.tile(value.reshape(-1, count), (1, places))
        return jnp.where((jnp.arange(LANES) // count)[None] == index % places, spread, 0)

    me = row * n + i
    whole = jnp.stack([ln1_gain, ln1_bias, out_bias, ln2_gain, ln2_bias, down_bias])
    pack = jnp.concatenate([lane_rows(whole, me), lane_rows(qv_bias, row), lane_rows(up_bias, row)])
    pack = jnp.pad(pack, ((0, -pack.shape[0] % 16), (0, 0)))
    lanes_up = 8 + max(up_piece // LANES, 1)

    dma = pltpu.SemaphoreType.DMA
    weight_sems = [dma((2, 2, m - 1)), dma((2, 2, m)), dma((2, 2))]
    attn_in, normal_one, vectors, bias_qv, bias_up, w_qkv, w_out = pl.pallas_call(
        functools.partial(tokens_kernel, n, m, (piece, qv_piece, up_piece)),
        out_shape=(shape((LEN, depth), BF), shape((LEN, depth), BF), shape((8, depth), F32), shape((8, width), F32),
                   shape((8, units), F32), shape((3, depth, width), BF), shape((width, depth), BF)),
        in_specs=[VM] * 4, out_specs=(ANY, ANY, VM, VM, VM, ANY, ANY),
        scratch_shapes=[pltpu.VMEM((total,) + pack.shape, BF), pltpu.VMEM((n, size, depth), BF), pltpu.VMEM((LEN, depth), BF),
                        pltpu.VMEM((LEN, depth), BF), dma((2, n))] + weight_sems +
                       [dma, dma((2, n, LineGather.PIECES)), dma((n, LineGather.PIECES)), dma((total,)), dma((total,))],
        compiler_params=params(0), name="gather_tokens",
    )(pack, tokens, qkv_weight, out_weight)

    pieces = 2
    sums = [pltpu.VMEM((n, size, depth), BF), pltpu.VMEM((n + 1, size, depth), BF)]
    qkv, mixture, residual, mlp_own, cot_all, w_up, w_down = pl.pallas_call(
        functools.partial(attend_kernel, n, m, pieces),
        out_shape=(shape((3, LEN, width), BF), shape((LEN, width), BF), shape((size, depth), F32),
                   shape((size, depth), BF), shape((n, size, depth), BF), shape((depth, units), BF), shape((units, depth), BF)),
        in_specs=[ANY] * 3 + [VM] * 6, out_specs=(ANY, ANY, VM, VM, ANY, ANY, ANY),
        scratch_shapes=weight_sems + [pltpu.VMEM((3, LEN, width), BF), pltpu.VMEM((LEN, width), BF), dma((2,)),
                        pltpu.VMEM((LEN, depth), BF), pltpu.VMEM((3, depth, width), BF), pltpu.VMEM((width, depth), BF)] +
                       sums + [dma((2, n, LineGather.PIECES)), dma((n, LineGather.PIECES)), dma((n, pieces)), dma((n + 1, pieces)), dma, dma, dma((4,))],
        compiler_params=params(1), name="attend",
    )(attn_in, w_qkv, w_out, up_weight, down_weight, tokens, cotangent, bias_qv, vectors)

    pieces = min(4, size // RB)
    mlp_in, hidden, grad_pre, mlp_part, grad_resid, branch_cot, vec_two, grad_up_b = pl.pallas_call(
        functools.partial(hidden_kernel, n, pieces),
        out_shape=(shape((n, size, depth), BF), shape((n, size, units), BF), shape((n, size, units), BF),
                   shape((n, size, depth), BF), shape((size, depth), F32), shape((size, depth), BF),
                   shape((8, depth), F32), shape((8, units), F32)),
        in_specs=[VM, VM, ANY, ANY, ANY, VM, VM], out_specs=(ANY, ANY, ANY, ANY, VM, VM, VM, VM),
        scratch_shapes=[pltpu.VMEM((n, size, depth), BF), pltpu.VMEM((n, size, units), BF),
                        pltpu.VMEM((n, size, units), BF), pltpu.VMEM((n, size, depth), BF),
                        pltpu.VMEM((depth, units), BF), pltpu.VMEM((units, depth), BF)] + sums +
                       [dma((2, n, LineGather.PIECES)), dma((n, LineGather.PIECES)), dma((n, pieces)), dma((n + 1, pieces)), dma((2,)), dma, dma,
                        dma((n,)), dma((n,)), dma((n,)), pltpu.VMEM((n, size, depth), BF), dma((n,))],
        compiler_params=params(2), name="hidden",
    )(mlp_own, residual, cot_all, w_up, w_down, bias_up, vectors)
    mlp_in, hidden, grad_pre, cot_rows = [v.reshape(LEN, -1) for v in (mlp_in, hidden, grad_pre, cot_all)]

    def plane_scratch(columns):
        rows = depth // m
        return [pltpu.VMEM((m // 2, rows, columns), BF), pltpu.VMEM((m // 2, rows, columns), BF),
                pltpu.VMEM((2, m // 2 - 1, rows // 2, columns), BF)]

    pieces = 2
    sum_sems = [dma((n, pieces)), dma((n + 1, pieces))]
    attn_cot, layer_out, grad_down_w, grad_up_w, grad_qkv = pl.pallas_call(
        functools.partial(branch_kernel, n, m, pieces),
        out_shape=(shape((n, size, depth), BF), shape((size, depth), BF), shape((units, depth // m), F32),
                   shape((depth // m, units), F32), shape((3, LEN, width), BF)),
        in_specs=[VM] * 3 + [ANY] * 7, out_specs=(ANY, VM, VM, VM, ANY),
        scratch_shapes=[pltpu.VMEM((depth // m, units), F32), dma((3,)), pltpu.VMEM((LEN, depth), BF), pltpu.VMEM((LEN, units), BF), pltpu.VMEM((width, depth), BF),
                        pltpu.VMEM((width // HD, LEN, HD), F32), pltpu.VMEM((width // HD, LEN, HD), F32)] + sums +
                       [pltpu.VMEM((m // 2, depth // m, units), BF)] + plane_scratch(units) * 2 +
                       [pltpu.VMEM((RB, depth), F32), dma((2, n, LineGather.PIECES)), dma((n, LineGather.PIECES))] + sum_sems +
                       [dma, dma, dma((3,)), dma((3,)), dma((n,)), dma((2, m // 2)), dma((2, m // 2)),
                        dma((2, 2, m // 2 - 1)), dma((2, 2, m // 2 - 1))],
        compiler_params=params(4), name="branch",
    )(branch_cot, residual, vectors, mlp_part, hidden, cot_rows, mlp_in, grad_pre, qkv, w_out)
    attn_cot = attn_cot.reshape(LEN, depth)

    tiles = [max(v, LANES) for v in (piece, up_piece, qv_piece)]
    grad_tokens, grad_qkv_w, grad_out_w, vector_grads, grad_up_b, grad_qv_b = pl.pallas_call(
        functools.partial(input_kernel, n, m, pieces, (piece, up_piece, qv_piece)),
        out_shape=(shape((size, depth), BF), shape((3, depth // m, width), F32), shape((width, depth // m), F32),
                   shape((8, piece), F32), shape((8, up_piece), F32), shape((8, qv_piece), F32)),
        in_specs=[VM, ANY, ANY, ANY, VM, VM, VM, ANY, ANY, ANY, ANY], out_specs=(VM,) * 6,
        scratch_shapes=[pltpu.VMEM((depth // m, width), F32)] + [pltpu.VMEM((8, tiles[k]), F32) for k in (0, 1, 2)] + [
                        pltpu.VMEM((8, depth), F32), pltpu.VMEM((8, width), F32),
                        pltpu.VMEM((3, depth, width), BF), pltpu.VMEM((LEN, depth), BF), pltpu.VMEM((LEN, depth), BF),
                        pltpu.VMEM((LEN, width), BF), pltpu.VMEM((LEN, depth), BF), pltpu.VMEM((size, depth), BF),
                        pltpu.VMEM((size, depth), F32)] + sums +
                       [pltpu.VMEM((m // 2, depth // m, 4 * width), BF)] +
                       plane_scratch(4 * width) +
                       [pltpu.VMEM((RB, depth), F32), pltpu.VMEM((total, 8, tiles[0]), F32),
                        pltpu.VMEM((m, 8, tiles[1]), F32),
                        pltpu.VMEM((m, 8, tiles[2]), F32)] + sum_sems +
                       [dma((7,)), dma((m // 2,)), dma((m // 2,)), dma((2, m // 2 - 1)), dma((2, m // 2 - 1))] +
                       [dma((total,))] * 2 + [dma((m,))] * 4,
        compiler_params=params(5), name="input",
    )(grad_qkv, w_qkv, tokens, grad_resid, vectors, vec_two, grad_up_b, attn_in, attn_cot, mixture, normal_one)

    vectors = [vector_grads[k] for k in range(6)]
    grad_up_b, grad_qv_b = grad_up_b[0], grad_qv_b[:2]
    return (layer_out, grad_tokens, vectors[0], vectors[1], grad_qkv_w, grad_qv_b, grad_out_w, vectors[2],
            vectors[3], vectors[4], grad_up_w, grad_up_b, grad_down_w, vectors[5])


def solution(mesh):
    vector, matrix = P(("dp", "tensor")), P(("dp", "tensor"), None)
    in_specs = (matrix, matrix, vector, vector, P(None, "dp", "tensor"), P(None, ("tensor", "dp")), P("tensor", "dp"),
                vector, vector, vector, P("dp", "tensor"), P(("tensor", "dp")), P("tensor", "dp"), vector)
    out_specs = (matrix, matrix, vector, vector, P(None, "dp", "tensor"), P(None, ("tensor", "dp")),
                 P("tensor", "dp"), vector, vector, vector, P("dp", "tensor"), P(("tensor", "dp")), P("tensor", "dp"),
                 vector)
    return jax.shard_map(body, mesh=mesh, in_specs=in_specs, out_specs=out_specs, check_vma=False)
```
